32 devices in a mesh: wide: 8 (over z, y), narrow: 4 (over x, core).
Axes of the slice: x: 2, y: 2, z: 4, core: 2. Of those that a mesh axis runs over, the one named last changes fastest.
Arguments:
- layer_in: bfloat16 [8, 512, 1536], P('wide', 'narrow'), may hold values from -6 to 6
- lengths: int32 [8, 8], P('wide'), may hold values from 1 to 256, 512 in all within a row
- w_qkv: bfloat16 [1536, 2048], P(('wide', 'narrow')), may hold values from -0.15625 to 0.15625
- b_qkv: bfloat16 [2048], P(('wide', 'narrow')), may hold values from -3 to 3
- w_out: bfloat16 [1536, 1536], P(None, ('wide', 'narrow')), may hold values from -0.625 to 0.625
- norm1_gain: bfloat16 [1536], P(('wide', 'narrow')), may hold values from 0.099609375 to 1.8984375
- norm2_gain: bfloat16 [1536], P(('wide', 'narrow')), may hold values from 0.099609375 to 1.8984375
- w_gate: bfloat16 [1536, 8960], P('wide', 'narrow'), may hold values from -0.15625 to 0.15625
- w_up: bfloat16 [1536, 8960], P('wide', 'narrow'), may hold values from -0.15625 to 0.15625
- w_down: bfloat16 [8960, 1536], P('narrow', 'wide'), may hold values from -0.0625 to 0.0625
- grad_out: bfloat16 [8, 512, 1536], P('wide', 'narrow'), may hold values from -6 to 6
Outputs:
- layer_out: bfloat16 [8, 512, 1536], P('wide', 'narrow')
- grad_in: float32 [8, 512, 1536], P('wide', 'narrow')
- grad_w_qkv: float32 [1536, 2048], P(('wide', 'narrow'))
- grad_b_qkv: float32 [2048], P(('wide', 'narrow'))
- grad_w_out: float32 [1536, 1536], P(None, ('wide', 'narrow'))
- grad_norm1: float32 [1536], P(('wide', 'narrow'))
- grad_norm2: float32 [1536], P(('wide', 'narrow'))
- grad_w_gate: float32 [1536, 8960], P('wide', 'narrow')
- grad_w_up: float32 [1536, 8960], P('wide', 'narrow')
- grad_w_down: float32 [8960, 1536], P('narrow', 'wide')
The draws below stay inside these ranges and needn't reach their ends.
Inputs may be any that keep to these rules, and one draw needn't show every extreme that they name: In each pack the 8 lengths sum to 512, and one of them is 256.
All inputs are finite; a program needn't handle non-finite values.
Results may differ from the reference program's by a relative error of at most 0.02.
Values may be sent and summed in bfloat16 or wider, within the bound.
A program may use at most 192 MiB of HBM per device.

```python
import math
import jax
import jax.numpy as jnp
import numpy as np
from jax import lax

D = 1536
QUERY_HEADS = 12
KEY_VALUE_HEADS = 2
HEAD_WIDTH = 128
FF = 8960
DOCS = 8
PACK_TOKENS = 512
PACKS = 8
QD = 1536
QKV = 2048


def block_scale(stream_key, dims, pieces, low, top_value):
    def one(dim, shards_of):
        draws = jax.random.uniform(jax.random.fold_in(jax.random.fold_in(stream_key, 6), dim), (shards_of,), jnp.float32, low / len(pieces), top_value / len(pieces))
        return jnp.repeat(jnp.exp(draws), dims[dim] // shards_of).reshape((-1,) + (1,) * (len(dims) - dim - 1))

    factor_of = one(*pieces[0])
    for cut in pieces[1:]:
        factor_of = factor_of * one(*cut)
    return factor_of


def profile(amount, total, bound, skew):
    weights = [(1 << 20) // math.isqrt(standing ** skew) + 1 for standing in range(2, amount + 1)]
    surplus, counts = total - bound - (amount - 1), [1] * (amount - 1)
    while surplus > 0:
        free = [i for i in range(amount - 1) if counts[i] < bound]
        whole, left = sum([weights[i] for i in free]), surplus
        for i in free:
            more = min(bound - counts[i], max(1, left * weights[i] // whole), surplus)
            counts[i] = counts[i] + more
            surplus = surplus - more
    return np.array([bound] + counts)


def uneven(own_key, number_of, total, reach, lean):
    if number_of == 2:
        one = jax.random.randint(own_key, (), max(1, total - reach), min(reach, total - 1) + 1)
        return jnp.stack([one, total - one])
    sizes = jnp.asarray(profile(number_of, total, reach, lean), jnp.int32)
    pairs = (number_of - 1) // 2
    source_of, receiver = sizes[1:1 + 2 * pairs:2], sizes[2:2 + 2 * pairs:2]
    margin = jnp.minimum(source_of - 1, reach - receiver)
    shifted = jax.random.randint(jax.random.fold_in(own_key, 1), (pairs,), 0, 1 << 20) % (margin + 1)
    sizes = sizes.at[1:1 + 2 * pairs:2].set(source_of - shifted).at[2:2 + 2 * pairs:2].set(receiver + shifted)
    return sizes[jax.random.permutation(jax.random.fold_in(own_key, 2), number_of)]


def normal_values(key, dims, width, reach, shards=(), kind=jnp.bfloat16):
    entries = width * jax.random.normal(key, dims, jnp.float32)
    if shards:
        entries = entries * block_scale(key, dims, shards, -0.22, 0.18)
    return jnp.clip(entries, -reach, reach).astype(kind)


def setup_inputs(seed: int = 0) -> dict:
    key_list = jax.random.split(jax.random.key(seed), 12)
    return {
        "layer_in": normal_values(key_list[0], (PACKS, PACK_TOKENS, D), 1.0, 6.0, ((0, 8), (1, 4))),
        "lengths": jax.vmap(lambda own: uneven(own, DOCS, PACK_TOKENS, PACK_TOKENS // 2, 2))(jax.random.split(key_list[1], PACKS)).reshape((PACKS, DOCS)).astype(jnp.int32),
        "w_qkv": normal_values(key_list[2], (D, QKV), D ** -0.5, 0.15625, ((0, 32),)),
        "b_qkv": normal_values(key_list[3], (QKV,), 0.5, 3.0, ((0, 32),)),
        "w_out": normal_values(key_list[4], (QD, D), (QD // 16) ** -0.5, 0.625, ((1, 32),)),
        "norm1_gain": jnp.clip(1.0 + 0.18 * jax.random.normal(key_list[5], (D,), jnp.float32), 0.099609375, 1.8984375).astype(jnp.bfloat16),
        "norm2_gain": jnp.clip(1.0 + 0.18 * jax.random.normal(key_list[6], (D,), jnp.float32), 0.099609375, 1.8984375).astype(jnp.bfloat16),
        "w_gate": normal_values(key_list[7], (D, FF), D ** -0.5, 0.15625, ((0, 8), (1, 4))),
        "w_up": normal_values(key_list[8], (D, FF), D ** -0.5, 0.15625, ((0, 8), (1, 4))),
        "w_down": normal_values(key_list[9], (FF, D), FF ** -0.5, 0.0625, ((0, 4), (1, 8))),
        "grad_out": normal_values(key_list[10], (PACKS, PACK_TOKENS, D), 1.0, 6.0, ((0, 8), (1, 4))),
    }


EPSILON = 1e-06
ROPE_BASE = 10000.0
NEGATIVE_BIG = -1e+30
HIGHEST = lax.Precision.HIGHEST

@jax.custom_vjp
def lowered_precision(v):
    return lax.optimization_barrier(v.astype(jnp.bfloat16)).astype(jnp.float32)

@jax.custom_vjp
def low_back(v):
    return v

def low_keep(v):
    return (lowered_precision(v), None)

def low_pass(kept, grad):
    return (grad,)

def back_keep(v):
    return (v, None)

def back_low(kept, grad):
    return (lowered_precision(grad),)
lowered_precision.defvjp(low_keep, low_pass)
low_back.defvjp(back_keep, back_low)

def matmul(left, right):
    return jnp.dot(left, right, precision=HIGHEST)

def rms_scale(value_rows, gain):
    return value_rows * lax.rsqrt(lax.optimization_barrier(jnp.mean(value_rows * value_rows, axis=-1, keepdims=True)) + EPSILON) * gain

def apply_rotation(value_rows, token_position):
    half_dim = value_rows.shape[-1] // 2
    freq = jnp.exp(jnp.arange(half_dim, dtype=jnp.float32) * (-2.0 * math.log(ROPE_BASE) / value_rows.shape[-1]))
    angle = token_position[:, None] * freq[None, :]
    cosine = jnp.cos(angle)[:, None, :]
    sine = jnp.sin(angle)[:, None, :]
    leading = value_rows[..., :half_dim]
    trailing = value_rows[..., half_dim:]
    return jnp.concatenate([leading * cosine - trailing * sine, trailing * cosine + leading * sine], axis=-1)

def doc_layout(index, doc_lengths):
    ends = jnp.cumsum(doc_lengths).astype(jnp.int32)
    starts = ends - doc_lengths.astype(jnp.int32)
    document_index = lax.optimization_barrier(jnp.sum((index[:, None] >= ends[None, :]).astype(jnp.int32), axis=1))
    onehot = (document_index[:, None] == jnp.arange(doc_lengths.shape[0], dtype=jnp.int32)[None, :]).astype(jnp.int32)
    token_position = index - lax.optimization_barrier(jnp.sum(onehot * starts[None, :], axis=1))
    return (document_index, token_position.astype(jnp.float32))

def attend_heads(query_rows, key_rows, value_rows, document_index):
    query_group = QUERY_HEADS // KEY_VALUE_HEADS
    current_query_block = min(512, PACK_TOKENS)
    count_of_blocks = PACK_TOKENS // current_query_block
    scale = HEAD_WIDTH ** (-0.5)
    blocked_queries = query_rows.reshape(count_of_blocks, current_query_block, KEY_VALUE_HEADS, query_group, HEAD_WIDTH)
    doc_blocks = document_index.reshape(count_of_blocks, current_query_block)
    block_starts = jnp.arange(count_of_blocks, dtype=jnp.int32) * current_query_block
    key_index = jnp.arange(PACK_TOKENS, dtype=jnp.int32)

    def one_block(inputs):
        query_part, doc_part, start_row = inputs
        scores = jnp.einsum('tkgd,skd->kgts', query_part, key_rows, precision=HIGHEST) * scale
        scores = low_back(scores)
        query_index = start_row + jnp.arange(current_query_block, dtype=jnp.int32)
        allowed = (doc_part[:, None] == document_index[None, :]) & (key_index[None, :] <= query_index[:, None])
        masked = jnp.where(allowed, scores, NEGATIVE_BIG)
        top_score = lax.optimization_barrier(jnp.max(masked, axis=-1, keepdims=True))
        weights = jnp.where(allowed, jnp.exp(masked - top_score), 0.0)
        weights = lowered_precision(weights / lax.optimization_barrier(jnp.sum(weights, axis=-1, keepdims=True)))
        result = jnp.einsum('kgts,skd->tkgd', weights, value_rows, precision=HIGHEST)
        return result.reshape(current_query_block, QUERY_HEADS * HEAD_WIDTH)
    results = lax.map(jax.checkpoint(one_block), (blocked_queries, doc_blocks, block_starts))
    return results.reshape(PACK_TOKENS, QUERY_HEADS * HEAD_WIDTH)

def pack_layer(hidden_in, doc_lengths, params):
    w_qkv, b_qkv, w_out, gain_one, gain_two, w_gate, w_up, w_down = params
    query_total_width = QUERY_HEADS * HEAD_WIDTH
    key_total_width = KEY_VALUE_HEADS * HEAD_WIDTH
    document_index, token_position = doc_layout(jnp.arange(PACK_TOKENS, dtype=jnp.int32), doc_lengths)
    normed = lowered_precision(rms_scale(hidden_in, gain_one))
    unrotated_projection = low_back(matmul(normed, w_qkv) + b_qkv)
    query_rows = lowered_precision(apply_rotation(unrotated_projection[:, :query_total_width].reshape(PACK_TOKENS, QUERY_HEADS, HEAD_WIDTH), token_position))
    key_rows = lowered_precision(apply_rotation(unrotated_projection[:, query_total_width:query_total_width + key_total_width].reshape(PACK_TOKENS, KEY_VALUE_HEADS, HEAD_WIDTH), token_position))
    value_rows = lowered_precision(unrotated_projection[:, query_total_width + key_total_width:].reshape(PACK_TOKENS, KEY_VALUE_HEADS, HEAD_WIDTH))
    attended_rows = attend_heads(query_rows.reshape(PACK_TOKENS, KEY_VALUE_HEADS, QUERY_HEADS // KEY_VALUE_HEADS, HEAD_WIDTH), key_rows, value_rows, document_index)
    attended_rows = lowered_precision(low_back(attended_rows))
    middle = hidden_in + low_back(matmul(attended_rows, w_out))
    normed_two = lowered_precision(rms_scale(middle, gain_two))
    gate = low_back(matmul(normed_two, w_gate))
    up_part = low_back(matmul(normed_two, w_up))
    hidden_act = lowered_precision(jax.nn.silu(gate) * up_part)
    return middle + low_back(matmul(hidden_act, w_down))

def reference(layer_in, lengths, w_qkv, b_qkv, w_out, norm1_gain, norm2_gain, w_gate, w_up, w_down, grad_out):
    params = tuple((item.astype(jnp.float32) for item in (w_qkv, b_qkv, w_out, norm1_gain, norm2_gain, w_gate, w_up, w_down)))

    def forward(inputs_all, weights):

        def one_pack(inputs):
            hidden_in, doc_lengths = inputs
            return pack_layer(hidden_in, doc_lengths, weights)
        return lax.map(jax.checkpoint(one_pack), (inputs_all, lengths))
    result, pullback = jax.vjp(forward, layer_in.astype(jnp.float32), params)
    grad_inputs, grad_params = pullback(grad_out.astype(jnp.float32))
    return (result.astype(jnp.bfloat16), grad_inputs, grad_params[0], grad_params[1], grad_params[2], grad_params[3], grad_params[4], grad_params[5], grad_params[6], grad_params[7])
```

```python
import math

import jax
import jax.numpy as jnp
from jax import lax
from jax.sharding import Mesh
from jax.sharding import PartitionSpec as P

QUERY_HEADS = 12
KEY_VALUE_HEADS = 2
HEAD_WIDTH = 128

EPSILON = 1e-06
ROPE_BASE = 10000.0
NEGATIVE_BIG = -1e30
HIGHEST = lax.Precision.HIGHEST


BF = jnp.bfloat16
F32 = jnp.float32


def fetch(value, axes, offsets):
    axes = (axes,) if isinstance(axes, str) else tuple(axes)
    offsets = (offsets,) if isinstance(offsets, int) else tuple(offsets)
    sizes = [lax.axis_size(a) for a in axes]
    total = math.prod(sizes)
    pairs = []
    for flat in range(total):
        rest, place = flat, []
        for size in reversed(sizes):
            place.append(rest % size)
            rest //= size
        place = place[::-1]
        source = 0
        for spot, off, size in zip(place, offsets, sizes):
            source = source * size + (spot + off) % size
        pairs.append((source, flat))
    return lax.ppermute(value, axes if len(axes) > 1 else axes[0], pairs)


def send(value, axes, offsets):
    offsets = (offsets,) if isinstance(offsets, int) else tuple(offsets)
    return fetch(value, axes, tuple(-o for o in offsets))


def pick(stack, place, axis=0):
    return lax.dynamic_index_in_dim(stack, place, axis, keepdims=False)


def nn(left, right):
    return lax.dot_general(left, right, (((1,), (0,)), ((), ())), preferred_element_type=F32)


def nt(left, right):
    return lax.dot_general(left, right, (((1,), (1,)), ((), ())), preferred_element_type=F32)


def tn(left, right):
    return lax.dot_general(left, right, (((0,), (0,)), ((), ())), preferred_element_type=F32)


def rms_parts(rows):
    return lax.rsqrt(jnp.mean(rows * rows, axis=-1, keepdims=True) + EPSILON)


def rms_back(rows, gain, grad):
    r = rms_parts(rows)
    scaled = gain * grad
    return (
        r * scaled - rows * (r * r * r) * jnp.mean(scaled * rows, axis=-1, keepdims=True),
        jnp.sum(grad * rows * r, axis=0),
    )


def doc_layout(index, doc_lengths):
    ends = jnp.cumsum(doc_lengths)
    starts = ends - doc_lengths
    document_index = jnp.sum((index[:, None] >= ends[None, :]).astype(jnp.int32), axis=1)
    onehot = (
        document_index[:, None] == jnp.arange(doc_lengths.shape[0], dtype=jnp.int32)[None, :]
    ).astype(jnp.int32)
    token_position = index - jnp.sum(onehot * starts[None, :], axis=1)
    return document_index, token_position.astype(F32)


def angles(position):
    half = HEAD_WIDTH // 2
    freq = jnp.exp(jnp.arange(half, dtype=F32) * (-2.0 * math.log(ROPE_BASE) / HEAD_WIDTH))
    angle = position[:, None] * freq[None, :]
    return jnp.cos(angle)[:, None, :], jnp.sin(angle)[:, None, :]


def rotate(rows, cosine, sine):
    half = HEAD_WIDTH // 2
    first, second = rows[..., :half], rows[..., half:]
    return jnp.concatenate(
        [first * cosine - second * sine, second * cosine + first * sine], axis=-1
    )


def ordered(pieces, axis):
    count, here = len(pieces), lax.axis_index(axis)
    if count == 1:
        return pieces[0][None]
    if count == 2:
        return jnp.where(here == 0, jnp.stack(pieces), jnp.stack(pieces[::-1]))
    whole = jnp.zeros((count,) + pieces[0].shape, pieces[0].dtype)
    for distance, piece in enumerate(pieces):
        whole = lax.dynamic_update_index_in_dim(whole, piece, (here + distance) % count, 0)
    return whole


def shards(
    layer_in, lengths, w_qkv, b_qkv, w_out, norm1_gain, norm2_gain, w_gate, w_up, w_down, grad_out
):
    size = lax.axis_size
    ZH, ZL, Y, X, C = (size(a) for a in ("zh", "zl", "y", "x", "c"))
    zh, zl, y, x, c = (lax.axis_index(a) for a in ("zh", "zl", "y", "x", "c"))
    everyone = ("zh", "zl", "y", "x", "c")
    devices = ZH * ZL * Y * X * C
    rows, width = layer_in.shape[1:]
    part = w_qkv.shape[0]
    group = QUERY_HEADS // KEY_VALUE_HEADS
    heads = QUERY_HEADS // X
    kv_heads = max(1, heads // group)
    share = heads // kv_heads
    q_cols, kv_cols = heads * HEAD_WIDTH, kv_heads * HEAD_WIDTH
    scale = HEAD_WIDTH ** (-0.5)

    bias_part = b_qkv.shape[0]
    small = jnp.concatenate([norm1_gain, norm2_gain, b_qkv])
    small = jnp.pad(small, (0, -small.shape[0] % 256))[None]
    small = lax.all_to_all(
        jnp.broadcast_to(small[None], (devices,) + small.shape), everyone, 0, 0, tiled=True
    )[:, 0].astype(F32)
    gain_one = small[:, :part].reshape(1, width)
    gain_two = small[:, part : 2 * part].reshape(1, width)
    bias = small[:, 2 * part : 2 * part + bias_part].reshape(-1)

    own_in = layer_in[0]
    query_in = jnp.concatenate([own_in] + [fetch(own_in, "x", d) for d in range(1, X)])
    pack_in = jnp.concatenate([query_in] + [fetch(query_in, "c", d) for d in range(1, C)])

    def row_index(cores):
        spans = [
            (((x + dx) % X) * C + (c + dc) % C) * rows + jnp.arange(rows, dtype=jnp.int32)
            for dc in range(cores)
            for dx in range(X)
        ]
        return jnp.concatenate(spans)

    doc_lengths = lengths[0]
    key_index = row_index(C)
    key_doc, key_pos = doc_layout(key_index, doc_lengths)
    query_rows = X * rows
    query_index, query_doc = key_index[:query_rows], key_doc[:query_rows]
    key_cos, key_sin = angles(key_pos)
    query_cos, query_sin = key_cos[:query_rows], key_sin[:query_rows]

    def gather_columns(pieces):
        held = ordered(
            [pick(pieces, x)] + [fetch(pick(pieces, (x - d) % X), "x", d) for d in range(1, X)],
            "x",
        )
        whole = jnp.zeros((ZH, ZL, Y) + held.shape, held.dtype)
        for dh in range(ZH):
            for dl in range(ZL):
                along = held if dh == dl == 0 else fetch(held, ("zh", "zl"), (dh, dl))
                for dy in range(Y):
                    piece = along if dy == 0 else fetch(along, "y", dy)
                    whole = lax.dynamic_update_slice(
                        whole,
                        piece[None, None, None],
                        ((zh + dh) % ZH, (zl + dl) % ZL, (y + dy) % Y, 0, 0, 0),
                    )
        whole = whole.reshape((ZH * ZL * Y * X,) + whole.shape[4:])
        both = ordered([whole] + [fetch(whole, "c", d) for d in range(1, C)], "c")
        return jnp.moveaxis(both, 0, 1).reshape(width, whole.shape[-1])

    def scatter_columns(grad):
        n = grad.shape[-1]
        grad = grad.astype(BF).reshape(ZH * ZL * Y * X, C, part, n)
        held = pick(grad, c, 1).astype(F32)
        for d in range(1, C):
            held = held + send(pick(grad, (c + d) % C, 1), "c", d)
        held = held.astype(BF).reshape(ZH, ZL, Y, X * part, n)
        kept = pick(held, y, 2).astype(F32)
        for d in range(1, Y):
            kept = kept + send(pick(held, (y + d) % Y, 2), "y", d)
        low = kept.astype(BF)
        total = 0.0
        for dh in range(ZH):
            for dl in range(ZL):
                if dh == dl == 0:
                    total = total + pick(pick(kept, zh), zl)
                else:
                    piece = pick(pick(low, (zh + dh) % ZH), (zl + dl) % ZL)
                    total = total + send(piece, ("zh", "zl"), (dh, dl)).astype(F32)
        total = total.reshape(X, part, n)
        lower = total.astype(BF)
        return ordered(
            [pick(total, x)]
            + [fetch(pick(lower, (x - d) % X), "x", d).astype(F32) for d in range(1, X)],
            "x",
        )

    def qkv_columns(array):
        blocks = []
        for at in range(X):
            kv = (at * heads) // group * HEAD_WIDTH
            key_at = QUERY_HEADS * HEAD_WIDTH + kv
            value_at = key_at + KEY_VALUE_HEADS * HEAD_WIDTH
            blocks.append(
                jnp.concatenate(
                    [
                        array[..., at * q_cols : (at + 1) * q_cols],
                        array[..., key_at : key_at + kv_cols],
                        array[..., value_at : value_at + kv_cols],
                    ],
                    axis=-1,
                )
            )
        return jnp.stack(blocks)

    def qkv_whole(blocks):
        queries = [blocks[at, ..., :q_cols] for at in range(X)]
        keys, values = [0.0] * KEY_VALUE_HEADS, [0.0] * KEY_VALUE_HEADS
        for at in range(X):
            for j in range(kv_heads):
                head = (at * heads) // group + j
                start = q_cols + j * HEAD_WIDTH
                keys[head] = keys[head] + blocks[at, ..., start : start + HEAD_WIDTH]
                start = start + kv_cols
                values[head] = values[head] + blocks[at, ..., start : start + HEAD_WIDTH]
        return jnp.concatenate(queries + keys + values, axis=-1)

    wqkv_mine = gather_columns(qkv_columns(w_qkv))
    wout_t = w_out.T
    wout_mine = gather_columns(
        jnp.stack([wout_t[:, at * q_cols : (at + 1) * q_cols] for at in range(X)])
    )
    bias_mine = pick(qkv_columns(bias), x)

    depth, units = w_gate.shape[0], w_gate.shape[1] // ZH

    def gather_units(weight):
        halves = weight.reshape(depth, ZH, units).transpose(1, 0, 2)
        whole = jnp.zeros((ZH, ZL, Y, depth, units), weight.dtype)
        for dh in range(ZH):
            first = pick(halves, zh) if dh == 0 else fetch(pick(halves, (zh - dh) % ZH), "zh", dh)
            for dl in range(ZL):
                second = first if dl == 0 else fetch(first, "zl", dl)
                for dy in range(Y):
                    third = second if dy == 0 else fetch(second, "y", dy)
                    whole = lax.dynamic_update_slice(
                        whole,
                        third[None, None, None],
                        ((zh + dh) % ZH, (zl + dl) % ZL, (y + dy) % Y, 0, 0),
                    )
        return whole.reshape(width, units)

    def scatter_units(grad):
        grad = grad.astype(BF).reshape(ZH, ZL, Y, depth, units)
        done = [None] * ZH
        for dh in reversed(range(ZH)):
            mine = pick(grad, (zh + dh) % ZH)
            kept = pick(mine, y, 1).astype(F32)
            for d in range(1, Y):
                kept = kept + send(pick(mine, (y + d) % Y, 1), "y", d).astype(F32)
            low = kept.astype(BF)
            total = pick(kept, zl)
            for d in range(1, ZL):
                total = total + send(pick(low, (zl + d) % ZL), "zl", d).astype(F32)
            done[dh] = total
        halves = [done[0]] + [
            send(done[dh].astype(BF), "zh", dh).astype(F32) for dh in range(1, ZH)
        ]
        halves = [halves[0]] + halves[:0:-1]
        return jnp.moveaxis(ordered(halves, "zh"), 0, 1).reshape(depth, ZH * units)

    wgate_mine, wup_mine = gather_units(w_gate), gather_units(w_up)
    wdown_mine = gather_units(w_down.T)

    near = [(dh, dx) for dh in range(ZH) for dx in range(X)]

    def gather_rows(own):
        held = jnp.concatenate([own if k == (0, 0) else fetch(own, ("zh", "x"), k) for k in near])
        return jnp.concatenate([held] + [fetch(held, "c", d) for d in range(1, C)])

    def scatter_rows(term):
        term = term.reshape(C, len(near), rows, width)
        held = term[0].astype(F32)
        for d in range(1, C):
            held = held + send(term[d].astype(BF), "c", d).astype(F32)
        total = held[0]
        for at, k in enumerate(near):
            if k != (0, 0):
                total = total + send(held[at].astype(BF), ("zh", "x"), k).astype(F32)
        return total

    def scatter_x(term):
        term = term.reshape(X, rows, width)
        total = term[0]
        for d in range(1, X):
            total = total + send(term[d].astype(BF), "x", d).astype(F32)
        return total

    cotangent = grad_out[0]
    group_cotangent = gather_rows(cotangent)

    pack_in = pack_in.astype(F32)
    normed_one = (pack_in * rms_parts(pack_in) * gain_one).astype(BF)
    query_normed = normed_one[:query_rows]
    pre_query = nn(query_normed, wqkv_mine[:, :q_cols]) + bias_mine[:q_cols]
    pre_kv = nn(normed_one, wqkv_mine[:, q_cols:]) + bias_mine[q_cols:]
    pack_rows = pack_in.shape[0]
    queries = rotate(
        pre_query.reshape(query_rows, heads, HEAD_WIDTH), query_cos, query_sin
    ).astype(BF)
    queries = queries.reshape(query_rows, kv_heads, share, HEAD_WIDTH)
    keys = rotate(
        pre_kv[:, :kv_cols].reshape(pack_rows, kv_heads, HEAD_WIDTH), key_cos, key_sin
    ).astype(BF)
    values = pre_kv[:, kv_cols:].reshape(pack_rows, kv_heads, HEAD_WIDTH).astype(BF)
    scores = jnp.einsum("tkgd,skd->kgts", queries, keys, preferred_element_type=F32) * scale
    allowed = (query_doc[:, None] == key_doc[None, :]) & (
        key_index[None, :] <= query_index[:, None]
    )
    masked = jnp.where(allowed, scores, NEGATIVE_BIG)
    top = jnp.max(masked, axis=-1, keepdims=True)
    weights = jnp.where(allowed, jnp.exp(masked - top), 0.0)
    probs = weights / jnp.sum(weights, axis=-1, keepdims=True)
    probs_low = probs.astype(BF)
    attended = jnp.einsum("kgts,skd->tkgd", probs_low, values, preferred_element_type=F32)
    attended_low = attended.reshape(query_rows, q_cols).astype(BF)
    own_rows = own_in.astype(F32)
    middle = own_rows + scatter_x(nt(attended_low, wout_mine))
    normed_two = (middle * rms_parts(middle) * gain_two).astype(BF)

    group_normed = gather_rows(normed_two)
    gate = nn(group_normed, wgate_mine)
    up_part = nn(group_normed, wup_mine)
    sig = jax.nn.sigmoid(gate)
    act = gate * sig
    hidden = (act * up_part).astype(BF)
    grad_wdown = tn(group_cotangent, hidden).astype(BF)
    grad_hidden = nn(group_cotangent, wdown_mine)
    grad_gate = (grad_hidden * up_part * sig * (1.0 + gate * (1.0 - sig))).astype(BF)
    grad_up = (grad_hidden * act).astype(BF)
    grad_normed_two = scatter_rows(nt(grad_gate, wgate_mine) + nt(grad_up, wup_mine))
    grad_wgate = tn(group_normed, grad_gate).astype(BF)
    grad_wup = tn(group_normed, grad_up).astype(BF)
    layer_out = (middle + scatter_rows(nt(hidden, wdown_mine))).astype(BF)
    sum_wdown = scatter_units(grad_wdown).T
    sum_wgate = scatter_units(grad_wgate)
    sum_wup = scatter_units(grad_wup)

    back_two, grad_gain_two = rms_back(middle, gain_two, grad_normed_two)
    grad_middle = cotangent.astype(F32) + back_two
    grad_att = grad_middle.astype(BF)
    query_grad_att = jnp.concatenate([grad_att] + [fetch(grad_att, "x", d) for d in range(1, X)])
    sum_wout = scatter_columns(tn(query_grad_att, attended_low))
    head_grads = nn(query_grad_att, wout_mine).astype(BF)
    head_grads = head_grads.reshape(query_rows, kv_heads, share, HEAD_WIDTH)
    delta = jnp.sum(head_grads.astype(F32) * attended, axis=-1).transpose(1, 2, 0)
    grad_probs = jnp.einsum("tkgd,skd->kgts", head_grads, values, preferred_element_type=F32)
    grad_scores = (probs * (grad_probs - delta[..., None])).astype(BF)
    grad_query = (
        jnp.einsum("kgts,skd->tkgd", grad_scores, keys, preferred_element_type=F32) * scale
    )
    grad_key = jnp.einsum("kgts,tkgd->skd", grad_scores, queries, preferred_element_type=F32)
    grad_key = rotate(grad_key * scale, key_cos, -key_sin)
    grad_value = jnp.einsum("kgts,tkgd->skd", probs_low, head_grads, preferred_element_type=F32)
    grad_kv = jnp.concatenate(
        [grad_key.reshape(pack_rows, kv_cols), grad_value.reshape(pack_rows, kv_cols)], axis=1
    ).reshape(C, query_rows, 2 * kv_cols)
    kv_total = grad_kv[0]
    for d in range(1, C):
        kv_total = kv_total + send(grad_kv[d].astype(BF), "c", d).astype(F32)
    grad_query = rotate(
        grad_query.reshape(query_rows, heads, HEAD_WIDTH), query_cos, -query_sin
    ).reshape(query_rows, q_cols)
    grad_pre = jnp.concatenate([grad_query, kv_total], axis=1).astype(BF)
    sum_wqkv = qkv_whole(scatter_columns(tn(query_normed, grad_pre)))
    grad_bias = jnp.sum(grad_pre.astype(F32), axis=0)
    grad_normed_one = scatter_x(nt(grad_pre, wqkv_mine))
    back_one, grad_gain_one = rms_back(own_rows, gain_one, grad_normed_one)
    grad_input = grad_middle + back_one

    bias_blocks = jnp.where(
        jnp.arange(X, dtype=jnp.int32)[:, None] == x, grad_bias[None, :], 0.0
    )
    bias_whole = qkv_whole(bias_blocks)
    piece = jnp.concatenate(
        [
            grad_gain_one.reshape(devices, part),
            grad_gain_two.reshape(devices, part),
            bias_whole.reshape(devices, bias_part),
        ],
        axis=1,
    )
    piece = jnp.pad(piece, ((0, 0), (0, -piece.shape[1] % 256)))
    piece = jnp.sum(lax.all_to_all(piece[:, None], everyone, 0, 0, tiled=True)[:, 0], axis=0)
    return (
        layer_out[None],
        grad_input[None],
        sum_wqkv,
        piece[2 * part : 2 * part + bias_part],
        jnp.moveaxis(sum_wout, 0, 1).reshape(part, -1).T,
        piece[:part],
        piece[part : 2 * part],
        sum_wgate,
        sum_wup,
        sum_wdown,
    )


def solution(mesh):
    wide, narrow = mesh.shape["wide"], mesh.shape["narrow"]
    cores = 2 if narrow % 2 == 0 else 1
    along_x = narrow // cores
    along_y = along_x if wide % along_x == 0 else 1
    along_z = wide // along_y
    far = 2 if along_z % 2 == 0 else 1
    split = Mesh(
        mesh.devices.reshape(far, along_z // far, along_y, along_x, cores),
        ("zh", "zl", "y", "x", "c"),
    )
    w, n = ("zh", "zl", "y"), ("x", "c")
    placed = (
        P(w, n, None),
        P(w, None),
        P(w + n, None),
        P(w + n),
        P(None, w + n),
        P(w + n),
        P(w + n),
        P(w, n),
        P(w, n),
        P(n, w),
        P(w, n, None),
    )
    return jax.shard_map(
        shards,
        mesh=split,
        in_specs=placed,
        out_specs=(
            P(w, n, None),
            P(w, n, None),
            P(w + n, None),
            P(w + n),
            P(None, w + n),
            P(w + n),
            P(w + n),
            P(w, n),
            P(w, n),
            P(n, w),
        ),
        check_vma=False,
    )
```

```python
import math

import jax
import jax.numpy as jnp
from jax import lax
from jax.experimental import pallas as pl
from jax.experimental.pallas import tpu as pltpu
from jax.sharding import Mesh
from jax.sharding import PartitionSpec as P

QUERY_HEADS = 12
KEY_VALUE_HEADS = 2
HEAD_WIDTH = 128

EPSILON = 1e-06
ROPE_BASE = 10000.0
NEGATIVE_BIG = -1e30
HIGHEST = lax.Precision.HIGHEST


BF = jnp.bfloat16
F32 = jnp.float32
AXES = ("zh", "zl", "y", "x", "c")
MESH_ID = pl.DeviceIdType.MESH
QKV_WIDTH = (QUERY_HEADS + 2 * KEY_VALUE_HEADS) * HEAD_WIDTH


def fetch(value, axes, offsets):
    axes = (axes,) if isinstance(axes, str) else tuple(axes)
    offsets = (offsets,) if isinstance(offsets, int) else tuple(offsets)
    sizes = [lax.axis_size(a) for a in axes]
    total = math.prod(sizes)
    pairs = []
    for flat in range(total):
        rest, place = flat, []
        for size in reversed(sizes):
            place.append(rest % size)
            rest //= size
        place = place[::-1]
        source = 0
        for spot, off, size in zip(place, offsets, sizes):
            source = source * size + (spot + off) % size
        pairs.append((source, flat))
    return lax.ppermute(value, axes if len(axes) > 1 else axes[0], pairs)


def send(value, axes, offsets):
    offsets = (offsets,) if isinstance(offsets, int) else tuple(offsets)
    return fetch(value, axes, tuple(-o for o in offsets))


def pick(stack, place, axis=0):
    return lax.dynamic_index_in_dim(stack, place, axis, keepdims=False)


def nn(left, right):
    return lax.dot_general(left, right, (((1,), (0,)), ((), ())), preferred_element_type=F32)


def nt(left, right):
    return lax.dot_general(left, right, (((1,), (1,)), ((), ())), preferred_element_type=F32)


def tn(left, right):
    return lax.dot_general(left, right, (((0,), (0,)), ((), ())), preferred_element_type=F32)


def rms_parts(rows):
    return lax.rsqrt(jnp.mean(rows * rows, axis=-1, keepdims=True) + EPSILON)


def rms_back(rows, gain, grad):
    r = rms_parts(rows)
    scaled = gain * grad
    return (
        r * scaled - rows * (r * r * r) * jnp.mean(scaled * rows, axis=-1, keepdims=True),
        jnp.sum(grad * rows * r, axis=0),
    )


def doc_layout(index, doc_lengths):
    ends = jnp.cumsum(doc_lengths)
    starts = ends - doc_lengths
    document_index = jnp.sum((index[:, None] >= ends[None, :]).astype(jnp.int32), axis=1)
    onehot = (
        document_index[:, None] == jnp.arange(doc_lengths.shape[0], dtype=jnp.int32)[None, :]
    ).astype(jnp.int32)
    token_position = index - jnp.sum(onehot * starts[None, :], axis=1)
    return document_index, token_position.astype(F32)


def angles(position):
    half = HEAD_WIDTH // 2
    freq = jnp.exp(jnp.arange(half, dtype=F32) * (-2.0 * math.log(ROPE_BASE) / HEAD_WIDTH))
    angle = position[:, None] * freq[None, :]
    return jnp.cos(angle)[:, None, :], jnp.sin(angle)[:, None, :]


def rotate(rows, cosine, sine):
    half = HEAD_WIDTH // 2
    first, second = rows[..., :half], rows[..., half:]
    return jnp.concatenate(
        [first * cosine - second * sine, second * cosine + first * sine], axis=-1
    )


def ordered(pieces, axis):
    count, here = len(pieces), lax.axis_index(axis)
    if count == 1:
        return pieces[0][None]
    if count == 2:
        return jnp.where(here == 0, jnp.stack(pieces), jnp.stack(pieces[::-1]))
    whole = jnp.zeros((count,) + pieces[0].shape, pieces[0].dtype)
    for distance, piece in enumerate(pieces):
        whole = lax.dynamic_update_index_in_dim(whole, piece, (here + distance) % count, 0)
    return whole


def front(own_in, cotangent, lengths, qkv_pieces, out_pieces, small, w_gate, w_up, w_down):
    size = lax.axis_size
    ZH, ZL, Y, X, C = (size(a) for a in AXES)
    rows, width = own_in.shape
    _, part, qkv_n = qkv_pieces.shape
    q_cols = out_pieces.shape[-1]
    heads = q_cols // HEAD_WIDTH
    kv_cols = (qkv_n - q_cols) // 2
    kv_heads = kv_cols // HEAD_WIDTH
    share = heads // kv_heads
    query_rows, pack_rows = X * rows, C * X * rows
    depth = w_gate.shape[0]
    units = w_gate.shape[1] // ZH
    near = [(dh, dx) for dh in range(ZH) for dx in range(X)]
    far = [(dh, dl) for dh in range(ZH) for dl in range(ZL)]
    devices = ZH * ZL * Y * X * C
    bias_part = QKV_WIDTH // devices
    scale = HEAD_WIDTH ** (-0.5)
    docs = lengths.shape[-1]
    n_sems = 400

    def kernel(
        own_ref, cot_ref, len_ref, qkv_ref, out_ref, small_ref, g_ref, u_ref, d_ref,
        wqkv_o, wout_o, n1_o, q_o, kv_o, p_o, att_o, h_o, nr_o, go_o, wg_o, wu_o, wd_o, vec_o,
        xr, w1, wo, sm, n1, qs, kv, ob, part_send, part_recv, n2s, hs,
        cos_s, sin_s, mask_s, rows_s, ps, raw, raw_d, half,
        send_sem, recv_sem, local_sem,
    ):
        zh, zl, y, x, c = (lax.axis_index(a) for a in AXES)
        sizes = dict(zip(AXES, (ZH, ZL, Y, X, C)))
        here = dict(zip(AXES, (zh, zl, y, x, c)))

        def device(**off):
            return tuple(
                lax.rem(here[a] + off[a], sizes[a]) if off.get(a, 0) % sizes[a] else here[a]
                for a in AXES
            )

        def at(a, d):
            d = d % sizes[a]
            return lax.rem(here[a] + d, sizes[a]) if d else here[a]

        peers = set()
        for d in range(1, C):
            peers.add((0, 0, 0, 0, d))
        for dh, dx in near[1:]:
            peers.add((dh, 0, 0, dx, 0))
        for dh, dl in far[1:]:
            peers.add((dh, dl, 0, 0, 0))
        for d in range(1, Y):
            peers.add((0, 0, d, 0, 0))
        peers = sorted(peers)
        barrier = pltpu.get_barrier_semaphore()
        for peer in peers:
            pl.semaphore_signal(
                barrier, inc=1, device_id=device(**dict(zip(AXES, peer))), device_id_type=MESH_ID
            )
        pl.semaphore_wait(barrier, len(peers))

        count = [0, 0]
        sent, local = [], []

        def put(src, dst, **off):
            k = count[0]
            count[0] += 1
            copy = pltpu.make_async_remote_copy(
                src_ref=src, dst_ref=dst, send_sem=send_sem.at[k], recv_sem=recv_sem.at[k],
                device_id=device(**off), device_id_type=MESH_ID,
            )
            copy.start()
            sent.append(copy)
            return copy

        def move(src, dst):
            k = count[1]
            count[1] += 1
            copy = pltpu.make_async_copy(src, dst, local_sem.at[k])
            copy.start()
            return copy

        class Gather:
            def __init__(self, buf, block, pieces):
                self.buf, self.block, self.pieces = buf, block, pieces

            def slot(self, dh, dl, dy, dx, dc):
                place = at("zh", dh)
                for a, d in (("zl", dl), ("y", dy), ("x", dx), ("c", dc)):
                    place = place * sizes[a] + at(a, d)
                start = pl.multiple_of(place * self.block, self.block)
                return self.buf.at[pl.ds(start, self.block)]

            def begin(self):
                self.own = move(self.pieces(x), self.slot(0, 0, 0, 0, 0))
                self.by_x = {
                    d: put(self.pieces(at("x", d)), self.slot(0, 0, 0, 0, 0), x=d)
                    for d in range(1, X)
                }

            def along_z(self):
                self.own.wait()
                for d in self.by_x:
                    self.by_x[d].wait_recv()
                self.by_z, self.by_y, self.by_c = {}, {}, {}
                for dh, dl in far[:0:-1]:
                    for dx in range(X):
                        s = self.slot(0, 0, 0, dx, 0)
                        self.by_z[dh, dl, dx] = put(s, s, zh=dh, zl=dl)
                for dx in range(X):
                    self.spread(0, 0, dx)

            def spread(self, dh, dl, dx):
                s = self.slot(-dh, -dl, 0, dx, 0)
                for d in range(1, Y):
                    self.by_y[dh, dl, d, dx] = put(s, s, y=d)
                self.to_core(dh, dl, 0, dx)

            def to_core(self, dh, dl, dy, dx):
                s = self.slot(-dh, -dl, -dy, dx, 0)
                for d in range(1, C):
                    self.by_c[dh, dl, dy, d, dx] = put(s, s, c=d)

            def along_y(self):
                for dh, dl in far[1:]:
                    for dx in range(X):
                        self.by_z[dh, dl, dx].wait_recv()
                        self.spread(dh, dl, dx)

            def along_c(self):
                for dh, dl in far:
                    for d in range(1, Y):
                        for dx in range(X):
                            self.by_y[dh, dl, d, dx].wait_recv()
                            self.to_core(dh, dl, d, dx)

            def end(self):
                for copy in self.by_c.values():
                    copy.wait_recv()

        class Units:
            def __init__(self, at_m, buf):
                self.m, self.buf = at_m, buf

            def slot(self, dh, dl, dy):
                return self.buf.at[at("zh", dh), at("zl", dl), at("y", dy)]

            def begin(self):
                mine = half.at[self.m, zh]
                s = self.slot(0, 0, 0)
                self.own = move(mine, s)
                self.by_h = {
                    d: put(half.at[self.m, at("zh", d)], s, zh=d) for d in range(1, ZH)
                }
                self.by_l, self.by_y = {}, {}
                for d in range(1, ZL):
                    self.by_l[0, d] = put(mine, s, zl=d)
                for d in range(1, Y):
                    self.by_y[0, 0, d] = put(mine, s, y=d)

            def middle(self):
                for dh in self.by_h:
                    self.by_h[dh].wait_recv()
                    s = self.slot(-dh, 0, 0)
                    for d in range(1, ZL):
                        self.by_l[dh, d] = put(s, s, zl=d)
                    for d in range(1, Y):
                        self.by_y[dh, 0, d] = put(s, s, y=d)

            def last(self):
                for dh, dl in list(self.by_l):
                    self.by_l[dh, dl].wait_recv()
                    s = self.slot(-dh, -dl, 0)
                    for d in range(1, Y):
                        self.by_y[dh, dl, d] = put(s, s, y=d)

            def end(self):
                self.own.wait()
                for copy in self.by_y.values():
                    copy.wait_recv()

        class Rows:
            def __init__(self, buf):
                self.buf = buf

            def begin(self, src):
                self.own = move(src, self.buf.at[0, 0, 0])
                self.by_n = {
                    (dh, dx): put(src, self.buf.at[0, -dh % ZH, -dx % X], zh=dh, x=dx)
                    for dh, dx in near[1:]
                }
                self.by_c = [put(src, self.buf.at[-d % C, 0, 0], c=d) for d in range(1, C)]

            def to_core(self):
                for dh, dx in near[1:]:
                    self.by_n[dh, dx].wait_recv()
                    a, b = -dh % ZH, -dx % X
                    for d in range(1, C):
                        self.by_c.append(put(self.buf.at[0, a, b], self.buf.at[-d % C, a, b], c=d))

            def end(self):
                self.own.wait()
                for copy in self.by_c:
                    copy.wait_recv()

        wq_g = Gather(w1, part, lambda to: qkv_ref.at[to])
        wo_g = Gather(wo, part, lambda to: out_ref.at[to])
        sm_g = Gather(sm, 8, lambda to: small_ref)
        wq_g.begin()
        sm_g.begin()
        xr_own = move(own_ref, xr.at[0, 0])
        xr_x = {d: put(own_ref, xr.at[0, -d % X], x=d) for d in range(1, X)}
        wo_g.begin()
        raws = [move(g_ref, raw.at[0]), move(u_ref, raw.at[1]), move(d_ref, raw_d)]
        sm_g.along_z()
        wq_g.along_z()

        lens = [len_ref[0, j] for j in range(docs)]
        ends = []
        for j in range(docs):
            ends.append(lens[j] if j == 0 else ends[-1] + lens[j])

        def slot_base(dc, dx):
            return (at("x", dx) * C + at("c", dc)) * rows

        def doc_of(index):
            doc = jnp.zeros(index.shape, jnp.int32)
            first = jnp.zeros(index.shape, jnp.int32)
            for j in range(docs):
                past = (index >= ends[j]).astype(jnp.int32)
                doc = doc + past
                first = first + past * lens[j]
            return doc, index - first

        lane = lax.broadcasted_iota(jnp.int32, (rows, HEAD_WIDTH), 1)
        folded = jnp.where(lane >= HEAD_WIDTH // 2, lane - HEAD_WIDTH // 2, lane)
        freq = jnp.exp(folded.astype(F32) * (-2.0 * math.log(ROPE_BASE) / HEAD_WIDTH))
        sign = jnp.where(lane >= HEAD_WIDTH // 2, 1.0, -1.0)
        slots = [(dc, dx) for dc in range(C) for dx in range(X)]
        for k, (dc, dx) in enumerate(slots):
            index = slot_base(dc, dx) + lax.broadcasted_iota(jnp.int32, (rows, HEAD_WIDTH), 0)
            angle = doc_of(index)[1].astype(F32) * freq
            cos_s[k * rows : (k + 1) * rows] = jnp.cos(angle)
            sin_s[k * rows : (k + 1) * rows] = jnp.sin(angle) * sign
        for a in range(X):
            q_index = slot_base(0, a) + lax.broadcasted_iota(jnp.int32, (rows, rows), 0)
            q_doc = doc_of(q_index)[0]
            for k, (dc, dx) in enumerate(slots):
                k_index = slot_base(dc, dx) + lax.broadcasted_iota(jnp.int32, (rows, rows), 1)
                k_doc = doc_of(k_index)[0]
                allowed = (q_doc == k_doc) & (k_index <= q_index)
                mask_s[a * rows : (a + 1) * rows, k * rows : (k + 1) * rows] = jnp.where(
                    allowed, 0.0, NEGATIVE_BIG
                )

        for r in raws:
            r.wait()
        for m in range(2):
            for h in range(ZH):
                half[m, h] = raw[m, :, h * units : (h + 1) * units]
        eye = (
            lax.broadcasted_iota(jnp.int32, (depth, depth), 0)
            == lax.broadcasted_iota(jnp.int32, (depth, depth), 1)
        ).astype(BF)
        for h in range(ZH):
            half[2, h] = nt(eye, raw_d[h * units : (h + 1) * units]).astype(BF)

        xr_own.wait()
        for d in xr_x:
            xr_x[d].wait_recv()
        xr_c = [
            put(xr.at[0, k], xr.at[-d % C, k], c=d) for d in range(1, C) for k in range(X)
        ]
        sm_g.along_y()
        wq_g.along_y()
        wo_g.along_z()
        wu, wgt, wdn = Units(1, wu_o), Units(0, wg_o), Units(2, wd_o)
        wgt.begin()
        sm_g.along_c()
        wq_g.along_c()
        wo_g.along_y()
        sm_g.end()

        def spread_row(k, block, total):
            pieces = sm[...].reshape(devices, 8, 128)[:, k, :].astype(BF)
            left = lax.broadcasted_iota(jnp.int32, (128, total), 0)
            right = lax.broadcasted_iota(jnp.int32, (128, total), 1)
            select = (lax.rem(right, block) == left).astype(BF)
            wide = nn(pieces, select)
            owner = lax.broadcasted_iota(jnp.int32, (devices, total), 0)
            place = lax.broadcasted_iota(jnp.int32, (devices, total), 1)
            inside = (place >= owner * block) & (place < (owner + 1) * block)
            return jnp.sum(jnp.where(inside, wide, 0.0), axis=0, keepdims=True)

        rows_s[0:1, :width] = spread_row(0, part, width)
        rows_s[1:2, :width] = spread_row(1, part, width)
        rows_s[2:3, :] = spread_row(2, bias_part, QKV_WIDTH)

        for copy in xr_c:
            copy.wait_recv()
        for k, (dc, dx) in enumerate(slots):
            v = xr[dc, dx].astype(F32)
            r = lax.rsqrt(jnp.mean(v * v, axis=-1, keepdims=True) + EPSILON)
            n1[k * rows : (k + 1) * rows] = (v * r * rows_s[0:1, :width]).astype(BF)
        n1_out = move(n1.at[0:query_rows], n1_o)
        wq_g.end()
        outs = [n1_out, move(w1, wqkv_o), move(rows_s, vec_o)]
        kv_at = lax.div(x * heads, QUERY_HEADS // KEY_VALUE_HEADS) * HEAD_WIDTH
        k_off = QUERY_HEADS * HEAD_WIDTH + kv_at
        v_off = k_off + KEY_VALUE_HEADS * HEAD_WIDTH
        wgt.middle()
        wu.begin()

        def turn(v, first, amount):
            return v * cos_s[first : first + amount] + pltpu.roll(
                v, HEAD_WIDTH // 2, 1
            ) * sin_s[first : first + amount]

        def bias_at(start, amount):
            return rows_s[2:3, pl.ds(pl.multiple_of(start, 128), amount)]

        @pl.loop(0, heads)
        def _(h):
            cols = pl.ds(pl.multiple_of(h * HEAD_WIDTH, HEAD_WIDTH), HEAD_WIDTH)
            v = nn(n1[0:query_rows], w1[:, cols])
            v = v + bias_at(x * q_cols + h * HEAD_WIDTH, HEAD_WIDTH)
            qs[:, cols] = turn(v, 0, query_rows).astype(BF)

        for j in range(kv_heads):
            at_k = q_cols + j * HEAD_WIDTH
            v = nn(n1[...], w1[:, at_k : at_k + HEAD_WIDTH]) + bias_at(k_off, kv_cols)[
                :, j * HEAD_WIDTH : (j + 1) * HEAD_WIDTH
            ]
            kv[:, j * HEAD_WIDTH : (j + 1) * HEAD_WIDTH] = turn(v, 0, pack_rows).astype(BF)
        v = nn(n1[...], w1[:, q_cols + kv_cols :]) + bias_at(v_off, kv_cols)
        kv[:, kv_cols:] = v.astype(BF)
        outs += [move(qs, q_o), move(kv, kv_o)]
        wo_g.along_c()
        wgt.last()
        wu.middle()
        wdn.begin()
        go_rows = Rows(go_o)
        go_rows.begin(cot_ref)

        @pl.loop(0, heads)
        def _(h):
            cols = pl.ds(pl.multiple_of(h * HEAD_WIDTH, HEAD_WIDTH), HEAD_WIDTH)
            g = lax.div(h, share)
            k_h = kv[:, pl.ds(pl.multiple_of(g * HEAD_WIDTH, HEAD_WIDTH), HEAD_WIDTH)]
            v_h = kv[:, pl.ds(pl.multiple_of(kv_cols + g * HEAD_WIDTH, HEAD_WIDTH), HEAD_WIDTH)]
            s = nt(qs[:, cols], k_h) * scale + mask_s[...]
            e = jnp.exp(s - jnp.max(s, axis=-1, keepdims=True))
            p = (e / jnp.sum(e, axis=-1, keepdims=True)).astype(BF)
            ps[h] = p
            ob[:, cols] = nn(p, v_h).astype(BF)

        outs += [move(ps, p_o), move(ob, att_o)]
        wo_g.end()
        outs.append(move(wo, wout_o))
        wu.last()
        wdn.middle()
        block = 256
        for d in list(range(1, X)) + [0]:
            @pl.loop(0, width // block)
            def _(j, d=d):
                cols = pl.ds(pl.multiple_of(j * block, block), block)
                v = nt(ob[d * rows : (d + 1) * rows], wo[cols])
                if d:
                    part_send[d - 1, :, cols] = v.astype(BF)
                else:
                    hs[:, cols] = v

            if d:
                part_recv_copy = put(part_send.at[d - 1], part_recv.at[d - 1], x=d)
                parts = [part_recv_copy] if d == 1 else parts + [part_recv_copy]
        h = hs[...] + own_row(xr)
        for d in range(1, X):
            parts[d - 1].wait_recv()
            h = h + part_recv[d - 1].astype(F32)
        hs[...] = h
        r = lax.rsqrt(jnp.mean(h * h, axis=-1, keepdims=True) + EPSILON)
        n2s[...] = (h * r * rows_s[1:2, :width]).astype(BF)
        nr_rows = Rows(nr_o)
        nr_rows.begin(n2s)
        outs.append(move(hs, h_o))
        wdn.last()
        nr_rows.to_core()
        go_rows.to_core()
        wgt.end()
        wu.end()
        wdn.end()
        nr_rows.end()
        go_rows.end()
        for copy in outs:
            copy.wait()
        for copy in sent:
            copy.wait_send()
        assert count[0] <= n_sems, count

    def own_row(xr):
        return xr[0, 0].astype(F32)

    any_spec = pl.BlockSpec(memory_space=pl.ANY)
    whole = (ZH, ZL, Y, depth, units)
    group = (C, ZH, X, rows, width)
    sds = jax.ShapeDtypeStruct
    return pl.pallas_call(
        kernel,
        out_shape=[
            sds((width, qkv_n), BF), sds((width, q_cols), BF), sds((query_rows, width), BF),
            sds((query_rows, q_cols), BF), sds((pack_rows, 2 * kv_cols), BF),
            sds((heads, query_rows, pack_rows), BF), sds((query_rows, q_cols), BF),
            sds((rows, width), F32), sds(group, BF), sds(group, BF),
            sds(whole, BF), sds(whole, BF), sds(whole, BF),
            sds((8, QKV_WIDTH), F32),
        ],
        in_specs=[any_spec, any_spec, pl.BlockSpec(memory_space=pltpu.SMEM)] + [any_spec] * 6,
        out_specs=[any_spec] * 14,
        scratch_shapes=[
            pltpu.VMEM((C, X, rows, width), BF),
            pltpu.VMEM((width, qkv_n), BF),
            pltpu.VMEM((width, q_cols), BF),
            pltpu.VMEM((devices * 8, 128), F32),
            pltpu.VMEM((pack_rows, width), BF),
            pltpu.VMEM((query_rows, q_cols), BF),
            pltpu.VMEM((pack_rows, 2 * kv_cols), BF),
            pltpu.VMEM((query_rows, q_cols), BF),
            pltpu.VMEM((max(X - 1, 1), rows, width), BF),
            pltpu.VMEM((max(X - 1, 1), rows, width), BF),
            pltpu.VMEM((rows, width), BF),
            pltpu.VMEM((rows, width), F32),
            pltpu.VMEM((pack_rows, HEAD_WIDTH), F32),
            pltpu.VMEM((pack_rows, HEAD_WIDTH), F32),
            pltpu.VMEM((query_rows, pack_rows), F32),
            pltpu.VMEM((8, QKV_WIDTH), F32),
            pltpu.VMEM((heads, query_rows, pack_rows), BF),
            pltpu.VMEM((2,) + w_gate.shape, BF),
            pltpu.VMEM(w_down.shape, BF),
            pltpu.VMEM((3, ZH, depth, units), BF),
            pltpu.SemaphoreType.DMA((n_sems,)),
            pltpu.SemaphoreType.DMA((n_sems,)),
            pltpu.SemaphoreType.DMA((32,)),
        ],
        compiler_params=pltpu.CompilerParams(
            collective_id=0, has_side_effects=True, vmem_limit_bytes=60 << 20
        ),
        name="front",
    )(own_in, cotangent, lengths, qkv_pieces, out_pieces, small, w_gate, w_up, w_down)


def small_rows(gain_one, gain_two, bias):
    wide = [jnp.pad(v.astype(F32), (0, 128 - v.shape[0])) for v in (gain_one, gain_two, bias)]
    return jnp.pad(jnp.stack(wide), ((0, 5), (0, 0)))


def shards(
    layer_in, lengths, w_qkv, b_qkv, w_out, norm1_gain, norm2_gain, w_gate, w_up, w_down, grad_out
):
    size = lax.axis_size
    ZH, ZL, Y, X, C = (size(a) for a in ("zh", "zl", "y", "x", "c"))
    zh, zl, y, x, c = (lax.axis_index(a) for a in ("zh", "zl", "y", "x", "c"))
    everyone = ("zh", "zl", "y", "x", "c")
    devices = ZH * ZL * Y * X * C
    rows, width = layer_in.shape[1:]
    part = w_qkv.shape[0]
    group = QUERY_HEADS // KEY_VALUE_HEADS
    heads = QUERY_HEADS // X
    kv_heads = max(1, heads // group)
    share = heads // kv_heads
    q_cols, kv_cols = heads * HEAD_WIDTH, kv_heads * HEAD_WIDTH
    scale = HEAD_WIDTH ** (-0.5)

    own_in = layer_in[0]
    cotangent = grad_out[0]
    own_rows = own_in.astype(F32)
    query_rows, pack_rows = X * rows, C * X * rows
    bias_part = b_qkv.shape[0]
    def row_index(cores):
        spans = [
            (((x + dx) % X) * C + (c + dc) % C) * rows + jnp.arange(rows, dtype=jnp.int32)
            for dc in range(cores)
            for dx in range(X)
        ]
        return jnp.concatenate(spans)

    doc_lengths = lengths[0]
    key_index = row_index(C)
    key_doc, key_pos = doc_layout(key_index, doc_lengths)
    query_index, query_doc = key_index[:query_rows], key_doc[:query_rows]
    key_cos, key_sin = angles(key_pos)
    query_cos, query_sin = key_cos[:query_rows], key_sin[:query_rows]

    def gather_columns(pieces):
        held = ordered(
            [pick(pieces, x)] + [fetch(pick(pieces, (x - d) % X), "x", d) for d in range(1, X)],
            "x",
        )
        whole = jnp.zeros((ZH, ZL, Y) + held.shape, held.dtype)
        for dh in range(ZH):
            for dl in range(ZL):
                along = held if dh == dl == 0 else fetch(held, ("zh", "zl"), (dh, dl))
                for dy in range(Y):
                    piece = along if dy == 0 else fetch(along, "y", dy)
                    whole = lax.dynamic_update_slice(
                        whole,
                        piece[None, None, None],
                        ((zh + dh) % ZH, (zl + dl) % ZL, (y + dy) % Y, 0, 0, 0),
                    )
        whole = whole.reshape((ZH * ZL * Y * X,) + whole.shape[4:])
        both = ordered([whole] + [fetch(whole, "c", d) for d in range(1, C)], "c")
        return jnp.moveaxis(both, 0, 1).reshape(width, whole.shape[-1])

    def scatter_columns(grad):
        n = grad.shape[-1]
        grad = grad.astype(BF).reshape(ZH * ZL * Y * X, C, part, n)
        held = pick(grad, c, 1).astype(F32)
        for d in range(1, C):
            held = held + send(pick(grad, (c + d) % C, 1), "c", d)
        held = held.astype(BF).reshape(ZH, ZL, Y, X * part, n)
        kept = pick(held, y, 2).astype(F32)
        for d in range(1, Y):
            kept = kept + send(pick(held, (y + d) % Y, 2), "y", d)
        low = kept.astype(BF)
        total = 0.0
        for dh in range(ZH):
            for dl in range(ZL):
                if dh == dl == 0:
                    total = total + pick(pick(kept, zh), zl)
                else:
                    piece = pick(pick(low, (zh + dh) % ZH), (zl + dl) % ZL)
                    total = total + send(piece, ("zh", "zl"), (dh, dl)).astype(F32)
        total = total.reshape(X, part, n)
        lower = total.astype(BF)
        return ordered(
            [pick(total, x)]
            + [fetch(pick(lower, (x - d) % X), "x", d).astype(F32) for d in range(1, X)],
            "x",
        )

    def qkv_columns(array):
        blocks = []
        for at in range(X):
            kv = (at * heads) // group * HEAD_WIDTH
            key_at = QUERY_HEADS * HEAD_WIDTH + kv
            value_at = key_at + KEY_VALUE_HEADS * HEAD_WIDTH
            blocks.append(
                jnp.concatenate(
                    [
                        array[..., at * q_cols : (at + 1) * q_cols],
                        array[..., key_at : key_at + kv_cols],
                        array[..., value_at : value_at + kv_cols],
                    ],
                    axis=-1,
                )
            )
        return jnp.stack(blocks)

    def qkv_whole(blocks):
        queries = [blocks[at, ..., :q_cols] for at in range(X)]
        keys, values = [0.0] * KEY_VALUE_HEADS, [0.0] * KEY_VALUE_HEADS
        for at in range(X):
            for j in range(kv_heads):
                head = (at * heads) // group + j
                start = q_cols + j * HEAD_WIDTH
                keys[head] = keys[head] + blocks[at, ..., start : start + HEAD_WIDTH]
                start = start + kv_cols
                values[head] = values[head] + blocks[at, ..., start : start + HEAD_WIDTH]
        return jnp.concatenate(queries + keys + values, axis=-1)

    depth, units = w_gate.shape[0], w_gate.shape[1] // ZH

    def gather_units(weight):
        halves = weight.reshape(depth, ZH, units).transpose(1, 0, 2)
        whole = jnp.zeros((ZH, ZL, Y, depth, units), weight.dtype)
        for dh in range(ZH):
            first = pick(halves, zh) if dh == 0 else fetch(pick(halves, (zh - dh) % ZH), "zh", dh)
            for dl in range(ZL):
                second = first if dl == 0 else fetch(first, "zl", dl)
                for dy in range(Y):
                    third = second if dy == 0 else fetch(second, "y", dy)
                    whole = lax.dynamic_update_slice(
                        whole,
                        third[None, None, None],
                        ((zh + dh) % ZH, (zl + dl) % ZL, (y + dy) % Y, 0, 0),
                    )
        return whole.reshape(width, units)

    def scatter_units(grad):
        grad = grad.astype(BF).reshape(ZH, ZL, Y, depth, units)
        done = [None] * ZH
        for dh in reversed(range(ZH)):
            mine = pick(grad, (zh + dh) % ZH)
            kept = pick(mine, y, 1).astype(F32)
            for d in range(1, Y):
                kept = kept + send(pick(mine, (y + d) % Y, 1), "y", d).astype(F32)
            low = kept.astype(BF)
            total = pick(kept, zl)
            for d in range(1, ZL):
                total = total + send(pick(low, (zl + d) % ZL), "zl", d).astype(F32)
            done[dh] = total
        halves = [done[0]] + [
            send(done[dh].astype(BF), "zh", dh).astype(F32) for dh in range(1, ZH)
        ]
        halves = [halves[0]] + halves[:0:-1]
        return jnp.moveaxis(ordered(halves, "zh"), 0, 1).reshape(depth, ZH * units)

    near = [(dh, dx) for dh in range(ZH) for dx in range(X)]

    def gather_rows(own):
        held = jnp.concatenate([own if k == (0, 0) else fetch(own, ("zh", "x"), k) for k in near])
        return jnp.concatenate([held] + [fetch(held, "c", d) for d in range(1, C)])

    def scatter_rows(term):
        term = term.reshape(C, len(near), rows, width)
        held = term[0].astype(F32)
        for d in range(1, C):
            held = held + send(term[d].astype(BF), "c", d).astype(F32)
        total = held[0]
        for at, k in enumerate(near):
            if k != (0, 0):
                total = total + send(held[at].astype(BF), ("zh", "x"), k).astype(F32)
        return total

    def scatter_x(term):
        term = term.reshape(X, rows, width)
        total = term[0]
        for d in range(1, X):
            total = total + send(term[d].astype(BF), "x", d).astype(F32)
        return total

    if part % 16 == 0 and depth % 16 == 0 and heads % kv_heads == 0:
        wqkv_mine, wout_mine, query_normed, queries, kv_low, probs_low, attended_low, middle, group_normed, group_cotangent, wgate_mine, wup_mine, wdown_mine, vectors = front(
            own_in,
            cotangent,
            lengths,
            qkv_columns(w_qkv),
            jnp.stack([w_out.T[:, at * q_cols : (at + 1) * q_cols] for at in range(X)]),
            small_rows(norm1_gain, norm2_gain, b_qkv),
            w_gate,
            w_up,
            w_down,
        )
        wgate_mine, wup_mine, wdown_mine = (
            w.reshape(width, units) for w in (wgate_mine, wup_mine, wdown_mine)
        )
        group_normed = group_normed.reshape(-1, width)
        group_cotangent = group_cotangent.reshape(-1, width)
        gain_one, gain_two = vectors[0:1, :width], vectors[1:2, :width]
        queries = queries.reshape(query_rows, kv_heads, share, HEAD_WIDTH)
        keys = kv_low[:, :kv_cols].reshape(pack_rows, kv_heads, HEAD_WIDTH)
        values = kv_low[:, kv_cols:].reshape(pack_rows, kv_heads, HEAD_WIDTH)
        probs_low = probs_low.reshape(kv_heads, share, query_rows, pack_rows)
    else:
        small = jnp.concatenate([norm1_gain, norm2_gain, b_qkv])
        small = jnp.pad(small, (0, -small.shape[0] % 256))[None]
        small = lax.all_to_all(
            jnp.broadcast_to(small[None], (devices,) + small.shape), everyone, 0, 0, tiled=True
        )[:, 0].astype(F32)
        gain_one = small[:, :part].reshape(1, width)
        gain_two = small[:, part : 2 * part].reshape(1, width)
        bias = small[:, 2 * part : 2 * part + bias_part].reshape(-1)

        query_in = jnp.concatenate([own_in] + [fetch(own_in, "x", d) for d in range(1, X)])
        pack_in = jnp.concatenate([query_in] + [fetch(query_in, "c", d) for d in range(1, C)])

        wqkv_mine = gather_columns(qkv_columns(w_qkv))
        wout_t = w_out.T
        wout_mine = gather_columns(
            jnp.stack([wout_t[:, at * q_cols : (at + 1) * q_cols] for at in range(X)])
        )
        bias_mine = pick(qkv_columns(bias), x)

        wgate_mine, wup_mine = gather_units(w_gate), gather_units(w_up)
        wdown_mine = gather_units(w_down.T)

        group_cotangent = gather_rows(cotangent)

        pack_in = pack_in.astype(F32)
        normed_one = (pack_in * rms_parts(pack_in) * gain_one).astype(BF)
        query_normed = normed_one[:query_rows]
        pre_query = nn(query_normed, wqkv_mine[:, :q_cols]) + bias_mine[:q_cols]
        pre_kv = nn(normed_one, wqkv_mine[:, q_cols:]) + bias_mine[q_cols:]
        queries = rotate(
            pre_query.reshape(query_rows, heads, HEAD_WIDTH), query_cos, query_sin
        ).astype(BF)
        queries = queries.reshape(query_rows, kv_heads, share, HEAD_WIDTH)
        keys = rotate(
            pre_kv[:, :kv_cols].reshape(pack_rows, kv_heads, HEAD_WIDTH), key_cos, key_sin
        ).astype(BF)
        values = pre_kv[:, kv_cols:].reshape(pack_rows, kv_heads, HEAD_WIDTH).astype(BF)
        scores = jnp.einsum("tkgd,skd->kgts", queries, keys, preferred_element_type=F32) * scale
        allowed = (query_doc[:, None] == key_doc[None, :]) & (
            key_index[None, :] <= query_index[:, None]
        )
        masked = jnp.where(allowed, scores, NEGATIVE_BIG)
        top = jnp.max(masked, axis=-1, keepdims=True)
        weights = jnp.where(allowed, jnp.exp(masked - top), 0.0)
        probs = weights / jnp.sum(weights, axis=-1, keepdims=True)
        probs_low = probs.astype(BF)
        attended = jnp.einsum("kgts,skd->tkgd", probs_low, values, preferred_element_type=F32)
        attended_low = attended.reshape(query_rows, q_cols).astype(BF)
        middle = own_rows + scatter_x(nt(attended_low, wout_mine))
        normed_two = (middle * rms_parts(middle) * gain_two).astype(BF)

        group_normed = gather_rows(normed_two)

    gate = nn(group_normed, wgate_mine)
    up_part = nn(group_normed, wup_mine)
    sig = jax.nn.sigmoid(gate)
    act = gate * sig
    hidden = (act * up_part).astype(BF)
    grad_wdown = tn(group_cotangent, hidden).astype(BF)
    grad_hidden = nn(group_cotangent, wdown_mine)
    grad_gate = (grad_hidden * up_part * sig * (1.0 + gate * (1.0 - sig))).astype(BF)
    grad_up = (grad_hidden * act).astype(BF)
    grad_normed_two = scatter_rows(nt(grad_gate, wgate_mine) + nt(grad_up, wup_mine))
    grad_wgate = tn(group_normed, grad_gate).astype(BF)
    grad_wup = tn(group_normed, grad_up).astype(BF)
    layer_out = (middle + scatter_rows(nt(hidden, wdown_mine))).astype(BF)
    sum_wdown = scatter_units(grad_wdown).T
    sum_wgate = scatter_units(grad_wgate)
    sum_wup = scatter_units(grad_wup)

    back_two, grad_gain_two = rms_back(middle, gain_two, grad_normed_two)
    grad_middle = cotangent.astype(F32) + back_two
    grad_att = grad_middle.astype(BF)
    query_grad_att = jnp.concatenate([grad_att] + [fetch(grad_att, "x", d) for d in range(1, X)])
    sum_wout = scatter_columns(tn(query_grad_att, attended_low))
    head_grads = nn(query_grad_att, wout_mine).astype(BF)
    head_grads = head_grads.reshape(query_rows, kv_heads, share, HEAD_WIDTH)
    grad_probs = jnp.einsum("tkgd,skd->kgts", head_grads, values, preferred_element_type=F32)
    probs = probs_low.astype(F32)
    delta = jnp.sum(probs * grad_probs, axis=-1, keepdims=True)
    grad_scores = (probs * (grad_probs - delta)).astype(BF)
    grad_query = (
        jnp.einsum("kgts,skd->tkgd", grad_scores, keys, preferred_element_type=F32) * scale
    )
    grad_key = jnp.einsum("kgts,tkgd->skd", grad_scores, queries, preferred_element_type=F32)
    grad_key = rotate(grad_key * scale, key_cos, -key_sin)
    grad_value = jnp.einsum("kgts,tkgd->skd", probs_low, head_grads, preferred_element_type=F32)
    grad_kv = jnp.concatenate(
        [grad_key.reshape(pack_rows, kv_cols), grad_value.reshape(pack_rows, kv_cols)], axis=1
    ).reshape(C, query_rows, 2 * kv_cols)
    kv_total = grad_kv[0]
    for d in range(1, C):
        kv_total = kv_total + send(grad_kv[d].astype(BF), "c", d).astype(F32)
    grad_query = rotate(
        grad_query.reshape(query_rows, heads, HEAD_WIDTH), query_cos, -query_sin
    ).reshape(query_rows, q_cols)
    grad_pre = jnp.concatenate([grad_query, kv_total], axis=1).astype(BF)
    sum_wqkv = qkv_whole(scatter_columns(tn(query_normed, grad_pre)))
    grad_bias = jnp.sum(grad_pre.astype(F32), axis=0)
    grad_normed_one = scatter_x(nt(grad_pre, wqkv_mine))
    back_one, grad_gain_one = rms_back(own_rows, gain_one, grad_normed_one)
    grad_input = grad_middle + back_one

    bias_blocks = jnp.where(
        jnp.arange(X, dtype=jnp.int32)[:, None] == x, grad_bias[None, :], 0.0
    )
    bias_whole = qkv_whole(bias_blocks)
    piece = jnp.concatenate(
        [
            grad_gain_one.reshape(devices, part),
            grad_gain_two.reshape(devices, part),
            bias_whole.reshape(devices, bias_part),
        ],
        axis=1,
    )
    piece = jnp.pad(piece, ((0, 0), (0, -piece.shape[1] % 256)))
    piece = jnp.sum(lax.all_to_all(piece[:, None], everyone, 0, 0, tiled=True)[:, 0], axis=0)
    return (
        layer_out[None],
        grad_input[None],
        sum_wqkv,
        piece[2 * part : 2 * part + bias_part],
        jnp.moveaxis(sum_wout, 0, 1).reshape(part, -1).T,
        piece[:part],
        piece[part : 2 * part],
        sum_wgate,
        sum_wup,
        sum_wdown,
    )


def solution(mesh):
    wide, narrow = mesh.shape["wide"], mesh.shape["narrow"]
    cores = 2 if narrow % 2 == 0 else 1
    along_x = narrow // cores
    along_y = along_x if wide % along_x == 0 else 1
    along_z = wide // along_y
    far = 2 if along_z % 2 == 0 else 1
    split = Mesh(
        mesh.devices.reshape(far, along_z // far, along_y, along_x, cores),
        ("zh", "zl", "y", "x", "c"),
    )
    w, n = ("zh", "zl", "y"), ("x", "c")
    placed = (
        P(w, n, None),
        P(w, None),
        P(w + n, None),
        P(w + n),
        P(None, w + n),
        P(w + n),
        P(w + n),
        P(w, n),
        P(w, n),
        P(n, w),
        P(w, n, None),
    )
    return jax.shard_map(
        shards,
        mesh=split,
        in_specs=placed,
        out_specs=(
            P(w, n, None),
            P(w, n, None),
            P(w + n, None),
            P(w + n),
            P(None, w + n),
            P(w + n),
            P(w + n),
            P(w, n),
            P(w, n),
            P(n, w),
        ),
        check_vma=False,
    )
```

```python
import math

import jax
import jax.numpy as jnp
from jax import lax
from jax.experimental import pallas as pl
from jax.experimental.pallas import tpu as pltpu
from jax.sharding import Mesh
from jax.sharding import PartitionSpec as P

QUERY_HEADS = 12
KEY_VALUE_HEADS = 2
HEAD_WIDTH = 128

EPSILON = 1e-06
ROPE_BASE = 10000.0
NEGATIVE_BIG = -1e30
HIGHEST = lax.Precision.HIGHEST


BF = jnp.bfloat16
F32 = jnp.float32
AXES = ("zh", "zl", "y", "x", "c")
MESH_ID = pl.DeviceIdType.MESH
QKV_WIDTH = (QUERY_HEADS + 2 * KEY_VALUE_HEADS) * HEAD_WIDTH


def fetch(value, axes, offsets):
    axes = (axes,) if isinstance(axes, str) else tuple(axes)
    offsets = (offsets,) if isinstance(offsets, int) else tuple(offsets)
    sizes = [lax.axis_size(a) for a in axes]
    total = math.prod(sizes)
    pairs = []
    for flat in range(total):
        rest, place = flat, []
        for size in reversed(sizes):
            place.append(rest % size)
            rest //= size
        place = place[::-1]
        source = 0
        for spot, off, size in zip(place, offsets, sizes):
            source = source * size + (spot + off) % size
        pairs.append((source, flat))
    return lax.ppermute(value, axes if len(axes) > 1 else axes[0], pairs)


def send(value, axes, offsets):
    offsets = (offsets,) if isinstance(offsets, int) else tuple(offsets)
    return fetch(value, axes, tuple(-o for o in offsets))


def pick(stack, place, axis=0):
    return lax.dynamic_index_in_dim(stack, place, axis, keepdims=False)


def nn(left, right):
    return lax.dot_general(left, right, (((1,), (0,)), ((), ())), preferred_element_type=F32)


def nt(left, right):
    return lax.dot_general(left, right, (((1,), (1,)), ((), ())), preferred_element_type=F32)


def tn(left, right):
    return lax.dot_general(left, right, (((0,), (0,)), ((), ())), preferred_element_type=F32)


def rms_parts(rows):
    return lax.rsqrt(jnp.mean(rows * rows, axis=-1, keepdims=True) + EPSILON)


def rms_back(rows, gain, grad):
    r = rms_parts(rows)
    scaled = gain * grad
    return (
        r * scaled - rows * (r * r * r) * jnp.mean(scaled * rows, axis=-1, keepdims=True),
        jnp.sum(grad * rows * r, axis=0),
    )


def doc_layout(index, doc_lengths):
    ends = jnp.cumsum(doc_lengths)
    starts = ends - doc_lengths
    document_index = jnp.sum((index[:, None] >= ends[None, :]).astype(jnp.int32), axis=1)
    onehot = (
        document_index[:, None] == jnp.arange(doc_lengths.shape[0], dtype=jnp.int32)[None, :]
    ).astype(jnp.int32)
    token_position = index - jnp.sum(onehot * starts[None, :], axis=1)
    return document_index, token_position.astype(F32)


def angles(position):
    half = HEAD_WIDTH // 2
    freq = jnp.exp(jnp.arange(half, dtype=F32) * (-2.0 * math.log(ROPE_BASE) / HEAD_WIDTH))
    angle = position[:, None] * freq[None, :]
    return jnp.cos(angle)[:, None, :], jnp.sin(angle)[:, None, :]


def rotate(rows, cosine, sine):
    half = HEAD_WIDTH // 2
    first, second = rows[..., :half], rows[..., half:]
    return jnp.concatenate(
        [first * cosine - second * sine, second * cosine + first * sine], axis=-1
    )


def ordered(pieces, axis):
    count, here = len(pieces), lax.axis_index(axis)
    if count == 1:
        return pieces[0][None]
    if count == 2:
        return jnp.where(here == 0, jnp.stack(pieces), jnp.stack(pieces[::-1]))
    whole = jnp.zeros((count,) + pieces[0].shape, pieces[0].dtype)
    for distance, piece in enumerate(pieces):
        whole = lax.dynamic_update_index_in_dim(whole, piece, (here + distance) % count, 0)
    return whole


def front(own_in, cotangent, lengths, qkv_pieces, out_pieces, small, w_gate, w_up, w_down):
    size = lax.axis_size
    ZH, ZL, Y, X, C = (size(a) for a in AXES)
    rows, width = own_in.shape
    _, part, qkv_n = qkv_pieces.shape
    q_cols = out_pieces.shape[-1]
    heads = q_cols // HEAD_WIDTH
    kv_cols = (qkv_n - q_cols) // 2
    kv_heads = kv_cols // HEAD_WIDTH
    share = heads // kv_heads
    query_rows, pack_rows = X * rows, C * X * rows
    depth = w_gate.shape[0]
    units = w_gate.shape[1] // ZH
    near = [(dh, dx) for dh in range(ZH) for dx in range(X)]
    far = [(dh, dl) for dh in range(ZH) for dl in range(ZL)]
    devices = ZH * ZL * Y * X * C
    bias_part = QKV_WIDTH // devices
    scale = HEAD_WIDTH ** (-0.5)
    docs = lengths.shape[-1]
    n_sems = 400

    def kernel(
        own_ref, cot_ref, len_ref, qkv_ref, out_ref, small_ref, g_ref, u_ref, d_ref,
        wqkv_o, wout_o, n1_o, q_o, kv_o, p_o, att_o, h_o, nr_o, go_o, wg_o, wu_o, wd_o, vec_o, cos_o, sin_o,
        xr, w1, wo, sm, n1, qs, kv, ob, part_send, part_recv, n2s, hs,
        cos_s, sin_s, mask_s, rows_s, ps, raw, raw_d, half,
        send_sem, recv_sem, local_sem,
    ):
        zh, zl, y, x, c = (lax.axis_index(a) for a in AXES)
        sizes = dict(zip(AXES, (ZH, ZL, Y, X, C)))
        here = dict(zip(AXES, (zh, zl, y, x, c)))

        def device(**off):
            return tuple(
                lax.rem(here[a] + off[a], sizes[a]) if off.get(a, 0) % sizes[a] else here[a]
                for a in AXES
            )

        def at(a, d):
            d = d % sizes[a]
            return lax.rem(here[a] + d, sizes[a]) if d else here[a]

        peers = set()
        for d in range(1, C):
            peers.add((0, 0, 0, 0, d))
        for dh, dx in near[1:]:
            peers.add((dh, 0, 0, dx, 0))
        for dh, dl in far[1:]:
            peers.add((dh, dl, 0, 0, 0))
        for d in range(1, Y):
            peers.add((0, 0, d, 0, 0))
        peers = sorted(peers)
        barrier = pltpu.get_barrier_semaphore()
        for peer in peers:
            pl.semaphore_signal(
                barrier, inc=1, device_id=device(**dict(zip(AXES, peer))), device_id_type=MESH_ID
            )
        pl.semaphore_wait(barrier, len(peers))

        count = [0, 0]
        sent, local = [], []

        def put(src, dst, **off):
            k = count[0]
            count[0] += 1
            copy = pltpu.make_async_remote_copy(
                src_ref=src, dst_ref=dst, send_sem=send_sem.at[k], recv_sem=recv_sem.at[k],
                device_id=device(**off), device_id_type=MESH_ID,
            )
            copy.start()
            sent.append(copy)
            return copy

        def move(src, dst):
            k = count[1]
            count[1] += 1
            copy = pltpu.make_async_copy(src, dst, local_sem.at[k])
            copy.start()
            return copy

        class Gather:
            def __init__(self, buf, block, pieces):
                self.buf, self.block, self.pieces = buf, block, pieces

            def slot(self, dh, dl, dy, dx, dc):
                place = at("zh", dh)
                for a, d in (("zl", dl), ("y", dy), ("x", dx), ("c", dc)):
                    place = place * sizes[a] + at(a, d)
                start = pl.multiple_of(place * self.block, self.block)
                return self.buf.at[pl.ds(start, self.block)]

            def begin(self):
                self.own = move(self.pieces(x), self.slot(0, 0, 0, 0, 0))
                self.by_x = {
                    d: put(self.pieces(at("x", d)), self.slot(0, 0, 0, 0, 0), x=d)
                    for d in range(1, X)
                }

            def along_z(self):
                self.own.wait()
                for d in self.by_x:
                    self.by_x[d].wait_recv()
                self.by_z, self.by_y, self.by_c = {}, {}, {}
                for dh, dl in far[:0:-1]:
                    for dx in range(X):
                        s = self.slot(0, 0, 0, dx, 0)
                        self.by_z[dh, dl, dx] = put(s, s, zh=dh, zl=dl)
                for dx in range(X):
                    self.spread(0, 0, dx)

            def spread(self, dh, dl, dx):
                s = self.slot(-dh, -dl, 0, dx, 0)
                for d in range(1, Y):
                    self.by_y[dh, dl, d, dx] = put(s, s, y=d)
                self.to_core(dh, dl, 0, dx)

            def to_core(self, dh, dl, dy, dx):
                s = self.slot(-dh, -dl, -dy, dx, 0)
                for d in range(1, C):
                    self.by_c[dh, dl, dy, d, dx] = put(s, s, c=d)

            def along_y(self):
                for dh, dl in far[1:]:
                    for dx in range(X):
                        self.by_z[dh, dl, dx].wait_recv()
                        self.spread(dh, dl, dx)

            def along_c(self):
                for dh, dl in far:
                    for d in range(1, Y):
                        for dx in range(X):
                            self.by_y[dh, dl, d, dx].wait_recv()
                            self.to_core(dh, dl, d, dx)

            def end(self):
                for copy in self.by_c.values():
                    copy.wait_recv()

        class Units:
            def __init__(self, at_m, buf):
                self.m, self.buf = at_m, buf

            def slot(self, dh, dl, dy):
                return self.buf.at[at("zh", dh), at("zl", dl), at("y", dy)]

            def begin(self):
                mine = half.at[self.m, zh]
                s = self.slot(0, 0, 0)
                self.own = move(mine, s)
                self.by_h = {
                    d: put(half.at[self.m, at("zh", d)], s, zh=d) for d in range(1, ZH)
                }
                self.by_l, self.by_y = {}, {}
                for d in range(1, ZL):
                    self.by_l[0, d] = put(mine, s, zl=d)
                for d in range(1, Y):
                    self.by_y[0, 0, d] = put(mine, s, y=d)

            def middle(self):
                for dh in self.by_h:
                    self.by_h[dh].wait_recv()
                    s = self.slot(-dh, 0, 0)
                    for d in range(1, ZL):
                        self.by_l[dh, d] = put(s, s, zl=d)
                    for d in range(1, Y):
                        self.by_y[dh, 0, d] = put(s, s, y=d)

            def last(self):
                for dh, dl in list(self.by_l):
                    self.by_l[dh, dl].wait_recv()
                    s = self.slot(-dh, -dl, 0)
                    for d in range(1, Y):
                        self.by_y[dh, dl, d] = put(s, s, y=d)

            def end(self):
                self.own.wait()
                for copy in self.by_y.values():
                    copy.wait_recv()

        class Rows:
            def __init__(self, buf):
                self.buf = buf

            def begin(self, src):
                self.own = move(src, self.buf.at[0, 0, 0])
                self.by_n = {
                    (dh, dx): put(src, self.buf.at[0, -dh % ZH, -dx % X], zh=dh, x=dx)
                    for dh, dx in near[1:]
                }
                self.by_c = [put(src, self.buf.at[-d % C, 0, 0], c=d) for d in range(1, C)]

            def to_core(self):
                for dh, dx in near[1:]:
                    self.by_n[dh, dx].wait_recv()
                    a, b = -dh % ZH, -dx % X
                    for d in range(1, C):
                        self.by_c.append(put(self.buf.at[0, a, b], self.buf.at[-d % C, a, b], c=d))

            def end(self):
                self.own.wait()
                for copy in self.by_c:
                    copy.wait_recv()

        wq_g = Gather(w1, part, lambda to: qkv_ref.at[to])
        wo_g = Gather(wo, part, lambda to: out_ref.at[to])
        sm_g = Gather(sm, 8, lambda to: small_ref)
        wq_g.begin()
        sm_g.begin()
        xr_own = move(own_ref, xr.at[0, 0])
        xr_x = {d: put(own_ref, xr.at[0, -d % X], x=d) for d in range(1, X)}
        wo_g.begin()
        raws = [move(g_ref, raw.at[0]), move(u_ref, raw.at[1]), move(d_ref, raw_d)]
        sm_g.along_z()
        wq_g.along_z()

        lens = [len_ref[0, j] for j in range(docs)]
        ends = []
        for j in range(docs):
            ends.append(lens[j] if j == 0 else ends[-1] + lens[j])

        def slot_base(dc, dx):
            return (at("x", dx) * C + at("c", dc)) * rows

        def doc_of(index):
            doc = jnp.zeros(index.shape, jnp.int32)
            first = jnp.zeros(index.shape, jnp.int32)
            for j in range(docs):
                past = (index >= ends[j]).astype(jnp.int32)
                doc = doc + past
                first = first + past * lens[j]
            return doc, index - first

        lane = lax.broadcasted_iota(jnp.int32, (rows, HEAD_WIDTH), 1)
        folded = jnp.where(lane >= HEAD_WIDTH // 2, lane - HEAD_WIDTH // 2, lane)
        freq = jnp.exp(folded.astype(F32) * (-2.0 * math.log(ROPE_BASE) / HEAD_WIDTH))
        sign = jnp.where(lane >= HEAD_WIDTH // 2, 1.0, -1.0)
        slots = [(dc, dx) for dc in range(C) for dx in range(X)]
        for k, (dc, dx) in enumerate(slots):
            index = slot_base(dc, dx) + lax.broadcasted_iota(jnp.int32, (rows, HEAD_WIDTH), 0)
            angle = doc_of(index)[1].astype(F32) * freq
            cos_s[k * rows : (k + 1) * rows] = jnp.cos(angle)
            sin_s[k * rows : (k + 1) * rows] = jnp.sin(angle) * sign
        for a in range(X):
            q_index = slot_base(0, a) + lax.broadcasted_iota(jnp.int32, (rows, rows), 0)
            q_doc = doc_of(q_index)[0]
            for k, (dc, dx) in enumerate(slots):
                k_index = slot_base(dc, dx) + lax.broadcasted_iota(jnp.int32, (rows, rows), 1)
                k_doc = doc_of(k_index)[0]
                allowed = (q_doc == k_doc) & (k_index <= q_index)
                mask_s[a * rows : (a + 1) * rows, k * rows : (k + 1) * rows] = jnp.where(
                    allowed, 0.0, NEGATIVE_BIG
                )

        for r in raws:
            r.wait()
        for m in range(2):
            for h in range(ZH):
                half[m, h] = raw[m, :, h * units : (h + 1) * units]
        eye = (
            lax.broadcasted_iota(jnp.int32, (depth, depth), 0)
            == lax.broadcasted_iota(jnp.int32, (depth, depth), 1)
        ).astype(BF)
        for h in range(ZH):
            half[2, h] = nt(eye, raw_d[h * units : (h + 1) * units]).astype(BF)

        xr_own.wait()
        for d in xr_x:
            xr_x[d].wait_recv()
        xr_c = [
            put(xr.at[0, k], xr.at[-d % C, k], c=d) for d in range(1, C) for k in range(X)
        ]
        sm_g.along_y()
        wq_g.along_y()
        wo_g.along_z()
        wu, wgt, wdn = Units(1, wu_o), Units(0, wg_o), Units(2, wd_o)
        wgt.begin()
        sm_g.along_c()
        wq_g.along_c()
        wo_g.along_y()
        sm_g.end()

        def spread_row(k, block, total):
            pieces = sm[...].reshape(devices, 8, 128)[:, k, :].astype(BF)
            left = lax.broadcasted_iota(jnp.int32, (128, total), 0)
            right = lax.broadcasted_iota(jnp.int32, (128, total), 1)
            select = (lax.rem(right, block) == left).astype(BF)
            wide = nn(pieces, select)
            owner = lax.broadcasted_iota(jnp.int32, (devices, total), 0)
            place = lax.broadcasted_iota(jnp.int32, (devices, total), 1)
            inside = (place >= owner * block) & (place < (owner + 1) * block)
            return jnp.sum(jnp.where(inside, wide, 0.0), axis=0, keepdims=True)

        rows_s[0:1, :width] = spread_row(0, part, width)
        rows_s[1:2, :width] = spread_row(1, part, width)
        rows_s[2:3, :] = spread_row(2, bias_part, QKV_WIDTH)

        for copy in xr_c:
            copy.wait_recv()
        for k, (dc, dx) in enumerate(slots):
            v = xr[dc, dx].astype(F32)
            r = lax.rsqrt(jnp.mean(v * v, axis=-1, keepdims=True) + EPSILON)
            n1[k * rows : (k + 1) * rows] = (v * r * rows_s[0:1, :width]).astype(BF)
        n1_out = move(n1.at[0:query_rows], n1_o)
        wq_g.end()
        outs = [n1_out, move(w1, wqkv_o), move(rows_s, vec_o), move(cos_s, cos_o), move(sin_s, sin_o)]
        kv_at = lax.div(x * heads, QUERY_HEADS // KEY_VALUE_HEADS) * HEAD_WIDTH
        k_off = QUERY_HEADS * HEAD_WIDTH + kv_at
        v_off = k_off + KEY_VALUE_HEADS * HEAD_WIDTH
        wgt.middle()
        wu.begin()

        def turn(v, first, amount):
            return v * cos_s[first : first + amount] + pltpu.roll(
                v, HEAD_WIDTH // 2, 1
            ) * sin_s[first : first + amount]

        def bias_at(start, amount):
            return rows_s[2:3, pl.ds(pl.multiple_of(start, 128), amount)]

        @pl.loop(0, heads)
        def _(h):
            cols = pl.ds(pl.multiple_of(h * HEAD_WIDTH, HEAD_WIDTH), HEAD_WIDTH)
            v = nn(n1[0:query_rows], w1[:, cols])
            v = v + bias_at(x * q_cols + h * HEAD_WIDTH, HEAD_WIDTH)
            qs[:, cols] = turn(v, 0, query_rows).astype(BF)

        for j in range(kv_heads):
            at_k = q_cols + j * HEAD_WIDTH
            v = nn(n1[...], w1[:, at_k : at_k + HEAD_WIDTH]) + bias_at(k_off, kv_cols)[
                :, j * HEAD_WIDTH : (j + 1) * HEAD_WIDTH
            ]
            kv[:, j * HEAD_WIDTH : (j + 1) * HEAD_WIDTH] = turn(v, 0, pack_rows).astype(BF)
        v = nn(n1[...], w1[:, q_cols + kv_cols :]) + bias_at(v_off, kv_cols)
        kv[:, kv_cols:] = v.astype(BF)
        outs += [move(qs, q_o), move(kv, kv_o)]
        wo_g.along_c()
        wgt.last()
        wu.middle()
        wdn.begin()
        go_rows = Rows(go_o)
        go_rows.begin(cot_ref)

        @pl.loop(0, heads)
        def _(h):
            cols = pl.ds(pl.multiple_of(h * HEAD_WIDTH, HEAD_WIDTH), HEAD_WIDTH)
            g = lax.div(h, share)
            k_h = kv[:, pl.ds(pl.multiple_of(g * HEAD_WIDTH, HEAD_WIDTH), HEAD_WIDTH)]
            v_h = kv[:, pl.ds(pl.multiple_of(kv_cols + g * HEAD_WIDTH, HEAD_WIDTH), HEAD_WIDTH)]
            s = nt(qs[:, cols], k_h) * scale + mask_s[...]
            e = jnp.exp(s - jnp.max(s, axis=-1, keepdims=True))
            p = (e / jnp.sum(e, axis=-1, keepdims=True)).astype(BF)
            ps[h] = p
            ob[:, cols] = nn(p, v_h).astype(BF)

        outs += [move(ps, p_o), move(ob, att_o)]
        wo_g.end()
        outs.append(move(wo, wout_o))
        wu.last()
        wdn.middle()
        block = 256
        for d in list(range(1, X)) + [0]:
            @pl.loop(0, width // block)
            def _(j, d=d):
                cols = pl.ds(pl.multiple_of(j * block, block), block)
                v = nt(ob[d * rows : (d + 1) * rows], wo[cols])
                if d:
                    part_send[d - 1, :, cols] = v.astype(BF)
                else:
                    hs[:, cols] = v

            if d:
                part_recv_copy = put(part_send.at[d - 1], part_recv.at[d - 1], x=d)
                parts = [part_recv_copy] if d == 1 else parts + [part_recv_copy]
        h = hs[...] + own_row(xr)
        for d in range(1, X):
            parts[d - 1].wait_recv()
            h = h + part_recv[d - 1].astype(F32)
        hs[...] = h
        r = lax.rsqrt(jnp.mean(h * h, axis=-1, keepdims=True) + EPSILON)
        n2s[...] = (h * r * rows_s[1:2, :width]).astype(BF)
        nr_rows = Rows(nr_o)
        nr_rows.begin(n2s)
        outs.append(move(hs, h_o))
        wdn.last()
        nr_rows.to_core()
        go_rows.to_core()
        wgt.end()
        wu.end()
        wdn.end()
        nr_rows.end()
        go_rows.end()
        for copy in outs:
            copy.wait()
        for copy in sent:
            copy.wait_send()
        assert count[0] <= n_sems, count

    def own_row(xr):
        return xr[0, 0].astype(F32)

    any_spec = pl.BlockSpec(memory_space=pl.ANY)
    whole = (ZH, ZL, Y, depth, units)
    group = (C, ZH, X, rows, width)
    sds = jax.ShapeDtypeStruct
    return pl.pallas_call(
        kernel,
        out_shape=[
            sds((width, qkv_n), BF), sds((width, q_cols), BF), sds((query_rows, width), BF),
            sds((query_rows, q_cols), BF), sds((pack_rows, 2 * kv_cols), BF),
            sds((heads, query_rows, pack_rows), BF), sds((query_rows, q_cols), BF),
            sds((rows, width), F32), sds(group, BF), sds(group, BF),
            sds(whole, BF), sds(whole, BF), sds(whole, BF),
            sds((8, QKV_WIDTH), F32),
            sds((pack_rows, HEAD_WIDTH), F32), sds((pack_rows, HEAD_WIDTH), F32),
        ],
        in_specs=[any_spec, any_spec, pl.BlockSpec(memory_space=pltpu.SMEM)] + [any_spec] * 6,
        out_specs=[any_spec] * 16,
        scratch_shapes=[
            pltpu.VMEM((C, X, rows, width), BF),
            pltpu.VMEM((width, qkv_n), BF),
            pltpu.VMEM((width, q_cols), BF),
            pltpu.VMEM((devices * 8, 128), F32),
            pltpu.VMEM((pack_rows, width), BF),
            pltpu.VMEM((query_rows, q_cols), BF),
            pltpu.VMEM((pack_rows, 2 * kv_cols), BF),
            pltpu.VMEM((query_rows, q_cols), BF),
            pltpu.VMEM((max(X - 1, 1), rows, width), BF),
            pltpu.VMEM((max(X - 1, 1), rows, width), BF),
            pltpu.VMEM((rows, width), BF),
            pltpu.VMEM((rows, width), F32),
            pltpu.VMEM((pack_rows, HEAD_WIDTH), F32),
            pltpu.VMEM((pack_rows, HEAD_WIDTH), F32),
            pltpu.VMEM((query_rows, pack_rows), F32),
            pltpu.VMEM((8, QKV_WIDTH), F32),
            pltpu.VMEM((heads, query_rows, pack_rows), BF),
            pltpu.VMEM((2,) + w_gate.shape, BF),
            pltpu.VMEM(w_down.shape, BF),
            pltpu.VMEM((3, ZH, depth, units), BF),
            pltpu.SemaphoreType.DMA((n_sems,)),
            pltpu.SemaphoreType.DMA((n_sems,)),
            pltpu.SemaphoreType.DMA((32,)),
        ],
        compiler_params=pltpu.CompilerParams(
            collective_id=0, has_side_effects=True, vmem_limit_bytes=60 << 20
        ),
        name="front",
    )(own_in, cotangent, lengths, qkv_pieces, out_pieces, small, w_gate, w_up, w_down)


def back(
    grad_d, grad_g, grad_u, normed_terms, out_terms, middle, cotangent, own_in,
    wqkv, wout, normed, queries, kv_rows, probs, attended, vectors, cosine, sine,
):
    size = lax.axis_size
    ZH, ZL, Y, X, C = (size(a) for a in AXES)
    rows, width = own_in.shape
    qkv_n, q_cols = wqkv.shape[1], wout.shape[1]
    heads = q_cols // HEAD_WIDTH
    kv_cols = (qkv_n - q_cols) // 2
    kv_heads = kv_cols // HEAD_WIDTH
    share = heads // kv_heads
    query_rows, pack_rows = X * rows, C * X * rows
    depth, units = grad_g.shape[-2:]
    near = [(dh, dx) for dh in range(ZH) for dx in range(X)]
    far = [(dh, dl) for dh in range(ZH) for dl in range(ZL)]
    devices = ZH * ZL * Y * X * C
    part = width // devices
    zs = ZH * ZL
    scale = HEAD_WIDTH ** (-0.5)
    n_sems = 200

    def kernel(
        gd_ref, gg_ref, gu_ref, nt_ref, ot_ref, mid_ref, cot_ref, in_ref,
        w1_ref, wo_ref, n1_ref, q_ref, kv_ref, p_ref, att_ref, vec_ref, cos_ref, sin_ref,
        lo_o, gi_o, dqkv_o, dout_o, vec_out, od_o, og_o, ou_o,
        own_g, from_y, from_l, from_h, out_gu, out_d,
        half_n, half_o, from_c, from_n, send_n, hs, cots, ins, w1, wo, n1s, n1t, qs, kv, ps,
        atts, vec, cos_s, sin_s, da, dat, dos, dpre, dkv, dkv_low, dkv_in, dh_s,
        d_qkv, c_qkv, y_qkv, z_qkv, t_qkv, b_qkv, x_qkv,
        d_out, c_out, y_out, z_out, t_out, b_out, x_out,
        n_send, n_recv, lo_s, gi_s, vs, v_in, v_send,
        send_sem, recv_sem, local_sem,
    ):
        zh, zl, y, x, c = (lax.axis_index(a) for a in AXES)
        sizes = dict(zip(AXES, (ZH, ZL, Y, X, C)))
        here = dict(zip(AXES, (zh, zl, y, x, c)))

        def at(a, d):
            d = d % sizes[a]
            return lax.rem(here[a] + d, sizes[a]) if d else here[a]

        def device(**off):
            return tuple(at(a, off.get(a, 0)) for a in AXES)

        peers = set()
        for d in range(1, C):
            peers.add((0, 0, 0, 0, d))
        for dh, dx in near[1:]:
            peers.add((dh, 0, 0, dx, 0))
        for dh, dl in far[1:]:
            peers.add((dh, dl, 0, 0, 0))
        for d in range(1, Y):
            peers.add((0, 0, d, 0, 0))
        peers = sorted(peers)
        barrier = pltpu.get_barrier_semaphore()
        for peer in peers:
            pl.semaphore_signal(
                barrier, inc=1, device_id=device(**dict(zip(AXES, peer))), device_id_type=MESH_ID
            )
        pl.semaphore_wait(barrier, len(peers))

        count = [0, 0]
        sent = []

        def put(src, dst, **off):
            k = count[0]
            count[0] += 1
            copy = pltpu.make_async_remote_copy(
                src_ref=src, dst_ref=dst, send_sem=send_sem.at[k], recv_sem=recv_sem.at[k],
                device_id=device(**off), device_id_type=MESH_ID,
            )
            copy.start()
            sent.append(copy)
            return copy

        def move(src, dst):
            k = count[1]
            count[1] += 1
            copy = pltpu.make_async_copy(src, dst, local_sem.at[k])
            copy.start()
            return copy

        def by_rows(total, step, body):
            @pl.loop(0, total // step)
            def _(i):
                body(pl.ds(pl.multiple_of(i * step, step), step))

        class Units:
            def __init__(self, m, src):
                self.m, self.src = m, src
                self.by_y, self.own, self.by_l, self.by_h = {}, {}, {}, {}

            def begin(self, blocks):
                for dh, dl in blocks:
                    k = dh * ZL + dl
                    a, b = at("zh", dh), at("zl", dl)
                    self.by_y[dh, dl] = [
                        put(self.src.at[a, b, at("y", d)], from_y.at[self.m, k, d - 1], y=d)
                        for d in range(1, Y)
                    ]
                    self.own[dh, dl] = move(self.src.at[a, b, y], own_g.at[self.m, k])

            def add_y(self, blocks):
                m = self.m
                for dh, dl in blocks:
                    k = dh * ZL + dl
                    self.own[dh, dl].wait()
                    for copy in self.by_y[dh, dl]:
                        copy.wait_recv()

                    def body(r, k=k):
                        v = own_g[m, k, r].astype(F32)
                        for d in range(1, Y):
                            v = v + from_y[m, k, d - 1, r].astype(F32)
                        own_g[m, k, r] = v.astype(BF)

                    by_rows(depth, 64, body)
                    if dl:
                        self.by_l[dh, dl] = put(
                            own_g.at[m, k], from_l.at[m, dh, dl - 1], zl=dl
                        )

            def add_l(self):
                m = self.m
                for dh in reversed(range(ZH)):
                    for d in range(1, ZL):
                        self.by_l[dh, d].wait_recv()
                    if dh:
                        def body(r, dh=dh):
                            v = own_g[m, dh * ZL, r].astype(F32)
                            for d in range(1, ZL):
                                v = v + from_l[m, dh, d - 1, r].astype(F32)
                            own_g[m, dh * ZL, r] = v.astype(BF)

                        by_rows(depth, 64, body)
                        self.by_h[dh] = put(own_g.at[m, dh * ZL], from_h.at[m, dh - 1], zh=dh)

            def half(self, h, r, cols=slice(None)):
                m = self.m
                v = own_g[m, 0, r, cols].astype(F32)
                for d in range(1, ZL):
                    v = v + from_l[m, 0, d - 1, r, cols].astype(F32)
                for d in range(1, ZH):
                    other = from_h[m, d - 1, r, cols].astype(F32)
                    v = jnp.where(lax.rem(zh + ZH - d, ZH) == h, other, v)
                return v

            def wait_h(self):
                for copy in self.by_h.values():
                    copy.wait_recv()

        class Scatter:
            def __init__(self, dd, in_c, in_y, in_z, tt, tb, in_x, out):
                self.r = (dd, in_c, in_y, in_z, tt, tb, in_x)
                self.out = out

            def fill(self, left, right):
                dd = self.r[0]
                span = X * C * part

                @pl.loop(0, zs)
                def _(z):
                    for b in range(Y):
                        start = pl.multiple_of((z * Y + b) * span, span)
                        v = nn(left[pl.ds(start, span)], right[...]).astype(BF)
                        for dx in range(X):
                            for dc in range(C):
                                first = (dx * C + dc) * part
                                dd[dc, b, z, dx * part : (dx + 1) * part] = v[
                                    first : first + part
                                ]

            def to_c(self):
                dd, in_c = self.r[:2]
                self.by_c = {
                    (f, d): put(dd.at[at("c", d), at("y", f)], in_c.at[f, d - 1], c=d)
                    for f in list(range(1, Y)) + [0]
                    for d in range(1, C)
                }

            def to_y(self):
                dd, in_c, in_y = self.r[:3]
                self.by_y = []
                for f in list(range(1, Y)) + [0]:
                    for d in range(1, C):
                        self.by_c[f, d].wait_recv()
                    b = at("y", f)

                    @pl.loop(0, zs)
                    def _(z):
                        v = dd[c, b, z].astype(F32)
                        for d in range(1, C):
                            v = v + in_c[f, d - 1, z].astype(F32)
                        dd[c, b, z] = v.astype(BF)

                    if f:
                        self.by_y.append(put(dd.at[c, b], in_y.at[f - 1], y=f))

            def to_z(self):
                dd, in_c, in_y, in_z = self.r[:4]
                for copy in self.by_y:
                    copy.wait_recv()

                @pl.loop(0, zs)
                def _(z):
                    v = dd[c, y, z].astype(F32)
                    for f in range(1, Y):
                        v = v + in_y[f - 1, z].astype(F32)
                    dd[c, y, z] = v.astype(BF)

                self.by_z = [
                    put(
                        dd.at[c, y, at("zh", dh) * ZL + at("zl", dl)], in_z.at[k - 1],
                        zh=dh, zl=dl,
                    )
                    for k, (dh, dl) in enumerate(far)
                    if k
                ]

            def to_x(self):
                dd, in_c, in_y, in_z, tt, tb, in_x = self.r
                for copy in self.by_z:
                    copy.wait_recv()
                v = dd[c, y, zh * ZL + zl].astype(F32)
                for k in range(1, zs):
                    v = v + in_z[k - 1].astype(F32)
                for dx in range(X):
                    tt[dx] = v[dx * part : (dx + 1) * part]
                    tb[dx] = v[dx * part : (dx + 1) * part].astype(BF)
                self.by_x = [put(tb.at[at("x", d)], in_x.at[d - 1], x=d) for d in range(1, X)]

            def end(self):
                tt, in_x = self.r[4], self.r[6]
                for d in range(1, X):
                    self.by_x[d - 1].wait_recv()
                for d in range(1, X):
                    tt[at("x", -d)] = in_x[d - 1].astype(F32)
                return move(tt, self.out)

        class Rows:
            def __init__(self, m, src, mine):
                self.m, self.mine = m, mine
                order = list(range(1, len(near))) + [0]
                self.by_c = {
                    (k, d): put(src.at[d, k], from_c.at[m, k, d - 1], c=d)
                    for k in order
                    for d in range(1, C)
                }
                self.own = move(src.at[0], mine)

            def summed(self, k, r):
                v = self.mine[k, r].astype(F32)
                for d in range(1, C):
                    v = v + from_c[self.m, k, d - 1, r].astype(F32)
                return v

            def spread(self):
                self.own.wait()
                self.by_n = []
                for k, (dh, dx) in enumerate(near):
                    for d in range(1, C):
                        if k:
                            self.by_c[k, d].wait_recv()
                    if k:
                        def body(r, k=k):
                            send_n[self.m, k - 1, r] = self.summed(k, r).astype(BF)

                        by_rows(rows, 32, body)
                        self.by_n.append(
                            put(send_n.at[self.m, k - 1], from_n.at[self.m, k - 1], zh=dh, x=dx)
                        )
                for d in range(1, C):
                    self.by_c[0, d].wait_recv()

            def arrive(self):
                for copy in self.by_n:
                    copy.wait_recv()

            def total(self, r):
                v = self.summed(0, r)
                for k in range(1, len(near)):
                    v = v + from_n[self.m, k - 1, r].astype(F32)
                return v

        terms = Rows(0, nt_ref, half_n)
        loads = {}
        for name, src, dst in (
            ("mid", mid_ref, hs), ("cot", cot_ref, cots), ("vec", vec_ref, vec),
            ("n1", n1_ref, n1s), ("wo", wo_ref, wo), ("kv", kv_ref, kv), ("p", p_ref, ps),
            ("att", att_ref, atts), ("q", q_ref, qs), ("cos", cos_ref, cos_s),
            ("sin", sin_ref, sin_s), ("w1", w1_ref, w1), ("in", in_ref, ins),
        ):
            loads[name] = move(src, dst)
        order = far[::-1]
        ud, ug, uu = Units(0, gd_ref), Units(1, gg_ref), Units(2, gu_ref)
        ud.begin(order)
        ug.begin(order)
        outs_terms = Rows(1, ot_ref, half_o)

        eye = (
            lax.broadcasted_iota(jnp.int32, (128, 128), 0)
            == lax.broadcasted_iota(jnp.int32, (128, 128), 1)
        ).astype(BF)

        def flip(src, dst, total):
            for j in range(total // 128):
                cols = slice(j * 128, (j + 1) * 128)
                dst[cols] = nt(eye, src[:, cols]).astype(BF)

        loads["n1"].wait()
        flip(n1s, n1t, width)
        terms.spread()
        for name in ("mid", "cot", "vec"):
            loads[name].wait()
        gain_one, gain_two = vec[0:1, :width], vec[1:2, :width]
        terms.arrive()
        vs[...] = jnp.zeros_like(vs)

        @pl.loop(0, rows // 32)
        def _(i):
            r = pl.ds(pl.multiple_of(i * 32, 32), 32)
            grad, h = terms.total(r), hs[r]
            inv = lax.rsqrt(jnp.mean(h * h, axis=-1, keepdims=True) + EPSILON)
            scaled = gain_two * grad
            v = (
                cots[r].astype(F32)
                + inv * scaled
                - h * (inv * inv * inv) * jnp.mean(scaled * h, axis=-1, keepdims=True)
            )
            dh_s[r] = v
            da[0, r] = v.astype(BF)
            vs[1:2, :width] = vs[1:2, :width] + jnp.sum(grad * h * inv, axis=0, keepdims=True)

        da_x = [put(da.at[0], da.at[-d % X], x=d) for d in range(1, X)]
        outs_terms.spread()
        loads["wo"].wait()
        loads["att"].wait()
        for copy in da_x:
            copy.wait_recv()

        @pl.loop(0, heads // 2)
        def _(j):
            cols = pl.ds(pl.multiple_of(j * 256, 256), 256)
            for k in range(X):
                dos[k * rows : (k + 1) * rows, cols] = nn(da[k], wo[:, cols]).astype(BF)

        for k in range(X):
            for j in range(width // 128):
                cols = slice(j * 128, (j + 1) * 128)
                dat[cols, k * rows : (k + 1) * rows] = nt(eye, da[k, :, cols]).astype(BF)
        s_out = Scatter(d_out, c_out, y_out, z_out, t_out, b_out, x_out, dout_o)
        s_out.fill(dat, atts)
        s_out.to_c()
        for name in ("kv", "p", "q", "cos", "sin", "w1", "in"):
            loads[name].wait()
        dkv[...] = jnp.zeros_like(dkv)

        @pl.loop(0, heads)
        def _(h):
            cols = pl.ds(pl.multiple_of(h * HEAD_WIDTH, HEAD_WIDTH), HEAD_WIDTH)
            g = lax.div(h, share)
            k_at = pl.ds(pl.multiple_of(g * HEAD_WIDTH, HEAD_WIDTH), HEAD_WIDTH)
            v_at = pl.ds(pl.multiple_of(kv_cols + g * HEAD_WIDTH, HEAD_WIDTH), HEAD_WIDTH)
            p_low, do_h = ps[h], dos[:, cols]
            p = p_low.astype(F32)
            dp = nt(do_h, kv[:, v_at])
            delta = jnp.sum(p * dp, axis=-1, keepdims=True)
            ds = (p * (dp - delta)).astype(BF)
            dq = nn(ds, kv[:, k_at]) * scale
            dq = dq * cos_s[:query_rows] - pltpu.roll(dq, HEAD_WIDTH // 2, 1) * sin_s[:query_rows]
            dpre[:, cols] = dq.astype(BF)
            dkv[:, k_at] += tn(ds, qs[:, cols]) * scale
            dkv[:, v_at] += tn(p_low, do_h)

        kv_c = []
        for d in range(1, C):
            dkv_low[d - 1] = dkv[d * query_rows : (d + 1) * query_rows].astype(BF)
            kv_c.append(put(dkv_low.at[d - 1], dkv_in.at[d - 1], c=d))
        ud.add_y(order)
        s_out.to_y()
        uu.begin(order[: len(order) // 2])
        for copy in kv_c:
            copy.wait_recv()
        total = dkv[:query_rows]
        for d in range(1, C):
            total = total + dkv_in[d - 1].astype(F32)
        for j in range(kv_heads):
            cols = slice(j * HEAD_WIDTH, (j + 1) * HEAD_WIDTH)
            v = total[:, cols]
            v = v * cos_s[:query_rows] - pltpu.roll(v, HEAD_WIDTH // 2, 1) * sin_s[:query_rows]
            dpre[:, q_cols + j * HEAD_WIDTH : q_cols + (j + 1) * HEAD_WIDTH] = v.astype(BF)
        dpre[:, q_cols + kv_cols :] = total[:, kv_cols:].astype(BF)
        s_qkv = Scatter(d_qkv, c_qkv, y_qkv, z_qkv, t_qkv, b_qkv, x_qkv, dqkv_o)
        s_qkv.fill(n1t, dpre)
        s_qkv.to_c()

        for k in list(range(1, X)) + [0]:
            @pl.loop(0, width // 256)
            def _(j, k=k):
                cols = pl.ds(pl.multiple_of(j * 256, 256), 256)
                v = nt(dpre[k * rows : (k + 1) * rows], w1[cols])
                if k:
                    n_send[k - 1, :, cols] = v.astype(BF)
                else:
                    gi_s[:, cols] = v

            if k:
                copy = put(n_send.at[k - 1], n_recv.at[k - 1], x=k)
                n_x = [copy] if k == 1 else n_x + [copy]
        kv_at = lax.div(x * heads, QUERY_HEADS // KEY_VALUE_HEADS) * HEAD_WIDTH
        k_off = QUERY_HEADS * HEAD_WIDTH + kv_at
        v_off = k_off + KEY_VALUE_HEADS * HEAD_WIDTH
        sums = jnp.sum(dpre[...].astype(F32), axis=0, keepdims=True)

        def place(start, first, amount):
            vs[2:3, pl.ds(pl.multiple_of(start, 128), amount)] = sums[:, first : first + amount]

        place(x * q_cols, 0, q_cols)
        place(k_off, q_cols, kv_cols)
        place(v_off, q_cols + kv_cols, kv_cols)
        s_qkv.to_y()
        uu.begin(order[len(order) // 2 :])
        for copy in n_x:
            copy.wait_recv()

        @pl.loop(0, rows // 32)
        def _(i):
            r = pl.ds(pl.multiple_of(i * 32, 32), 32)
            grad, h = gi_s[r], ins[r].astype(F32)
            for d in range(1, X):
                grad = grad + n_recv[d - 1, r].astype(F32)
            inv = lax.rsqrt(jnp.mean(h * h, axis=-1, keepdims=True) + EPSILON)
            scaled = gain_one * grad
            gi_s[r] = (
                dh_s[r]
                + inv * scaled
                - h * (inv * inv * inv) * jnp.mean(scaled * h, axis=-1, keepdims=True)
            )
            vs[0:1, :width] = vs[0:1, :width] + jnp.sum(grad * h * inv, axis=0, keepdims=True)

        done = [move(gi_s, gi_o)]

        outs_terms.arrive()

        def finish(r):
            lo_s[r] = (hs[r] + outs_terms.total(r)).astype(BF)

        by_rows(rows, 32, finish)
        done.append(move(lo_s, lo_o))
        places = iter(range(V_IN))
        stages = iter(range(4))

        def small_stage(offsets):
            k = next(stages)
            v_send[k] = vs[...]
            return [(p, put(v_send.at[k], v_in.at[p], **off)) for off, p in zip(offsets, places)]

        def small_finish(copies):
            for p, copy in copies:
                copy.wait_recv()
                vs[...] = vs[...] + v_in[p]

        state = small_stage([dict(c=d) for d in range(1, C)])
        ud.add_l()
        small_finish(state)
        state = small_stage([dict(x=d) for d in range(1, X)])
        ug.add_y(order)
        small_finish(state)
        state = small_stage([dict(y=d) for d in range(1, Y)])
        s_out.to_z()
        ug.add_l()
        ud.wait_h()
        for h in range(ZH):
            for j in range(-(-units // 128)):
                first = j * 128
                amount = min(128, units - first)
                v = ud.half(h, slice(None), slice(first, first + amount)).astype(BF)
                out_d[h * units + first : h * units + first + amount] = nt(
                    eye[:amount, :amount], v
                )
        done.append(move(out_d, od_o))
        s_qkv.to_z()
        s_out.to_x()
        small_finish(state)
        state = small_stage([dict(zh=dh, zl=dl) for dh, dl in far[1:]])

        def put_out(u, m, out):
            u.wait_h()
            for h in range(ZH):
                def body(r, h=h):
                    out_gu[m, r, h * units : (h + 1) * units] = u.half(h, r)

                by_rows(depth, 64, body)
            done.append(move(out_gu.at[m], out))

        put_out(ug, 0, og_o)
        uu.add_y(order[: len(order) // 2])
        done.append(s_out.end())
        s_qkv.to_x()
        small_finish(state)
        done.append(move(vs, vec_out))
        uu.add_y(order[len(order) // 2 :])
        done.append(s_qkv.end())
        uu.add_l()
        put_out(uu, 1, ou_o)
        for copy in done:
            copy.wait()
        for copy in sent:
            copy.wait_send()
        assert count[0] <= n_sems and count[1] <= 64, count

    V_IN = (C - 1) + (X - 1) + (Y - 1) + (zs - 1)
    any_spec = pl.BlockSpec(memory_space=pl.ANY)
    sds = jax.ShapeDtypeStruct
    vm = pltpu.VMEM

    def scatter_scratch(n):
        return [
            vm((C, Y, zs, X * part, n), BF), vm((Y, max(C - 1, 1), zs, X * part, n), BF),
            vm((max(Y - 1, 1), zs, X * part, n), BF), vm((max(zs - 1, 1), X * part, n), BF),
            vm((X, part, n), F32), vm((X, part, n), BF), vm((max(X - 1, 1), part, n), BF),
        ]

    nk = len(near)
    return pl.pallas_call(
        kernel,
        out_shape=[
            sds((rows, width), BF), sds((rows, width), F32), sds((X, part, qkv_n), F32),
            sds((X, part, q_cols), F32), sds((8, QKV_WIDTH), F32),
            sds((ZH * units, depth), F32), sds((depth, ZH * units), F32),
            sds((depth, ZH * units), F32),
        ],
        in_specs=[any_spec] * 18,
        out_specs=[any_spec] * 8,
        scratch_shapes=[
            vm((3, zs, depth, units), BF), vm((3, zs, max(Y - 1, 1), depth, units), BF),
            vm((3, ZH, max(ZL - 1, 1), depth, units), BF), vm((3, max(ZH - 1, 1), depth, units), BF),
            vm((2, depth, ZH * units), F32), vm((ZH * units, depth), F32),
            vm((nk, rows, width), BF), vm((nk, rows, width), BF),
            vm((2, nk, max(C - 1, 1), rows, width), BF), vm((2, max(nk - 1, 1), rows, width), BF),
            vm((2, max(nk - 1, 1), rows, width), BF),
            vm((rows, width), F32), vm((rows, width), BF), vm((rows, width), BF),
            vm((width, qkv_n), BF), vm((width, q_cols), BF), vm((query_rows, width), BF),
            vm((width, query_rows), BF), vm((query_rows, q_cols), BF),
            vm((pack_rows, 2 * kv_cols), BF), vm((heads, query_rows, pack_rows), BF),
            vm((query_rows, q_cols), BF), vm((8, QKV_WIDTH), F32),
            vm((pack_rows, HEAD_WIDTH), F32), vm((pack_rows, HEAD_WIDTH), F32),
            vm((X, rows, width), BF), vm((width, query_rows), BF), vm((query_rows, q_cols), BF),
            vm((query_rows, qkv_n), BF), vm((pack_rows, 2 * kv_cols), F32),
            vm((max(C - 1, 1), query_rows, 2 * kv_cols), BF),
            vm((max(C - 1, 1), query_rows, 2 * kv_cols), BF),
            vm((rows, width), F32),
        ]
        + scatter_scratch(qkv_n)
        + scatter_scratch(q_cols)
        + [
            vm((max(X - 1, 1), rows, width), BF), vm((max(X - 1, 1), rows, width), BF),
            vm((rows, width), BF), vm((rows, width), F32), vm((8, QKV_WIDTH), F32),
            vm((max(V_IN, 1), 8, QKV_WIDTH), F32), vm((4, 8, QKV_WIDTH), F32),
            pltpu.SemaphoreType.DMA((n_sems,)), pltpu.SemaphoreType.DMA((n_sems,)),
            pltpu.SemaphoreType.DMA((64,)),
        ],
        compiler_params=pltpu.CompilerParams(
            collective_id=1, has_side_effects=True, vmem_limit_bytes=63 << 20
        ),
        name="back",
    )(
        grad_d, grad_g, grad_u, normed_terms, out_terms, middle, cotangent, own_in,
        wqkv, wout, normed, queries, kv_rows, probs, attended, vectors, cosine, sine,
    )


def ff(normed, cotangent, w_gate, w_up, w_down):
    gate = nn(normed, w_gate)
    up_part = nn(normed, w_up)
    sig = jax.nn.sigmoid(gate)
    act = gate * sig
    hidden = (act * up_part).astype(BF)
    grad_wdown = tn(cotangent, hidden).astype(BF)
    grad_hidden = nn(cotangent, w_down)
    grad_gate = (grad_hidden * up_part * sig * (1.0 + gate * (1.0 - sig))).astype(BF)
    grad_up = (grad_hidden * act).astype(BF)
    grad_wgate = tn(normed, grad_gate).astype(BF)
    grad_wup = tn(normed, grad_up).astype(BF)
    normed_term = (nt(grad_gate, w_gate) + nt(grad_up, w_up)).astype(BF)
    out_term = nt(hidden, w_down).astype(BF)
    return hidden, grad_gate, grad_up, grad_wdown, grad_wgate, grad_wup, out_term, normed_term


def small_rows(gain_one, gain_two, bias):
    wide = [jnp.pad(v.astype(F32), (0, 128 - v.shape[0])) for v in (gain_one, gain_two, bias)]
    return jnp.pad(jnp.stack(wide), ((0, 5), (0, 0)))


def shards(
    layer_in, lengths, w_qkv, b_qkv, w_out, norm1_gain, norm2_gain, w_gate, w_up, w_down, grad_out
):
    size = lax.axis_size
    ZH, ZL, Y, X, C = (size(a) for a in ("zh", "zl", "y", "x", "c"))
    zh, zl, y, x, c = (lax.axis_index(a) for a in ("zh", "zl", "y", "x", "c"))
    everyone = ("zh", "zl", "y", "x", "c")
    devices = ZH * ZL * Y * X * C
    rows, width = layer_in.shape[1:]
    part = w_qkv.shape[0]
    group = QUERY_HEADS // KEY_VALUE_HEADS
    heads = QUERY_HEADS // X
    kv_heads = max(1, heads // group)
    share = heads // kv_heads
    q_cols, kv_cols = heads * HEAD_WIDTH, kv_heads * HEAD_WIDTH
    scale = HEAD_WIDTH ** (-0.5)

    own_in = layer_in[0]
    cotangent = grad_out[0]
    own_rows = own_in.astype(F32)
    query_rows, pack_rows = X * rows, C * X * rows
    bias_part = b_qkv.shape[0]
    def row_index(cores):
        spans = [
            (((x + dx) % X) * C + (c + dc) % C) * rows + jnp.arange(rows, dtype=jnp.int32)
            for dc in range(cores)
            for dx in range(X)
        ]
        return jnp.concatenate(spans)

    doc_lengths = lengths[0]
    key_index = row_index(C)
    key_doc, key_pos = doc_layout(key_index, doc_lengths)
    query_index, query_doc = key_index[:query_rows], key_doc[:query_rows]
    key_cos, key_sin = angles(key_pos)
    query_cos, query_sin = key_cos[:query_rows], key_sin[:query_rows]

    def gather_columns(pieces):
        held = ordered(
            [pick(pieces, x)] + [fetch(pick(pieces, (x - d) % X), "x", d) for d in range(1, X)],
            "x",
        )
        whole = jnp.zeros((ZH, ZL, Y) + held.shape, held.dtype)
        for dh in range(ZH):
            for dl in range(ZL):
                along = held if dh == dl == 0 else fetch(held, ("zh", "zl"), (dh, dl))
                for dy in range(Y):
                    piece = along if dy == 0 else fetch(along, "y", dy)
                    whole = lax.dynamic_update_slice(
                        whole,
                        piece[None, None, None],
                        ((zh + dh) % ZH, (zl + dl) % ZL, (y + dy) % Y, 0, 0, 0),
                    )
        whole = whole.reshape((ZH * ZL * Y * X,) + whole.shape[4:])
        both = ordered([whole] + [fetch(whole, "c", d) for d in range(1, C)], "c")
        return jnp.moveaxis(both, 0, 1).reshape(width, whole.shape[-1])

    def scatter_columns(grad):
        n = grad.shape[-1]
        grad = grad.astype(BF).reshape(ZH * ZL * Y * X, C, part, n)
        held = pick(grad, c, 1).astype(F32)
        for d in range(1, C):
            held = held + send(pick(grad, (c + d) % C, 1), "c", d)
        held = held.astype(BF).reshape(ZH, ZL, Y, X * part, n)
        kept = pick(held, y, 2).astype(F32)
        for d in range(1, Y):
            kept = kept + send(pick(held, (y + d) % Y, 2), "y", d)
        low = kept.astype(BF)
        total = 0.0
        for dh in range(ZH):
            for dl in range(ZL):
                if dh == dl == 0:
                    total = total + pick(pick(kept, zh), zl)
                else:
                    piece = pick(pick(low, (zh + dh) % ZH), (zl + dl) % ZL)
                    total = total + send(piece, ("zh", "zl"), (dh, dl)).astype(F32)
        total = total.reshape(X, part, n)
        lower = total.astype(BF)
        return ordered(
            [pick(total, x)]
            + [fetch(pick(lower, (x - d) % X), "x", d).astype(F32) for d in range(1, X)],
            "x",
        )

    def qkv_columns(array):
        blocks = []
        for at in range(X):
            kv = (at * heads) // group * HEAD_WIDTH
            key_at = QUERY_HEADS * HEAD_WIDTH + kv
            value_at = key_at + KEY_VALUE_HEADS * HEAD_WIDTH
            blocks.append(
                jnp.concatenate(
                    [
                        array[..., at * q_cols : (at + 1) * q_cols],
                        array[..., key_at : key_at + kv_cols],
                        array[..., value_at : value_at + kv_cols],
                    ],
                    axis=-1,
                )
            )
        return jnp.stack(blocks)

    def qkv_whole(blocks):
        queries = [blocks[at, ..., :q_cols] for at in range(X)]
        keys, values = [0.0] * KEY_VALUE_HEADS, [0.0] * KEY_VALUE_HEADS
        for at in range(X):
            for j in range(kv_heads):
                head = (at * heads) // group + j
                start = q_cols + j * HEAD_WIDTH
                keys[head] = keys[head] + blocks[at, ..., start : start + HEAD_WIDTH]
                start = start + kv_cols
                values[head] = values[head] + blocks[at, ..., start : start + HEAD_WIDTH]
        return jnp.concatenate(queries + keys + values, axis=-1)

    depth, units = w_gate.shape[0], w_gate.shape[1] // ZH

    def gather_units(weight):
        halves = weight.reshape(depth, ZH, units).transpose(1, 0, 2)
        whole = jnp.zeros((ZH, ZL, Y, depth, units), weight.dtype)
        for dh in range(ZH):
            first = pick(halves, zh) if dh == 0 else fetch(pick(halves, (zh - dh) % ZH), "zh", dh)
            for dl in range(ZL):
                second = first if dl == 0 else fetch(first, "zl", dl)
                for dy in range(Y):
                    third = second if dy == 0 else fetch(second, "y", dy)
                    whole = lax.dynamic_update_slice(
                        whole,
                        third[None, None, None],
                        ((zh + dh) % ZH, (zl + dl) % ZL, (y + dy) % Y, 0, 0),
                    )
        return whole.reshape(width, units)

    def scatter_units(grad):
        grad = grad.astype(BF).reshape(ZH, ZL, Y, depth, units)
        done = [None] * ZH
        for dh in reversed(range(ZH)):
            mine = pick(grad, (zh + dh) % ZH)
            kept = pick(mine, y, 1).astype(F32)
            for d in range(1, Y):
                kept = kept + send(pick(mine, (y + d) % Y, 1), "y", d).astype(F32)
            low = kept.astype(BF)
            total = pick(kept, zl)
            for d in range(1, ZL):
                total = total + send(pick(low, (zl + d) % ZL), "zl", d).astype(F32)
            done[dh] = total
        halves = [done[0]] + [
            send(done[dh].astype(BF), "zh", dh).astype(F32) for dh in range(1, ZH)
        ]
        halves = [halves[0]] + halves[:0:-1]
        return jnp.moveaxis(ordered(halves, "zh"), 0, 1).reshape(depth, ZH * units)

    near = [(dh, dx) for dh in range(ZH) for dx in range(X)]

    def gather_rows(own):
        held = jnp.concatenate([own if k == (0, 0) else fetch(own, ("zh", "x"), k) for k in near])
        return jnp.concatenate([held] + [fetch(held, "c", d) for d in range(1, C)])

    def scatter_rows(term):
        term = term.reshape(C, len(near), rows, width)
        held = term[0].astype(F32)
        for d in range(1, C):
            held = held + send(term[d].astype(BF), "c", d).astype(F32)
        total = held[0]
        for at, k in enumerate(near):
            if k != (0, 0):
                total = total + send(held[at].astype(BF), ("zh", "x"), k).astype(F32)
        return total

    def scatter_x(term):
        term = term.reshape(X, rows, width)
        total = term[0]
        for d in range(1, X):
            total = total + send(term[d].astype(BF), "x", d).astype(F32)
        return total

    if part % 16 == 0 and depth % 64 == 0 and heads % 2 == 0 and X > 1:
        (
            wqkv_mine, wout_mine, query_normed, queries, kv_low, probs_low, attended_low,
            middle, group_normed, group_cotangent, wgate_mine, wup_mine, wdown_mine, vectors,
            cosine, sine,
        ) = front(
            own_in,
            cotangent,
            lengths,
            qkv_columns(w_qkv),
            jnp.stack([w_out.T[:, at * q_cols : (at + 1) * q_cols] for at in range(X)]),
            small_rows(norm1_gain, norm2_gain, b_qkv),
            w_gate,
            w_up,
            w_down,
        )
        hidden, grad_gate, grad_up, grad_wdown, grad_wgate, grad_wup, out_term, normed_term = ff(
            group_normed.reshape(-1, width),
            group_cotangent.reshape(-1, width),
            *(w.reshape(width, units) for w in (wgate_mine, wup_mine, wdown_mine)),
        )
        whole = (ZH, ZL, Y, depth, units)
        terms = (C, ZH * X, rows, width)
        layer_out, grad_input, sum_wqkv, sum_wout, small, sum_wdown, sum_wgate, sum_wup = back(
            grad_wdown.reshape(whole),
            grad_wgate.reshape(whole),
            grad_wup.reshape(whole),
            normed_term.reshape(terms),
            out_term.reshape(terms),
            middle,
            cotangent,
            own_in,
            wqkv_mine,
            wout_mine,
            query_normed,
            queries,
            kv_low,
            probs_low,
            attended_low,
            vectors,
            cosine,
            sine,
        )
        place = (((zh * ZL + zl) * Y + y) * X + x) * C + c
        return (
            layer_out[None],
            grad_input[None],
            qkv_whole(sum_wqkv),
            lax.dynamic_slice_in_dim(small[2], place * bias_part, bias_part),
            jnp.moveaxis(sum_wout, 0, 1).reshape(part, -1).T,
            lax.dynamic_slice_in_dim(small[0, :width], place * part, part),
            lax.dynamic_slice_in_dim(small[1, :width], place * part, part),
            sum_wgate,
            sum_wup,
            sum_wdown,
        )

    small = jnp.concatenate([norm1_gain, norm2_gain, b_qkv])
    small = jnp.pad(small, (0, -small.shape[0] % 256))[None]
    small = lax.all_to_all(
        jnp.broadcast_to(small[None], (devices,) + small.shape), everyone, 0, 0, tiled=True
    )[:, 0].astype(F32)
    gain_one = small[:, :part].reshape(1, width)
    gain_two = small[:, part : 2 * part].reshape(1, width)
    bias = small[:, 2 * part : 2 * part + bias_part].reshape(-1)

    query_in = jnp.concatenate([own_in] + [fetch(own_in, "x", d) for d in range(1, X)])
    pack_in = jnp.concatenate([query_in] + [fetch(query_in, "c", d) for d in range(1, C)])

    wqkv_mine = gather_columns(qkv_columns(w_qkv))
    wout_t = w_out.T
    wout_mine = gather_columns(
        jnp.stack([wout_t[:, at * q_cols : (at + 1) * q_cols] for at in range(X)])
    )
    bias_mine = pick(qkv_columns(bias), x)

    wgate_mine, wup_mine = gather_units(w_gate), gather_units(w_up)
    wdown_mine = gather_units(w_down.T)

    group_cotangent = gather_rows(cotangent)

    pack_in = pack_in.astype(F32)
    normed_one = (pack_in * rms_parts(pack_in) * gain_one).astype(BF)
    query_normed = normed_one[:query_rows]
    pre_query = nn(query_normed, wqkv_mine[:, :q_cols]) + bias_mine[:q_cols]
    pre_kv = nn(normed_one, wqkv_mine[:, q_cols:]) + bias_mine[q_cols:]
    queries = rotate(
        pre_query.reshape(query_rows, heads, HEAD_WIDTH), query_cos, query_sin
    ).astype(BF)
    queries = queries.reshape(query_rows, kv_heads, share, HEAD_WIDTH)
    keys = rotate(
        pre_kv[:, :kv_cols].reshape(pack_rows, kv_heads, HEAD_WIDTH), key_cos, key_sin
    ).astype(BF)
    values = pre_kv[:, kv_cols:].reshape(pack_rows, kv_heads, HEAD_WIDTH).astype(BF)
    scores = jnp.einsum("tkgd,skd->kgts", queries, keys, preferred_element_type=F32) * scale
    allowed = (query_doc[:, None] == key_doc[None, :]) & (
        key_index[None, :] <= query_index[:, None]
    )
    masked = jnp.where(allowed, scores, NEGATIVE_BIG)
    top = jnp.max(masked, axis=-1, keepdims=True)
    weights = jnp.where(allowed, jnp.exp(masked - top), 0.0)
    probs = weights / jnp.sum(weights, axis=-1, keepdims=True)
    probs_low = probs.astype(BF)
    attended = jnp.einsum("kgts,skd->tkgd", probs_low, values, preferred_element_type=F32)
    attended_low = attended.reshape(query_rows, q_cols).astype(BF)
    middle = own_rows + scatter_x(nt(attended_low, wout_mine))
    normed_two = (middle * rms_parts(middle) * gain_two).astype(BF)

    group_normed = gather_rows(normed_two)

    hidden, grad_gate, grad_up, grad_wdown, grad_wgate, grad_wup, out_term, normed_term = ff(
        group_normed, group_cotangent, wgate_mine, wup_mine, wdown_mine
    )
    grad_normed_two = scatter_rows(normed_term)
    layer_out = (middle + scatter_rows(out_term)).astype(BF)
    sum_wdown = scatter_units(grad_wdown).T
    sum_wgate = scatter_units(grad_wgate)
    sum_wup = scatter_units(grad_wup)

    back_two, grad_gain_two = rms_back(middle, gain_two, grad_normed_two)
    grad_middle = cotangent.astype(F32) + back_two
    grad_att = grad_middle.astype(BF)
    query_grad_att = jnp.concatenate([grad_att] + [fetch(grad_att, "x", d) for d in range(1, X)])
    sum_wout = scatter_columns(tn(query_grad_att, attended_low))
    head_grads = nn(query_grad_att, wout_mine).astype(BF)
    head_grads = head_grads.reshape(query_rows, kv_heads, share, HEAD_WIDTH)
    grad_probs = jnp.einsum("tkgd,skd->kgts", head_grads, values, preferred_element_type=F32)
    probs = probs_low.astype(F32)
    delta = jnp.sum(probs * grad_probs, axis=-1, keepdims=True)
    grad_scores = (probs * (grad_probs - delta)).astype(BF)
    grad_query = (
        jnp.einsum("kgts,skd->tkgd", grad_scores, keys, preferred_element_type=F32) * scale
    )
    grad_key = jnp.einsum("kgts,tkgd->skd", grad_scores, queries, preferred_element_type=F32)
    grad_key = rotate(grad_key * scale, key_cos, -key_sin)
    grad_value = jnp.einsum("kgts,tkgd->skd", probs_low, head_grads, preferred_element_type=F32)
    grad_kv = jnp.concatenate(
        [grad_key.reshape(pack_rows, kv_cols), grad_value.reshape(pack_rows, kv_cols)], axis=1
    ).reshape(C, query_rows, 2 * kv_cols)
    kv_total = grad_kv[0]
    for d in range(1, C):
        kv_total = kv_total + send(grad_kv[d].astype(BF), "c", d).astype(F32)
    grad_query = rotate(
        grad_query.reshape(query_rows, heads, HEAD_WIDTH), query_cos, -query_sin
    ).reshape(query_rows, q_cols)
    grad_pre = jnp.concatenate([grad_query, kv_total], axis=1).astype(BF)
    sum_wqkv = qkv_whole(scatter_columns(tn(query_normed, grad_pre)))
    grad_bias = jnp.sum(grad_pre.astype(F32), axis=0)
    grad_normed_one = scatter_x(nt(grad_pre, wqkv_mine))
    back_one, grad_gain_one = rms_back(own_rows, gain_one, grad_normed_one)
    grad_input = grad_middle + back_one

    bias_blocks = jnp.where(
        jnp.arange(X, dtype=jnp.int32)[:, None] == x, grad_bias[None, :], 0.0
    )
    bias_whole = qkv_whole(bias_blocks)
    piece = jnp.concatenate(
        [
            grad_gain_one.reshape(devices, part),
            grad_gain_two.reshape(devices, part),
            bias_whole.reshape(devices, bias_part),
        ],
        axis=1,
    )
    piece = jnp.pad(piece, ((0, 0), (0, -piece.shape[1] % 256)))
    piece = jnp.sum(lax.all_to_all(piece[:, None], everyone, 0, 0, tiled=True)[:, 0], axis=0)
    return (
        layer_out[None],
        grad_input[None],
        sum_wqkv,
        piece[2 * part : 2 * part + bias_part],
        jnp.moveaxis(sum_wout, 0, 1).reshape(part, -1).T,
        piece[:part],
        piece[part : 2 * part],
        sum_wgate,
        sum_wup,
        sum_wdown,
    )


def solution(mesh):
    wide, narrow = mesh.shape["wide"], mesh.shape["narrow"]
    cores = 2 if narrow % 2 == 0 else 1
    along_x = narrow // cores
    along_y = along_x if wide % along_x == 0 else 1
    along_z = wide // along_y
    far = 2 if along_z % 2 == 0 else 1
    split = Mesh(
        mesh.devices.reshape(far, along_z // far, along_y, along_x, cores),
        ("zh", "zl", "y", "x", "c"),
    )
    w, n = ("zh", "zl", "y"), ("x", "c")
    placed = (
        P(w, n, None),
        P(w, None),
        P(w + n, None),
        P(w + n),
        P(None, w + n),
        P(w + n),
        P(w + n),
        P(w, n),
        P(w, n),
        P(n, w),
        P(w, n, None),
    )
    return jax.shard_map(
        shards,
        mesh=split,
        in_specs=placed,
        out_specs=(
            P(w, n, None),
            P(w, n, None),
            P(w + n, None),
            P(w + n),
            P(None, w + n),
            P(w + n),
            P(w + n),
            P(w, n),
            P(w, n),
            P(n, w),
        ),
        check_vma=False,
    )
```

```python
import math

import jax
import jax.numpy as jnp
from jax import lax
from jax.experimental import pallas as pl
from jax.experimental.pallas import tpu as pltpu
from jax.sharding import Mesh
from jax.sharding import PartitionSpec as P

QUERY_HEADS = 12
KEY_VALUE_HEADS = 2
HEAD_WIDTH = 128

EPSILON = 1e-06
ROPE_BASE = 10000.0
NEGATIVE_BIG = -1e30
HIGHEST = lax.Precision.HIGHEST


BF = jnp.bfloat16
F32 = jnp.float32
AXES = ("zh", "zl", "y", "x", "c")
MESH_ID = pl.DeviceIdType.MESH
QKV_WIDTH = (QUERY_HEADS + 2 * KEY_VALUE_HEADS) * HEAD_WIDTH


def fetch(value, axes, offsets):
    axes = (axes,) if isinstance(axes, str) else tuple(axes)
    offsets = (offsets,) if isinstance(offsets, int) else tuple(offsets)
    sizes = [lax.axis_size(a) for a in axes]
    total = math.prod(sizes)
    pairs = []
    for flat in range(total):
        rest, place = flat, []
        for size in reversed(sizes):
            place.append(rest % size)
            rest //= size
        place = place[::-1]
        source = 0
        for spot, off, size in zip(place, offsets, sizes):
            source = source * size + (spot + off) % size
        pairs.append((source, flat))
    return lax.ppermute(value, axes if len(axes) > 1 else axes[0], pairs)


def send(value, axes, offsets):
    offsets = (offsets,) if isinstance(offsets, int) else tuple(offsets)
    return fetch(value, axes, tuple(-o for o in offsets))


def pick(stack, place, axis=0):
    return lax.dynamic_index_in_dim(stack, place, axis, keepdims=False)


def nn(left, right):
    return lax.dot_general(left, right, (((1,), (0,)), ((), ())), preferred_element_type=F32)


def nt(left, right):
    return lax.dot_general(left, right, (((1,), (1,)), ((), ())), preferred_element_type=F32)


def tn(left, right):
    return lax.dot_general(left, right, (((0,), (0,)), ((), ())), preferred_element_type=F32)


def rms_parts(rows):
    return lax.rsqrt(jnp.mean(rows * rows, axis=-1, keepdims=True) + EPSILON)


def rms_back(rows, gain, grad):
    r = rms_parts(rows)
    scaled = gain * grad
    return (
        r * scaled - rows * (r * r * r) * jnp.mean(scaled * rows, axis=-1, keepdims=True),
        jnp.sum(grad * rows * r, axis=0),
    )


def doc_layout(index, doc_lengths):
    ends = jnp.cumsum(doc_lengths)
    starts = ends - doc_lengths
    document_index = jnp.sum((index[:, None] >= ends[None, :]).astype(jnp.int32), axis=1)
    onehot = (
        document_index[:, None] == jnp.arange(doc_lengths.shape[0], dtype=jnp.int32)[None, :]
    ).astype(jnp.int32)
    token_position = index - jnp.sum(onehot * starts[None, :], axis=1)
    return document_index, token_position.astype(F32)


def angles(position):
    half = HEAD_WIDTH // 2
    freq = jnp.exp(jnp.arange(half, dtype=F32) * (-2.0 * math.log(ROPE_BASE) / HEAD_WIDTH))
    angle = position[:, None] * freq[None, :]
    return jnp.cos(angle)[:, None, :], jnp.sin(angle)[:, None, :]


def rotate(rows, cosine, sine):
    half = HEAD_WIDTH // 2
    first, second = rows[..., :half], rows[..., half:]
    return jnp.concatenate(
        [first * cosine - second * sine, second * cosine + first * sine], axis=-1
    )


def ordered(pieces, axis):
    count, here = len(pieces), lax.axis_index(axis)
    if count == 1:
        return pieces[0][None]
    if count == 2:
        return jnp.where(here == 0, jnp.stack(pieces), jnp.stack(pieces[::-1]))
    whole = jnp.zeros((count,) + pieces[0].shape, pieces[0].dtype)
    for distance, piece in enumerate(pieces):
        whole = lax.dynamic_update_index_in_dim(whole, piece, (here + distance) % count, 0)
    return whole


def front(own_in, cotangent, lengths, w_qkv, w_out, small, w_gate, w_up, w_down, qkv_columns):
    size = lax.axis_size
    ZH, ZL, Y, X, C = (size(a) for a in AXES)
    rows, width = own_in.shape
    part = w_qkv.shape[0]
    q_cols = w_out.shape[1] // X
    qkv_n = qkv_columns(w_qkv).shape[-1]
    heads = q_cols // HEAD_WIDTH
    kv_cols = (qkv_n - q_cols) // 2
    kv_heads = kv_cols // HEAD_WIDTH
    share = heads // kv_heads
    query_rows, pack_rows = X * rows, C * X * rows
    depth = w_gate.shape[0]
    units = w_gate.shape[1] // ZH
    near = [(dh, dx) for dh in range(ZH) for dx in range(X)]
    far = [(dh, dl) for dh in range(ZH) for dl in range(ZL)]
    devices = ZH * ZL * Y * X * C
    bias_part = QKV_WIDTH // devices
    scale = HEAD_WIDTH ** (-0.5)
    docs = lengths.shape[-1]
    n_sems = 400

    def kernel(
        own_ref, cot_ref, len_ref, qkv_ref, out_ref, small_ref, g_ref, u_ref, d_ref,
        wqkv_o, wout_o, n1_o, n2t_o, q_o, kv_o, p_o, att_o, h_o, nr_o, go_o, wg_o, wu_o, wd_o, vec_o, cos_o, sin_o,
        xr, w1, wo, sm, n1, qs, kv, ob, part_send, part_recv, n2s, hs,
        cos_s, sin_s, mask_s, rows_s, ps, raw, half, wq_raw, wq_cut, n1t, n2t, nr_v, go_v,
        send_sem, recv_sem, local_sem,
    ):
        zh, zl, y, x, c = (lax.axis_index(a) for a in AXES)
        sizes = dict(zip(AXES, (ZH, ZL, Y, X, C)))
        here = dict(zip(AXES, (zh, zl, y, x, c)))

        def device(**off):
            return tuple(
                lax.rem(here[a] + off[a], sizes[a]) if off.get(a, 0) % sizes[a] else here[a]
                for a in AXES
            )

        def at(a, d):
            d = d % sizes[a]
            return lax.rem(here[a] + d, sizes[a]) if d else here[a]

        peers = set()
        for d in range(1, C):
            peers.add((0, 0, 0, 0, d))
        for dh, dx in near[1:]:
            peers.add((dh, 0, 0, dx, 0))
        for dh, dl in far[1:]:
            peers.add((dh, dl, 0, 0, 0))
        for d in range(1, Y):
            peers.add((0, 0, d, 0, 0))
        peers = sorted(peers)
        barrier = pltpu.get_barrier_semaphore()
        for peer in peers:
            pl.semaphore_signal(
                barrier, inc=1, device_id=device(**dict(zip(AXES, peer))), device_id_type=MESH_ID
            )
        pl.semaphore_wait(barrier, len(peers))

        count = [0, 0]
        sent, local = [], []

        def put(src, dst, **off):
            k = count[0]
            count[0] += 1
            copy = pltpu.make_async_remote_copy(
                src_ref=src, dst_ref=dst, send_sem=send_sem.at[k], recv_sem=recv_sem.at[k],
                device_id=device(**off), device_id_type=MESH_ID,
            )
            copy.start()
            sent.append(copy)
            return copy

        def move(src, dst):
            k = count[1]
            count[1] += 1
            copy = pltpu.make_async_copy(src, dst, local_sem.at[k])
            copy.start()
            return copy

        class Gather:
            def __init__(self, buf, block, pieces):
                self.buf, self.block, self.pieces = buf, block, pieces

            def slot(self, dh, dl, dy, dx, dc):
                place = at("zh", dh)
                for a, d in (("zl", dl), ("y", dy), ("x", dx), ("c", dc)):
                    place = place * sizes[a] + at(a, d)
                start = pl.multiple_of(place * self.block, self.block)
                return self.buf.at[pl.ds(start, self.block)]

            def begin(self):
                self.own = move(self.pieces(x), self.slot(0, 0, 0, 0, 0))
                self.by_x = {
                    d: put(self.pieces(at("x", d)), self.slot(0, 0, 0, 0, 0), x=d)
                    for d in range(1, X)
                }

            def along_z(self):
                self.own.wait()
                for d in self.by_x:
                    self.by_x[d].wait_recv()
                self.by_z, self.by_y, self.by_c = {}, {}, {}
                for dh, dl in far[:0:-1]:
                    for dx in range(X):
                        s = self.slot(0, 0, 0, dx, 0)
                        self.by_z[dh, dl, dx] = put(s, s, zh=dh, zl=dl)
                for dx in range(X):
                    self.spread(0, 0, dx)

            def spread(self, dh, dl, dx):
                s = self.slot(-dh, -dl, 0, dx, 0)
                for d in range(1, Y):
                    self.by_y[dh, dl, d, dx] = put(s, s, y=d)
                self.to_core(dh, dl, 0, dx)

            def to_core(self, dh, dl, dy, dx):
                s = self.slot(-dh, -dl, -dy, dx, 0)
                for d in range(1, C):
                    self.by_c[dh, dl, dy, d, dx] = put(s, s, c=d)

            def along_y(self):
                for dh, dl in far[1:]:
                    for dx in range(X):
                        self.by_z[dh, dl, dx].wait_recv()
                        self.spread(dh, dl, dx)

            def along_c(self):
                for dh, dl in far:
                    for d in range(1, Y):
                        for dx in range(X):
                            self.by_y[dh, dl, d, dx].wait_recv()
                            self.to_core(dh, dl, d, dx)

            def end(self):
                for copy in self.by_c.values():
                    copy.wait_recv()

        class Units:
            def __init__(self, at_m, buf):
                self.m, self.buf = at_m, buf

            def slot(self, dh, dl, dy):
                return self.buf.at[at("zh", dh), at("zl", dl), at("y", dy)]

            def begin(self):
                mine = half.at[self.m, zh]
                s = self.slot(0, 0, 0)
                self.own = move(mine, s)
                self.by_h = {
                    d: put(half.at[self.m, at("zh", d)], s, zh=d) for d in range(1, ZH)
                }
                self.by_l = {}
                for d in range(1, ZL):
                    self.by_l[0, d] = put(mine, s, zl=d)

            def own_y(self):
                self.by_y = {
                    (0, 0, d): put(half.at[self.m, zh], self.slot(0, 0, 0), y=d)
                    for d in range(1, Y)
                }

            def middle(self):
                for dh in self.by_h:
                    self.by_h[dh].wait_recv()
                    s = self.slot(-dh, 0, 0)
                    for d in range(1, ZL):
                        self.by_l[dh, d] = put(s, s, zl=d)
                    for d in range(1, Y):
                        self.by_y[dh, 0, d] = put(s, s, y=d)

            def last(self, spread=True):
                for dh, dl in list(self.by_l):
                    self.by_l[dh, dl].wait_recv()
                    s = self.slot(-dh, -dl, 0)
                    for d in range(1, Y) if spread else ():
                        self.by_y[dh, dl, d] = put(s, s, y=d)

            def end(self):
                self.own.wait()
                for copy in self.by_y.values():
                    copy.wait_recv()

        class Rows:
            def __init__(self, buf):
                self.buf = buf

            def begin(self, src):
                self.own = move(src, self.buf.at[0, 0, 0])
                self.by_h = {d: put(src, self.buf.at[0, -d % ZH, 0], zh=d) for d in range(1, ZH)}
                self.by_x = {(0, d): put(src, self.buf.at[0, 0, -d % X], x=d) for d in range(1, X)}
                self.by_c = [put(src, self.buf.at[-d % C, 0, 0], c=d) for d in range(1, C)]

            def spread(self, a, b):
                for d in range(1, C):
                    self.by_c.append(put(self.buf.at[0, a, b], self.buf.at[-d % C, a, b], c=d))

            def along_x(self):
                for dh in self.by_h:
                    self.by_h[dh].wait_recv()
                    a = -dh % ZH
                    for d in range(1, X):
                        self.by_x[dh, d] = put(self.buf.at[0, a, 0], self.buf.at[0, a, -d % X], x=d)
                    self.spread(a, 0)

            def to_core(self):
                for dh, d in self.by_x:
                    self.by_x[dh, d].wait_recv()
                    self.spread(-dh % ZH, -d % X)

            def end(self):
                self.own.wait()
                for copy in self.by_c:
                    copy.wait_recv()

        raws = [move(qkv_ref, wq_raw), move(g_ref, raw.at[0]), move(u_ref, raw.at[1])]
        raws.append(move(d_ref, raw.at[2]))

        def out_piece(to):
            return out_ref.at[:, pl.ds(pl.multiple_of(to * q_cols, 128), q_cols)]

        wq_g = Gather(w1, part, lambda to: wq_cut.at[to])
        wo_g = Gather(wo, part, out_piece)
        sm_g = Gather(sm, 8, lambda to: small_ref)
        raws[0].wait()
        cut = qkv_columns(wq_raw)
        for k in range(X):
            wq_cut[k] = cut[k]
        wq_g.begin()
        sm_g.begin()
        xr_own = move(own_ref, xr.at[0, 0])
        xr_x = {d: put(own_ref, xr.at[0, -d % X], x=d) for d in range(1, X)}
        wo_g.begin()
        wu, wgt, wdn = Units(1, wu_o), Units(0, wg_o), Units(2, wd_o)
        for m, unit in ((0, wgt), (1, wu), (2, wdn)):
            raws[m + 1].wait()
            for h in range(ZH):
                half[m, h] = raw[m, :, h * units : (h + 1) * units]
            if m < 2:
                unit.own_y()
        sm_g.along_z()
        wq_g.along_z()

        lens = [len_ref[0, j] for j in range(docs)]
        ends = []
        for j in range(docs):
            ends.append(lens[j] if j == 0 else ends[-1] + lens[j])

        def slot_base(dc, dx):
            return (at("x", dx) * C + at("c", dc)) * rows

        def doc_of(index):
            doc = jnp.zeros(index.shape, jnp.int32)
            first = jnp.zeros(index.shape, jnp.int32)
            for j in range(docs):
                past = (index >= ends[j]).astype(jnp.int32)
                doc = doc + past
                first = first + past * lens[j]
            return doc, index - first

        lane = lax.broadcasted_iota(jnp.int32, (rows, HEAD_WIDTH), 1)
        folded = jnp.where(lane >= HEAD_WIDTH // 2, lane - HEAD_WIDTH // 2, lane)
        freq = jnp.exp(folded.astype(F32) * (-2.0 * math.log(ROPE_BASE) / HEAD_WIDTH))
        sign = jnp.where(lane >= HEAD_WIDTH // 2, 1.0, -1.0)
        slots = [(dc, dx) for dc in range(C) for dx in range(X)]
        for k, (dc, dx) in enumerate(slots):
            index = slot_base(dc, dx) + lax.broadcasted_iota(jnp.int32, (rows, HEAD_WIDTH), 0)
            angle = doc_of(index)[1].astype(F32) * freq
            cos_s[k * rows : (k + 1) * rows] = jnp.cos(angle)
            sin_s[k * rows : (k + 1) * rows] = jnp.sin(angle) * sign
        for a in range(X):
            q_index = slot_base(0, a) + lax.broadcasted_iota(jnp.int32, (rows, rows), 0)
            q_doc = doc_of(q_index)[0]
            for k, (dc, dx) in enumerate(slots):
                k_index = slot_base(dc, dx) + lax.broadcasted_iota(jnp.int32, (rows, rows), 1)
                k_doc = doc_of(k_index)[0]
                allowed = (q_doc == k_doc) & (k_index <= q_index)
                mask_s[a * rows : (a + 1) * rows, k * rows : (k + 1) * rows] = jnp.where(
                    allowed, 0.0, NEGATIVE_BIG
                )

        xr_own.wait()
        for d in xr_x:
            xr_x[d].wait_recv()
        xr_c = [
            put(xr.at[0, k], xr.at[-d % C, k], c=d) for d in range(1, C) for k in range(X)
        ]
        wo_g.along_z()
        sm_g.along_y()
        wq_g.along_y()
        wgt.begin()
        go_rows = Rows(go_v)
        go_rows.begin(cot_ref)
        sm_g.along_c()
        wq_g.along_c()
        sm_g.end()

        def spread_row(k, block, total):
            pieces = sm[...].reshape(devices, 8, 128)[:, k, :].astype(BF)
            left = lax.broadcasted_iota(jnp.int32, (128, total), 0)
            right = lax.broadcasted_iota(jnp.int32, (128, total), 1)
            select = (lax.rem(right, block) == left).astype(BF)
            wide = nn(pieces, select)
            owner = lax.broadcasted_iota(jnp.int32, (devices, total), 0)
            place = lax.broadcasted_iota(jnp.int32, (devices, total), 1)
            inside = (place >= owner * block) & (place < (owner + 1) * block)
            return jnp.sum(jnp.where(inside, wide, 0.0), axis=0, keepdims=True)

        rows_s[0:1, :width] = spread_row(0, part, width)
        rows_s[1:2, :width] = spread_row(1, part, width)
        rows_s[2:3, :] = spread_row(2, bias_part, QKV_WIDTH)

        for copy in xr_c:
            copy.wait_recv()
        for k, (dc, dx) in enumerate(slots):
            v = xr[dc, dx].astype(F32)
            r = lax.rsqrt(jnp.mean(v * v, axis=-1, keepdims=True) + EPSILON)
            n1[k * rows : (k + 1) * rows] = (v * r * rows_s[0:1, :width]).astype(BF)
        eye = (
            lax.broadcasted_iota(jnp.int32, (128, 128), 0)
            == lax.broadcasted_iota(jnp.int32, (128, 128), 1)
        ).astype(BF)

        def flip(read, dst, amount):
            @pl.loop(0, width // 128)
            def _(j):
                cols = pl.ds(pl.multiple_of(j * 128, 128), 128)
                dst[cols] = nt(eye, read(cols)).astype(BF)

        wq_g.end()
        outs = [move(w1, wqkv_o), move(rows_s, vec_o), move(cos_s, cos_o), move(sin_s, sin_o)]
        kv_at = lax.div(x * heads, QUERY_HEADS // KEY_VALUE_HEADS) * HEAD_WIDTH
        k_off = QUERY_HEADS * HEAD_WIDTH + kv_at
        v_off = k_off + KEY_VALUE_HEADS * HEAD_WIDTH
        wo_g.along_y()
        wu.begin()

        def turn(v, first, amount):
            return v * cos_s[first : first + amount] + pltpu.roll(
                v, HEAD_WIDTH // 2, 1
            ) * sin_s[first : first + amount]

        def bias_at(start, amount):
            return rows_s[2:3, pl.ds(pl.multiple_of(start, 128), amount)]

        @pl.loop(0, heads)
        def _(h):
            cols = pl.ds(pl.multiple_of(h * HEAD_WIDTH, HEAD_WIDTH), HEAD_WIDTH)
            v = nn(n1[0:query_rows], w1[:, cols])
            v = v + bias_at(x * q_cols + h * HEAD_WIDTH, HEAD_WIDTH)
            qs[:, cols] = turn(v, 0, query_rows).astype(BF)

        for j in range(kv_heads):
            at_k = q_cols + j * HEAD_WIDTH
            v = nn(n1[...], w1[:, at_k : at_k + HEAD_WIDTH]) + bias_at(k_off, kv_cols)[
                :, j * HEAD_WIDTH : (j + 1) * HEAD_WIDTH
            ]
            kv[:, j * HEAD_WIDTH : (j + 1) * HEAD_WIDTH] = turn(v, 0, pack_rows).astype(BF)
        v = nn(n1[...], w1[:, q_cols + kv_cols :]) + bias_at(v_off, kv_cols)
        kv[:, kv_cols:] = v.astype(BF)
        outs += [move(qs, q_o), move(kv, kv_o)]
        wo_g.along_c()

        @pl.loop(0, heads)
        def _(h):
            cols = pl.ds(pl.multiple_of(h * HEAD_WIDTH, HEAD_WIDTH), HEAD_WIDTH)
            g = lax.div(h, share)
            k_h = kv[:, pl.ds(pl.multiple_of(g * HEAD_WIDTH, HEAD_WIDTH), HEAD_WIDTH)]
            v_h = kv[:, pl.ds(pl.multiple_of(kv_cols + g * HEAD_WIDTH, HEAD_WIDTH), HEAD_WIDTH)]
            s = nt(qs[:, cols], k_h) * scale + mask_s[...]
            e = jnp.exp(s - jnp.max(s, axis=-1, keepdims=True))
            p = (e / jnp.sum(e, axis=-1, keepdims=True)).astype(BF)
            ps[h] = p
            ob[:, cols] = nn(p, v_h).astype(BF)

        outs += [move(ps, p_o), move(ob, att_o)]
        wo_g.end()
        outs.append(move(wo, wout_o))
        block = 256
        for d in list(range(1, X)) + [0]:
            @pl.loop(0, width // block)
            def _(j, d=d):
                cols = pl.ds(pl.multiple_of(j * block, block), block)
                v = nt(ob[d * rows : (d + 1) * rows], wo[cols])
                if d:
                    part_send[d - 1, :, cols] = v.astype(BF)
                else:
                    hs[:, cols] = v

            if d:
                part_recv_copy = put(part_send.at[d - 1], part_recv.at[d - 1], x=d)
                parts = [part_recv_copy] if d == 1 else parts + [part_recv_copy]
        wgt.middle()
        wdn.begin()
        wdn.own_y()
        h = hs[...] + own_row(xr)
        for d in range(1, X):
            parts[d - 1].wait_recv()
            h = h + part_recv[d - 1].astype(F32)
        hs[...] = h
        r = lax.rsqrt(jnp.mean(h * h, axis=-1, keepdims=True) + EPSILON)
        n2s[...] = (h * r * rows_s[1:2, :width]).astype(BF)
        nr_rows = Rows(nr_v)
        nr_rows.begin(n2s)
        outs.append(move(hs, h_o))
        flip(lambda cols: n1[0:query_rows, cols], n1t, query_rows)
        outs.append(move(n1t, n1_o))
        wgt.last()
        go_rows.along_x()
        wu.middle()
        nr_rows.along_x()
        wu.last()
        go_rows.to_core()
        wdn.middle()
        nr_rows.to_core()
        nr_rows.end()
        outs.append(move(nr_v, nr_o))
        group_rows = C * ZH * X * rows
        flip(lambda cols: nr_v[:, :, :, :, cols].reshape(group_rows, 128), n2t, group_rows)
        outs.append(move(n2t, n2t_o))
        wdn.last(False)
        go_rows.end()
        outs.append(move(go_v, go_o))
        wgt.end()
        wu.end()
        wdn.end()
        for copy in outs:
            copy.wait()
        for copy in sent:
            copy.wait_send()
        assert count[0] <= n_sems, count

    def own_row(xr):
        return xr[0, 0].astype(F32)

    any_spec = pl.BlockSpec(memory_space=pl.ANY)
    whole = (ZH, ZL, Y, depth, units)
    group = (C, ZH, X, rows, width)
    sds = jax.ShapeDtypeStruct
    return pl.pallas_call(
        kernel,
        out_shape=[
            sds((width, qkv_n), BF), sds((width, q_cols), BF), sds((width, query_rows), BF),
            sds((width, C * ZH * X * rows), BF),
            sds((query_rows, q_cols), BF), sds((pack_rows, 2 * kv_cols), BF),
            sds((heads, query_rows, pack_rows), BF), sds((query_rows, q_cols), BF),
            sds((rows, width), F32), sds(group, BF), sds(group, BF),
            sds(whole, BF), sds(whole, BF), sds(whole, BF),
            sds((8, QKV_WIDTH), F32),
            sds((pack_rows, HEAD_WIDTH), F32), sds((pack_rows, HEAD_WIDTH), F32),
        ],
        in_specs=[any_spec, any_spec, pl.BlockSpec(memory_space=pltpu.SMEM)] + [any_spec] * 6,
        out_specs=[any_spec] * 17,
        scratch_shapes=[
            pltpu.VMEM((C, X, rows, width), BF),
            pltpu.VMEM((width, qkv_n), BF),
            pltpu.VMEM((width, q_cols), BF),
            pltpu.VMEM((devices * 8, 128), F32),
            pltpu.VMEM((pack_rows, width), BF),
            pltpu.VMEM((query_rows, q_cols), BF),
            pltpu.VMEM((pack_rows, 2 * kv_cols), BF),
            pltpu.VMEM((query_rows, q_cols), BF),
            pltpu.VMEM((max(X - 1, 1), rows, width), BF),
            pltpu.VMEM((max(X - 1, 1), rows, width), BF),
            pltpu.VMEM((rows, width), BF),
            pltpu.VMEM((rows, width), F32),
            pltpu.VMEM((pack_rows, HEAD_WIDTH), F32),
            pltpu.VMEM((pack_rows, HEAD_WIDTH), F32),
            pltpu.VMEM((query_rows, pack_rows), F32),
            pltpu.VMEM((8, QKV_WIDTH), F32),
            pltpu.VMEM((heads, query_rows, pack_rows), BF),
            pltpu.VMEM((3,) + w_gate.shape, BF),
            pltpu.VMEM((3, ZH, depth, units), BF),
            pltpu.VMEM(w_qkv.shape, BF),
            pltpu.VMEM((X, part, qkv_n), BF),
            pltpu.VMEM((width, query_rows), BF),
            pltpu.VMEM((width, C * ZH * X * rows), BF),
            pltpu.VMEM(group, BF),
            pltpu.VMEM(group, BF),
            pltpu.SemaphoreType.DMA((n_sems,)),
            pltpu.SemaphoreType.DMA((n_sems,)),
            pltpu.SemaphoreType.DMA((32,)),
        ],
        compiler_params=pltpu.CompilerParams(
            collective_id=0, has_side_effects=True, vmem_limit_bytes=60 << 20
        ),
        name="front",
    )(own_in, cotangent, lengths, w_qkv, w_out, small, w_gate, w_up, w_down)


def back(
    grad_d, near_d, grad_g, grad_u, group_t, normed_terms, out_terms, middle, cotangent, own_in,
    wqkv, wout, normed, queries, kv_rows, probs, attended, vectors, cosine, sine,
):
    size = lax.axis_size
    ZH, ZL, Y, X, C = (size(a) for a in AXES)
    rows, width = own_in.shape
    qkv_n, q_cols = wqkv.shape[1], wout.shape[1]
    heads = q_cols // HEAD_WIDTH
    kv_cols = (qkv_n - q_cols) // 2
    kv_heads = kv_cols // HEAD_WIDTH
    share = heads // kv_heads
    query_rows, pack_rows = X * rows, C * X * rows
    depth, units = grad_d.shape[-2:]
    group_rows = group_t.shape[1]
    near = [(dh, dx) for dh in range(ZH) for dx in range(X)]
    far = [(dh, dl) for dh in range(ZH) for dl in range(ZL)]
    devices = ZH * ZL * Y * X * C
    part = width // devices
    zs = ZH * ZL
    scale = HEAD_WIDTH ** (-0.5)
    n_sems = 200

    blocks = {}
    for dx in range(X):
        for h in range(heads):
            blocks.setdefault(dx * heads + h, []).append((dx, h * HEAD_WIDTH))
        for j in range(kv_heads):
            head = dx * heads // (QUERY_HEADS // KEY_VALUE_HEADS) + j
            for at_kv, start in ((0, q_cols), (KEY_VALUE_HEADS, q_cols + kv_cols)):
                blocks.setdefault(QUERY_HEADS + at_kv + head, []).append(
                    (dx, start + j * HEAD_WIDTH)
                )
    qkv_layout = [(k * HEAD_WIDTH, b) for k, b in sorted(blocks.items())]
    out_layout = [(k * HEAD_WIDTH, b) for k, b in sorted(blocks.items()) if k < QUERY_HEADS]
    def kernel(
        gd_ref, dd_ref, gg_ref, gu_ref, gt_ref, nt_ref, ot_ref, mid_ref, cot_ref, in_ref,
        w1_ref, wo_ref, n1_ref, q_ref, kv_ref, p_ref, att_ref, vec_ref, cos_ref, sin_ref,
        lo_o, gi_o, dqkv_o, dout_o, vec_out, od_o, og_o, ou_o,
        own_g, from_y, from_l, from_h, out_w, turned, units_t,
        half_n, half_o, from_c, from_n, hs, cots, ins, w1, wo, n1t, qs, kv, ps,
        atts, vec, cos_s, sin_s, da, dat, dos, dpre, dkv, dkv_low, dkv_in, dh_s,
        d_qkv, c_qkv, y_qkv, z_qkv, t_qkv, b_qkv, x_qkv,
        d_out, c_out, y_out, z_out, t_out, b_out, x_out, w_qkv_s, w_out_s,
        n_send, n_recv, lo_s, gi_s, vs, v_in, v_send,
        send_sem, recv_sem, local_sem,
    ):
        zh, zl, y, x, c = (lax.axis_index(a) for a in AXES)
        sizes = dict(zip(AXES, (ZH, ZL, Y, X, C)))
        here = dict(zip(AXES, (zh, zl, y, x, c)))

        def at(a, d):
            d = d % sizes[a]
            return lax.rem(here[a] + d, sizes[a]) if d else here[a]

        def device(**off):
            return tuple(at(a, off.get(a, 0)) for a in AXES)

        peers = set()
        for d in range(1, C):
            peers.add((0, 0, 0, 0, d))
        for dh, dx in near[1:]:
            peers.add((dh, 0, 0, dx, 0))
        for dh, dl in far[1:]:
            peers.add((dh, dl, 0, 0, 0))
        for d in range(1, Y):
            peers.add((0, 0, d, 0, 0))
        peers = sorted(peers)
        barrier = pltpu.get_barrier_semaphore()
        for peer in peers:
            pl.semaphore_signal(
                barrier, inc=1, device_id=device(**dict(zip(AXES, peer))), device_id_type=MESH_ID
            )
        pl.semaphore_wait(barrier, len(peers))

        count = [0, 0]
        sent = []

        def put(src, dst, **off):
            k = count[0]
            count[0] += 1
            copy = pltpu.make_async_remote_copy(
                src_ref=src, dst_ref=dst, send_sem=send_sem.at[k], recv_sem=recv_sem.at[k],
                device_id=device(**off), device_id_type=MESH_ID,
            )
            copy.start()
            sent.append(copy)
            return copy

        def move(src, dst):
            k = count[1]
            count[1] += 1
            copy = pltpu.make_async_copy(src, dst, local_sem.at[k])
            copy.start()
            return copy

        def by_rows(total, step, body):
            @pl.loop(0, total // step)
            def _(i):
                body(pl.ds(pl.multiple_of(i * step, step), step))

        class Units:
            def __init__(self, m, src):
                self.m, self.src = m, src
                self.by_y, self.own, self.by_l, self.by_h = {}, {}, {}, {}

            def begin(self, blocks, arrived=()):
                for dh, dl in blocks:
                    k = dh * ZL + dl
                    a, b = at("zh", dh), at("zl", dl)
                    if (dh, dl) in arrived:
                        self.by_y[dh, dl] = [move(dd_ref.at[arrived.index((dh, dl))], from_y.at[self.m, k, 0])]
                    else:
                        self.by_y[dh, dl] = [
                            put(self.src.at[a, b, at("y", d)], from_y.at[self.m, k, d - 1], y=d)
                            for d in range(1, Y)
                        ]
                    self.own[dh, dl] = move(self.src.at[a, b, y], own_g.at[self.m, k])

            def add_y(self, blocks):
                m = self.m
                for dh, dl in blocks:
                    k = dh * ZL + dl
                    self.own[dh, dl].wait()
                    for copy in self.by_y[dh, dl]:
                        if any(copy is other for other in sent):
                            copy.wait_recv()
                        else:
                            copy.wait()

                    def body(r, k=k):
                        v = own_g[m, k, r].astype(F32)
                        for d in range(1, Y):
                            v = v + from_y[m, k, d - 1, r].astype(F32)
                        own_g[m, k, r] = v.astype(BF)

                    by_rows(depth, 64, body)
                    if dl:
                        self.by_l[dh, dl] = put(
                            own_g.at[m, k], from_l.at[m, dh, dl - 1], zl=dl
                        )

            def add_l(self, far):
                m = self.m
                for dh in range(ZH - 1, 0, -1) if far else (0,):
                    for d in range(1, ZL):
                        self.by_l[dh, d].wait_recv()
                    if dh:
                        def body(r, dh=dh):
                            v = own_g[m, dh * ZL, r].astype(F32)
                            for d in range(1, ZL):
                                v = v + from_l[m, dh, d - 1, r].astype(F32)
                            own_g[m, dh * ZL, r] = v.astype(BF)

                        by_rows(depth, 64, body)
                        self.by_h[dh] = put(own_g.at[m, dh * ZL], from_h.at[m, dh - 1], zh=dh)

            def half(self, h, r, cols=slice(None)):
                m = self.m
                v = own_g[m, 0, r, cols].astype(F32)
                for d in range(1, ZL):
                    v = v + from_l[m, 0, d - 1, r, cols].astype(F32)
                for d in range(1, ZH):
                    other = from_h[m, d - 1, r, cols].astype(F32)
                    v = jnp.where(lax.rem(zh + ZH - d, ZH) == h, other, v)
                return v

            def wait_h(self):
                for copy in self.by_h.values():
                    copy.wait_recv()

        def block(m, k, place_y):
            a = lax.rem(zh + k // ZL, ZH)
            b = lax.rem(zl + k % ZL, ZL)
            start = pl.multiple_of(((a * ZL + b) * Y + place_y) * depth, depth)
            return nt(turned[pl.ds(start, depth)], units_t[m])

        def compute_other():
            @pl.loop(0, 2 * zs)
            def _(i):
                m, k = lax.rem(i, 2), zs - 1 - lax.div(i, 2)
                a = lax.rem(zh + lax.div(k, ZL), ZH)
                b = lax.rem(zl + lax.rem(k, ZL), ZL)
                start = pl.multiple_of(((a * ZL + b) * Y + at("y", 1)) * depth, depth)
                own_g[m + 1, k] = nt(turned[pl.ds(start, depth)], units_t[m]).astype(BF)

        def send_pair(k):
            for u in (ug, uu):
                u.by_y[k] = put(own_g.at[u.m, k], from_y.at[u.m, k, 0], y=1)

        def add_pair(k):
            for u in (ug, uu):
                u.by_y[k].wait()
                sent[:] = [other for other in sent if other is not u.by_y[k]]

            @pl.loop(0, 2)
            def _(m):
                v = block(m, k, y) + from_y[m + 1, k, 0].astype(F32)
                own_g[m + 1, k] = v.astype(BF)

            if k % ZL:
                for u in (ug, uu):
                    u.by_l[k // ZL, k % ZL] = put(
                        own_g.at[u.m, k], from_l.at[u.m, k // ZL, k % ZL - 1], zl=k % ZL
                    )

        class Scatter:
            def __init__(self, dd, in_c, in_y, in_z, tt, tb, in_x, whole, out, layout):
                self.r = (dd, in_c, in_y, in_z, tt, tb, in_x)
                self.whole, self.out, self.layout = whole, out, layout

            def fill(self, left, right):
                dd = self.r[0]
                span = X * C * part

                @pl.loop(0, zs)
                def _(z):
                    for b in range(Y):
                        start = pl.multiple_of((z * Y + b) * span, span)
                        v = nn(left[pl.ds(start, span)], right[...]).astype(BF)
                        for dx in range(X):
                            for dc in range(C):
                                first = (dx * C + dc) * part
                                dd[dc, b, z, dx * part : (dx + 1) * part] = v[
                                    first : first + part
                                ]

            def to_c(self):
                dd, in_c = self.r[:2]
                self.by_c = {
                    (f, d): put(dd.at[at("c", d), at("y", f)], in_c.at[f, d - 1], c=d)
                    for f in list(range(1, Y)) + [0]
                    for d in range(1, C)
                }

            def to_y(self):
                dd, in_c, in_y = self.r[:3]
                self.by_y = []
                for f in list(range(1, Y)) + [0]:
                    for d in range(1, C):
                        self.by_c[f, d].wait_recv()
                    b = at("y", f)

                    @pl.loop(0, zs)
                    def _(z):
                        v = dd[c, b, z].astype(F32)
                        for d in range(1, C):
                            v = v + in_c[f, d - 1, z].astype(F32)
                        dd[c, b, z] = v.astype(BF)

                    if f:
                        self.by_y.append(put(dd.at[c, b], in_y.at[f - 1], y=f))

            def to_z(self):
                dd, in_c, in_y, in_z = self.r[:4]
                for copy in self.by_y:
                    copy.wait_recv()

                @pl.loop(0, zs)
                def _(z):
                    v = dd[c, y, z].astype(F32)
                    for f in range(1, Y):
                        v = v + in_y[f - 1, z].astype(F32)
                    dd[c, y, z] = v.astype(BF)

                self.by_z = [
                    put(
                        dd.at[c, y, at("zh", dh) * ZL + at("zl", dl)], in_z.at[k - 1],
                        zh=dh, zl=dl,
                    )
                    for k, (dh, dl) in enumerate(far)
                    if k
                ]

            def to_x(self):
                dd, in_c, in_y, in_z, tt, tb, in_x = self.r
                for copy in self.by_z:
                    copy.wait_recv()
                v = dd[c, y, zh * ZL + zl].astype(F32)
                for k in range(1, zs):
                    v = v + in_z[k - 1].astype(F32)
                for dx in range(X):
                    tt[dx] = v[dx * part : (dx + 1) * part]
                    tb[dx] = v[dx * part : (dx + 1) * part].astype(BF)
                self.by_x = [put(tb.at[at("x", d)], in_x.at[d - 1], x=d) for d in range(1, X)]

            def end(self):
                tt, in_x = self.r[4], self.r[6]
                for d in range(1, X):
                    self.by_x[d - 1].wait_recv()
                for d in range(1, X):
                    tt[at("x", -d)] = in_x[d - 1].astype(F32)
                for first, blocks in self.layout:
                    v = 0.0
                    for dx, start in blocks:
                        v = v + tt[dx, :, start : start + HEAD_WIDTH]
                    self.whole[:, first : first + HEAD_WIDTH] = v
                return move(self.whole, self.out)

        class Rows:
            def __init__(self, m, src, mine):
                self.m, self.mine = m, mine
                order = list(range(1, len(near))) + [0]
                self.by_c = {
                    (k, d): put(src.at[d, k], from_c.at[m, k, d - 1], c=d)
                    for k in order
                    for d in range(1, C)
                }
                self.own = move(src.at[0], mine)

            def summed(self, k, r):
                v = self.mine[k, r].astype(F32)
                for d in range(1, C):
                    v = v + from_c[self.m, k, d - 1, r].astype(F32)
                return v

            def spread(self):
                self.own.wait()
                self.by_n = []
                for k, (dh, dx) in enumerate(near):
                    for d in range(1, C):
                        if k:
                            self.by_c[k, d].wait_recv()
                    if k:
                        def body(r, k=k):
                            self.mine[k, r] = self.summed(k, r).astype(BF)

                        by_rows(rows, 32, body)
                        self.by_n.append(
                            put(self.mine.at[k], from_n.at[self.m, k - 1], zh=dh, x=dx)
                        )
                for d in range(1, C):
                    self.by_c[0, d].wait_recv()

            def spread_x(self):
                self.own.wait()
                self.by_n = {}
                for dh in reversed(range(ZH)):
                    for dx in range(1, X):
                        k = dh * X + dx
                        for d in range(1, C):
                            self.by_c[k, d].wait_recv()

                        def body(r, k=k):
                            self.mine[k, r] = self.summed(k, r).astype(BF)

                        by_rows(rows, 32, body)
                        to = from_n.at[self.m, dh * (X - 1) + dx - 1]
                        self.by_n[dh, dx] = put(self.mine.at[k], to, x=dx)

            def came_x(self, dh, r):
                v = self.summed(dh * X, r)
                for dx in range(1, X):
                    v = v + from_n[self.m, dh * (X - 1) + dx - 1, r].astype(F32)
                return v

            def relay(self):
                for dh in reversed(range(ZH)):
                    for d in range(1, C):
                        self.by_c[dh * X, d].wait_recv()
                    for dx in range(1, X):
                        self.by_n[dh, dx].wait_recv()
                    if dh:
                        def body(r, dh=dh):
                            self.mine[dh * X, r] = self.came_x(dh, r).astype(BF)

                        by_rows(rows, 32, body)
                        to = from_n.at[self.m, ZH * (X - 1) + dh - 1]
                        self.by_n[dh, 0] = put(self.mine.at[dh * X], to, zh=dh)

            def landed(self):
                for dh in range(1, ZH):
                    self.by_n[dh, 0].wait_recv()

            def final(self, r):
                v = self.came_x(0, r)
                for dh in range(1, ZH):
                    v = v + from_n[self.m, ZH * (X - 1) + dh - 1, r].astype(F32)
                return v

            def arrive(self):
                for copy in self.by_n:
                    copy.wait_recv()

            def total(self, r):
                v = self.summed(0, r)
                for k in range(1, len(near)):
                    v = v + from_n[self.m, k - 1, r].astype(F32)
                return v

        terms = Rows(0, nt_ref, half_n)
        loads = {
            "turned": move(gt_ref, turned),
            "g": move(gg_ref, units_t.at[0]),
            "u": move(gu_ref, units_t.at[1]),
        }
        for name, src, dst in (
            ("mid", mid_ref, hs), ("cot", cot_ref, cots), ("vec", vec_ref, vec),
            ("n1", n1_ref, n1t), ("wo", wo_ref, wo), ("kv", kv_ref, kv), ("p", p_ref, ps),
            ("att", att_ref, atts), ("q", q_ref, qs), ("cos", cos_ref, cos_s),
            ("sin", sin_ref, sin_s), ("w1", w1_ref, w1), ("in", in_ref, ins),
        ):
            loads[name] = move(src, dst)
        ud, ug, uu = Units(0, gd_ref), Units(1, None), Units(2, None)
        arrived = [(dh, dl) for dh, dl in far if dh]
        ud.begin(arrived[::-1] + [(0, 1)], arrived)
        outs_terms = Rows(1, ot_ref, half_o)

        eye = (
            lax.broadcasted_iota(jnp.int32, (128, 128), 0)
            == lax.broadcasted_iota(jnp.int32, (128, 128), 1)
        ).astype(BF)

        terms.spread()
        for name in ("turned", "g", "u", "n1"):
            loads[name].wait()
        compute_other()
        for k in (3, 2):
            send_pair(k)
        ud.add_y(arrived[::-1])
        for name in ("mid", "cot", "vec"):
            loads[name].wait()
        gain_one, gain_two = vec[0:1, :width], vec[1:2, :width]
        terms.arrive()
        vs[...] = jnp.zeros_like(vs)

        @pl.loop(0, rows // 32)
        def _(i):
            r = pl.ds(pl.multiple_of(i * 32, 32), 32)
            grad, h = terms.total(r), hs[r]
            inv = lax.rsqrt(jnp.mean(h * h, axis=-1, keepdims=True) + EPSILON)
            scaled = gain_two * grad
            v = (
                cots[r].astype(F32)
                + inv * scaled
                - h * (inv * inv * inv) * jnp.mean(scaled * h, axis=-1, keepdims=True)
            )
            dh_s[r] = v
            da[0, r] = v.astype(BF)
            vs[1:2, :width] = vs[1:2, :width] + jnp.sum(grad * h * inv, axis=0, keepdims=True)

        da_x = [put(da.at[0], da.at[-d % X], x=d) for d in range(1, X)]
        add_pair(3)
        add_pair(2)
        send_pair(1)
        loads["wo"].wait()
        loads["att"].wait()
        for copy in da_x:
            copy.wait_recv()

        @pl.loop(0, heads // 2)
        def _(j):
            cols = pl.ds(pl.multiple_of(j * 256, 256), 256)
            for k in range(X):
                dos[k * rows : (k + 1) * rows, cols] = nn(da[k], wo[:, cols]).astype(BF)

        for k in range(X):
            for j in range(width // 128):
                cols = slice(j * 128, (j + 1) * 128)
                dat[cols, k * rows : (k + 1) * rows] = nt(eye, da[k, :, cols]).astype(BF)
        s_out = Scatter(d_out, c_out, y_out, z_out, t_out, b_out, x_out, w_out_s, dout_o, out_layout)
        s_out.fill(dat, atts)
        s_out.to_c()
        for name in ("kv", "p", "q", "cos", "sin", "w1", "in"):
            loads[name].wait()
        dkv[...] = jnp.zeros_like(dkv)

        @pl.loop(0, heads)
        def _(h):
            cols = pl.ds(pl.multiple_of(h * HEAD_WIDTH, HEAD_WIDTH), HEAD_WIDTH)
            g = lax.div(h, share)
            k_at = pl.ds(pl.multiple_of(g * HEAD_WIDTH, HEAD_WIDTH), HEAD_WIDTH)
            v_at = pl.ds(pl.multiple_of(kv_cols + g * HEAD_WIDTH, HEAD_WIDTH), HEAD_WIDTH)
            p_low, do_h = ps[h], dos[:, cols]
            p = p_low.astype(F32)
            dp = nt(do_h, kv[:, v_at])
            delta = jnp.sum(p * dp, axis=-1, keepdims=True)
            ds = (p * (dp - delta)).astype(BF)
            dq = nn(ds, kv[:, k_at]) * scale
            dq = dq * cos_s[:query_rows] - pltpu.roll(dq, HEAD_WIDTH // 2, 1) * sin_s[:query_rows]
            dpre[:, cols] = dq.astype(BF)
            dkv[:, k_at] += tn(ds, qs[:, cols]) * scale
            dkv[:, v_at] += tn(p_low, do_h)

        kv_c = []
        for d in range(1, C):
            dkv_low[d - 1] = dkv[d * query_rows : (d + 1) * query_rows].astype(BF)
            kv_c.append(put(dkv_low.at[d - 1], dkv_in.at[d - 1], c=d))
        ud.add_l(far=True)
        s_out.to_y()
        ud.add_y([(0, 1)])
        for copy in kv_c:
            copy.wait_recv()
        total = dkv[:query_rows]
        for d in range(1, C):
            total = total + dkv_in[d - 1].astype(F32)
        for j in range(kv_heads):
            cols = slice(j * HEAD_WIDTH, (j + 1) * HEAD_WIDTH)
            v = total[:, cols]
            v = v * cos_s[:query_rows] - pltpu.roll(v, HEAD_WIDTH // 2, 1) * sin_s[:query_rows]
            dpre[:, q_cols + j * HEAD_WIDTH : q_cols + (j + 1) * HEAD_WIDTH] = v.astype(BF)
        dpre[:, q_cols + kv_cols :] = total[:, kv_cols:].astype(BF)
        s_qkv = Scatter(d_qkv, c_qkv, y_qkv, z_qkv, t_qkv, b_qkv, x_qkv, w_qkv_s, dqkv_o, qkv_layout)
        s_qkv.fill(n1t, dpre)
        s_qkv.to_c()

        for k in list(range(1, X)) + [0]:
            @pl.loop(0, width // 256)
            def _(j, k=k):
                cols = pl.ds(pl.multiple_of(j * 256, 256), 256)
                v = nt(dpre[k * rows : (k + 1) * rows], w1[cols])
                if k:
                    n_send[k - 1, :, cols] = v.astype(BF)
                else:
                    gi_s[:, cols] = v

            if k:
                copy = put(n_send.at[k - 1], n_recv.at[k - 1], x=k)
                n_x = [copy] if k == 1 else n_x + [copy]
        kv_at = lax.div(x * heads, QUERY_HEADS // KEY_VALUE_HEADS) * HEAD_WIDTH
        k_off = QUERY_HEADS * HEAD_WIDTH + kv_at
        v_off = k_off + KEY_VALUE_HEADS * HEAD_WIDTH
        sums = jnp.sum(dpre[...].astype(F32), axis=0, keepdims=True)

        def place(start, first, amount):
            vs[2:3, pl.ds(pl.multiple_of(start, 128), amount)] = sums[:, first : first + amount]

        place(x * q_cols, 0, q_cols)
        place(k_off, q_cols, kv_cols)
        place(v_off, q_cols + kv_cols, kv_cols)
        s_qkv.to_y()
        outs_terms.spread_x()
        ug.add_l(far=True)
        uu.add_l(far=True)
        for copy in n_x:
            copy.wait_recv()

        @pl.loop(0, rows // 32)
        def _(i):
            r = pl.ds(pl.multiple_of(i * 32, 32), 32)
            grad, h = gi_s[r], ins[r].astype(F32)
            for d in range(1, X):
                grad = grad + n_recv[d - 1, r].astype(F32)
            inv = lax.rsqrt(jnp.mean(h * h, axis=-1, keepdims=True) + EPSILON)
            scaled = gain_one * grad
            gi_s[r] = (
                dh_s[r]
                + inv * scaled
                - h * (inv * inv * inv) * jnp.mean(scaled * h, axis=-1, keepdims=True)
            )
            vs[0:1, :width] = vs[0:1, :width] + jnp.sum(grad * h * inv, axis=0, keepdims=True)

        done = [move(gi_s, gi_o)]

        def put_out(u, out):
            u.wait_h()
            for h in range(ZH):
                def body(r, h=h):
                    out_w[u.m, r, h * units : (h + 1) * units] = u.half(h, r).astype(BF)

                by_rows(depth, 64, body)
            done.append(move(out_w.at[u.m], out))

        places = iter(range(V_IN))
        stages = iter(range(4))

        def small_stage(offsets):
            k = next(stages)
            v_send[k] = vs[...]
            return [(p, put(v_send.at[k], v_in.at[p], **off)) for off, p in zip(offsets, places)]

        def small_finish(copies):
            for p, copy in copies:
                copy.wait_recv()
                vs[...] = vs[...] + v_in[p]

        state = small_stage([dict(c=d) for d in range(1, C)])
        send_pair(0)
        ud.begin([(0, 0)])
        add_pair(1)
        small_finish(state)
        state = small_stage([dict(x=d) for d in range(1, X)])
        s_out.to_z()
        outs_terms.relay()
        small_finish(state)
        state = small_stage([dict(y=d) for d in range(1, Y)])
        s_qkv.to_z()
        s_out.to_x()
        small_finish(state)
        state = small_stage([dict(zh=dh, zl=dl) for dh, dl in far[1:]])
        outs_terms.landed()

        def finish(r):
            lo_s[r] = (hs[r] + outs_terms.final(r)).astype(BF)

        by_rows(rows, 32, finish)
        done.append(move(lo_s, lo_o))
        done.append(s_out.end())
        s_qkv.to_x()
        ud.add_l(far=False)
        ug.add_l(far=False)
        uu.add_l(far=False)
        small_finish(state)
        done.append(move(vs, vec_out))
        done.append(s_qkv.end())
        add_pair(0)
        put_out(ug, og_o)
        put_out(uu, ou_o)
        ud.add_y([(0, 0)])
        put_out(ud, od_o)
        for copy in done:
            copy.wait()
        for copy in sent:
            copy.wait_send()
        assert count[0] <= n_sems and count[1] <= 64, count

    V_IN = (C - 1) + (X - 1) + (Y - 1) + (zs - 1)
    any_spec = pl.BlockSpec(memory_space=pl.ANY)
    sds = jax.ShapeDtypeStruct
    vm = pltpu.VMEM

    def scatter_scratch(n):
        return [
            vm((C, Y, zs, X * part, n), BF), vm((Y, max(C - 1, 1), zs, X * part, n), BF),
            vm((max(Y - 1, 1), zs, X * part, n), BF), vm((max(zs - 1, 1), X * part, n), BF),
            vm((X, part, n), F32), vm((X, part, n), BF), vm((max(X - 1, 1), part, n), BF),
        ]

    nk = len(near)
    return pl.pallas_call(
        kernel,
        out_shape=[
            sds((rows, width), BF), sds((rows, width), F32), sds((part, QKV_WIDTH), F32),
            sds((part, X * q_cols), F32), sds((8, QKV_WIDTH), F32),
            sds((depth, ZH * units), BF), sds((depth, ZH * units), BF),
            sds((depth, ZH * units), BF),
        ],
        in_specs=[any_spec] * 20,
        out_specs=[any_spec] * 8,
        scratch_shapes=[
            vm((3, zs, depth, units), BF), vm((3, zs, max(Y - 1, 1), depth, units), BF),
            vm((3, ZH, max(ZL - 1, 1), depth, units), BF), vm((3, max(ZH - 1, 1), depth, units), BF),
            vm((3, depth, ZH * units), BF), vm((width, group_rows), BF), vm((2, units, group_rows), BF),
            vm((nk, rows, width), BF), vm((nk, rows, width), BF),
            vm((2, nk, max(C - 1, 1), rows, width), BF), vm((2, max(nk - 1, 1), rows, width), BF),
            vm((rows, width), F32), vm((rows, width), BF), vm((rows, width), BF),
            vm((width, qkv_n), BF), vm((width, q_cols), BF),
            vm((width, query_rows), BF), vm((query_rows, q_cols), BF),
            vm((pack_rows, 2 * kv_cols), BF), vm((heads, query_rows, pack_rows), BF),
            vm((query_rows, q_cols), BF), vm((8, QKV_WIDTH), F32),
            vm((pack_rows, HEAD_WIDTH), F32), vm((pack_rows, HEAD_WIDTH), F32),
            vm((X, rows, width), BF), vm((width, query_rows), BF), vm((query_rows, q_cols), BF),
            vm((query_rows, qkv_n), BF), vm((pack_rows, 2 * kv_cols), F32),
            vm((max(C - 1, 1), query_rows, 2 * kv_cols), BF),
            vm((max(C - 1, 1), query_rows, 2 * kv_cols), BF),
            vm((rows, width), F32),
        ]
        + scatter_scratch(qkv_n)
        + scatter_scratch(q_cols)
        + [
            vm((part, QKV_WIDTH), F32), vm((part, X * q_cols), F32),
            vm((max(X - 1, 1), rows, width), BF), vm((max(X - 1, 1), rows, width), BF),
            vm((rows, width), BF), vm((rows, width), F32), vm((8, QKV_WIDTH), F32),
            vm((max(V_IN, 1), 8, QKV_WIDTH), F32), vm((4, 8, QKV_WIDTH), F32),
            pltpu.SemaphoreType.DMA((n_sems,)), pltpu.SemaphoreType.DMA((n_sems,)),
            pltpu.SemaphoreType.DMA((64,)),
        ],
        compiler_params=pltpu.CompilerParams(
            collective_id=1, has_side_effects=True, vmem_limit_bytes=63 << 20
        ),
        name="back",
    )(
        grad_d, near_d, grad_g, grad_u, group_t, normed_terms, out_terms, middle, cotangent, own_in,
        wqkv, wout, normed, queries, kv_rows, probs, attended, vectors, cosine, sine,
    )


def product(left, right, block):
    count, depth = left.shape[0] // block, left.shape[1]
    columns = right.shape[0]

    def kernel(left_ref, right_ref, out_ref):
        out_ref[...] = nt(left_ref[...], right_ref[...]).astype(BF)

    return pl.pallas_call(
        kernel,
        grid=(count,),
        out_shape=jax.ShapeDtypeStruct((count * block, columns), BF),
        in_specs=[
            pl.BlockSpec((block, depth), lambda i: (i, 0)),
            pl.BlockSpec((columns, depth), lambda i: (0, 0)),
        ],
        out_specs=pl.BlockSpec((block, columns), lambda i: (i, 0)),
        cost_estimate=pl.CostEstimate(
            flops=2 * count * block * depth * columns,
            bytes_accessed=2 * (count * block * (depth + columns) + columns * depth),
            transcendentals=0,
        ),
        name="product",
    )(left, right)


def ff(normed, cotangent, w_gate, w_up, w_down):
    gate = nn(normed, w_gate)
    up_part = nn(normed, w_up)
    sig = jax.nn.sigmoid(gate)
    act = gate * sig
    hidden = (act * up_part).astype(BF)
    grad_wdown = tn(cotangent, hidden).astype(BF)
    grad_hidden = nn(cotangent, w_down)
    grad_gate = (grad_hidden * up_part * sig * (1.0 + gate * (1.0 - sig))).astype(BF)
    grad_up = (grad_hidden * act).astype(BF)
    grad_wgate = tn(normed, grad_gate).astype(BF)
    grad_wup = tn(normed, grad_up).astype(BF)
    normed_term = (nt(grad_gate, w_gate) + nt(grad_up, w_up)).astype(BF)
    out_term = nt(hidden, w_down).astype(BF)
    return hidden, grad_gate, grad_up, grad_wdown, grad_wgate, grad_wup, out_term, normed_term


def small_rows(gain_one, gain_two, bias):
    wide = [jnp.pad(v.astype(F32), (0, 128 - v.shape[0])) for v in (gain_one, gain_two, bias)]
    return jnp.pad(jnp.stack(wide), ((0, 5), (0, 0)))


def shards(
    layer_in, lengths, w_qkv, b_qkv, w_out, norm1_gain, norm2_gain, w_gate, w_up, w_down, grad_out
):
    size = lax.axis_size
    ZH, ZL, Y, X, C = (size(a) for a in ("zh", "zl", "y", "x", "c"))
    zh, zl, y, x, c = (lax.axis_index(a) for a in ("zh", "zl", "y", "x", "c"))
    everyone = ("zh", "zl", "y", "x", "c")
    devices = ZH * ZL * Y * X * C
    rows, width = layer_in.shape[1:]
    part = w_qkv.shape[0]
    group = QUERY_HEADS // KEY_VALUE_HEADS
    heads = QUERY_HEADS // X
    kv_heads = max(1, heads // group)
    share = heads // kv_heads
    q_cols, kv_cols = heads * HEAD_WIDTH, kv_heads * HEAD_WIDTH
    scale = HEAD_WIDTH ** (-0.5)

    own_in = layer_in[0]
    cotangent = grad_out[0]
    own_rows = own_in.astype(F32)
    query_rows, pack_rows = X * rows, C * X * rows
    bias_part = b_qkv.shape[0]
    def row_index(cores):
        spans = [
            (((x + dx) % X) * C + (c + dc) % C) * rows + jnp.arange(rows, dtype=jnp.int32)
            for dc in range(cores)
            for dx in range(X)
        ]
        return jnp.concatenate(spans)

    doc_lengths = lengths[0]
    key_index = row_index(C)
    key_doc, key_pos = doc_layout(key_index, doc_lengths)
    query_index, query_doc = key_index[:query_rows], key_doc[:query_rows]
    key_cos, key_sin = angles(key_pos)
    query_cos, query_sin = key_cos[:query_rows], key_sin[:query_rows]

    def gather_columns(pieces):
        held = ordered(
            [pick(pieces, x)] + [fetch(pick(pieces, (x - d) % X), "x", d) for d in range(1, X)],
            "x",
        )
        whole = jnp.zeros((ZH, ZL, Y) + held.shape, held.dtype)
        for dh in range(ZH):
            for dl in range(ZL):
                along = held if dh == dl == 0 else fetch(held, ("zh", "zl"), (dh, dl))
                for dy in range(Y):
                    piece = along if dy == 0 else fetch(along, "y", dy)
                    whole = lax.dynamic_update_slice(
                        whole,
                        piece[None, None, None],
                        ((zh + dh) % ZH, (zl + dl) % ZL, (y + dy) % Y, 0, 0, 0),
                    )
        whole = whole.reshape((ZH * ZL * Y * X,) + whole.shape[4:])
        both = ordered([whole] + [fetch(whole, "c", d) for d in range(1, C)], "c")
        return jnp.moveaxis(both, 0, 1).reshape(width, whole.shape[-1])

    def scatter_columns(grad):
        n = grad.shape[-1]
        grad = grad.astype(BF).reshape(ZH * ZL * Y * X, C, part, n)
        held = pick(grad, c, 1).astype(F32)
        for d in range(1, C):
            held = held + send(pick(grad, (c + d) % C, 1), "c", d)
        held = held.astype(BF).reshape(ZH, ZL, Y, X * part, n)
        kept = pick(held, y, 2).astype(F32)
        for d in range(1, Y):
            kept = kept + send(pick(held, (y + d) % Y, 2), "y", d)
        low = kept.astype(BF)
        total = 0.0
        for dh in range(ZH):
            for dl in range(ZL):
                if dh == dl == 0:
                    total = total + pick(pick(kept, zh), zl)
                else:
                    piece = pick(pick(low, (zh + dh) % ZH), (zl + dl) % ZL)
                    total = total + send(piece, ("zh", "zl"), (dh, dl)).astype(F32)
        total = total.reshape(X, part, n)
        lower = total.astype(BF)
        return ordered(
            [pick(total, x)]
            + [fetch(pick(lower, (x - d) % X), "x", d).astype(F32) for d in range(1, X)],
            "x",
        )

    def qkv_columns(array):
        blocks = []
        for at in range(X):
            kv = (at * heads) // group * HEAD_WIDTH
            key_at = QUERY_HEADS * HEAD_WIDTH + kv
            value_at = key_at + KEY_VALUE_HEADS * HEAD_WIDTH
            blocks.append(
                jnp.concatenate(
                    [
                        array[..., at * q_cols : (at + 1) * q_cols],
                        array[..., key_at : key_at + kv_cols],
                        array[..., value_at : value_at + kv_cols],
                    ],
                    axis=-1,
                )
            )
        return jnp.stack(blocks)

    def qkv_whole(blocks):
        queries = [blocks[at, ..., :q_cols] for at in range(X)]
        keys, values = [0.0] * KEY_VALUE_HEADS, [0.0] * KEY_VALUE_HEADS
        for at in range(X):
            for j in range(kv_heads):
                head = (at * heads) // group + j
                start = q_cols + j * HEAD_WIDTH
                keys[head] = keys[head] + blocks[at, ..., start : start + HEAD_WIDTH]
                start = start + kv_cols
                values[head] = values[head] + blocks[at, ..., start : start + HEAD_WIDTH]
        return jnp.concatenate(queries + keys + values, axis=-1)

    depth, units = w_gate.shape[0], w_gate.shape[1] // ZH

    def gather_units(weight):
        halves = weight.reshape(depth, ZH, units).transpose(1, 0, 2)
        whole = jnp.zeros((ZH, ZL, Y, depth, units), weight.dtype)
        for dh in range(ZH):
            first = pick(halves, zh) if dh == 0 else fetch(pick(halves, (zh - dh) % ZH), "zh", dh)
            for dl in range(ZL):
                second = first if dl == 0 else fetch(first, "zl", dl)
                for dy in range(Y):
                    third = second if dy == 0 else fetch(second, "y", dy)
                    whole = lax.dynamic_update_slice(
                        whole,
                        third[None, None, None],
                        ((zh + dh) % ZH, (zl + dl) % ZL, (y + dy) % Y, 0, 0),
                    )
        return whole.reshape(width, units)

    def scatter_units(grad):
        grad = grad.astype(BF).reshape(ZH, ZL, Y, depth, units)
        done = [None] * ZH
        for dh in reversed(range(ZH)):
            mine = pick(grad, (zh + dh) % ZH)
            kept = pick(mine, y, 1).astype(F32)
            for d in range(1, Y):
                kept = kept + send(pick(mine, (y + d) % Y, 1), "y", d).astype(F32)
            low = kept.astype(BF)
            total = pick(kept, zl)
            for d in range(1, ZL):
                total = total + send(pick(low, (zl + d) % ZL), "zl", d).astype(F32)
            done[dh] = total
        halves = [done[0]] + [
            send(done[dh].astype(BF), "zh", dh).astype(F32) for dh in range(1, ZH)
        ]
        halves = [halves[0]] + halves[:0:-1]
        return jnp.moveaxis(ordered(halves, "zh"), 0, 1).reshape(depth, ZH * units)

    near = [(dh, dx) for dh in range(ZH) for dx in range(X)]

    def gather_rows(own):
        held = jnp.concatenate([own if k == (0, 0) else fetch(own, ("zh", "x"), k) for k in near])
        return jnp.concatenate([held] + [fetch(held, "c", d) for d in range(1, C)])

    def scatter_rows(term):
        term = term.reshape(C, len(near), rows, width)
        held = term[0].astype(F32)
        for d in range(1, C):
            held = held + send(term[d].astype(BF), "c", d).astype(F32)
        total = held[0]
        for at, k in enumerate(near):
            if k != (0, 0):
                total = total + send(held[at].astype(BF), ("zh", "x"), k).astype(F32)
        return total

    def scatter_x(term):
        term = term.reshape(X, rows, width)
        total = term[0]
        for d in range(1, X):
            total = total + send(term[d].astype(BF), "x", d).astype(F32)
        return total

    if part % 16 == 0 and depth % 64 == 0 and heads % 2 == 0 and X > 1 and ZH == ZL == Y == 2:
        (
            wqkv_mine, wout_mine, normed_t, group_normed_t, queries, kv_low, probs_low,
            attended_low, middle, group_normed, group_cotangent, wgate_mine, wup_mine,
            wdown_part, vectors, cosine, sine,
        ) = front(
            own_in,
            cotangent,
            lengths,
            w_qkv,
            w_out.T,
            small_rows(norm1_gain, norm2_gain, b_qkv),
            w_gate,
            w_up,
            w_down.T,
            qkv_columns,
        )
        step = pick(pick(wdown_part, (zl + 1) % ZL, 1), y, 1)
        step = fetch(step, "y", 1)
        wdown_mine = lax.dynamic_update_slice(
            wdown_part, step[:, None, None], (0, (zl + 1) % ZL, (y + 1) % Y, 0, 0)
        ).reshape(width, units)
        group_normed = group_normed.reshape(-1, width)
        group_cotangent = group_cotangent.reshape(-1, width)
        wgate_mine, wup_mine = (w.reshape(width, units) for w in (wgate_mine, wup_mine))
        gate = nn(group_normed, wgate_mine)
        up_part = nn(group_normed, wup_mine)
        sig = jax.nn.sigmoid(gate)
        act = gate * sig
        hidden = lax.optimization_barrier((act * up_part).astype(BF))
        whole = (ZH, ZL, Y, depth, units)
        terms = (C, ZH * X, rows, width)
        grad_wdown = tn(group_cotangent, hidden).astype(BF).reshape(whole)
        near_d = fetch(
            jnp.stack(
                [
                    pick(pick(pick(grad_wdown, (zh + dh) % ZH), (zl + dl) % ZL), (y + 1) % Y)
                    for dh in range(1, ZH)
                    for dl in range(ZL)
                ]
            ),
            "y",
            1,
        )
        grad_hidden = nn(group_cotangent, wdown_mine)
        grad_gate = (grad_hidden * up_part * sig * (1.0 + gate * (1.0 - sig))).astype(BF)
        grad_up = (grad_hidden * act).astype(BF)
        normed_term = (nt(grad_gate, wgate_mine) + nt(grad_up, wup_mine)).astype(BF)
        out_term = nt(hidden, wdown_mine).astype(BF)
        layer_out, grad_input, sum_wqkv, sum_wout, small, sum_wdown, sum_wgate, sum_wup = back(
            grad_wdown,
            near_d,
            grad_gate.T,
            grad_up.T,
            group_normed_t,
            normed_term.reshape(terms),
            out_term.reshape(terms),
            middle,
            cotangent,
            own_in,
            wqkv_mine,
            wout_mine,
            normed_t,
            queries,
            kv_low,
            probs_low,
            attended_low,
            vectors,
            cosine,
            sine,
        )
        place = (((zh * ZL + zl) * Y + y) * X + x) * C + c
        return (
            layer_out[None],
            grad_input[None],
            sum_wqkv,
            lax.dynamic_slice_in_dim(small[2], place * bias_part, bias_part),
            sum_wout.T,
            lax.dynamic_slice_in_dim(small[0, :width], place * part, part),
            lax.dynamic_slice_in_dim(small[1, :width], place * part, part),
            sum_wgate.astype(F32),
            sum_wup.astype(F32),
            sum_wdown.T.astype(F32),
        )

    small = jnp.concatenate([norm1_gain, norm2_gain, b_qkv])
    small = jnp.pad(small, (0, -small.shape[0] % 256))[None]
    small = lax.all_to_all(
        jnp.broadcast_to(small[None], (devices,) + small.shape), everyone, 0, 0, tiled=True
    )[:, 0].astype(F32)
    gain_one = small[:, :part].reshape(1, width)
    gain_two = small[:, part : 2 * part].reshape(1, width)
    bias = small[:, 2 * part : 2 * part + bias_part].reshape(-1)

    query_in = jnp.concatenate([own_in] + [fetch(own_in, "x", d) for d in range(1, X)])
    pack_in = jnp.concatenate([query_in] + [fetch(query_in, "c", d) for d in range(1, C)])

    wqkv_mine = gather_columns(qkv_columns(w_qkv))
    wout_t = w_out.T
    wout_mine = gather_columns(
        jnp.stack([wout_t[:, at * q_cols : (at + 1) * q_cols] for at in range(X)])
    )
    bias_mine = pick(qkv_columns(bias), x)

    wgate_mine, wup_mine = gather_units(w_gate), gather_units(w_up)
    wdown_mine = gather_units(w_down.T)

    group_cotangent = gather_rows(cotangent)

    pack_in = pack_in.astype(F32)
    normed_one = (pack_in * rms_parts(pack_in) * gain_one).astype(BF)
    query_normed = normed_one[:query_rows]
    pre_query = nn(query_normed, wqkv_mine[:, :q_cols]) + bias_mine[:q_cols]
    pre_kv = nn(normed_one, wqkv_mine[:, q_cols:]) + bias_mine[q_cols:]
    queries = rotate(
        pre_query.reshape(query_rows, heads, HEAD_WIDTH), query_cos, query_sin
    ).astype(BF)
    queries = queries.reshape(query_rows, kv_heads, share, HEAD_WIDTH)
    keys = rotate(
        pre_kv[:, :kv_cols].reshape(pack_rows, kv_heads, HEAD_WIDTH), key_cos, key_sin
    ).astype(BF)
    values = pre_kv[:, kv_cols:].reshape(pack_rows, kv_heads, HEAD_WIDTH).astype(BF)
    scores = jnp.einsum("tkgd,skd->kgts", queries, keys, preferred_element_type=F32) * scale
    allowed = (query_doc[:, None] == key_doc[None, :]) & (
        key_index[None, :] <= query_index[:, None]
    )
    masked = jnp.where(allowed, scores, NEGATIVE_BIG)
    top = jnp.max(masked, axis=-1, keepdims=True)
    weights = jnp.where(allowed, jnp.exp(masked - top), 0.0)
    probs = weights / jnp.sum(weights, axis=-1, keepdims=True)
    probs_low = probs.astype(BF)
    attended = jnp.einsum("kgts,skd->tkgd", probs_low, values, preferred_element_type=F32)
    attended_low = attended.reshape(query_rows, q_cols).astype(BF)
    middle = own_rows + scatter_x(nt(attended_low, wout_mine))
    normed_two = (middle * rms_parts(middle) * gain_two).astype(BF)

    group_normed = gather_rows(normed_two)

    hidden, grad_gate, grad_up, grad_wdown, grad_wgate, grad_wup, out_term, normed_term = ff(
        group_normed, group_cotangent, wgate_mine, wup_mine, wdown_mine
    )
    grad_normed_two = scatter_rows(normed_term)
    layer_out = (middle + scatter_rows(out_term)).astype(BF)
    sum_wdown = scatter_units(grad_wdown).T
    sum_wgate = scatter_units(grad_wgate)
    sum_wup = scatter_units(grad_wup)

    back_two, grad_gain_two = rms_back(middle, gain_two, grad_normed_two)
    grad_middle = cotangent.astype(F32) + back_two
    grad_att = grad_middle.astype(BF)
    query_grad_att = jnp.concatenate([grad_att] + [fetch(grad_att, "x", d) for d in range(1, X)])
    sum_wout = scatter_columns(tn(query_grad_att, attended_low))
    head_grads = nn(query_grad_att, wout_mine).astype(BF)
    head_grads = head_grads.reshape(query_rows, kv_heads, share, HEAD_WIDTH)
    grad_probs = jnp.einsum("tkgd,skd->kgts", head_grads, values, preferred_element_type=F32)
    probs = probs_low.astype(F32)
    delta = jnp.sum(probs * grad_probs, axis=-1, keepdims=True)
    grad_scores = (probs * (grad_probs - delta)).astype(BF)
    grad_query = (
        jnp.einsum("kgts,skd->tkgd", grad_scores, keys, preferred_element_type=F32) * scale
    )
    grad_key = jnp.einsum("kgts,tkgd->skd", grad_scores, queries, preferred_element_type=F32)
    grad_key = rotate(grad_key * scale, key_cos, -key_sin)
    grad_value = jnp.einsum("kgts,tkgd->skd", probs_low, head_grads, preferred_element_type=F32)
    grad_kv = jnp.concatenate(
        [grad_key.reshape(pack_rows, kv_cols), grad_value.reshape(pack_rows, kv_cols)], axis=1
    ).reshape(C, query_rows, 2 * kv_cols)
    kv_total = grad_kv[0]
    for d in range(1, C):
        kv_total = kv_total + send(grad_kv[d].astype(BF), "c", d).astype(F32)
    grad_query = rotate(
        grad_query.reshape(query_rows, heads, HEAD_WIDTH), query_cos, -query_sin
    ).reshape(query_rows, q_cols)
    grad_pre = jnp.concatenate([grad_query, kv_total], axis=1).astype(BF)
    sum_wqkv = qkv_whole(scatter_columns(tn(query_normed, grad_pre)))
    grad_bias = jnp.sum(grad_pre.astype(F32), axis=0)
    grad_normed_one = scatter_x(nt(grad_pre, wqkv_mine))
    back_one, grad_gain_one = rms_back(own_rows, gain_one, grad_normed_one)
    grad_input = grad_middle + back_one

    bias_blocks = jnp.where(
        jnp.arange(X, dtype=jnp.int32)[:, None] == x, grad_bias[None, :], 0.0
    )
    bias_whole = qkv_whole(bias_blocks)
    piece = jnp.concatenate(
        [
            grad_gain_one.reshape(devices, part),
            grad_gain_two.reshape(devices, part),
            bias_whole.reshape(devices, bias_part),
        ],
        axis=1,
    )
    piece = jnp.pad(piece, ((0, 0), (0, -piece.shape[1] % 256)))
    piece = jnp.sum(lax.all_to_all(piece[:, None], everyone, 0, 0, tiled=True)[:, 0], axis=0)
    return (
        layer_out[None],
        grad_input[None],
        sum_wqkv,
        piece[2 * part : 2 * part + bias_part],
        jnp.moveaxis(sum_wout, 0, 1).reshape(part, -1).T,
        piece[:part],
        piece[part : 2 * part],
        sum_wgate,
        sum_wup,
        sum_wdown,
    )


def solution(mesh):
    wide, narrow = mesh.shape["wide"], mesh.shape["narrow"]
    cores = 2 if narrow % 2 == 0 else 1
    along_x = narrow // cores
    along_y = along_x if wide % along_x == 0 else 1
    along_z = wide // along_y
    far = 2 if along_z % 2 == 0 else 1
    split = Mesh(
        mesh.devices.reshape(far, along_z // far, along_y, along_x, cores),
        ("zh", "zl", "y", "x", "c"),
    )
    w, n = ("zh", "zl", "y"), ("x", "c")
    placed = (
        P(w, n, None),
        P(w, None),
        P(w + n, None),
        P(w + n),
        P(None, w + n),
        P(w + n),
        P(w + n),
        P(w, n),
        P(w, n),
        P(n, w),
        P(w, n, None),
    )
    return jax.shard_map(
        shards,
        mesh=split,
        in_specs=placed,
        out_specs=(
            P(w, n, None),
            P(w, n, None),
            P(w + n, None),
            P(w + n),
            P(None, w + n),
            P(w + n),
            P(w + n),
            P(w, n),
            P(w, n),
            P(n, w),
        ),
        check_vma=False,
    )
```

```python
import math

import jax
import jax.numpy as jnp
from jax import lax
from jax.experimental import pallas as pl
from jax.experimental.pallas import tpu as pltpu
from jax.sharding import Mesh
from jax.sharding import PartitionSpec as P

QUERY_HEADS = 12
KEY_VALUE_HEADS = 2
HEAD_WIDTH = 128

EPSILON = 1e-06
ROPE_BASE = 10000.0
NEGATIVE_BIG = -1e30
HIGHEST = lax.Precision.HIGHEST


BF = jnp.bfloat16
F32 = jnp.float32
AXES = ("zh", "zl", "y", "x", "c")
MESH_ID = pl.DeviceIdType.MESH
QKV_WIDTH = (QUERY_HEADS + 2 * KEY_VALUE_HEADS) * HEAD_WIDTH


def fetch(value, axes, offsets):
    axes = (axes,) if isinstance(axes, str) else tuple(axes)
    offsets = (offsets,) if isinstance(offsets, int) else tuple(offsets)
    sizes = [lax.axis_size(a) for a in axes]
    total = math.prod(sizes)
    pairs = []
    for flat in range(total):
        rest, place = flat, []
        for size in reversed(sizes):
            place.append(rest % size)
            rest //= size
        place = place[::-1]
        source = 0
        for spot, off, size in zip(place, offsets, sizes):
            source = source * size + (spot + off) % size
        pairs.append((source, flat))
    return lax.ppermute(value, axes if len(axes) > 1 else axes[0], pairs)


def send(value, axes, offsets):
    offsets = (offsets,) if isinstance(offsets, int) else tuple(offsets)
    return fetch(value, axes, tuple(-o for o in offsets))


def pick(stack, place, axis=0):
    return lax.dynamic_index_in_dim(stack, place, axis, keepdims=False)


def nn(left, right):
    return lax.dot_general(left, right, (((1,), (0,)), ((), ())), preferred_element_type=F32)


def nt(left, right):
    return lax.dot_general(left, right, (((1,), (1,)), ((), ())), preferred_element_type=F32)


def tn(left, right):
    return lax.dot_general(left, right, (((0,), (0,)), ((), ())), preferred_element_type=F32)


def rms_parts(rows):
    return lax.rsqrt(jnp.mean(rows * rows, axis=-1, keepdims=True) + EPSILON)


def rms_back(rows, gain, grad):
    r = rms_parts(rows)
    scaled = gain * grad
    return (
        r * scaled - rows * (r * r * r) * jnp.mean(scaled * rows, axis=-1, keepdims=True),
        jnp.sum(grad * rows * r, axis=0),
    )


def doc_layout(index, doc_lengths):
    ends = jnp.cumsum(doc_lengths)
    starts = ends - doc_lengths
    document_index = jnp.sum((index[:, None] >= ends[None, :]).astype(jnp.int32), axis=1)
    onehot = (
        document_index[:, None] == jnp.arange(doc_lengths.shape[0], dtype=jnp.int32)[None, :]
    ).astype(jnp.int32)
    token_position = index - jnp.sum(onehot * starts[None, :], axis=1)
    return document_index, token_position.astype(F32)


def angles(position):
    half = HEAD_WIDTH // 2
    freq = jnp.exp(jnp.arange(half, dtype=F32) * (-2.0 * math.log(ROPE_BASE) / HEAD_WIDTH))
    angle = position[:, None] * freq[None, :]
    return jnp.cos(angle)[:, None, :], jnp.sin(angle)[:, None, :]


def rotate(rows, cosine, sine):
    half = HEAD_WIDTH // 2
    first, second = rows[..., :half], rows[..., half:]
    return jnp.concatenate(
        [first * cosine - second * sine, second * cosine + first * sine], axis=-1
    )


def ordered(pieces, axis):
    count, here = len(pieces), lax.axis_index(axis)
    if count == 1:
        return pieces[0][None]
    if count == 2:
        return jnp.where(here == 0, jnp.stack(pieces), jnp.stack(pieces[::-1]))
    whole = jnp.zeros((count,) + pieces[0].shape, pieces[0].dtype)
    for distance, piece in enumerate(pieces):
        whole = lax.dynamic_update_index_in_dim(whole, piece, (here + distance) % count, 0)
    return whole


def front(own_in, cotangent, lengths, w_qkv, w_out, small, w_gate, w_up, w_down, qkv_columns):
    size = lax.axis_size
    ZH, ZL, Y, X, C = (size(a) for a in AXES)
    rows, width = own_in.shape
    part = w_qkv.shape[0]
    q_cols = w_out.shape[1] // X
    qkv_n = qkv_columns(w_qkv).shape[-1]
    heads = q_cols // HEAD_WIDTH
    kv_cols = (qkv_n - q_cols) // 2
    kv_heads = kv_cols // HEAD_WIDTH
    share = heads // kv_heads
    query_rows, pack_rows = X * rows, C * X * rows
    depth = w_gate.shape[0]
    units = w_gate.shape[1] // ZH
    near = [(dh, dx) for dh in range(ZH) for dx in range(X)]
    far = [(dh, dl) for dh in range(ZH) for dl in range(ZL)]
    devices = ZH * ZL * Y * X * C
    bias_part = QKV_WIDTH // devices
    scale = HEAD_WIDTH ** (-0.5)
    docs = lengths.shape[-1]
    n_sems = 400

    def kernel(
        own_ref, cot_ref, len_ref, qkv_ref, out_ref, small_ref, g_ref, u_ref, d_ref,
        wqkv_o, wout_o, n1_o, n2t_o, q_o, kv_o, p_o, att_o, h_o, nr_o, go_o, wg_o, wu_o, wd_o, vec_o, cos_o, sin_o, relay,
        xr, w1, wo, sm, n1, qs, kv, ob, part_send, part_recv, n2s, hs,
        cos_s, sin_s, mask_s, rows_s, ps, raw, half, wq_raw, wq_cut, n1t, n2t, nr_v, go_v,
        send_sem, recv_sem, local_sem,
    ):
        zh, zl, y, x, c = (lax.axis_index(a) for a in AXES)
        sizes = dict(zip(AXES, (ZH, ZL, Y, X, C)))
        here = dict(zip(AXES, (zh, zl, y, x, c)))

        def device(**off):
            return tuple(
                lax.rem(here[a] + off[a], sizes[a]) if off.get(a, 0) % sizes[a] else here[a]
                for a in AXES
            )

        def at(a, d):
            d = d % sizes[a]
            return lax.rem(here[a] + d, sizes[a]) if d else here[a]

        peers = set()
        for d in range(1, C):
            peers.add((0, 0, 0, 0, d))
        for dh, dx in near[1:]:
            peers.add((dh, 0, 0, dx, 0))
        for dh, dl in far[1:]:
            peers.add((dh, dl, 0, 0, 0))
        for d in range(1, Y):
            peers.add((0, 0, d, 0, 0))
        peers = sorted(peers)
        barrier = pltpu.get_barrier_semaphore()
        for peer in peers:
            pl.semaphore_signal(
                barrier, inc=1, device_id=device(**dict(zip(AXES, peer))), device_id_type=MESH_ID
            )
        pl.semaphore_wait(barrier, len(peers))

        count = [0, 0]
        sent, local = [], []

        def put(src, dst, **off):
            k = count[0]
            count[0] += 1
            copy = pltpu.make_async_remote_copy(
                src_ref=src, dst_ref=dst, send_sem=send_sem.at[k], recv_sem=recv_sem.at[k],
                device_id=device(**off), device_id_type=MESH_ID,
            )
            copy.start()
            sent.append(copy)
            return copy

        def move(src, dst):
            k = count[1]
            count[1] += 1
            copy = pltpu.make_async_copy(src, dst, local_sem.at[k])
            copy.start()
            return copy

        inner = zh + zl == 1

        class Far:
            def __init__(self, src, dst, relay, onward):
                k = count[0]
                count[0] += 3
                self.relay, self.k = relay, k
                self.main = self.copy(src, dst, k, k, device(zh=1))
                self.step = self.copy(src, relay, k, k + 1, device(zl=1))
                self.onward = self.copy(relay, onward, k + 2, k, device(zh=1, zl=1))
                pl.when(inner)(self.main.start)
                pl.when(jnp.logical_not(inner))(self.step.start)
                sent.append(self)

            def copy(self, src, dst, k, r, to):
                return pltpu.make_async_remote_copy(
                    src_ref=src, dst_ref=dst, send_sem=send_sem.at[k], recv_sem=recv_sem.at[r],
                    device_id=to, device_id_type=MESH_ID,
                )

            def forward(self):
                @pl.when(inner)
                def _():
                    self.step.wait_recv()
                    self.onward.start()

            def wait_recv(self):
                self.main.wait_recv()

            def wait_send(self):
                self.main.wait_send()
                pl.when(inner)(self.onward.wait_send)

        class Gather:
            def __init__(self, buf, block, pieces):
                self.buf, self.block, self.pieces = buf, block, pieces

            def slot(self, dh, dl, dy, dx, dc):
                place = at("zh", dh)
                for a, d in (("zl", dl), ("y", dy), ("x", dx), ("c", dc)):
                    place = place * sizes[a] + at(a, d)
                start = pl.multiple_of(place * self.block, self.block)
                return self.buf.at[pl.ds(start, self.block)]

            def begin(self):
                self.own = move(self.pieces(x), self.slot(0, 0, 0, 0, 0))
                self.by_x = {
                    d: put(self.pieces(at("x", d)), self.slot(0, 0, 0, 0, 0), x=d)
                    for d in range(1, X)
                }

            def along_z(self):
                self.own.wait()
                for d in self.by_x:
                    self.by_x[d].wait_recv()
                self.by_h, self.by_l, self.by_y, self.by_c = {}, {}, {}, {}
                for dx in range(X):
                    s = self.slot(0, 0, 0, dx, 0)
                    for d in range(1, ZH):
                        self.by_h[d, dx] = put(s, s, zh=d)
                for dx in range(X):
                    self.along_l(0, dx)
                for dx in range(X):
                    self.spread(0, 0, dx)

            def along_l(self, dh, dx):
                s = self.slot(-dh, 0, 0, dx, 0)
                for d in range(1, ZL):
                    self.by_l[dh, d, dx] = put(s, s, zl=d)

            def spread(self, dh, dl, dx):
                s = self.slot(-dh, -dl, 0, dx, 0)
                for d in range(1, Y):
                    self.by_y[dh, dl, d, dx] = put(s, s, y=d)
                self.to_core(dh, dl, 0, dx)

            def to_core(self, dh, dl, dy, dx):
                s = self.slot(-dh, -dl, -dy, dx, 0)
                for d in range(1, C):
                    self.by_c[dh, dl, dy, d, dx] = put(s, s, c=d)

            def along_h(self):
                for d, dx in self.by_h:
                    self.by_h[d, dx].wait_recv()
                    self.along_l(d, dx)
                    self.spread(d, 0, dx)

            def along_y(self):
                for dh, dl, dx in self.by_l:
                    self.by_l[dh, dl, dx].wait_recv()
                    self.spread(dh, dl, dx)

            def along_c(self):
                for dh, dl in far:
                    for d in range(1, Y):
                        for dx in range(X):
                            self.by_y[dh, dl, d, dx].wait_recv()
                            self.to_core(dh, dl, d, dx)

            def end(self):
                for copy in self.by_c.values():
                    copy.wait_recv()

        class Units:
            def __init__(self, at_m, buf):
                self.m, self.buf = at_m, buf

            def slot(self, dh, dl, dy):
                return self.buf.at[at("zh", dh), at("zl", dl), at("y", dy)]

            def begin(self):
                mine = half.at[self.m, zh]
                s = self.slot(0, 0, 0)
                self.own = move(mine, s)
                self.by_h = {
                    1: Far(half.at[self.m, at("zh", 1)], s, relay.at[self.m], self.slot(0, 1, 0))
                }

            def own_l(self):
                self.by_l = {
                    (0, d): put(half.at[self.m, zh], self.slot(0, 0, 0), zl=d)
                    for d in range(1, ZL)
                }

            def own_y(self):
                self.by_y = {
                    (0, 0, d): put(half.at[self.m, zh], self.slot(0, 0, 0), y=d)
                    for d in range(1, Y)
                }

            def middle(self):
                for dh in self.by_h:
                    self.by_h[dh].wait_recv()
                    s = self.slot(-dh, 0, 0)
                    for d in range(1, ZL):
                        self.by_l[dh, d] = put(s, s, zl=d)
                    for d in range(1, Y):
                        self.by_y[dh, 0, d] = put(s, s, y=d)

            def last(self, dh, spread=True):
                for dl in range(1, ZL):
                    self.by_l[dh, dl].wait_recv()
                    s = self.slot(-dh, -dl, 0)
                    for d in range(1, Y) if spread else ():
                        self.by_y[dh, dl, d] = put(s, s, y=d)

            def end(self):
                self.own.wait()
                for copy in self.by_y.values():
                    copy.wait_recv()

        class Rows:
            def __init__(self, buf):
                self.buf = buf

            def begin(self, src):
                self.own = move(src, self.buf.at[0, 0, 0])
                self.by_h = {d: put(src, self.buf.at[0, -d % ZH, 0], zh=d) for d in range(1, ZH)}
                self.by_x = {(0, d): put(src, self.buf.at[0, 0, -d % X], x=d) for d in range(1, X)}
                self.by_c = [put(src, self.buf.at[-d % C, 0, 0], c=d) for d in range(1, C)]

            def spread(self, a, b):
                for d in range(1, C):
                    self.by_c.append(put(self.buf.at[0, a, b], self.buf.at[-d % C, a, b], c=d))

            def along_x(self):
                for dh in self.by_h:
                    self.by_h[dh].wait_recv()
                    a = -dh % ZH
                    for d in range(1, X):
                        self.by_x[dh, d] = put(self.buf.at[0, a, 0], self.buf.at[0, a, -d % X], x=d)
                    self.spread(a, 0)

            def to_core(self):
                for dh, d in self.by_x:
                    self.by_x[dh, d].wait_recv()
                    self.spread(-dh % ZH, -d % X)

            def end(self):
                self.own.wait()
                for copy in self.by_c:
                    copy.wait_recv()

        raws = [move(qkv_ref, wq_raw), move(g_ref, raw.at[0]), move(u_ref, raw.at[1])]
        raws.append(move(d_ref, raw.at[2]))

        def out_piece(to):
            return out_ref.at[:, pl.ds(pl.multiple_of(to * q_cols, 128), q_cols)]

        wq_g = Gather(w1, part, lambda to: wq_cut.at[to])
        wo_g = Gather(wo, part, out_piece)
        sm_g = Gather(sm, 8, lambda to: small_ref)
        raws[0].wait()
        cut = qkv_columns(wq_raw)
        for k in range(X):
            wq_cut[k] = cut[k]
        wq_g.begin()
        sm_g.begin()
        xr_own = move(own_ref, xr.at[0, 0])
        xr_x = {d: put(own_ref, xr.at[0, -d % X], x=d) for d in range(1, X)}
        wo_g.begin()
        wu, wgt, wdn = Units(1, wu_o), Units(0, wg_o), Units(2, wd_o)
        for m, unit in ((0, wgt), (1, wu), (2, wdn)):
            raws[m + 1].wait()
            @pl.loop(0, depth // 32)
            def _(i, m=m):
                r = pl.ds(pl.multiple_of(i * 32, 32), 32)
                for h in range(ZH):
                    half[m, h, r] = raw[m, r, h * units : (h + 1) * units]

            if m < 2:
                unit.own_y()
        sm_g.along_z()
        wq_g.along_z()

        lens = [len_ref[0, j] for j in range(docs)]
        ends = []
        for j in range(docs):
            ends.append(lens[j] if j == 0 else ends[-1] + lens[j])

        def slot_base(dc, dx):
            return (at("x", dx) * C + at("c", dc)) * rows

        def doc_of(index):
            doc = jnp.zeros(index.shape, jnp.int32)
            first = jnp.zeros(index.shape, jnp.int32)
            for j in range(docs):
                past = (index >= ends[j]).astype(jnp.int32)
                doc = doc + past
                first = first + past * lens[j]
            return doc, index - first

        lane = lax.broadcasted_iota(jnp.int32, (rows, HEAD_WIDTH), 1)
        folded = jnp.where(lane >= HEAD_WIDTH // 2, lane - HEAD_WIDTH // 2, lane)
        freq = jnp.exp(folded.astype(F32) * (-2.0 * math.log(ROPE_BASE) / HEAD_WIDTH))
        sign = jnp.where(lane >= HEAD_WIDTH // 2, 1.0, -1.0)
        slots = [(dc, dx) for dc in range(C) for dx in range(X)]
        def slot_of(k):
            there = lax.rem(x + lax.rem(k, X), X) * C + lax.rem(c + lax.div(k, X), C)
            return there * rows

        @pl.loop(0, C * X)
        def _(k):
            r = pl.ds(pl.multiple_of(k * rows, rows), rows)
            index = slot_of(k) + lax.broadcasted_iota(jnp.int32, (rows, HEAD_WIDTH), 0)
            angle = doc_of(index)[1].astype(F32) * freq
            cos_s[r] = jnp.cos(angle)
            sin_s[r] = jnp.sin(angle) * sign
            k_index = slot_of(k) + lax.broadcasted_iota(jnp.int32, (rows, rows), 1)
            k_doc = doc_of(k_index)[0]
            for a in range(X):
                q_index = slot_base(0, a) + lax.broadcasted_iota(jnp.int32, (rows, rows), 0)
                q_doc = doc_of(q_index)[0]
                allowed = (q_doc == k_doc) & (k_index <= q_index)
                mask_s[a * rows : (a + 1) * rows, r] = jnp.where(allowed, 0.0, NEGATIVE_BIG)

        xr_own.wait()
        for d in xr_x:
            xr_x[d].wait_recv()
        xr_c = [
            put(xr.at[0, k], xr.at[-d % C, k], c=d) for d in range(1, C) for k in range(X)
        ]
        sm_g.along_h()
        wq_g.along_h()
        wo_g.along_z()
        wgt.begin()
        wgt.own_l()
        sm_g.along_y()
        wq_g.along_y()
        sm_g.along_c()
        wo_g.along_h()
        wdn.own_y()
        wgt.by_h[1].forward()
        wu.begin()
        wu.own_l()
        wq_g.along_c()
        sm_g.end()

        def spread_row(first, block, total):
            pieces = sm[...].reshape(devices, 8, 256)[:, 0, :].astype(BF)
            left = lax.broadcasted_iota(jnp.int32, (256, total), 0)
            right = lax.broadcasted_iota(jnp.int32, (256, total), 1)
            select = (lax.rem(right, block) + first == left).astype(BF)
            wide = nn(pieces, select)
            owner = lax.broadcasted_iota(jnp.int32, (devices, total), 0)
            place = lax.broadcasted_iota(jnp.int32, (devices, total), 1)
            inside = (place >= owner * block) & (place < (owner + 1) * block)
            return jnp.sum(jnp.where(inside, wide, 0.0), axis=0, keepdims=True)

        rows_s[0:1, :width] = spread_row(0, part, width)
        rows_s[1:2, :width] = spread_row(part, part, width)
        rows_s[2:3, :] = spread_row(2 * part, bias_part, QKV_WIDTH)

        for copy in xr_c:
            copy.wait_recv()
        gain_one = rows_s[0:1, :width]
        for k, (dc, dx) in enumerate(slots):
            @pl.loop(0, rows // 32)
            def _(i, k=k, dc=dc, dx=dx):
                v = xr[dc, dx, pl.ds(pl.multiple_of(i * 32, 32), 32)].astype(F32)
                r = lax.rsqrt(jnp.mean(v * v, axis=-1, keepdims=True) + EPSILON)
                to = pl.ds(pl.multiple_of(k * rows + i * 32, 32), 32)
                n1[to] = (v * r * gain_one).astype(BF)

        eye = (
            lax.broadcasted_iota(jnp.int32, (128, 128), 0)
            == lax.broadcasted_iota(jnp.int32, (128, 128), 1)
        ).astype(BF)

        def flip(read, dst, amount):
            @pl.loop(0, width // 128)
            def _(j):
                cols = pl.ds(pl.multiple_of(j * 128, 128), 128)
                dst[cols] = nt(eye, read(cols)).astype(BF)

        wq_g.end()
        outs = [move(w1, wqkv_o), move(rows_s, vec_o), move(cos_s, cos_o), move(sin_s, sin_o)]
        kv_at = lax.div(x * heads, QUERY_HEADS // KEY_VALUE_HEADS) * HEAD_WIDTH
        k_off = QUERY_HEADS * HEAD_WIDTH + kv_at
        v_off = k_off + KEY_VALUE_HEADS * HEAD_WIDTH
        def turn(v, first, amount):
            return v * cos_s[first : first + amount] + pltpu.roll(
                v, HEAD_WIDTH // 2, 1
            ) * sin_s[first : first + amount]

        def bias_at(start, amount):
            return rows_s[2:3, pl.ds(pl.multiple_of(start, 128), amount)]

        @pl.loop(0, heads)
        def _(h):
            cols = pl.ds(pl.multiple_of(h * HEAD_WIDTH, HEAD_WIDTH), HEAD_WIDTH)
            v = nn(n1[0:query_rows], w1[:, cols])
            v = v + bias_at(x * q_cols + h * HEAD_WIDTH, HEAD_WIDTH)
            qs[:, cols] = turn(v, 0, query_rows).astype(BF)

        for j in range(kv_heads):
            at_k = q_cols + j * HEAD_WIDTH
            v = nn(n1[...], w1[:, at_k : at_k + HEAD_WIDTH]) + bias_at(k_off, kv_cols)[
                :, j * HEAD_WIDTH : (j + 1) * HEAD_WIDTH
            ]
            kv[:, j * HEAD_WIDTH : (j + 1) * HEAD_WIDTH] = turn(v, 0, pack_rows).astype(BF)
        v = nn(n1[...], w1[:, q_cols + kv_cols :]) + bias_at(v_off, kv_cols)
        kv[:, kv_cols:] = v.astype(BF)
        outs += [move(qs, q_o), move(kv, kv_o)]
        wo_g.along_y()
        wu.by_h[1].forward()
        wgt.last(0)
        wgt.middle()
        wdn.begin()
        wdn.own_l()

        @pl.loop(0, heads)
        def _(h):
            cols = pl.ds(pl.multiple_of(h * HEAD_WIDTH, HEAD_WIDTH), HEAD_WIDTH)
            g = lax.div(h, share)
            k_h = kv[:, pl.ds(pl.multiple_of(g * HEAD_WIDTH, HEAD_WIDTH), HEAD_WIDTH)]
            v_h = kv[:, pl.ds(pl.multiple_of(kv_cols + g * HEAD_WIDTH, HEAD_WIDTH), HEAD_WIDTH)]
            s = nt(qs[:, cols], k_h) * scale + mask_s[...]
            e = jnp.exp(s - jnp.max(s, axis=-1, keepdims=True))
            p = (e / jnp.sum(e, axis=-1, keepdims=True)).astype(BF)
            ps[h] = p
            ob[:, cols] = nn(p, v_h).astype(BF)

        outs += [move(ps, p_o), move(ob, att_o)]
        wo_g.along_c()
        wo_g.end()
        outs.append(move(wo, wout_o))
        block = 256
        for d in list(range(1, X)) + [0]:
            @pl.loop(0, width // block)
            def _(j, d=d):
                cols = pl.ds(pl.multiple_of(j * block, block), block)
                v = nt(ob[d * rows : (d + 1) * rows], wo[cols])
                if d:
                    part_send[d - 1, :, cols] = v.astype(BF)
                else:
                    hs[:, cols] = v

            if d:
                part_recv_copy = put(part_send.at[d - 1], part_recv.at[d - 1], x=d)
                parts = [part_recv_copy] if d == 1 else parts + [part_recv_copy]
        wu.last(0)
        go_rows = Rows(go_v)
        go_rows.begin(cot_ref)
        for d in range(1, X):
            parts[d - 1].wait_recv()
        gain_two = rows_s[1:2, :width]

        @pl.loop(0, rows // 32)
        def _(i):
            r = pl.ds(pl.multiple_of(i * 32, 32), 32)
            h = hs[r] + xr[0, 0, r].astype(F32)
            for d in range(1, X):
                h = h + part_recv[d - 1, r].astype(F32)
            hs[r] = h
            inv = lax.rsqrt(jnp.mean(h * h, axis=-1, keepdims=True) + EPSILON)
            n2s[r] = (h * inv * gain_two).astype(BF)

        nr_rows = Rows(nr_v)
        nr_rows.begin(n2s)
        outs.append(move(hs, h_o))
        flip(lambda cols: n1[0:query_rows, cols], n1t, query_rows)
        outs.append(move(n1t, n1_o))
        wdn.by_h[1].forward()
        wgt.last(1)
        wu.middle()
        wu.last(1)
        nr_rows.along_x()
        go_rows.along_x()
        wdn.last(0, False)
        wdn.middle()
        nr_rows.to_core()
        nr_rows.end()
        outs.append(move(nr_v, nr_o))
        group_rows = C * ZH * X * rows
        flip(lambda cols: nr_v[:, :, :, :, cols].reshape(group_rows, 128), n2t, group_rows)
        outs.append(move(n2t, n2t_o))
        go_rows.to_core()
        wdn.last(1, False)
        go_rows.end()
        outs.append(move(go_v, go_o))
        wgt.end()
        wu.end()
        wdn.end()
        for copy in outs:
            copy.wait()
        for copy in sent:
            copy.wait_send()
        assert count[0] <= n_sems, count

    any_spec = pl.BlockSpec(memory_space=pl.ANY)
    whole = (ZH, ZL, Y, depth, units)
    group = (C, ZH, X, rows, width)
    sds = jax.ShapeDtypeStruct
    return pl.pallas_call(
        kernel,
        out_shape=[
            sds((width, qkv_n), BF), sds((width, q_cols), BF), sds((width, query_rows), BF),
            sds((width, C * ZH * X * rows), BF),
            sds((query_rows, q_cols), BF), sds((pack_rows, 2 * kv_cols), BF),
            sds((heads, query_rows, pack_rows), BF), sds((query_rows, q_cols), BF),
            sds((rows, width), F32), sds(group, BF), sds(group, BF),
            sds(whole, BF), sds(whole, BF), sds(whole, BF),
            sds((8, QKV_WIDTH), F32),
            sds((pack_rows, HEAD_WIDTH), F32), sds((pack_rows, HEAD_WIDTH), F32),
            sds((3, depth, units), BF),
        ],
        in_specs=[any_spec, any_spec, pl.BlockSpec(memory_space=pltpu.SMEM)] + [any_spec] * 6,
        out_specs=[any_spec] * 18,
        scratch_shapes=[
            pltpu.VMEM((C, X, rows, width), BF),
            pltpu.VMEM((width, qkv_n), BF),
            pltpu.VMEM((width, q_cols), BF),
            pltpu.VMEM((devices * 8, 256), F32),
            pltpu.VMEM((pack_rows, width), BF),
            pltpu.VMEM((query_rows, q_cols), BF),
            pltpu.VMEM((pack_rows, 2 * kv_cols), BF),
            pltpu.VMEM((query_rows, q_cols), BF),
            pltpu.VMEM((max(X - 1, 1), rows, width), BF),
            pltpu.VMEM((max(X - 1, 1), rows, width), BF),
            pltpu.VMEM((rows, width), BF),
            pltpu.VMEM((rows, width), F32),
            pltpu.VMEM((pack_rows, HEAD_WIDTH), F32),
            pltpu.VMEM((pack_rows, HEAD_WIDTH), F32),
            pltpu.VMEM((query_rows, pack_rows), F32),
            pltpu.VMEM((8, QKV_WIDTH), F32),
            pltpu.VMEM((heads, query_rows, pack_rows), BF),
            pltpu.VMEM((3,) + w_gate.shape, BF),
            pltpu.VMEM((3, ZH, depth, units), BF),
            pltpu.VMEM(w_qkv.shape, BF),
            pltpu.VMEM((X, part, qkv_n), BF),
            pltpu.VMEM((width, query_rows), BF),
            pltpu.VMEM((width, C * ZH * X * rows), BF),
            pltpu.VMEM(group, BF),
            pltpu.VMEM(group, BF),
            pltpu.SemaphoreType.DMA((n_sems,)),
            pltpu.SemaphoreType.DMA((n_sems,)),
            pltpu.SemaphoreType.DMA((32,)),
        ],
        compiler_params=pltpu.CompilerParams(
            collective_id=0, has_side_effects=True, vmem_limit_bytes=60 << 20
        ),
        name="front",
    )(own_in, cotangent, lengths, w_qkv, w_out, small, w_gate, w_up, w_down)


def forward_backward(normed, cotangent, w_gate, w_up, w_down):
    size = lax.axis_size
    ZH, ZL, Y, X, C = (size(a) for a in AXES)
    total, width = normed.shape
    depth, units = w_down.shape[-2:]
    step = 256

    def kernel(
        n_ref, g_ref, wg_ref, wu_ref, wd_ref,
        dg_o, du_o, dw_o, near_o, nt_o, ot_o,
        n_s, g_s, turned, wg, wu, wd, gates, ups, hidden, dg, du, dw, nt_s, ot_s,
        send_sem, recv_sem, local_sem, out_sem,
    ):
        here = dict(zip(AXES, (lax.axis_index(a) for a in AXES)))
        sizes = dict(zip(AXES, (ZH, ZL, Y, X, C)))

        def at(a, d):
            d = d % sizes[a]
            return lax.rem(here[a] + d, sizes[a]) if d else here[a]

        other = tuple(at(a, 1) if a == "y" else here[a] for a in AXES)
        barrier = pltpu.get_barrier_semaphore()
        pl.semaphore_signal(barrier, inc=1, device_id=other, device_id_type=MESH_ID)
        pl.semaphore_wait(barrier, 1)
        sent = []

        def put(src, dst):
            k = len(sent)
            copy = pltpu.make_async_remote_copy(
                src_ref=src, dst_ref=dst, send_sem=send_sem.at[k], recv_sem=recv_sem.at[k],
                device_id=other, device_id_type=MESH_ID,
            )
            copy.start()
            sent.append(copy)
            return copy

        count = [0]

        def move(src, dst):
            k = count[0]
            count[0] += 1
            copy = pltpu.make_async_copy(src, dst, local_sem.at[k])
            copy.start()
            return copy

        def row(a, b, e):
            start = pl.multiple_of(((a * ZL + b) * Y + e) * depth, depth)
            return pl.ds(start, depth)

        def at_rows(t):
            return pl.ds(pl.multiple_of(t * step, step), step)

        zh, zl, y = here["zh"], here["zl"], here["y"]
        loads = [move(n_ref, n_s), move(wg_ref, wg), move(wu_ref, wu), move(g_ref, g_s)]
        down = []
        for d in range(ZH):
            a = at("zh", d)
            for e in range(1, ZL):
                b = at("zl", e)
                down.append(put(wd_ref.at[a, b, y], wd.at[row(a, b, y)]))
                loads.append(move(wd_ref.at[a, b, y], wd.at[row(a, b, y)]))
            for e in range(Y):
                loads.append(move(wd_ref.at[a, zl, e], wd.at[row(a, zl, e)]))
        for copy in loads[:3]:
            copy.wait()

        @pl.loop(0, total // step)
        def _(t):
            r = at_rows(t)
            gate = nn(n_s[r], wg[...])
            up = nn(n_s[r], wu[...])
            gates[r] = gate
            ups[r] = up
            hidden[r] = (gate * jax.nn.sigmoid(gate) * up).astype(BF)

        loads[3].wait()
        eye = (
            lax.broadcasted_iota(jnp.int32, (128, 128), 0)
            == lax.broadcasted_iota(jnp.int32, (128, 128), 1)
        ).astype(BF)

        @pl.loop(0, width // 128)
        def _(j):
            cols = pl.ds(pl.multiple_of(j * 128, 128), 128)
            turned[cols] = nt(eye, g_s[:, cols]).astype(BF)

        def blocks(first, last):
            @pl.loop(first, last)
            def _(k):
                a = lax.rem(zh + lax.rem(k + 2, 4) // ZL, ZH)
                b = lax.rem(zl + lax.rem(k, ZL), ZL)
                e = lax.rem(y + 1 + k // 4, Y)
                at_block = row(a, b, e)
                dw[at_block] = nn(turned[at_block], hidden[...]).astype(BF)

        blocks(0, 2)
        for k in range(ZL):
            put(dw.at[row(at("zh", 1), at("zl", k), at("y", 1))], near_o.at[k])
        blocks(2, 8)
        outs = [move(dw, dw_o)]
        for copy in loads[4:]:
            copy.wait()
        for copy in down:
            copy.wait_recv()

        def stream(k, src, dst, r):
            pltpu.make_async_copy(src.at[r], dst.at[r], out_sem.at[k]).start()

        results = ((dg, dg_o), (du, du_o), (nt_s, nt_o), (ot_s, ot_o))

        @pl.loop(0, total // step)
        def _(t):
            r = at_rows(t)
            grad = nn(g_s[r], wd[...])
            ot_s[r] = nt(hidden[r], wd[...]).astype(BF)
            gate, up = gates[r], ups[r]
            sig = jax.nn.sigmoid(gate)
            low_g = (grad * up * sig * (1.0 + gate * (1.0 - sig))).astype(BF)
            low_u = (grad * gate * sig).astype(BF)
            dg[r] = low_g
            du[r] = low_u
            nt_s[r] = (nt(low_g, wg[...]) + nt(low_u, wu[...])).astype(BF)
            for k, (src, dst) in enumerate(results):
                stream(k, src, dst, r)

        for k, (src, dst) in enumerate(results):
            pltpu.make_async_copy(src, dst, out_sem.at[k]).wait()
        for copy in outs:
            copy.wait()
        for copy in sent[len(down) :]:
            copy.wait_recv()
        for copy in sent:
            copy.wait_send()

    any_spec = pl.BlockSpec(memory_space=pl.ANY)
    sds, vm = jax.ShapeDtypeStruct, pltpu.VMEM
    return pl.pallas_call(
        kernel,
        out_shape=[
            sds((total, units), BF), sds((total, units), BF), sds((width, units), BF),
            sds((ZL, depth, units), BF), sds((total, width), BF), sds((total, width), BF),
        ],
        in_specs=[any_spec] * 5,
        out_specs=[any_spec] * 6,
        scratch_shapes=[
            vm((total, width), BF), vm((total, width), BF), vm((width, total), BF),
            vm((width, units), BF), vm((width, units), BF), vm((width, units), BF),
            vm((total, units), F32), vm((total, units), F32), vm((total, units), BF),
            vm((total, units), BF), vm((total, units), BF), vm((width, units), BF),
            vm((total, width), BF), vm((total, width), BF),
            pltpu.SemaphoreType.DMA((8,)), pltpu.SemaphoreType.DMA((8,)),
            pltpu.SemaphoreType.DMA((16,)), pltpu.SemaphoreType.DMA((4,)),
        ],
        compiler_params=pltpu.CompilerParams(
            collective_id=2, has_side_effects=True, vmem_limit_bytes=62 << 20
        ),
        name="forward_backward",
    )(normed, cotangent, w_gate, w_up, w_down)


def back(
    grad_d, near_d, grad_g, grad_u, group_t, normed_terms, out_terms, middle, cotangent, own_in,
    wqkv, wout, normed, queries, kv_rows, probs, attended, vectors, cosine, sine,
):
    size = lax.axis_size
    ZH, ZL, Y, X, C = (size(a) for a in AXES)
    rows, width = own_in.shape
    qkv_n, q_cols = wqkv.shape[1], wout.shape[1]
    heads = q_cols // HEAD_WIDTH
    kv_cols = (qkv_n - q_cols) // 2
    kv_heads = kv_cols // HEAD_WIDTH
    share = heads // kv_heads
    query_rows, pack_rows = X * rows, C * X * rows
    depth, units = grad_d.shape[-2:]
    group_rows = group_t.shape[1]
    near = [(dh, dx) for dh in range(ZH) for dx in range(X)]
    far = [(dh, dl) for dh in range(ZH) for dl in range(ZL)]
    devices = ZH * ZL * Y * X * C
    part = width // devices
    zs = ZH * ZL
    scale = HEAD_WIDTH ** (-0.5)
    n_sems = 200

    blocks = {}
    for dx in range(X):
        for h in range(heads):
            blocks.setdefault(dx * heads + h, []).append((dx, h * HEAD_WIDTH))
        for j in range(kv_heads):
            head = dx * heads // (QUERY_HEADS // KEY_VALUE_HEADS) + j
            for at_kv, start in ((0, q_cols), (KEY_VALUE_HEADS, q_cols + kv_cols)):
                blocks.setdefault(QUERY_HEADS + at_kv + head, []).append(
                    (dx, start + j * HEAD_WIDTH)
                )
    qkv_layout = [(k * HEAD_WIDTH, b) for k, b in sorted(blocks.items())]
    out_layout = [(k * HEAD_WIDTH, b) for k, b in sorted(blocks.items()) if k < QUERY_HEADS]
    def kernel(
        gd_ref, dd_ref, gg_ref, gu_ref, gt_ref, nt_ref, ot_ref, mid_ref, cot_ref, in_ref,
        w1_ref, wo_ref, n1_ref, q_ref, kv_ref, p_ref, att_ref, vec_ref, cos_ref, sin_ref,
        lo_o, gi_o, dqkv_o, dout_o, vec_out, od_o, og_o, ou_o, relay,
        own_g, from_y, from_l, from_h, out_w, turned, units_t,
        half_n, half_o, from_c, from_n, hs, cots, ins, w1, wo, n1t, qs, kv, ps,
        atts, vec, cos_s, sin_s, da, dat, dos, dpre, dkv, dkv_low, dkv_in, dh_s,
        d_qkv, c_qkv, y_qkv, z_qkv, t_qkv, b_qkv, x_qkv,
        d_out, c_out, y_out, z_out, t_out, b_out, x_out, w_qkv_s, w_out_s,
        n_send, n_recv, lo_s, gi_s, vs, v_in, v_send,
        send_sem, recv_sem, local_sem,
    ):
        zh, zl, y, x, c = (lax.axis_index(a) for a in AXES)
        sizes = dict(zip(AXES, (ZH, ZL, Y, X, C)))
        here = dict(zip(AXES, (zh, zl, y, x, c)))

        def at(a, d):
            d = d % sizes[a]
            return lax.rem(here[a] + d, sizes[a]) if d else here[a]

        def device(**off):
            return tuple(at(a, off.get(a, 0)) for a in AXES)

        peers = set()
        for d in range(1, C):
            peers.add((0, 0, 0, 0, d))
        for dh, dx in near[1:]:
            peers.add((dh, 0, 0, dx, 0))
        for dh, dl in far[1:]:
            peers.add((dh, dl, 0, 0, 0))
        for d in range(1, Y):
            peers.add((0, 0, d, 0, 0))
        peers = sorted(peers)
        barrier = pltpu.get_barrier_semaphore()
        for peer in peers:
            pl.semaphore_signal(
                barrier, inc=1, device_id=device(**dict(zip(AXES, peer))), device_id_type=MESH_ID
            )
        pl.semaphore_wait(barrier, len(peers))

        count = [0, 0]
        sent = []

        def put(src, dst, **off):
            k = count[0]
            count[0] += 1
            copy = pltpu.make_async_remote_copy(
                src_ref=src, dst_ref=dst, send_sem=send_sem.at[k], recv_sem=recv_sem.at[k],
                device_id=device(**off), device_id_type=MESH_ID,
            )
            copy.start()
            sent.append(copy)
            return copy

        def move(src, dst):
            k = count[1]
            count[1] += 1
            copy = pltpu.make_async_copy(src, dst, local_sem.at[k])
            copy.start()
            return copy

        def by_rows(total, step, body):
            @pl.loop(0, total // step)
            def _(i):
                body(pl.ds(pl.multiple_of(i * step, step), step))

        inner = zh + zl == 1

        class Far:
            def __init__(self, src, dst, relay, onward):
                k = count[0]
                count[0] += 3
                self.relay, self.k = relay, k
                self.main = self.copy(src, dst, k, k, device(zh=1))
                self.step = self.copy(src, relay, k, k + 1, device(zl=1))
                self.onward = self.copy(relay, onward, k + 2, k, device(zh=1, zl=1))
                pl.when(inner)(self.main.start)
                pl.when(jnp.logical_not(inner))(self.step.start)
                sent.append(self)

            def copy(self, src, dst, k, r, to):
                return pltpu.make_async_remote_copy(
                    src_ref=src, dst_ref=dst, send_sem=send_sem.at[k], recv_sem=recv_sem.at[r],
                    device_id=to, device_id_type=MESH_ID,
                )

            def forward(self):
                @pl.when(inner)
                def _():
                    self.step.wait_recv()
                    self.onward.start()

            def wait_recv(self):
                self.main.wait_recv()

            def wait_send(self):
                self.main.wait_send()
                pl.when(inner)(self.onward.wait_send)

        class Units:
            def __init__(self, m, src):
                self.m, self.src = m, src
                self.by_y, self.own, self.by_l, self.by_h = {}, {}, {}, {}

            def begin(self, blocks, arrived=()):
                for dh, dl in blocks:
                    k = dh * ZL + dl
                    a, b = at("zh", dh), at("zl", dl)
                    if (dh, dl) in arrived:
                        self.by_y[dh, dl] = [move(dd_ref.at[arrived.index((dh, dl))], from_y.at[self.m, k, 0])]
                    else:
                        self.by_y[dh, dl] = [
                            put(self.src.at[a, b, at("y", d)], from_y.at[self.m, k, d - 1], y=d)
                            for d in range(1, Y)
                        ]
                    self.own[dh, dl] = move(self.src.at[a, b, y], own_g.at[self.m, k])

            def add_y(self, blocks):
                m = self.m
                for dh, dl in blocks:
                    k = dh * ZL + dl
                    self.own[dh, dl].wait()
                    for copy in self.by_y[dh, dl]:
                        if any(copy is other for other in sent):
                            copy.wait_recv()
                        else:
                            copy.wait()

                    def body(r, k=k):
                        v = own_g[m, k, r].astype(F32)
                        for d in range(1, Y):
                            v = v + from_y[m, k, d - 1, r].astype(F32)
                        own_g[m, k, r] = v.astype(BF)

                    by_rows(depth, 64, body)
                    if dl:
                        self.by_l[dh, dl] = put(
                            own_g.at[m, k], from_l.at[m, dh, dl - 1], zl=dl
                        )

            def add_l(self, far):
                m = self.m
                for dh in range(ZH - 1, 0, -1) if far else (0,):
                    for d in range(1, ZL):
                        self.by_l[dh, d].wait_recv()
                    if dh:
                        def body(r, dh=dh):
                            v = own_g[m, dh * ZL, r].astype(F32)
                            for d in range(1, ZL):
                                v = v + from_l[m, dh, d - 1, r].astype(F32)
                            own_g[m, dh * ZL, r] = v.astype(BF)

                        by_rows(depth, 64, body)
                        to = from_h.at[m, dh - 1]
                        self.by_h[dh] = Far(own_g.at[m, dh * ZL], to, relay.at[m], to)

            def half(self, h, r, cols=slice(None)):
                m = self.m
                v = own_g[m, 0, r, cols].astype(F32)
                for d in range(1, ZL):
                    v = v + from_l[m, 0, d - 1, r, cols].astype(F32)
                for d in range(1, ZH):
                    other = from_h[m, d - 1, r, cols].astype(F32)
                    v = jnp.where(lax.rem(zh + ZH - d, ZH) == h, other, v)
                return v

            def wait_h(self):
                for copy in self.by_h.values():
                    copy.wait_recv()

        def block(m, k, place_y):
            a = lax.rem(zh + k // ZL, ZH)
            b = lax.rem(zl + k % ZL, ZL)
            start = pl.multiple_of(((a * ZL + b) * Y + place_y) * depth, depth)
            return nn(turned[pl.ds(start, depth)], units_t[m])

        def compute_other(first, last):
            @pl.loop(2 * first, 2 * last)
            def _(i):
                m, k = lax.rem(i, 2), zs - 1 - lax.div(i, 2)
                a = lax.rem(zh + lax.div(k, ZL), ZH)
                b = lax.rem(zl + lax.rem(k, ZL), ZL)
                start = pl.multiple_of(((a * ZL + b) * Y + at("y", 1)) * depth, depth)
                own_g[m + 1, k] = nn(turned[pl.ds(start, depth)], units_t[m]).astype(BF)

        def send_pair(k):
            for u in (ug, uu):
                u.by_y[k] = put(own_g.at[u.m, k], from_y.at[u.m, k, 0], y=1)

        def add_pair(k):
            for u in (ug, uu):
                u.by_y[k].wait()
                sent[:] = [other for other in sent if other is not u.by_y[k]]

            @pl.loop(0, 2)
            def _(m):
                v = block(m, k, y) + from_y[m + 1, k, 0].astype(F32)
                own_g[m + 1, k] = v.astype(BF)

            if k % ZL:
                for u in (ug, uu):
                    u.by_l[k // ZL, k % ZL] = put(
                        own_g.at[u.m, k], from_l.at[u.m, k // ZL, k % ZL - 1], zl=k % ZL
                    )

        class Scatter:
            def __init__(self, dd, in_c, in_y, in_z, tt, tb, in_x, whole, out, layout):
                self.r = (dd, in_c, in_y, in_z, tt, tb, in_x)
                self.whole, self.out, self.layout = whole, out, layout

            def fill(self, left, right):
                dd = self.r[0]
                span = X * C * part

                @pl.loop(0, zs)
                def _(z):
                    for b in range(Y):
                        start = pl.multiple_of((z * Y + b) * span, span)
                        v = nn(left[pl.ds(start, span)], right[...]).astype(BF)
                        for dx in range(X):
                            for dc in range(C):
                                first = (dx * C + dc) * part
                                dd[dc, b, z, dx * part : (dx + 1) * part] = v[
                                    first : first + part
                                ]

            def to_c(self):
                dd, in_c = self.r[:2]
                self.by_c = {
                    (f, d): put(dd.at[at("c", d), at("y", f)], in_c.at[f, d - 1], c=d)
                    for f in list(range(1, Y)) + [0]
                    for d in range(1, C)
                }

            def to_y(self):
                dd, in_c, in_y = self.r[:3]
                self.by_y = []
                for f in list(range(1, Y)) + [0]:
                    for d in range(1, C):
                        self.by_c[f, d].wait_recv()
                    b = at("y", f)

                    @pl.loop(0, zs)
                    def _(z):
                        v = dd[c, b, z].astype(F32)
                        for d in range(1, C):
                            v = v + in_c[f, d - 1, z].astype(F32)
                        dd[c, b, z] = v.astype(BF)

                    if f:
                        self.by_y.append(put(dd.at[c, b], in_y.at[f - 1], y=f))

            def to_z(self):
                dd, in_c, in_y, in_z = self.r[:4]
                for copy in self.by_y:
                    copy.wait_recv()

                @pl.loop(0, zs)
                def _(z):
                    v = dd[c, y, z].astype(F32)
                    for f in range(1, Y):
                        v = v + in_y[f - 1, z].astype(F32)
                    dd[c, y, z] = v.astype(BF)

                self.by_l = {
                    (dh, d): put(
                        dd.at[c, y, at("zh", dh) * ZL + at("zl", d)],
                        in_z.at[dh * (ZL - 1) + d - 1],
                        zl=d,
                    )
                    for dh in range(ZH - 1, -1, -1)
                    for d in range(1, ZL)
                }

            def summed_l(self, dh):
                dd, in_z = self.r[0], self.r[3]
                v = dd[c, y, at("zh", dh) * ZL + zl].astype(F32)
                for d in range(1, ZL):
                    v = v + in_z[dh * (ZL - 1) + d - 1].astype(F32)
                return v

            def to_h(self):
                dd, in_z = self.r[0], self.r[3]
                for copy in self.by_l.values():
                    copy.wait_recv()
                self.by_h = []
                for dh in range(1, ZH):
                    place = at("zh", dh) * ZL + zl
                    dd[c, y, place] = self.summed_l(dh).astype(BF)
                    self.by_h.append(
                        put(dd.at[c, y, place], in_z.at[ZH * (ZL - 1) + dh - 1], zh=dh)
                    )

            def to_x(self):
                dd, in_c, in_y, in_z, tt, tb, in_x = self.r
                for copy in self.by_h:
                    copy.wait_recv()
                v = self.summed_l(0)
                for dh in range(1, ZH):
                    v = v + in_z[ZH * (ZL - 1) + dh - 1].astype(F32)
                for dx in range(X):
                    tt[dx] = v[dx * part : (dx + 1) * part]
                    tb[dx] = v[dx * part : (dx + 1) * part].astype(BF)
                self.by_x = [put(tb.at[at("x", d)], in_x.at[d - 1], x=d) for d in range(1, X)]

            def end(self):
                tt, in_x = self.r[4], self.r[6]
                for d in range(1, X):
                    self.by_x[d - 1].wait_recv()
                for d in range(1, X):
                    tt[at("x", -d)] = in_x[d - 1].astype(F32)
                for first, blocks in self.layout:
                    v = 0.0
                    for dx, start in blocks:
                        v = v + tt[dx, :, start : start + HEAD_WIDTH]
                    self.whole[:, first : first + HEAD_WIDTH] = v
                return move(self.whole, self.out)

        class Rows:
            def __init__(self, m, src, mine):
                self.m, self.mine = m, mine
                order = list(range(1, len(near))) + [0]
                self.by_c = {
                    (k, d): put(src.at[d, k], from_c.at[m, k, d - 1], c=d)
                    for k in order
                    for d in range(1, C)
                }
                self.own = move(src.at[0], mine)

            def summed(self, k, r):
                v = self.mine[k, r].astype(F32)
                for d in range(1, C):
                    v = v + from_c[self.m, k, d - 1, r].astype(F32)
                return v

            def spread(self):
                self.own.wait()
                self.by_n = []
                for k, (dh, dx) in enumerate(near):
                    for d in range(1, C):
                        if k:
                            self.by_c[k, d].wait_recv()
                    if k:
                        def body(r, k=k):
                            self.mine[k, r] = self.summed(k, r).astype(BF)

                        by_rows(rows, 32, body)
                        self.by_n.append(
                            put(self.mine.at[k], from_n.at[self.m, k - 1], zh=dh, x=dx)
                        )
                for d in range(1, C):
                    self.by_c[0, d].wait_recv()

            def spread_x(self):
                self.own.wait()
                self.by_n = {}
                for dh in reversed(range(ZH)):
                    for dx in range(1, X):
                        k = dh * X + dx
                        for d in range(1, C):
                            self.by_c[k, d].wait_recv()

                        def body(r, k=k):
                            self.mine[k, r] = self.summed(k, r).astype(BF)

                        by_rows(rows, 32, body)
                        to = from_n.at[self.m, dh * (X - 1) + dx - 1]
                        self.by_n[dh, dx] = put(self.mine.at[k], to, x=dx)

            def came_x(self, dh, r):
                v = self.summed(dh * X, r)
                for dx in range(1, X):
                    v = v + from_n[self.m, dh * (X - 1) + dx - 1, r].astype(F32)
                return v

            def relay(self):
                for dh in reversed(range(ZH)):
                    for d in range(1, C):
                        self.by_c[dh * X, d].wait_recv()
                    for dx in range(1, X):
                        self.by_n[dh, dx].wait_recv()
                    if dh:
                        def body(r, dh=dh):
                            self.mine[dh * X, r] = self.came_x(dh, r).astype(BF)

                        by_rows(rows, 32, body)
                        to = from_n.at[self.m, ZH * (X - 1) + dh - 1]
                        self.by_n[dh, 0] = put(self.mine.at[dh * X], to, zh=dh)

            def landed(self):
                for dh in range(1, ZH):
                    self.by_n[dh, 0].wait_recv()

            def final(self, r):
                v = self.came_x(0, r)
                for dh in range(1, ZH):
                    v = v + from_n[self.m, ZH * (X - 1) + dh - 1, r].astype(F32)
                return v

            def arrive(self):
                for copy in self.by_n:
                    copy.wait_recv()

            def total(self, r):
                v = self.summed(0, r)
                for k in range(1, len(near)):
                    v = v + from_n[self.m, k - 1, r].astype(F32)
                return v

        terms = Rows(0, nt_ref, half_n)
        loads = {
            "turned": move(gt_ref, turned),
            "g": move(gg_ref, units_t.at[0]),
            "u": move(gu_ref, units_t.at[1]),
        }
        for name, src, dst in (
            ("mid", mid_ref, hs), ("cot", cot_ref, cots), ("vec", vec_ref, vec),
            ("n1", n1_ref, n1t), ("wo", wo_ref, wo), ("kv", kv_ref, kv), ("p", p_ref, ps),
            ("att", att_ref, atts), ("q", q_ref, qs), ("cos", cos_ref, cos_s),
            ("sin", sin_ref, sin_s), ("w1", w1_ref, w1), ("in", in_ref, ins),
        ):
            loads[name] = move(src, dst)
        ud, ug, uu = Units(0, gd_ref), Units(1, None), Units(2, None)
        arrived = [(dh, dl) for dh, dl in far if dh]
        ud.begin(arrived[::-1] + [(0, 1)], arrived)
        outs_terms = Rows(1, ot_ref, half_o)

        eye = (
            lax.broadcasted_iota(jnp.int32, (128, 128), 0)
            == lax.broadcasted_iota(jnp.int32, (128, 128), 1)
        ).astype(BF)

        terms.spread_x()
        for name in ("turned", "g", "u", "n1"):
            loads[name].wait()
        compute_other(0, 2)
        for k in (3, 2):
            send_pair(k)
        ud.add_y(arrived[::-1])
        compute_other(2, 4)
        send_pair(1)
        ud.add_y([(0, 1)])
        ud.add_l(far=True)
        terms.relay()
        add_pair(3)
        ud.by_h[1].forward()
        for name in ("mid", "cot", "vec"):
            loads[name].wait()
        gain_one, gain_two = vec[0:1, :width], vec[1:2, :width]
        terms.landed()
        vs[...] = jnp.zeros_like(vs)

        @pl.loop(0, rows // 32)
        def _(i):
            r = pl.ds(pl.multiple_of(i * 32, 32), 32)
            grad, h = terms.final(r), hs[r]
            inv = lax.rsqrt(jnp.mean(h * h, axis=-1, keepdims=True) + EPSILON)
            scaled = gain_two * grad
            v = (
                cots[r].astype(F32)
                + inv * scaled
                - h * (inv * inv * inv) * jnp.mean(scaled * h, axis=-1, keepdims=True)
            )
            dh_s[r] = v
            da[0, r] = v.astype(BF)
            vs[1:2, :width] = vs[1:2, :width] + jnp.sum(grad * h * inv, axis=0, keepdims=True)

        da_x = [put(da.at[0], da.at[-d % X], x=d) for d in range(1, X)]
        add_pair(2)
        loads["wo"].wait()
        loads["att"].wait()
        for copy in da_x:
            copy.wait_recv()

        @pl.loop(0, heads // 2)
        def _(j):
            cols = pl.ds(pl.multiple_of(j * 256, 256), 256)
            for k in range(X):
                dos[k * rows : (k + 1) * rows, cols] = nn(da[k], wo[:, cols]).astype(BF)

        for k in range(X):
            for j in range(width // 128):
                cols = slice(j * 128, (j + 1) * 128)
                dat[cols, k * rows : (k + 1) * rows] = nt(eye, da[k, :, cols]).astype(BF)
        s_out = Scatter(d_out, c_out, y_out, z_out, t_out, b_out, x_out, w_out_s, dout_o, out_layout)
        s_out.fill(dat, atts)
        s_out.to_c()
        ug.add_l(far=True)
        uu.add_l(far=True)
        for name in ("kv", "p", "q", "cos", "sin", "w1", "in"):
            loads[name].wait()
        dkv[...] = jnp.zeros_like(dkv)

        @pl.loop(0, heads)
        def _(h):
            cols = pl.ds(pl.multiple_of(h * HEAD_WIDTH, HEAD_WIDTH), HEAD_WIDTH)
            g = lax.div(h, share)
            k_at = pl.ds(pl.multiple_of(g * HEAD_WIDTH, HEAD_WIDTH), HEAD_WIDTH)
            v_at = pl.ds(pl.multiple_of(kv_cols + g * HEAD_WIDTH, HEAD_WIDTH), HEAD_WIDTH)
            p_low, do_h = ps[h], dos[:, cols]
            p = p_low.astype(F32)
            dp = nt(do_h, kv[:, v_at])
            delta = jnp.sum(p * dp, axis=-1, keepdims=True)
            ds = (p * (dp - delta)).astype(BF)
            dq = nn(ds, kv[:, k_at]) * scale
            dq = dq * cos_s[:query_rows] - pltpu.roll(dq, HEAD_WIDTH // 2, 1) * sin_s[:query_rows]
            dpre[:, cols] = dq.astype(BF)
            dkv[:, k_at] += tn(ds, qs[:, cols]) * scale
            dkv[:, v_at] += tn(p_low, do_h)

        kv_c = []
        for d in range(1, C):
            dkv_low[d - 1] = dkv[d * query_rows : (d + 1) * query_rows].astype(BF)
            kv_c.append(put(dkv_low.at[d - 1], dkv_in.at[d - 1], c=d))
        s_out.to_y()
        ug.by_h[1].forward()
        for copy in kv_c:
            copy.wait_recv()
        total = dkv[:query_rows]
        for d in range(1, C):
            total = total + dkv_in[d - 1].astype(F32)
        for j in range(kv_heads):
            cols = slice(j * HEAD_WIDTH, (j + 1) * HEAD_WIDTH)
            v = total[:, cols]
            v = v * cos_s[:query_rows] - pltpu.roll(v, HEAD_WIDTH // 2, 1) * sin_s[:query_rows]
            dpre[:, q_cols + j * HEAD_WIDTH : q_cols + (j + 1) * HEAD_WIDTH] = v.astype(BF)
        dpre[:, q_cols + kv_cols :] = total[:, kv_cols:].astype(BF)
        s_qkv = Scatter(d_qkv, c_qkv, y_qkv, z_qkv, t_qkv, b_qkv, x_qkv, w_qkv_s, dqkv_o, qkv_layout)
        s_qkv.fill(n1t, dpre)
        s_qkv.to_c()

        for k in list(range(1, X)) + [0]:
            @pl.loop(0, width // 256)
            def _(j, k=k):
                cols = pl.ds(pl.multiple_of(j * 256, 256), 256)
                v = nt(dpre[k * rows : (k + 1) * rows], w1[cols])
                if k:
                    n_send[k - 1, :, cols] = v.astype(BF)
                else:
                    gi_s[:, cols] = v

            if k:
                copy = put(n_send.at[k - 1], n_recv.at[k - 1], x=k)
                n_x = [copy] if k == 1 else n_x + [copy]
        kv_at = lax.div(x * heads, QUERY_HEADS // KEY_VALUE_HEADS) * HEAD_WIDTH
        k_off = QUERY_HEADS * HEAD_WIDTH + kv_at
        v_off = k_off + KEY_VALUE_HEADS * HEAD_WIDTH
        sums = jnp.sum(dpre[...].astype(F32), axis=0, keepdims=True)

        def place(start, first, amount):
            vs[2:3, pl.ds(pl.multiple_of(start, 128), amount)] = sums[:, first : first + amount]

        place(x * q_cols, 0, q_cols)
        place(k_off, q_cols, kv_cols)
        place(v_off, q_cols + kv_cols, kv_cols)
        s_qkv.to_y()
        uu.by_h[1].forward()
        send_pair(0)
        ud.begin([(0, 0)])
        add_pair(1)
        s_out.to_z()
        outs_terms.spread_x()
        for copy in n_x:
            copy.wait_recv()

        @pl.loop(0, rows // 32)
        def _(i):
            r = pl.ds(pl.multiple_of(i * 32, 32), 32)
            grad, h = gi_s[r], ins[r].astype(F32)
            for d in range(1, X):
                grad = grad + n_recv[d - 1, r].astype(F32)
            inv = lax.rsqrt(jnp.mean(h * h, axis=-1, keepdims=True) + EPSILON)
            scaled = gain_one * grad
            gi_s[r] = (
                dh_s[r]
                + inv * scaled
                - h * (inv * inv * inv) * jnp.mean(scaled * h, axis=-1, keepdims=True)
            )
            vs[0:1, :width] = vs[0:1, :width] + jnp.sum(grad * h * inv, axis=0, keepdims=True)

        done = [move(gi_s, gi_o)]

        def put_out(u, out):
            u.wait_h()
            for h in range(ZH):
                def body(r, h=h):
                    out_w[u.m, r, h * units : (h + 1) * units] = u.half(h, r).astype(BF)

                by_rows(depth, 64, body)
            done.append(move(out_w.at[u.m], out))

        places = iter(range(V_IN))
        stages = iter(range(4))

        def small_stage(offsets):
            k = next(stages)
            v_send[k] = vs[...]
            return [(p, put(v_send.at[k], v_in.at[p], **off)) for off, p in zip(offsets, places)]

        def small_finish(copies):
            for p, copy in copies:
                copy.wait_recv()
                vs[...] = vs[...] + v_in[p]

        state = small_stage([dict(c=d) for d in range(1, C)])
        small_finish(state)
        state = small_stage([dict(x=d) for d in range(1, X)])
        s_out.to_h()
        outs_terms.relay()
        small_finish(state)
        state = small_stage([dict(y=d) for d in range(1, Y)])
        s_qkv.to_z()
        s_qkv.to_h()
        s_out.to_x()
        small_finish(state)
        state = small_stage([dict(zh=dh, zl=dl) for dh, dl in far[1:]])
        outs_terms.landed()

        def finish(r):
            lo_s[r] = (hs[r] + outs_terms.final(r)).astype(BF)

        by_rows(rows, 32, finish)
        done.append(move(lo_s, lo_o))
        done.append(s_out.end())
        s_qkv.to_x()
        ud.add_l(far=False)
        ug.add_l(far=False)
        uu.add_l(far=False)
        small_finish(state)
        done.append(move(vs, vec_out))
        done.append(s_qkv.end())
        add_pair(0)
        put_out(ug, og_o)
        put_out(uu, ou_o)
        ud.add_y([(0, 0)])
        put_out(ud, od_o)
        for copy in done:
            copy.wait()
        for copy in sent:
            copy.wait_send()
        assert count[0] <= n_sems and count[1] <= 64, count

    V_IN = (C - 1) + (X - 1) + (Y - 1) + (zs - 1)
    any_spec = pl.BlockSpec(memory_space=pl.ANY)
    sds = jax.ShapeDtypeStruct
    vm = pltpu.VMEM

    def scatter_scratch(n):
        return [
            vm((C, Y, zs, X * part, n), BF), vm((Y, max(C - 1, 1), zs, X * part, n), BF),
            vm((max(Y - 1, 1), zs, X * part, n), BF), vm((max(zs - 1, 1), X * part, n), BF),
            vm((X, part, n), F32), vm((X, part, n), BF), vm((max(X - 1, 1), part, n), BF),
        ]

    nk = len(near)
    return pl.pallas_call(
        kernel,
        out_shape=[
            sds((rows, width), BF), sds((rows, width), F32), sds((part, QKV_WIDTH), F32),
            sds((part, X * q_cols), F32), sds((8, QKV_WIDTH), F32),
            sds((depth, ZH * units), BF), sds((depth, ZH * units), BF),
            sds((depth, ZH * units), BF), sds((3, depth, units), BF),
        ],
        in_specs=[any_spec] * 20,
        out_specs=[any_spec] * 9,
        scratch_shapes=[
            vm((3, zs, depth, units), BF), vm((3, zs, max(Y - 1, 1), depth, units), BF),
            vm((3, ZH, max(ZL - 1, 1), depth, units), BF), vm((3, max(ZH - 1, 1), depth, units), BF),
            vm((3, depth, ZH * units), BF), vm((width, group_rows), BF), vm((2, group_rows, units), BF),
            vm((nk, rows, width), BF), vm((nk, rows, width), BF),
            vm((2, nk, max(C - 1, 1), rows, width), BF), vm((2, max(nk - 1, 1), rows, width), BF),
            vm((rows, width), F32), vm((rows, width), BF), vm((rows, width), BF),
            vm((width, qkv_n), BF), vm((width, q_cols), BF),
            vm((width, query_rows), BF), vm((query_rows, q_cols), BF),
            vm((pack_rows, 2 * kv_cols), BF), vm((heads, query_rows, pack_rows), BF),
            vm((query_rows, q_cols), BF), vm((8, QKV_WIDTH), F32),
            vm((pack_rows, HEAD_WIDTH), F32), vm((pack_rows, HEAD_WIDTH), F32),
            vm((X, rows, width), BF), vm((width, query_rows), BF), vm((query_rows, q_cols), BF),
            vm((query_rows, qkv_n), BF), vm((pack_rows, 2 * kv_cols), F32),
            vm((max(C - 1, 1), query_rows, 2 * kv_cols), BF),
            vm((max(C - 1, 1), query_rows, 2 * kv_cols), BF),
            vm((rows, width), F32),
        ]
        + scatter_scratch(qkv_n)
        + scatter_scratch(q_cols)
        + [
            vm((part, QKV_WIDTH), F32), vm((part, X * q_cols), F32),
            vm((max(X - 1, 1), rows, width), BF), vm((max(X - 1, 1), rows, width), BF),
            vm((rows, width), BF), vm((rows, width), F32), vm((8, QKV_WIDTH), F32),
            vm((max(V_IN, 1), 8, QKV_WIDTH), F32), vm((4, 8, QKV_WIDTH), F32),
            pltpu.SemaphoreType.DMA((n_sems,)), pltpu.SemaphoreType.DMA((n_sems,)),
            pltpu.SemaphoreType.DMA((64,)),
        ],
        compiler_params=pltpu.CompilerParams(
            collective_id=1, has_side_effects=True, vmem_limit_bytes=63 << 20
        ),
        name="back",
    )(
        grad_d, near_d, grad_g, grad_u, group_t, normed_terms, out_terms, middle, cotangent, own_in,
        wqkv, wout, normed, queries, kv_rows, probs, attended, vectors, cosine, sine,
    )


def finish(arrays, types):
    def spec(v):
        if v.shape[0] % 64 == 0:
            return pl.BlockSpec((v.shape[0] // 4,) + v.shape[1:], lambda i: (i,) + (0,) * (v.ndim - 1))
        return pl.BlockSpec(v.shape, lambda i: (0,) * v.ndim)

    def kernel(*refs):
        for src, dst in zip(refs[: len(arrays)], refs[len(arrays) :]):
            dst[...] = src[...].astype(dst.dtype)

    return pl.pallas_call(
        kernel,
        grid=(4,),
        out_shape=[jax.ShapeDtypeStruct(v.shape, t) for v, t in zip(arrays, types)],
        in_specs=[spec(v) for v in arrays],
        out_specs=[spec(v) for v in arrays],
        name="finish",
    )(*arrays)


def ff(normed, cotangent, w_gate, w_up, w_down):
    gate = nn(normed, w_gate)
    up_part = nn(normed, w_up)
    sig = jax.nn.sigmoid(gate)
    act = gate * sig
    hidden = (act * up_part).astype(BF)
    grad_wdown = tn(cotangent, hidden).astype(BF)
    grad_hidden = nn(cotangent, w_down)
    grad_gate = (grad_hidden * up_part * sig * (1.0 + gate * (1.0 - sig))).astype(BF)
    grad_up = (grad_hidden * act).astype(BF)
    grad_wgate = tn(normed, grad_gate).astype(BF)
    grad_wup = tn(normed, grad_up).astype(BF)
    normed_term = (nt(grad_gate, w_gate) + nt(grad_up, w_up)).astype(BF)
    out_term = nt(hidden, w_down).astype(BF)
    return hidden, grad_gate, grad_up, grad_wdown, grad_wgate, grad_wup, out_term, normed_term


def small_rows(gain_one, gain_two, bias):
    row = jnp.concatenate([gain_one, gain_two, bias]).astype(F32)
    return jnp.broadcast_to(jnp.pad(row, (0, -row.shape[0] % 256))[None], (8, 256))


def shards(
    layer_in, lengths, w_qkv, b_qkv, w_out, norm1_gain, norm2_gain, w_gate, w_up, w_down, grad_out
):
    size = lax.axis_size
    ZH, ZL, Y, X, C = (size(a) for a in ("zh", "zl", "y", "x", "c"))
    zh, zl, y, x, c = (lax.axis_index(a) for a in ("zh", "zl", "y", "x", "c"))
    everyone = ("zh", "zl", "y", "x", "c")
    devices = ZH * ZL * Y * X * C
    rows, width = layer_in.shape[1:]
    part = w_qkv.shape[0]
    group = QUERY_HEADS // KEY_VALUE_HEADS
    heads = QUERY_HEADS // X
    kv_heads = max(1, heads // group)
    share = heads // kv_heads
    q_cols, kv_cols = heads * HEAD_WIDTH, kv_heads * HEAD_WIDTH
    scale = HEAD_WIDTH ** (-0.5)

    own_in = layer_in[0]
    cotangent = grad_out[0]
    own_rows = own_in.astype(F32)
    query_rows, pack_rows = X * rows, C * X * rows
    bias_part = b_qkv.shape[0]
    def row_index(cores):
        spans = [
            (((x + dx) % X) * C + (c + dc) % C) * rows + jnp.arange(rows, dtype=jnp.int32)
            for dc in range(cores)
            for dx in range(X)
        ]
        return jnp.concatenate(spans)

    doc_lengths = lengths[0]
    key_index = row_index(C)
    key_doc, key_pos = doc_layout(key_index, doc_lengths)
    query_index, query_doc = key_index[:query_rows], key_doc[:query_rows]
    key_cos, key_sin = angles(key_pos)
    query_cos, query_sin = key_cos[:query_rows], key_sin[:query_rows]

    def gather_columns(pieces):
        held = ordered(
            [pick(pieces, x)] + [fetch(pick(pieces, (x - d) % X), "x", d) for d in range(1, X)],
            "x",
        )
        whole = jnp.zeros((ZH, ZL, Y) + held.shape, held.dtype)
        for dh in range(ZH):
            for dl in range(ZL):
                along = held if dh == dl == 0 else fetch(held, ("zh", "zl"), (dh, dl))
                for dy in range(Y):
                    piece = along if dy == 0 else fetch(along, "y", dy)
                    whole = lax.dynamic_update_slice(
                        whole,
                        piece[None, None, None],
                        ((zh + dh) % ZH, (zl + dl) % ZL, (y + dy) % Y, 0, 0, 0),
                    )
        whole = whole.reshape((ZH * ZL * Y * X,) + whole.shape[4:])
        both = ordered([whole] + [fetch(whole, "c", d) for d in range(1, C)], "c")
        return jnp.moveaxis(both, 0, 1).reshape(width, whole.shape[-1])

    def scatter_columns(grad):
        n = grad.shape[-1]
        grad = grad.astype(BF).reshape(ZH * ZL * Y * X, C, part, n)
        held = pick(grad, c, 1).astype(F32)
        for d in range(1, C):
            held = held + send(pick(grad, (c + d) % C, 1), "c", d)
        held = held.astype(BF).reshape(ZH, ZL, Y, X * part, n)
        kept = pick(held, y, 2).astype(F32)
        for d in range(1, Y):
            kept = kept + send(pick(held, (y + d) % Y, 2), "y", d)
        low = kept.astype(BF)
        total = 0.0
        for dh in range(ZH):
            for dl in range(ZL):
                if dh == dl == 0:
                    total = total + pick(pick(kept, zh), zl)
                else:
                    piece = pick(pick(low, (zh + dh) % ZH), (zl + dl) % ZL)
                    total = total + send(piece, ("zh", "zl"), (dh, dl)).astype(F32)
        total = total.reshape(X, part, n)
        lower = total.astype(BF)
        return ordered(
            [pick(total, x)]
            + [fetch(pick(lower, (x - d) % X), "x", d).astype(F32) for d in range(1, X)],
            "x",
        )

    def qkv_columns(array):
        blocks = []
        for at in range(X):
            kv = (at * heads) // group * HEAD_WIDTH
            key_at = QUERY_HEADS * HEAD_WIDTH + kv
            value_at = key_at + KEY_VALUE_HEADS * HEAD_WIDTH
            blocks.append(
                jnp.concatenate(
                    [
                        array[..., at * q_cols : (at + 1) * q_cols],
                        array[..., key_at : key_at + kv_cols],
                        array[..., value_at : value_at + kv_cols],
                    ],
                    axis=-1,
                )
            )
        return jnp.stack(blocks)

    def qkv_whole(blocks):
        queries = [blocks[at, ..., :q_cols] for at in range(X)]
        keys, values = [0.0] * KEY_VALUE_HEADS, [0.0] * KEY_VALUE_HEADS
        for at in range(X):
            for j in range(kv_heads):
                head = (at * heads) // group + j
                start = q_cols + j * HEAD_WIDTH
                keys[head] = keys[head] + blocks[at, ..., start : start + HEAD_WIDTH]
                start = start + kv_cols
                values[head] = values[head] + blocks[at, ..., start : start + HEAD_WIDTH]
        return jnp.concatenate(queries + keys + values, axis=-1)

    depth, units = w_gate.shape[0], w_gate.shape[1] // ZH

    def gather_units(weight):
        halves = weight.reshape(depth, ZH, units).transpose(1, 0, 2)
        whole = jnp.zeros((ZH, ZL, Y, depth, units), weight.dtype)
        for dh in range(ZH):
            first = pick(halves, zh) if dh == 0 else fetch(pick(halves, (zh - dh) % ZH), "zh", dh)
            for dl in range(ZL):
                second = first if dl == 0 else fetch(first, "zl", dl)
                for dy in range(Y):
                    third = second if dy == 0 else fetch(second, "y", dy)
                    whole = lax.dynamic_update_slice(
                        whole,
                        third[None, None, None],
                        ((zh + dh) % ZH, (zl + dl) % ZL, (y + dy) % Y, 0, 0),
                    )
        return whole.reshape(width, units)

    def scatter_units(grad):
        grad = grad.astype(BF).reshape(ZH, ZL, Y, depth, units)
        done = [None] * ZH
        for dh in reversed(range(ZH)):
            mine = pick(grad, (zh + dh) % ZH)
            kept = pick(mine, y, 1).astype(F32)
            for d in range(1, Y):
                kept = kept + send(pick(mine, (y + d) % Y, 1), "y", d).astype(F32)
            low = kept.astype(BF)
            total = pick(kept, zl)
            for d in range(1, ZL):
                total = total + send(pick(low, (zl + d) % ZL), "zl", d).astype(F32)
            done[dh] = total
        halves = [done[0]] + [
            send(done[dh].astype(BF), "zh", dh).astype(F32) for dh in range(1, ZH)
        ]
        halves = [halves[0]] + halves[:0:-1]
        return jnp.moveaxis(ordered(halves, "zh"), 0, 1).reshape(depth, ZH * units)

    near = [(dh, dx) for dh in range(ZH) for dx in range(X)]

    def gather_rows(own):
        held = jnp.concatenate([own if k == (0, 0) else fetch(own, ("zh", "x"), k) for k in near])
        return jnp.concatenate([held] + [fetch(held, "c", d) for d in range(1, C)])

    def scatter_rows(term):
        term = term.reshape(C, len(near), rows, width)
        held = term[0].astype(F32)
        for d in range(1, C):
            held = held + send(term[d].astype(BF), "c", d).astype(F32)
        total = held[0]
        for at, k in enumerate(near):
            if k != (0, 0):
                total = total + send(held[at].astype(BF), ("zh", "x"), k).astype(F32)
        return total

    def scatter_x(term):
        term = term.reshape(X, rows, width)
        total = term[0]
        for d in range(1, X):
            total = total + send(term[d].astype(BF), "x", d).astype(F32)
        return total

    if part % 16 == 0 and depth % 64 == 0 and heads % 2 == 0 and X > 1 and ZH == ZL == Y == 2:
        (
            wqkv_mine, wout_mine, normed_t, group_normed_t, queries, kv_low, probs_low,
            attended_low, middle, group_normed, group_cotangent, wgate_mine, wup_mine,
            wdown_part, vectors, cosine, sine, _,
        ) = front(
            own_in,
            cotangent,
            lengths,
            w_qkv,
            w_out.T,
            small_rows(norm1_gain, norm2_gain, b_qkv),
            w_gate,
            w_up,
            w_down.T,
            qkv_columns,
        )
        grad_gate, grad_up, grad_wdown, near_d, normed_term, out_term = forward_backward(
            group_normed.reshape(-1, width),
            group_cotangent.reshape(-1, width),
            wgate_mine.reshape(width, units),
            wup_mine.reshape(width, units),
            wdown_part,
        )
        whole = (ZH, ZL, Y, depth, units)
        terms = (C, ZH * X, rows, width)
        layer_out, grad_input, sum_wqkv, sum_wout, small, sum_wdown, sum_wgate, sum_wup, _ = back(
            grad_wdown.reshape(whole),
            near_d,
            grad_gate,
            grad_up,
            group_normed_t,
            normed_term.reshape(terms),
            out_term.reshape(terms),
            middle,
            cotangent,
            own_in,
            wqkv_mine,
            wout_mine,
            normed_t,
            queries,
            kv_low,
            probs_low,
            attended_low,
            vectors,
            cosine,
            sine,
        )
        place = (((zh * ZL + zl) * Y + y) * X + x) * C + c
        layer_out, grad_input, sum_wqkv, sum_wout, sum_wgate, sum_wup, sum_wdown = finish(
            (layer_out, grad_input, sum_wqkv, sum_wout, sum_wgate, sum_wup, sum_wdown),
            (BF,) + (F32,) * 6,
        )
        return (
            layer_out[None],
            grad_input[None],
            sum_wqkv,
            lax.dynamic_slice(small, (2, place * bias_part), (1, bias_part))[0],
            sum_wout.T,
            lax.dynamic_slice(small, (0, place * part), (1, part))[0],
            lax.dynamic_slice(small, (1, place * part), (1, part))[0],
            sum_wgate,
            sum_wup,
            sum_wdown.T,
        )

    small = jnp.concatenate([norm1_gain, norm2_gain, b_qkv])
    small = jnp.pad(small, (0, -small.shape[0] % 256))[None]
    small = lax.all_to_all(
        jnp.broadcast_to(small[None], (devices,) + small.shape), everyone, 0, 0, tiled=True
    )[:, 0].astype(F32)
    gain_one = small[:, :part].reshape(1, width)
    gain_two = small[:, part : 2 * part].reshape(1, width)
    bias = small[:, 2 * part : 2 * part + bias_part].reshape(-1)

    query_in = jnp.concatenate([own_in] + [fetch(own_in, "x", d) for d in range(1, X)])
    pack_in = jnp.concatenate([query_in] + [fetch(query_in, "c", d) for d in range(1, C)])

    wqkv_mine = gather_columns(qkv_columns(w_qkv))
    wout_t = w_out.T
    wout_mine = gather_columns(
        jnp.stack([wout_t[:, at * q_cols : (at + 1) * q_cols] for at in range(X)])
    )
    bias_mine = pick(qkv_columns(bias), x)

    wgate_mine, wup_mine = gather_units(w_gate), gather_units(w_up)
    wdown_mine = gather_units(w_down.T)

    group_cotangent = gather_rows(cotangent)

    pack_in = pack_in.astype(F32)
    normed_one = (pack_in * rms_parts(pack_in) * gain_one).astype(BF)
    query_normed = normed_one[:query_rows]
    pre_query = nn(query_normed, wqkv_mine[:, :q_cols]) + bias_mine[:q_cols]
    pre_kv = nn(normed_one, wqkv_mine[:, q_cols:]) + bias_mine[q_cols:]
    queries = rotate(
        pre_query.reshape(query_rows, heads, HEAD_WIDTH), query_cos, query_sin
    ).astype(BF)
    queries = queries.reshape(query_rows, kv_heads, share, HEAD_WIDTH)
    keys = rotate(
        pre_kv[:, :kv_cols].reshape(pack_rows, kv_heads, HEAD_WIDTH), key_cos, key_sin
    ).astype(BF)
    values = pre_kv[:, kv_cols:].reshape(pack_rows, kv_heads, HEAD_WIDTH).astype(BF)
    scores = jnp.einsum("tkgd,skd->kgts", queries, keys, preferred_element_type=F32) * scale
    allowed = (query_doc[:, None] == key_doc[None, :]) & (
        key_index[None, :] <= query_index[:, None]
    )
    masked = jnp.where(allowed, scores, NEGATIVE_BIG)
    top = jnp.max(masked, axis=-1, keepdims=True)
    weights = jnp.where(allowed, jnp.exp(masked - top), 0.0)
    probs = weights / jnp.sum(weights, axis=-1, keepdims=True)
    probs_low = probs.astype(BF)
    attended = jnp.einsum("kgts,skd->tkgd", probs_low, values, preferred_element_type=F32)
    attended_low = attended.reshape(query_rows, q_cols).astype(BF)
    middle = own_rows + scatter_x(nt(attended_low, wout_mine))
    normed_two = (middle * rms_parts(middle) * gain_two).astype(BF)

    group_normed = gather_rows(normed_two)

    hidden, grad_gate, grad_up, grad_wdown, grad_wgate, grad_wup, out_term, normed_term = ff(
        group_normed, group_cotangent, wgate_mine, wup_mine, wdown_mine
    )
    grad_normed_two = scatter_rows(normed_term)
    layer_out = (middle + scatter_rows(out_term)).astype(BF)
    sum_wdown = scatter_units(grad_wdown).T
    sum_wgate = scatter_units(grad_wgate)
    sum_wup = scatter_units(grad_wup)

    back_two, grad_gain_two = rms_back(middle, gain_two, grad_normed_two)
    grad_middle = cotangent.astype(F32) + back_two
    grad_att = grad_middle.astype(BF)
    query_grad_att = jnp.concatenate([grad_att] + [fetch(grad_att, "x", d) for d in range(1, X)])
    sum_wout = scatter_columns(tn(query_grad_att, attended_low))
    head_grads = nn(query_grad_att, wout_mine).astype(BF)
    head_grads = head_grads.reshape(query_rows, kv_heads, share, HEAD_WIDTH)
    grad_probs = jnp.einsum("tkgd,skd->kgts", head_grads, values, preferred_element_type=F32)
    probs = probs_low.astype(F32)
    delta = jnp.sum(probs * grad_probs, axis=-1, keepdims=True)
    grad_scores = (probs * (grad_probs - delta)).astype(BF)
    grad_query = (
        jnp.einsum("kgts,skd->tkgd", grad_scores, keys, preferred_element_type=F32) * scale
    )
    grad_key = jnp.einsum("kgts,tkgd->skd", grad_scores, queries, preferred_element_type=F32)
    grad_key = rotate(grad_key * scale, key_cos, -key_sin)
    grad_value = jnp.einsum("kgts,tkgd->skd", probs_low, head_grads, preferred_element_type=F32)
    grad_kv = jnp.concatenate(
        [grad_key.reshape(pack_rows, kv_cols), grad_value.reshape(pack_rows, kv_cols)], axis=1
    ).reshape(C, query_rows, 2 * kv_cols)
    kv_total = grad_kv[0]
    for d in range(1, C):
        kv_total = kv_total + send(grad_kv[d].astype(BF), "c", d).astype(F32)
    grad_query = rotate(
        grad_query.reshape(query_rows, heads, HEAD_WIDTH), query_cos, -query_sin
    ).reshape(query_rows, q_cols)
    grad_pre = jnp.concatenate([grad_query, kv_total], axis=1).astype(BF)
    sum_wqkv = qkv_whole(scatter_columns(tn(query_normed, grad_pre)))
    grad_bias = jnp.sum(grad_pre.astype(F32), axis=0)
    grad_normed_one = scatter_x(nt(grad_pre, wqkv_mine))
    back_one, grad_gain_one = rms_back(own_rows, gain_one, grad_normed_one)
    grad_input = grad_middle + back_one

    bias_blocks = jnp.where(
        jnp.arange(X, dtype=jnp.int32)[:, None] == x, grad_bias[None, :], 0.0
    )
    bias_whole = qkv_whole(bias_blocks)
    piece = jnp.concatenate(
        [
            grad_gain_one.reshape(devices, part),
            grad_gain_two.reshape(devices, part),
            bias_whole.reshape(devices, bias_part),
        ],
        axis=1,
    )
    piece = jnp.pad(piece, ((0, 0), (0, -piece.shape[1] % 256)))
    piece = jnp.sum(lax.all_to_all(piece[:, None], everyone, 0, 0, tiled=True)[:, 0], axis=0)
    return (
        layer_out[None],
        grad_input[None],
        sum_wqkv,
        piece[2 * part : 2 * part + bias_part],
        jnp.moveaxis(sum_wout, 0, 1).reshape(part, -1).T,
        piece[:part],
        piece[part : 2 * part],
        sum_wgate,
        sum_wup,
        sum_wdown,
    )


def solution(mesh):
    wide, narrow = mesh.shape["wide"], mesh.shape["narrow"]
    cores = 2 if narrow % 2 == 0 else 1
    along_x = narrow // cores
    along_y = along_x if wide % along_x == 0 else 1
    along_z = wide // along_y
    far = 2 if along_z % 2 == 0 else 1
    split = Mesh(
        mesh.devices.reshape(far, along_z // far, along_y, along_x, cores),
        ("zh", "zl", "y", "x", "c"),
    )
    w, n = ("zh", "zl", "y"), ("x", "c")
    placed = (
        P(w, n, None),
        P(w, None),
        P(w + n, None),
        P(w + n),
        P(None, w + n),
        P(w + n),
        P(w + n),
        P(w, n),
        P(w, n),
        P(n, w),
        P(w, n, None),
    )
    return jax.shard_map(
        shards,
        mesh=split,
        in_specs=placed,
        out_specs=(
            P(w, n, None),
            P(w, n, None),
            P(w + n, None),
            P(w + n),
            P(None, w + n),
            P(w + n),
            P(w + n),
            P(w, n),
            P(w, n),
            P(n, w),
        ),
        check_vma=False,
    )
```

```python
import math

import jax
import jax.numpy as jnp
from jax import lax
from jax.experimental import pallas as pl
from jax.experimental.pallas import tpu as pltpu
from jax.sharding import Mesh
from jax.sharding import PartitionSpec as P

QUERY_HEADS = 12
KEY_VALUE_HEADS = 2
HEAD_WIDTH = 128

EPSILON = 1e-06
ROPE_BASE = 10000.0
NEGATIVE_BIG = -1e30
HIGHEST = lax.Precision.HIGHEST


BF = jnp.bfloat16
F32 = jnp.float32
AXES = ("zh", "zl", "y", "x", "c")
MESH_ID = pl.DeviceIdType.MESH
QKV_WIDTH = (QUERY_HEADS + 2 * KEY_VALUE_HEADS) * HEAD_WIDTH


def fetch(value, axes, offsets):
    axes = (axes,) if isinstance(axes, str) else tuple(axes)
    offsets = (offsets,) if isinstance(offsets, int) else tuple(offsets)
    sizes = [lax.axis_size(a) for a in axes]
    total = math.prod(sizes)
    pairs = []
    for flat in range(total):
        rest, place = flat, []
        for size in reversed(sizes):
            place.append(rest % size)
            rest //= size
        place = place[::-1]
        source = 0
        for spot, off, size in zip(place, offsets, sizes):
            source = source * size + (spot + off) % size
        pairs.append((source, flat))
    return lax.ppermute(value, axes if len(axes) > 1 else axes[0], pairs)


def send(value, axes, offsets):
    offsets = (offsets,) if isinstance(offsets, int) else tuple(offsets)
    return fetch(value, axes, tuple(-o for o in offsets))


def pick(stack, place, axis=0):
    return lax.dynamic_index_in_dim(stack, place, axis, keepdims=False)


def nn(left, right):
    return lax.dot_general(left, right, (((1,), (0,)), ((), ())), preferred_element_type=F32)


def nt(left, right):
    return lax.dot_general(left, right, (((1,), (1,)), ((), ())), preferred_element_type=F32)


def tn(left, right):
    return lax.dot_general(left, right, (((0,), (0,)), ((), ())), preferred_element_type=F32)


def rms_parts(rows):
    return lax.rsqrt(jnp.mean(rows * rows, axis=-1, keepdims=True) + EPSILON)


def rms_back(rows, gain, grad):
    r = rms_parts(rows)
    scaled = gain * grad
    return (
        r * scaled - rows * (r * r * r) * jnp.mean(scaled * rows, axis=-1, keepdims=True),
        jnp.sum(grad * rows * r, axis=0),
    )


def doc_layout(index, doc_lengths):
    ends = jnp.cumsum(doc_lengths)
    starts = ends - doc_lengths
    document_index = jnp.sum((index[:, None] >= ends[None, :]).astype(jnp.int32), axis=1)
    onehot = (
        document_index[:, None] == jnp.arange(doc_lengths.shape[0], dtype=jnp.int32)[None, :]
    ).astype(jnp.int32)
    token_position = index - jnp.sum(onehot * starts[None, :], axis=1)
    return document_index, token_position.astype(F32)


def angles(position):
    half = HEAD_WIDTH // 2
    freq = jnp.exp(jnp.arange(half, dtype=F32) * (-2.0 * math.log(ROPE_BASE) / HEAD_WIDTH))
    angle = position[:, None] * freq[None, :]
    return jnp.cos(angle)[:, None, :], jnp.sin(angle)[:, None, :]


def rotate(rows, cosine, sine):
    half = HEAD_WIDTH // 2
    first, second = rows[..., :half], rows[..., half:]
    return jnp.concatenate(
        [first * cosine - second * sine, second * cosine + first * sine], axis=-1
    )


def ordered(pieces, axis):
    count, here = len(pieces), lax.axis_index(axis)
    if count == 1:
        return pieces[0][None]
    if count == 2:
        return jnp.where(here == 0, jnp.stack(pieces), jnp.stack(pieces[::-1]))
    whole = jnp.zeros((count,) + pieces[0].shape, pieces[0].dtype)
    for distance, piece in enumerate(pieces):
        whole = lax.dynamic_update_index_in_dim(whole, piece, (here + distance) % count, 0)
    return whole


def front(own_in, cotangent, lengths, w_qkv, w_out, small, w_gate, w_up, w_down, qkv_columns):
    size = lax.axis_size
    ZH, ZL, Y, X, C = (size(a) for a in AXES)
    rows, width = own_in.shape
    part = w_qkv.shape[0]
    q_cols = w_out.shape[1] // X
    qkv_n = qkv_columns(w_qkv).shape[-1]
    heads = q_cols // HEAD_WIDTH
    kv_cols = (qkv_n - q_cols) // 2
    kv_heads = kv_cols // HEAD_WIDTH
    share = heads // kv_heads
    query_rows, pack_rows = X * rows, C * X * rows
    depth = w_gate.shape[0]
    units = w_gate.shape[1] // ZH
    near = [(dh, dx) for dh in range(ZH) for dx in range(X)]
    far = [(dh, dl) for dh in range(ZH) for dl in range(ZL)]
    devices = ZH * ZL * Y * X * C
    bias_part = QKV_WIDTH // devices
    scale = HEAD_WIDTH ** (-0.5)
    docs = lengths.shape[-1]
    n_sems = 400

    def kernel(
        own_ref, cot_ref, len_ref, qkv_ref, out_ref, small_ref, g_ref, u_ref, d_ref,
        wqkv_o, wout_o, n1_o, n2t_o, q_o, kv_o, p_o, att_o, h_o, nr_o, go_o, wg_o, wu_o, wd_o, vec_o, cos_o, sin_o, relay,
        xr, w1, wo, sm, n1, qs, kv, ob, part_send, part_recv, n2s, hs,
        cos_s, sin_s, mask_s, rows_s, ps, raw, half, wq_raw, wq_cut, n1t, n2t, nr_v, go_v,
        send_sem, recv_sem, local_sem,
    ):
        zh, zl, y, x, c = (lax.axis_index(a) for a in AXES)
        sizes = dict(zip(AXES, (ZH, ZL, Y, X, C)))
        here = dict(zip(AXES, (zh, zl, y, x, c)))

        def device(**off):
            return tuple(
                lax.rem(here[a] + off[a], sizes[a]) if off.get(a, 0) % sizes[a] else here[a]
                for a in AXES
            )

        def at(a, d):
            d = d % sizes[a]
            return lax.rem(here[a] + d, sizes[a]) if d else here[a]

        peers = set()
        for d in range(1, C):
            peers.add((0, 0, 0, 0, d))
        for dh, dx in near[1:]:
            peers.add((dh, 0, 0, dx, 0))
        for dh, dl in far[1:]:
            peers.add((dh, dl, 0, 0, 0))
        for d in range(1, Y):
            peers.add((0, 0, d, 0, 0))
        peers = sorted(peers)
        barrier = pltpu.get_barrier_semaphore()
        for peer in peers:
            pl.semaphore_signal(
                barrier, inc=1, device_id=device(**dict(zip(AXES, peer))), device_id_type=MESH_ID
            )
        pl.semaphore_wait(barrier, len(peers))

        count = [0, 0]
        sent, local = [], []

        def put(src, dst, **off):
            k = count[0]
            count[0] += 1
            copy = pltpu.make_async_remote_copy(
                src_ref=src, dst_ref=dst, send_sem=send_sem.at[k], recv_sem=recv_sem.at[k],
                device_id=device(**off), device_id_type=MESH_ID,
            )
            copy.start()
            sent.append(copy)
            return copy

        def move(src, dst):
            k = count[1]
            count[1] += 1
            copy = pltpu.make_async_copy(src, dst, local_sem.at[k])
            copy.start()
            return copy

        inner = zh + zl == 1

        class Far:
            def __init__(self, src, dst, relay, onward):
                k = count[0]
                count[0] += 3
                self.relay, self.k = relay, k
                self.main = self.copy(src, dst, k, k, device(zh=1))
                self.step = self.copy(src, relay, k, k + 1, device(zl=1))
                self.onward = self.copy(relay, onward, k + 2, k, device(zh=1, zl=1))
                pl.when(inner)(self.main.start)
                pl.when(jnp.logical_not(inner))(self.step.start)
                sent.append(self)

            def copy(self, src, dst, k, r, to):
                return pltpu.make_async_remote_copy(
                    src_ref=src, dst_ref=dst, send_sem=send_sem.at[k], recv_sem=recv_sem.at[r],
                    device_id=to, device_id_type=MESH_ID,
                )

            def forward(self):
                @pl.when(inner)
                def _():
                    self.step.wait_recv()
                    self.onward.start()

            def wait_recv(self):
                self.main.wait_recv()

            def wait_send(self):
                self.main.wait_send()
                pl.when(inner)(self.onward.wait_send)

        class Gather:
            def __init__(self, buf, block, pieces):
                self.buf, self.block, self.pieces = buf, block, pieces

            def slot(self, dh, dl, dy, dx, dc):
                place = at("zh", dh)
                for a, d in (("zl", dl), ("y", dy), ("x", dx), ("c", dc)):
                    place = place * sizes[a] + at(a, d)
                start = pl.multiple_of(place * self.block, self.block)
                return self.buf.at[pl.ds(start, self.block)]

            def begin(self):
                self.own = move(self.pieces(x), self.slot(0, 0, 0, 0, 0))
                self.by_x = {
                    d: put(self.pieces(at("x", d)), self.slot(0, 0, 0, 0, 0), x=d)
                    for d in range(1, X)
                }

            def along_z(self):
                self.own.wait()
                for d in self.by_x:
                    self.by_x[d].wait_recv()
                self.by_h, self.by_l, self.by_y, self.by_c = {}, {}, {}, {}
                for dx in range(X):
                    s = self.slot(0, 0, 0, dx, 0)
                    for d in range(1, ZH):
                        self.by_h[d, dx] = put(s, s, zh=d)
                for dx in range(X):
                    self.along_l(0, dx)
                for dx in range(X):
                    self.spread(0, 0, dx)

            def along_l(self, dh, dx):
                s = self.slot(-dh, 0, 0, dx, 0)
                for d in range(1, ZL):
                    self.by_l[dh, d, dx] = put(s, s, zl=d)

            def spread(self, dh, dl, dx):
                s = self.slot(-dh, -dl, 0, dx, 0)
                for d in range(1, Y):
                    self.by_y[dh, dl, d, dx] = put(s, s, y=d)
                self.to_core(dh, dl, 0, dx)

            def to_core(self, dh, dl, dy, dx):
                s = self.slot(-dh, -dl, -dy, dx, 0)
                for d in range(1, C):
                    self.by_c[dh, dl, dy, d, dx] = put(s, s, c=d)

            def along_h(self):
                for d, dx in self.by_h:
                    self.by_h[d, dx].wait_recv()
                    self.along_l(d, dx)
                    self.spread(d, 0, dx)

            def along_y(self):
                for dh, dl, dx in self.by_l:
                    self.by_l[dh, dl, dx].wait_recv()
                    self.spread(dh, dl, dx)

            def along_c(self):
                for dh, dl in far:
                    for d in range(1, Y):
                        for dx in range(X):
                            self.by_y[dh, dl, d, dx].wait_recv()
                            self.to_core(dh, dl, d, dx)

            def end(self):
                for copy in self.by_c.values():
                    copy.wait_recv()

        class Units:
            def __init__(self, at_m, buf):
                self.m, self.buf = at_m, buf

            def slot(self, dh, dl, dy):
                return self.buf.at[at("zh", dh), at("zl", dl), at("y", dy)]

            def begin(self):
                mine = half.at[self.m, zh]
                s = self.slot(0, 0, 0)
                self.own = move(mine, s)
                self.by_h = {
                    1: Far(half.at[self.m, at("zh", 1)], s, relay.at[self.m], self.slot(0, 1, 0))
                }

            def own_l(self):
                self.by_l = {
                    (0, d): put(half.at[self.m, zh], self.slot(0, 0, 0), zl=d)
                    for d in range(1, ZL)
                }

            def own_y(self):
                self.by_y = {
                    (0, 0, d): put(half.at[self.m, zh], self.slot(0, 0, 0), y=d)
                    for d in range(1, Y)
                }

            def middle(self):
                for dh in self.by_h:
                    self.by_h[dh].wait_recv()
                    s = self.slot(-dh, 0, 0)
                    for d in range(1, ZL):
                        self.by_l[dh, d] = put(s, s, zl=d)
                    for d in range(1, Y):
                        self.by_y[dh, 0, d] = put(s, s, y=d)

            def last(self, dh, spread=True):
                for dl in range(1, ZL):
                    self.by_l[dh, dl].wait_recv()
                    s = self.slot(-dh, -dl, 0)
                    for d in range(1, Y) if spread else ():
                        self.by_y[dh, dl, d] = put(s, s, y=d)

            def end(self):
                self.own.wait()
                for copy in self.by_y.values():
                    copy.wait_recv()

        class Rows:
            def __init__(self, buf):
                self.buf = buf

            def begin(self, src):
                self.own = move(src, self.buf.at[0, 0, 0])
                self.by_h = {d: put(src, self.buf.at[0, -d % ZH, 0], zh=d) for d in range(1, ZH)}
                self.by_x = {(0, d): put(src, self.buf.at[0, 0, -d % X], x=d) for d in range(1, X)}
                self.by_c = [put(src, self.buf.at[-d % C, 0, 0], c=d) for d in range(1, C)]

            def spread(self, a, b):
                for d in range(1, C):
                    self.by_c.append(put(self.buf.at[0, a, b], self.buf.at[-d % C, a, b], c=d))

            def along_x(self):
                for dh in self.by_h:
                    self.by_h[dh].wait_recv()
                    a = -dh % ZH
                    for d in range(1, X):
                        self.by_x[dh, d] = put(self.buf.at[0, a, 0], self.buf.at[0, a, -d % X], x=d)
                    self.spread(a, 0)

            def to_core(self):
                for dh, d in self.by_x:
                    self.by_x[dh, d].wait_recv()
                    self.spread(-dh % ZH, -d % X)

            def end(self):
                self.own.wait()
                for copy in self.by_c:
                    copy.wait_recv()

        raws = [move(qkv_ref, wq_raw), move(g_ref, raw.at[0]), move(u_ref, raw.at[1])]
        raws.append(move(d_ref, raw.at[2]))

        def out_piece(to):
            return out_ref.at[:, pl.ds(pl.multiple_of(to * q_cols, 128), q_cols)]

        wq_g = Gather(w1, part, lambda to: wq_cut.at[to])
        wo_g = Gather(wo, part, out_piece)
        sm_g = Gather(sm, 8, lambda to: small_ref)
        raws[0].wait()
        cut = qkv_columns(wq_raw)
        for k in range(X):
            wq_cut[k] = cut[k]
        wq_g.begin()
        sm_g.begin()
        xr_own = move(own_ref, xr.at[0, 0])
        xr_x = {d: put(own_ref, xr.at[0, -d % X], x=d) for d in range(1, X)}
        wo_g.begin()
        wu, wgt, wdn = Units(1, wu_o), Units(0, wg_o), Units(2, wd_o)
        for m, unit in ((0, wgt), (1, wu), (2, wdn)):
            raws[m + 1].wait()
            @pl.loop(0, depth // 32)
            def _(i, m=m):
                r = pl.ds(pl.multiple_of(i * 32, 32), 32)
                for h in range(ZH):
                    half[m, h, r] = raw[m, r, h * units : (h + 1) * units]

            if m < 2:
                unit.own_y()
        wgt.own_l()
        sm_g.along_z()
        wq_g.along_z()

        lens = [len_ref[0, j] for j in range(docs)]
        ends = []
        for j in range(docs):
            ends.append(lens[j] if j == 0 else ends[-1] + lens[j])

        def slot_base(dc, dx):
            return (at("x", dx) * C + at("c", dc)) * rows

        def doc_of(index):
            doc = jnp.zeros(index.shape, jnp.int32)
            first = jnp.zeros(index.shape, jnp.int32)
            for j in range(docs):
                past = (index >= ends[j]).astype(jnp.int32)
                doc = doc + past
                first = first + past * lens[j]
            return doc, index - first

        lane = lax.broadcasted_iota(jnp.int32, (rows, HEAD_WIDTH), 1)
        folded = jnp.where(lane >= HEAD_WIDTH // 2, lane - HEAD_WIDTH // 2, lane)
        freq = jnp.exp(folded.astype(F32) * (-2.0 * math.log(ROPE_BASE) / HEAD_WIDTH))
        sign = jnp.where(lane >= HEAD_WIDTH // 2, 1.0, -1.0)
        slots = [(dc, dx) for dc in range(C) for dx in range(X)]
        def slot_of(k):
            there = lax.rem(x + lax.rem(k, X), X) * C + lax.rem(c + lax.div(k, X), C)
            return there * rows

        @pl.loop(0, C * X)
        def _(k):
            r = pl.ds(pl.multiple_of(k * rows, rows), rows)
            index = slot_of(k) + lax.broadcasted_iota(jnp.int32, (rows, HEAD_WIDTH), 0)
            angle = doc_of(index)[1].astype(F32) * freq
            cos_s[r] = jnp.cos(angle)
            sin_s[r] = jnp.sin(angle) * sign
            k_index = slot_of(k) + lax.broadcasted_iota(jnp.int32, (rows, rows), 1)
            k_doc = doc_of(k_index)[0]
            for a in range(X):
                q_index = slot_base(0, a) + lax.broadcasted_iota(jnp.int32, (rows, rows), 0)
                q_doc = doc_of(q_index)[0]
                allowed = (q_doc == k_doc) & (k_index <= q_index)
                mask_s[a * rows : (a + 1) * rows, r] = jnp.where(allowed, 0.0, NEGATIVE_BIG)

        xr_own.wait()
        for d in xr_x:
            xr_x[d].wait_recv()
        xr_c = [
            put(xr.at[0, k], xr.at[-d % C, k], c=d) for d in range(1, C) for k in range(X)
        ]
        sm_g.along_h()
        wq_g.along_h()
        wo_g.along_z()
        wgt.begin()
        wu.begin()
        sm_g.along_y()
        wq_g.along_y()
        sm_g.along_c()
        wo_g.along_h()
        wdn.own_y()
        wgt.by_h[1].forward()
        wu.own_l()
        wq_g.along_c()
        sm_g.end()
        wu.by_h[1].forward()

        def spread_row(first, block, total):
            pieces = sm[...].reshape(devices, 8, 256)[:, 0, :].astype(BF)
            left = lax.broadcasted_iota(jnp.int32, (256, total), 0)
            right = lax.broadcasted_iota(jnp.int32, (256, total), 1)
            select = (lax.rem(right, block) + first == left).astype(BF)
            wide = nn(pieces, select)
            owner = lax.broadcasted_iota(jnp.int32, (devices, total), 0)
            place = lax.broadcasted_iota(jnp.int32, (devices, total), 1)
            inside = (place >= owner * block) & (place < (owner + 1) * block)
            return jnp.sum(jnp.where(inside, wide, 0.0), axis=0, keepdims=True)

        rows_s[0:1, :width] = spread_row(0, part, width)
        rows_s[1:2, :width] = spread_row(part, part, width)
        rows_s[2:3, :] = spread_row(2 * part, bias_part, QKV_WIDTH)

        for copy in xr_c:
            copy.wait_recv()
        gain_one = rows_s[0:1, :width]
        for k, (dc, dx) in enumerate(slots):
            @pl.loop(0, rows // 32)
            def _(i, k=k, dc=dc, dx=dx):
                v = xr[dc, dx, pl.ds(pl.multiple_of(i * 32, 32), 32)].astype(F32)
                r = lax.rsqrt(jnp.mean(v * v, axis=-1, keepdims=True) + EPSILON)
                to = pl.ds(pl.multiple_of(k * rows + i * 32, 32), 32)
                n1[to] = (v * r * gain_one).astype(BF)

        eye = (
            lax.broadcasted_iota(jnp.int32, (128, 128), 0)
            == lax.broadcasted_iota(jnp.int32, (128, 128), 1)
        ).astype(BF)

        def flip(read, dst, amount):
            @pl.loop(0, width // 128)
            def _(j):
                cols = pl.ds(pl.multiple_of(j * 128, 128), 128)
                dst[cols] = nt(eye, read(cols)).astype(BF)

        wq_g.end()
        outs = [move(w1, wqkv_o), move(rows_s, vec_o), move(cos_s, cos_o), move(sin_s, sin_o)]
        kv_at = lax.div(x * heads, QUERY_HEADS // KEY_VALUE_HEADS) * HEAD_WIDTH
        k_off = QUERY_HEADS * HEAD_WIDTH + kv_at
        v_off = k_off + KEY_VALUE_HEADS * HEAD_WIDTH
        def turn(v, first, amount):
            return v * cos_s[first : first + amount] + pltpu.roll(
                v, HEAD_WIDTH // 2, 1
            ) * sin_s[first : first + amount]

        def bias_at(start, amount):
            return rows_s[2:3, pl.ds(pl.multiple_of(start, 128), amount)]

        @pl.loop(0, heads)
        def _(h):
            cols = pl.ds(pl.multiple_of(h * HEAD_WIDTH, HEAD_WIDTH), HEAD_WIDTH)
            v = nn(n1[0:query_rows], w1[:, cols])
            v = v + bias_at(x * q_cols + h * HEAD_WIDTH, HEAD_WIDTH)
            qs[:, cols] = turn(v, 0, query_rows).astype(BF)

        for j in range(kv_heads):
            at_k = q_cols + j * HEAD_WIDTH
            v = nn(n1[...], w1[:, at_k : at_k + HEAD_WIDTH]) + bias_at(k_off, kv_cols)[
                :, j * HEAD_WIDTH : (j + 1) * HEAD_WIDTH
            ]
            kv[:, j * HEAD_WIDTH : (j + 1) * HEAD_WIDTH] = turn(v, 0, pack_rows).astype(BF)
        v = nn(n1[...], w1[:, q_cols + kv_cols :]) + bias_at(v_off, kv_cols)
        kv[:, kv_cols:] = v.astype(BF)
        outs += [move(qs, q_o), move(kv, kv_o)]
        wo_g.along_y()
        wgt.last(0)
        wgt.middle()
        wdn.begin()
        wdn.own_l()

        @pl.loop(0, heads)
        def _(h):
            cols = pl.ds(pl.multiple_of(h * HEAD_WIDTH, HEAD_WIDTH), HEAD_WIDTH)
            g = lax.div(h, share)
            k_h = kv[:, pl.ds(pl.multiple_of(g * HEAD_WIDTH, HEAD_WIDTH), HEAD_WIDTH)]
            v_h = kv[:, pl.ds(pl.multiple_of(kv_cols + g * HEAD_WIDTH, HEAD_WIDTH), HEAD_WIDTH)]
            s = nt(qs[:, cols], k_h) * scale + mask_s[...]
            e = jnp.exp(s - jnp.max(s, axis=-1, keepdims=True))
            p = (e / jnp.sum(e, axis=-1, keepdims=True)).astype(BF)
            ps[h] = p
            ob[:, cols] = nn(p, v_h).astype(BF)

        outs += [move(ps, p_o), move(ob, att_o)]
        wo_g.along_c()
        wo_g.end()
        outs.append(move(wo, wout_o))
        block = 256
        for d in list(range(1, X)) + [0]:
            @pl.loop(0, width // block)
            def _(j, d=d):
                cols = pl.ds(pl.multiple_of(j * block, block), block)
                v = nt(ob[d * rows : (d + 1) * rows], wo[cols])
                if d:
                    part_send[d - 1, :, cols] = v.astype(BF)
                else:
                    hs[:, cols] = v

            if d:
                part_recv_copy = put(part_send.at[d - 1], part_recv.at[d - 1], x=d)
                parts = [part_recv_copy] if d == 1 else parts + [part_recv_copy]
        wu.last(0)
        go_rows = Rows(go_v)
        go_rows.begin(cot_ref)
        for d in range(1, X):
            parts[d - 1].wait_recv()
        gain_two = rows_s[1:2, :width]

        @pl.loop(0, rows // 32)
        def _(i):
            r = pl.ds(pl.multiple_of(i * 32, 32), 32)
            h = hs[r] + xr[0, 0, r].astype(F32)
            for d in range(1, X):
                h = h + part_recv[d - 1, r].astype(F32)
            hs[r] = h
            inv = lax.rsqrt(jnp.mean(h * h, axis=-1, keepdims=True) + EPSILON)
            n2s[r] = (h * inv * gain_two).astype(BF)

        nr_rows = Rows(nr_v)
        nr_rows.begin(n2s)
        outs.append(move(hs, h_o))
        flip(lambda cols: n1[0:query_rows, cols], n1t, query_rows)
        outs.append(move(n1t, n1_o))
        wdn.by_h[1].forward()
        wgt.last(1)
        wu.middle()
        wu.last(1)
        nr_rows.along_x()
        go_rows.along_x()
        wdn.last(0, False)
        wdn.middle()
        nr_rows.to_core()
        nr_rows.end()
        outs.append(move(nr_v, nr_o))
        group_rows = C * ZH * X * rows
        flip(lambda cols: nr_v[:, :, :, :, cols].reshape(group_rows, 128), n2t, group_rows)
        outs.append(move(n2t, n2t_o))
        go_rows.to_core()
        wdn.last(1, False)
        go_rows.end()
        outs.append(move(go_v, go_o))
        wgt.end()
        wu.end()
        wdn.end()
        for copy in outs:
            copy.wait()
        for copy in sent:
            copy.wait_send()
        assert count[0] <= n_sems, count

    any_spec = pl.BlockSpec(memory_space=pl.ANY)
    whole = (ZH, ZL, Y, depth, units)
    group = (C, ZH, X, rows, width)
    sds = jax.ShapeDtypeStruct
    return pl.pallas_call(
        kernel,
        out_shape=[
            sds((width, qkv_n), BF), sds((width, q_cols), BF), sds((width, query_rows), BF),
            sds((width, C * ZH * X * rows), BF),
            sds((query_rows, q_cols), BF), sds((pack_rows, 2 * kv_cols), BF),
            sds((heads, query_rows, pack_rows), BF), sds((query_rows, q_cols), BF),
            sds((rows, width), F32), sds(group, BF), sds(group, BF),
            sds(whole, BF), sds(whole, BF), sds(whole, BF),
            sds((8, QKV_WIDTH), F32),
            sds((pack_rows, HEAD_WIDTH), F32), sds((pack_rows, HEAD_WIDTH), F32),
            sds((3, depth, units), BF),
        ],
        in_specs=[any_spec, any_spec, pl.BlockSpec(memory_space=pltpu.SMEM)] + [any_spec] * 6,
        out_specs=[any_spec] * 18,
        scratch_shapes=[
            pltpu.VMEM((C, X, rows, width), BF),
            pltpu.VMEM((width, qkv_n), BF),
            pltpu.VMEM((width, q_cols), BF),
            pltpu.VMEM((devices * 8, 256), F32),
            pltpu.VMEM((pack_rows, width), BF),
            pltpu.VMEM((query_rows, q_cols), BF),
            pltpu.VMEM((pack_rows, 2 * kv_cols), BF),
            pltpu.VMEM((query_rows, q_cols), BF),
            pltpu.VMEM((max(X - 1, 1), rows, width), BF),
            pltpu.VMEM((max(X - 1, 1), rows, width), BF),
            pltpu.VMEM((rows, width), BF),
            pltpu.VMEM((rows, width), F32),
            pltpu.VMEM((pack_rows, HEAD_WIDTH), F32),
            pltpu.VMEM((pack_rows, HEAD_WIDTH), F32),
            pltpu.VMEM((query_rows, pack_rows), F32),
            pltpu.VMEM((8, QKV_WIDTH), F32),
            pltpu.VMEM((heads, query_rows, pack_rows), BF),
            pltpu.VMEM((3,) + w_gate.shape, BF),
            pltpu.VMEM((3, ZH, depth, units), BF),
            pltpu.VMEM(w_qkv.shape, BF),
            pltpu.VMEM((X, part, qkv_n), BF),
            pltpu.VMEM((width, query_rows), BF),
            pltpu.VMEM((width, C * ZH * X * rows), BF),
            pltpu.VMEM(group, BF),
            pltpu.VMEM(group, BF),
            pltpu.SemaphoreType.DMA((n_sems,)),
            pltpu.SemaphoreType.DMA((n_sems,)),
            pltpu.SemaphoreType.DMA((32,)),
        ],
        compiler_params=pltpu.CompilerParams(
            collective_id=0, has_side_effects=True, vmem_limit_bytes=60 << 20
        ),
        name="front",
    )(own_in, cotangent, lengths, w_qkv, w_out, small, w_gate, w_up, w_down)


def forward_backward(normed, cotangent, w_gate, w_up, w_down):
    size = lax.axis_size
    ZH, ZL, Y, X, C = (size(a) for a in AXES)
    total, width = normed.shape
    depth, units = w_down.shape[-2:]
    step = 256

    def kernel(
        n_ref, g_ref, wg_ref, wu_ref, wd_ref,
        dg_o, du_o, dw_o, near_o, nt_o, ot_o,
        n_s, g_s, turned, wg, wu, wd, gates, ups, hidden, dg, du, dw, nt_s, ot_s,
        send_sem, recv_sem, local_sem, out_sem,
    ):
        here = dict(zip(AXES, (lax.axis_index(a) for a in AXES)))
        sizes = dict(zip(AXES, (ZH, ZL, Y, X, C)))

        def at(a, d):
            d = d % sizes[a]
            return lax.rem(here[a] + d, sizes[a]) if d else here[a]

        other = tuple(at(a, 1) if a == "y" else here[a] for a in AXES)
        barrier = pltpu.get_barrier_semaphore()
        pl.semaphore_signal(barrier, inc=1, device_id=other, device_id_type=MESH_ID)
        pl.semaphore_wait(barrier, 1)
        sent = []

        def put(src, dst):
            k = len(sent)
            copy = pltpu.make_async_remote_copy(
                src_ref=src, dst_ref=dst, send_sem=send_sem.at[k], recv_sem=recv_sem.at[k],
                device_id=other, device_id_type=MESH_ID,
            )
            copy.start()
            sent.append(copy)
            return copy

        count = [0]

        def move(src, dst):
            k = count[0]
            count[0] += 1
            copy = pltpu.make_async_copy(src, dst, local_sem.at[k])
            copy.start()
            return copy

        def row(a, b, e):
            start = pl.multiple_of(((a * ZL + b) * Y + e) * depth, depth)
            return pl.ds(start, depth)

        def at_rows(t):
            return pl.ds(pl.multiple_of(t * step, step), step)

        zh, zl, y = here["zh"], here["zl"], here["y"]
        loads = [move(n_ref, n_s), move(wg_ref, wg), move(wu_ref, wu), move(g_ref, g_s)]
        down = []
        for d in range(ZH):
            a = at("zh", d)
            for e in range(1, ZL):
                b = at("zl", e)
                down.append(put(wd_ref.at[a, b, y], wd.at[row(a, b, y)]))
                loads.append(move(wd_ref.at[a, b, y], wd.at[row(a, b, y)]))
            for e in range(Y):
                loads.append(move(wd_ref.at[a, zl, e], wd.at[row(a, zl, e)]))
        for copy in loads[:3]:
            copy.wait()

        @pl.loop(0, total // step)
        def _(t):
            r = at_rows(t)
            gate = nn(n_s[r], wg[...])
            up = nn(n_s[r], wu[...])
            gates[r] = gate
            ups[r] = up
            hidden[r] = (gate * jax.nn.sigmoid(gate) * up).astype(BF)

        loads[3].wait()
        eye = (
            lax.broadcasted_iota(jnp.int32, (128, 128), 0)
            == lax.broadcasted_iota(jnp.int32, (128, 128), 1)
        ).astype(BF)

        @pl.loop(0, width // 128)
        def _(j):
            cols = pl.ds(pl.multiple_of(j * 128, 128), 128)
            turned[cols] = nt(eye, g_s[:, cols]).astype(BF)

        def blocks(first, last):
            @pl.loop(first, last)
            def _(k):
                a = lax.rem(zh + lax.rem(k + 2, 4) // ZL, ZH)
                b = lax.rem(zl + lax.rem(k, ZL), ZL)
                e = lax.rem(y + 1 + k // 4, Y)
                at_block = row(a, b, e)
                dw[at_block] = nn(turned[at_block], hidden[...]).astype(BF)

        blocks(0, 2)
        for k in range(ZL):
            put(dw.at[row(at("zh", 1), at("zl", k), at("y", 1))], near_o.at[k])
        blocks(2, 8)
        outs = [move(dw, dw_o)]
        for copy in loads[4:]:
            copy.wait()
        for copy in down:
            copy.wait_recv()

        def stream(k, src, dst, r):
            pltpu.make_async_copy(src.at[r], dst.at[r], out_sem.at[k]).start()

        results = ((dg, dg_o), (du, du_o), (nt_s, nt_o), (ot_s, ot_o))

        @pl.loop(0, total // step)
        def _(t):
            r = at_rows(t)
            grad = nn(g_s[r], wd[...])
            ot_s[r] = nt(hidden[r], wd[...]).astype(BF)
            gate, up = gates[r], ups[r]
            sig = jax.nn.sigmoid(gate)
            low_g = (grad * up * sig * (1.0 + gate * (1.0 - sig))).astype(BF)
            low_u = (grad * gate * sig).astype(BF)
            dg[r] = low_g
            du[r] = low_u
            nt_s[r] = (nt(low_g, wg[...]) + nt(low_u, wu[...])).astype(BF)
            for k, (src, dst) in enumerate(results):
                stream(k, src, dst, r)

        for k, (src, dst) in enumerate(results):
            pltpu.make_async_copy(src, dst, out_sem.at[k]).wait()
        for copy in outs:
            copy.wait()
        for copy in sent[len(down) :]:
            copy.wait_recv()
        for copy in sent:
            copy.wait_send()

    any_spec = pl.BlockSpec(memory_space=pl.ANY)
    sds, vm = jax.ShapeDtypeStruct, pltpu.VMEM
    return pl.pallas_call(
        kernel,
        out_shape=[
            sds((total, units), BF), sds((total, units), BF), sds((width, units), BF),
            sds((ZL, depth, units), BF), sds((total, width), BF), sds((total, width), BF),
        ],
        in_specs=[any_spec] * 5,
        out_specs=[any_spec] * 6,
        scratch_shapes=[
            vm((total, width), BF), vm((total, width), BF), vm((width, total), BF),
            vm((width, units), BF), vm((width, units), BF), vm((width, units), BF),
            vm((total, units), F32), vm((total, units), F32), vm((total, units), BF),
            vm((total, units), BF), vm((total, units), BF), vm((width, units), BF),
            vm((total, width), BF), vm((total, width), BF),
            pltpu.SemaphoreType.DMA((8,)), pltpu.SemaphoreType.DMA((8,)),
            pltpu.SemaphoreType.DMA((16,)), pltpu.SemaphoreType.DMA((4,)),
        ],
        compiler_params=pltpu.CompilerParams(
            collective_id=2, has_side_effects=True, vmem_limit_bytes=62 << 20
        ),
        name="forward_backward",
    )(normed, cotangent, w_gate, w_up, w_down)


def back(
    grad_d, near_d, grad_g, grad_u, group_t, normed_terms, out_terms, middle, cotangent, own_in,
    wqkv, wout, normed, queries, kv_rows, probs, attended, vectors, cosine, sine,
):
    size = lax.axis_size
    ZH, ZL, Y, X, C = (size(a) for a in AXES)
    rows, width = own_in.shape
    qkv_n, q_cols = wqkv.shape[1], wout.shape[1]
    heads = q_cols // HEAD_WIDTH
    kv_cols = (qkv_n - q_cols) // 2
    kv_heads = kv_cols // HEAD_WIDTH
    share = heads // kv_heads
    query_rows, pack_rows = X * rows, C * X * rows
    depth, units = grad_d.shape[-2:]
    group_rows = group_t.shape[1]
    near = [(dh, dx) for dh in range(ZH) for dx in range(X)]
    far = [(dh, dl) for dh in range(ZH) for dl in range(ZL)]
    devices = ZH * ZL * Y * X * C
    part = width // devices
    zs = ZH * ZL
    scale = HEAD_WIDTH ** (-0.5)
    n_sems = 200

    blocks = {}
    for dx in range(X):
        for h in range(heads):
            blocks.setdefault(dx * heads + h, []).append((dx, h * HEAD_WIDTH))
        for j in range(kv_heads):
            head = dx * heads // (QUERY_HEADS // KEY_VALUE_HEADS) + j
            for at_kv, start in ((0, q_cols), (KEY_VALUE_HEADS, q_cols + kv_cols)):
                blocks.setdefault(QUERY_HEADS + at_kv + head, []).append(
                    (dx, start + j * HEAD_WIDTH)
                )
    qkv_layout = [(k * HEAD_WIDTH, b) for k, b in sorted(blocks.items())]
    out_layout = [(k * HEAD_WIDTH, b) for k, b in sorted(blocks.items()) if k < QUERY_HEADS]
    def kernel(
        gd_ref, dd_ref, gg_ref, gu_ref, gt_ref, nt_ref, ot_ref, mid_ref, cot_ref, in_ref,
        w1_ref, wo_ref, n1_ref, q_ref, kv_ref, p_ref, att_ref, vec_ref, cos_ref, sin_ref,
        lo_o, gi_o, dqkv_o, dout_o, vec_out, od_o, og_o, ou_o, relay,
        own_g, from_y, from_l, from_h, out_w, turned, units_t,
        half_n, half_o, from_c, from_n, hs, cots, ins, w1, wo, n1t, qs, kv, ps,
        atts, vec, cos_s, sin_s, da, dat, dos, dpre, dkv, dkv_low, dkv_in, dh_s,
        d_qkv, c_qkv, y_qkv, z_qkv, t_qkv, b_qkv, x_qkv,
        d_out, c_out, y_out, z_out, t_out, b_out, x_out, w_qkv_s, w_out_s,
        n_send, n_recv, lo_s, gi_s, vs, v_in, v_send,
        send_sem, recv_sem, local_sem,
    ):
        zh, zl, y, x, c = (lax.axis_index(a) for a in AXES)
        sizes = dict(zip(AXES, (ZH, ZL, Y, X, C)))
        here = dict(zip(AXES, (zh, zl, y, x, c)))

        def at(a, d):
            d = d % sizes[a]
            return lax.rem(here[a] + d, sizes[a]) if d else here[a]

        def device(**off):
            return tuple(at(a, off.get(a, 0)) for a in AXES)

        peers = set()
        for d in range(1, C):
            peers.add((0, 0, 0, 0, d))
        for dh, dx in near[1:]:
            peers.add((dh, 0, 0, dx, 0))
        for dh, dl in far[1:]:
            peers.add((dh, dl, 0, 0, 0))
        for d in range(1, Y):
            peers.add((0, 0, d, 0, 0))
        peers = sorted(peers)
        barrier = pltpu.get_barrier_semaphore()
        for peer in peers:
            pl.semaphore_signal(
                barrier, inc=1, device_id=device(**dict(zip(AXES, peer))), device_id_type=MESH_ID
            )
        pl.semaphore_wait(barrier, len(peers))

        count = [0, 0]
        sent = []

        def put(src, dst, **off):
            k = count[0]
            count[0] += 1
            copy = pltpu.make_async_remote_copy(
                src_ref=src, dst_ref=dst, send_sem=send_sem.at[k], recv_sem=recv_sem.at[k],
                device_id=device(**off), device_id_type=MESH_ID,
            )
            copy.start()
            sent.append(copy)
            return copy

        def move(src, dst):
            k = count[1]
            count[1] += 1
            copy = pltpu.make_async_copy(src, dst, local_sem.at[k])
            copy.start()
            return copy

        def by_rows(total, step, body):
            @pl.loop(0, total // step)
            def _(i):
                body(pl.ds(pl.multiple_of(i * step, step), step))

        inner = zh + zl == 1

        class Far:
            def __init__(self, src, dst, relay, onward):
                k = count[0]
                count[0] += 3
                self.relay, self.k = relay, k
                self.main = self.copy(src, dst, k, k, device(zh=1))
                self.step = self.copy(src, relay, k, k + 1, device(zl=1))
                self.onward = self.copy(relay, onward, k + 2, k, device(zh=1, zl=1))
                pl.when(inner)(self.main.start)
                pl.when(jnp.logical_not(inner))(self.step.start)
                sent.append(self)

            def copy(self, src, dst, k, r, to):
                return pltpu.make_async_remote_copy(
                    src_ref=src, dst_ref=dst, send_sem=send_sem.at[k], recv_sem=recv_sem.at[r],
                    device_id=to, device_id_type=MESH_ID,
                )

            def forward(self):
                @pl.when(inner)
                def _():
                    self.step.wait_recv()
                    self.onward.start()

            def wait_recv(self):
                self.main.wait_recv()

            def wait_send(self):
                self.main.wait_send()
                pl.when(inner)(self.onward.wait_send)

        class Units:
            def __init__(self, m, src):
                self.m, self.src = m, src
                self.by_y, self.own, self.by_l, self.by_h = {}, {}, {}, {}

            def begin(self, blocks, arrived=()):
                for dh, dl in blocks:
                    k = dh * ZL + dl
                    a, b = at("zh", dh), at("zl", dl)
                    if (dh, dl) in arrived:
                        self.by_y[dh, dl] = [move(dd_ref.at[arrived.index((dh, dl))], from_y.at[self.m, k, 0])]
                    else:
                        self.by_y[dh, dl] = [
                            put(self.src.at[a, b, at("y", d)], from_y.at[self.m, k, d - 1], y=d)
                            for d in range(1, Y)
                        ]
                    self.own[dh, dl] = move(self.src.at[a, b, y], own_g.at[self.m, k])

            def add_y(self, blocks):
                m = self.m
                for dh, dl in blocks:
                    k = dh * ZL + dl
                    self.own[dh, dl].wait()
                    for copy in self.by_y[dh, dl]:
                        if any(copy is other for other in sent):
                            copy.wait_recv()
                        else:
                            copy.wait()

                    def body(r, k=k):
                        v = own_g[m, k, r].astype(F32)
                        for d in range(1, Y):
                            v = v + from_y[m, k, d - 1, r].astype(F32)
                        own_g[m, k, r] = v.astype(BF)

                    by_rows(depth, 64, body)
                    if dl:
                        self.by_l[dh, dl] = put(
                            own_g.at[m, k], from_l.at[m, dh, dl - 1], zl=dl
                        )

            def add_l(self, far):
                m = self.m
                for dh in range(ZH - 1, 0, -1) if far else (0,):
                    for d in range(1, ZL):
                        self.by_l[dh, d].wait_recv()
                    if dh:
                        def body(r, dh=dh):
                            v = own_g[m, dh * ZL, r].astype(F32)
                            for d in range(1, ZL):
                                v = v + from_l[m, dh, d - 1, r].astype(F32)
                            own_g[m, dh * ZL, r] = v.astype(BF)

                        by_rows(depth, 64, body)
                        to = from_h.at[m, dh - 1]
                        self.by_h[dh] = Far(own_g.at[m, dh * ZL], to, relay.at[m], to)

            def half(self, h, r, cols=slice(None)):
                m = self.m
                v = own_g[m, 0, r, cols].astype(F32)
                for d in range(1, ZL):
                    v = v + from_l[m, 0, d - 1, r, cols].astype(F32)
                for d in range(1, ZH):
                    other = from_h[m, d - 1, r, cols].astype(F32)
                    v = jnp.where(lax.rem(zh + ZH - d, ZH) == h, other, v)
                return v

            def wait_h(self):
                for copy in self.by_h.values():
                    copy.wait_recv()

        def block(m, k, place_y):
            a = lax.rem(zh + k // ZL, ZH)
            b = lax.rem(zl + k % ZL, ZL)
            start = pl.multiple_of(((a * ZL + b) * Y + place_y) * depth, depth)
            return nn(turned[pl.ds(start, depth)], units_t[m])

        def compute_other(first, last):
            @pl.loop(2 * first, 2 * last)
            def _(i):
                m, k = lax.rem(i, 2), zs - 1 - lax.div(i, 2)
                a = lax.rem(zh + lax.div(k, ZL), ZH)
                b = lax.rem(zl + lax.rem(k, ZL), ZL)
                start = pl.multiple_of(((a * ZL + b) * Y + at("y", 1)) * depth, depth)
                own_g[m + 1, k] = nn(turned[pl.ds(start, depth)], units_t[m]).astype(BF)

        def send_block(u, k):
            u.by_y[k] = put(own_g.at[u.m, k], from_y.at[u.m, k, 0], y=1)

        def add_block(u, k):
            u.by_y[k].wait()
            sent[:] = [other for other in sent if other is not u.by_y[k]]
            v = block(u.m - 1, k, y) + from_y[u.m, k, 0].astype(F32)
            own_g[u.m, k] = v.astype(BF)
            if k % ZL:
                u.by_l[k // ZL, k % ZL] = put(
                    own_g.at[u.m, k], from_l.at[u.m, k // ZL, k % ZL - 1], zl=k % ZL
                )

        class Scatter:
            def __init__(self, dd, in_c, in_y, in_z, tt, tb, in_x, whole, out, layout):
                self.r = (dd, in_c, in_y, in_z, tt, tb, in_x)
                self.whole, self.out, self.layout = whole, out, layout

            def fill(self, left, right):
                dd = self.r[0]
                span = X * C * part

                @pl.loop(0, zs)
                def _(z):
                    for b in range(Y):
                        start = pl.multiple_of((z * Y + b) * span, span)
                        v = nn(left[pl.ds(start, span)], right[...]).astype(BF)
                        for dx in range(X):
                            for dc in range(C):
                                first = (dx * C + dc) * part
                                dd[dc, b, z, dx * part : (dx + 1) * part] = v[
                                    first : first + part
                                ]

            def to_c(self):
                dd, in_c = self.r[:2]
                self.by_c = {
                    (f, d): put(dd.at[at("c", d), at("y", f)], in_c.at[f, d - 1], c=d)
                    for f in list(range(1, Y)) + [0]
                    for d in range(1, C)
                }

            def to_y(self):
                dd, in_c, in_y = self.r[:3]
                self.by_y = []
                for f in list(range(1, Y)) + [0]:
                    for d in range(1, C):
                        self.by_c[f, d].wait_recv()
                    b = at("y", f)

                    @pl.loop(0, zs)
                    def _(z):
                        v = dd[c, b, z].astype(F32)
                        for d in range(1, C):
                            v = v + in_c[f, d - 1, z].astype(F32)
                        dd[c, b, z] = v.astype(BF)

                    if f:
                        self.by_y.append(put(dd.at[c, b], in_y.at[f - 1], y=f))

            def to_z(self):
                dd, in_c, in_y, in_z = self.r[:4]
                for copy in self.by_y:
                    copy.wait_recv()

                @pl.loop(0, zs)
                def _(z):
                    v = dd[c, y, z].astype(F32)
                    for f in range(1, Y):
                        v = v + in_y[f - 1, z].astype(F32)
                    dd[c, y, z] = v.astype(BF)

                self.by_l = {
                    (dh, d): put(
                        dd.at[c, y, at("zh", dh) * ZL + at("zl", d)],
                        in_z.at[dh * (ZL - 1) + d - 1],
                        zl=d,
                    )
                    for dh in range(ZH - 1, -1, -1)
                    for d in range(1, ZL)
                }

            def summed_l(self, dh):
                dd, in_z = self.r[0], self.r[3]
                v = dd[c, y, at("zh", dh) * ZL + zl].astype(F32)
                for d in range(1, ZL):
                    v = v + in_z[dh * (ZL - 1) + d - 1].astype(F32)
                return v

            def to_h(self):
                dd, in_z = self.r[0], self.r[3]
                for copy in self.by_l.values():
                    copy.wait_recv()
                self.by_h = []
                for dh in range(1, ZH):
                    place = at("zh", dh) * ZL + zl
                    dd[c, y, place] = self.summed_l(dh).astype(BF)
                    self.by_h.append(
                        put(dd.at[c, y, place], in_z.at[ZH * (ZL - 1) + dh - 1], zh=dh)
                    )

            def to_x(self):
                dd, in_c, in_y, in_z, tt, tb, in_x = self.r
                for copy in self.by_h:
                    copy.wait_recv()
                v = self.summed_l(0)
                for dh in range(1, ZH):
                    v = v + in_z[ZH * (ZL - 1) + dh - 1].astype(F32)
                for dx in range(X):
                    tt[dx] = v[dx * part : (dx + 1) * part]
                    tb[dx] = v[dx * part : (dx + 1) * part].astype(BF)
                self.by_x = [put(tb.at[at("x", d)], in_x.at[d - 1], x=d) for d in range(1, X)]

            def end(self):
                tt, in_x = self.r[4], self.r[6]
                for d in range(1, X):
                    self.by_x[d - 1].wait_recv()
                for d in range(1, X):
                    tt[at("x", -d)] = in_x[d - 1].astype(F32)
                for first, blocks in self.layout:
                    v = 0.0
                    for dx, start in blocks:
                        v = v + tt[dx, :, start : start + HEAD_WIDTH]
                    self.whole[:, first : first + HEAD_WIDTH] = v
                return move(self.whole, self.out)

        class Rows:
            def __init__(self, m, src, mine):
                self.m, self.mine = m, mine
                order = list(range(1, len(near))) + [0]
                self.by_c = {
                    (k, d): put(src.at[d, k], from_c.at[m, k, d - 1], c=d)
                    for k in order
                    for d in range(1, C)
                }
                self.own = move(src.at[0], mine)

            def summed(self, k, r):
                v = self.mine[k, r].astype(F32)
                for d in range(1, C):
                    v = v + from_c[self.m, k, d - 1, r].astype(F32)
                return v

            def spread(self):
                self.own.wait()
                self.by_n = []
                for k, (dh, dx) in enumerate(near):
                    for d in range(1, C):
                        if k:
                            self.by_c[k, d].wait_recv()
                    if k:
                        def body(r, k=k):
                            self.mine[k, r] = self.summed(k, r).astype(BF)

                        by_rows(rows, 32, body)
                        self.by_n.append(
                            put(self.mine.at[k], from_n.at[self.m, k - 1], zh=dh, x=dx)
                        )
                for d in range(1, C):
                    self.by_c[0, d].wait_recv()

            def spread_x(self):
                self.own.wait()
                self.by_n = {}
                for dh in reversed(range(ZH)):
                    for dx in range(1, X):
                        k = dh * X + dx
                        for d in range(1, C):
                            self.by_c[k, d].wait_recv()

                        def body(r, k=k):
                            self.mine[k, r] = self.summed(k, r).astype(BF)

                        by_rows(rows, 32, body)
                        to = from_n.at[self.m, dh * (X - 1) + dx - 1]
                        self.by_n[dh, dx] = put(self.mine.at[k], to, x=dx)

            def came_x(self, dh, r):
                v = self.summed(dh * X, r)
                for dx in range(1, X):
                    v = v + from_n[self.m, dh * (X - 1) + dx - 1, r].astype(F32)
                return v

            def relay(self):
                for dh in reversed(range(ZH)):
                    for d in range(1, C):
                        self.by_c[dh * X, d].wait_recv()
                    for dx in range(1, X):
                        self.by_n[dh, dx].wait_recv()
                    if dh:
                        def body(r, dh=dh):
                            self.mine[dh * X, r] = self.came_x(dh, r).astype(BF)

                        by_rows(rows, 32, body)
                        to = from_n.at[self.m, ZH * (X - 1) + dh - 1]
                        self.by_n[dh, 0] = put(self.mine.at[dh * X], to, zh=dh)

            def landed(self):
                for dh in range(1, ZH):
                    self.by_n[dh, 0].wait_recv()

            def final(self, r):
                v = self.came_x(0, r)
                for dh in range(1, ZH):
                    v = v + from_n[self.m, ZH * (X - 1) + dh - 1, r].astype(F32)
                return v

            def arrive(self):
                for copy in self.by_n:
                    copy.wait_recv()

            def total(self, r):
                v = self.summed(0, r)
                for k in range(1, len(near)):
                    v = v + from_n[self.m, k - 1, r].astype(F32)
                return v

        terms = Rows(0, nt_ref, half_n)
        loads = {
            "turned": move(gt_ref, turned),
            "g": move(gg_ref, units_t.at[0]),
            "u": move(gu_ref, units_t.at[1]),
        }
        for name, src, dst in (
            ("mid", mid_ref, hs), ("cot", cot_ref, cots), ("vec", vec_ref, vec),
            ("n1", n1_ref, n1t), ("wo", wo_ref, wo), ("kv", kv_ref, kv), ("p", p_ref, ps),
            ("att", att_ref, atts), ("q", q_ref, qs), ("cos", cos_ref, cos_s),
            ("sin", sin_ref, sin_s), ("w1", w1_ref, w1), ("in", in_ref, ins),
        ):
            loads[name] = move(src, dst)
        ud, ug, uu = Units(0, gd_ref), Units(1, None), Units(2, None)
        arrived = [(dh, dl) for dh, dl in far if dh]
        ud.begin(arrived[::-1] + [(0, 1)], arrived)
        outs_terms = Rows(1, ot_ref, half_o)

        eye = (
            lax.broadcasted_iota(jnp.int32, (128, 128), 0)
            == lax.broadcasted_iota(jnp.int32, (128, 128), 1)
        ).astype(BF)

        terms.spread_x()
        for name in ("turned", "g", "u", "n1"):
            loads[name].wait()
        compute_other(0, 2)
        for u in (ug, uu):
            for k in (3, 2):
                send_block(u, k)
        ud.add_y(arrived[::-1])
        compute_other(2, 4)
        terms.relay()
        add_block(ug, 3)
        ud.add_l(far=True)
        add_block(ug, 2)
        for name in ("mid", "cot", "vec"):
            loads[name].wait()
        gain_one, gain_two = vec[0:1, :width], vec[1:2, :width]
        terms.landed()
        vs[...] = jnp.zeros_like(vs)

        @pl.loop(0, rows // 32)
        def _(i):
            r = pl.ds(pl.multiple_of(i * 32, 32), 32)
            grad, h = terms.final(r), hs[r]
            inv = lax.rsqrt(jnp.mean(h * h, axis=-1, keepdims=True) + EPSILON)
            scaled = gain_two * grad
            v = (
                cots[r].astype(F32)
                + inv * scaled
                - h * (inv * inv * inv) * jnp.mean(scaled * h, axis=-1, keepdims=True)
            )
            dh_s[r] = v
            da[0, r] = v.astype(BF)
            vs[1:2, :width] = vs[1:2, :width] + jnp.sum(grad * h * inv, axis=0, keepdims=True)

        da_x = [put(da.at[0], da.at[-d % X], x=d) for d in range(1, X)]
        ud.by_h[1].forward()
        add_block(uu, 3)
        loads["wo"].wait()
        loads["att"].wait()
        for copy in da_x:
            copy.wait_recv()

        @pl.loop(0, heads // 2)
        def _(j):
            cols = pl.ds(pl.multiple_of(j * 256, 256), 256)
            for k in range(X):
                dos[k * rows : (k + 1) * rows, cols] = nn(da[k], wo[:, cols]).astype(BF)

        for k in range(X):
            for j in range(width // 128):
                cols = slice(j * 128, (j + 1) * 128)
                dat[cols, k * rows : (k + 1) * rows] = nt(eye, da[k, :, cols]).astype(BF)
        s_out = Scatter(d_out, c_out, y_out, z_out, t_out, b_out, x_out, w_out_s, dout_o, out_layout)
        s_out.fill(dat, atts)
        s_out.to_c()
        ug.add_l(far=True)
        add_block(uu, 2)
        ud.add_y([(0, 1)])
        for name in ("kv", "p", "q", "cos", "sin", "w1", "in"):
            loads[name].wait()
        dkv[...] = jnp.zeros_like(dkv)

        @pl.loop(0, heads)
        def _(h):
            cols = pl.ds(pl.multiple_of(h * HEAD_WIDTH, HEAD_WIDTH), HEAD_WIDTH)
            g = lax.div(h, share)
            k_at = pl.ds(pl.multiple_of(g * HEAD_WIDTH, HEAD_WIDTH), HEAD_WIDTH)
            v_at = pl.ds(pl.multiple_of(kv_cols + g * HEAD_WIDTH, HEAD_WIDTH), HEAD_WIDTH)
            p_low, do_h = ps[h], dos[:, cols]
            p = p_low.astype(F32)
            dp = nt(do_h, kv[:, v_at])
            delta = jnp.sum(p * dp, axis=-1, keepdims=True)
            ds = (p * (dp - delta)).astype(BF)
            dq = nn(ds, kv[:, k_at]) * scale
            dq = dq * cos_s[:query_rows] - pltpu.roll(dq, HEAD_WIDTH // 2, 1) * sin_s[:query_rows]
            dpre[:, cols] = dq.astype(BF)
            dkv[:, k_at] += tn(ds, qs[:, cols]) * scale
            dkv[:, v_at] += tn(p_low, do_h)

        kv_c = []
        for d in range(1, C):
            dkv_low[d - 1] = dkv[d * query_rows : (d + 1) * query_rows].astype(BF)
            kv_c.append(put(dkv_low.at[d - 1], dkv_in.at[d - 1], c=d))
        s_out.to_y()
        for copy in kv_c:
            copy.wait_recv()
        total = dkv[:query_rows]
        for d in range(1, C):
            total = total + dkv_in[d - 1].astype(F32)
        for j in range(kv_heads):
            cols = slice(j * HEAD_WIDTH, (j + 1) * HEAD_WIDTH)
            v = total[:, cols]
            v = v * cos_s[:query_rows] - pltpu.roll(v, HEAD_WIDTH // 2, 1) * sin_s[:query_rows]
            dpre[:, q_cols + j * HEAD_WIDTH : q_cols + (j + 1) * HEAD_WIDTH] = v.astype(BF)
        dpre[:, q_cols + kv_cols :] = total[:, kv_cols:].astype(BF)
        s_qkv = Scatter(d_qkv, c_qkv, y_qkv, z_qkv, t_qkv, b_qkv, x_qkv, w_qkv_s, dqkv_o, qkv_layout)
        s_qkv.fill(n1t, dpre)
        s_qkv.to_c()

        for k in list(range(1, X)) + [0]:
            @pl.loop(0, width // 256)
            def _(j, k=k):
                cols = pl.ds(pl.multiple_of(j * 256, 256), 256)
                v = nt(dpre[k * rows : (k + 1) * rows], w1[cols])
                if k:
                    n_send[k - 1, :, cols] = v.astype(BF)
                else:
                    gi_s[:, cols] = v

            if k:
                copy = put(n_send.at[k - 1], n_recv.at[k - 1], x=k)
                n_x = [copy] if k == 1 else n_x + [copy]
        kv_at = lax.div(x * heads, QUERY_HEADS // KEY_VALUE_HEADS) * HEAD_WIDTH
        k_off = QUERY_HEADS * HEAD_WIDTH + kv_at
        v_off = k_off + KEY_VALUE_HEADS * HEAD_WIDTH
        sums = jnp.sum(dpre[...].astype(F32), axis=0, keepdims=True)

        def place(start, first, amount):
            vs[2:3, pl.ds(pl.multiple_of(start, 128), amount)] = sums[:, first : first + amount]

        place(x * q_cols, 0, q_cols)
        place(k_off, q_cols, kv_cols)
        place(v_off, q_cols + kv_cols, kv_cols)
        s_qkv.to_y()
        for k in (1, 0):
            for u in (ug, uu):
                send_block(u, k)
        ud.begin([(0, 0)])
        ug.by_h[1].forward()
        s_out.to_z()
        outs_terms.spread_x()
        for copy in n_x:
            copy.wait_recv()

        @pl.loop(0, rows // 32)
        def _(i):
            r = pl.ds(pl.multiple_of(i * 32, 32), 32)
            grad, h = gi_s[r], ins[r].astype(F32)
            for d in range(1, X):
                grad = grad + n_recv[d - 1, r].astype(F32)
            inv = lax.rsqrt(jnp.mean(h * h, axis=-1, keepdims=True) + EPSILON)
            scaled = gain_one * grad
            gi_s[r] = (
                dh_s[r]
                + inv * scaled
                - h * (inv * inv * inv) * jnp.mean(scaled * h, axis=-1, keepdims=True)
            )
            vs[0:1, :width] = vs[0:1, :width] + jnp.sum(grad * h * inv, axis=0, keepdims=True)

        done = [move(gi_s, gi_o)]

        def put_out(u, out):
            u.wait_h()
            for h in range(ZH):
                def body(r, h=h):
                    out_w[u.m, r, h * units : (h + 1) * units] = u.half(h, r).astype(BF)

                by_rows(depth, 64, body)
            done.append(move(out_w.at[u.m], out))

        places = iter(range(V_IN))
        stages = iter(range(4))

        def small_stage(offsets):
            k = next(stages)
            v_send[k] = vs[...]
            return [(p, put(v_send.at[k], v_in.at[p], **off)) for off, p in zip(offsets, places)]

        def small_finish(copies):
            for p, copy in copies:
                copy.wait_recv()
                vs[...] = vs[...] + v_in[p]

        state = small_stage([dict(c=d) for d in range(1, C)])
        uu.add_l(far=True)
        small_finish(state)
        state = small_stage([dict(x=d) for d in range(1, X)])
        s_qkv.to_z()
        s_out.to_h()
        small_finish(state)
        state = small_stage([dict(y=d) for d in range(1, Y)])
        uu.by_h[1].forward()
        outs_terms.relay()
        add_block(ug, 1)
        s_qkv.to_h()
        add_block(uu, 1)
        s_out.to_x()
        small_finish(state)
        state = small_stage([dict(zh=dh, zl=dl) for dh, dl in far[1:]])
        outs_terms.landed()

        def finish(r):
            lo_s[r] = (hs[r] + outs_terms.final(r)).astype(BF)

        by_rows(rows, 32, finish)
        done.append(move(lo_s, lo_o))
        done.append(s_out.end())
        s_qkv.to_x()
        ud.add_l(far=False)
        ug.add_l(far=False)
        uu.add_l(far=False)
        small_finish(state)
        done.append(move(vs, vec_out))
        done.append(s_qkv.end())
        add_block(ug, 0)
        put_out(ug, og_o)
        add_block(uu, 0)
        put_out(uu, ou_o)
        ud.add_y([(0, 0)])
        put_out(ud, od_o)
        for copy in done:
            copy.wait()
        for copy in sent:
            copy.wait_send()
        assert count[0] <= n_sems and count[1] <= 64, count

    V_IN = (C - 1) + (X - 1) + (Y - 1) + (zs - 1)
    any_spec = pl.BlockSpec(memory_space=pl.ANY)
    sds = jax.ShapeDtypeStruct
    vm = pltpu.VMEM

    def scatter_scratch(n):
        return [
            vm((C, Y, zs, X * part, n), BF), vm((Y, max(C - 1, 1), zs, X * part, n), BF),
            vm((max(Y - 1, 1), zs, X * part, n), BF), vm((max(zs - 1, 1), X * part, n), BF),
            vm((X, part, n), F32), vm((X, part, n), BF), vm((max(X - 1, 1), part, n), BF),
        ]

    nk = len(near)
    return pl.pallas_call(
        kernel,
        out_shape=[
            sds((rows, width), BF), sds((rows, width), F32), sds((part, QKV_WIDTH), F32),
            sds((part, X * q_cols), F32), sds((8, QKV_WIDTH), F32),
            sds((depth, ZH * units), BF), sds((depth, ZH * units), BF),
            sds((depth, ZH * units), BF), sds((3, depth, units), BF),
        ],
        in_specs=[any_spec] * 20,
        out_specs=[any_spec] * 9,
        scratch_shapes=[
            vm((3, zs, depth, units), BF), vm((3, zs, max(Y - 1, 1), depth, units), BF),
            vm((3, ZH, max(ZL - 1, 1), depth, units), BF), vm((3, max(ZH - 1, 1), depth, units), BF),
            vm((3, depth, ZH * units), BF), vm((width, group_rows), BF), vm((2, group_rows, units), BF),
            vm((nk, rows, width), BF), vm((nk, rows, width), BF),
            vm((2, nk, max(C - 1, 1), rows, width), BF), vm((2, max(nk - 1, 1), rows, width), BF),
            vm((rows, width), F32), vm((rows, width), BF), vm((rows, width), BF),
            vm((width, qkv_n), BF), vm((width, q_cols), BF),
            vm((width, query_rows), BF), vm((query_rows, q_cols), BF),
            vm((pack_rows, 2 * kv_cols), BF), vm((heads, query_rows, pack_rows), BF),
            vm((query_rows, q_cols), BF), vm((8, QKV_WIDTH), F32),
            vm((pack_rows, HEAD_WIDTH), F32), vm((pack_rows, HEAD_WIDTH), F32),
            vm((X, rows, width), BF), vm((width, query_rows), BF), vm((query_rows, q_cols), BF),
            vm((query_rows, qkv_n), BF), vm((pack_rows, 2 * kv_cols), F32),
            vm((max(C - 1, 1), query_rows, 2 * kv_cols), BF),
            vm((max(C - 1, 1), query_rows, 2 * kv_cols), BF),
            vm((rows, width), F32),
        ]
        + scatter_scratch(qkv_n)
        + scatter_scratch(q_cols)
        + [
            vm((part, QKV_WIDTH), F32), vm((part, X * q_cols), F32),
            vm((max(X - 1, 1), rows, width), BF), vm((max(X - 1, 1), rows, width), BF),
            vm((rows, width), BF), vm((rows, width), F32), vm((8, QKV_WIDTH), F32),
            vm((max(V_IN, 1), 8, QKV_WIDTH), F32), vm((4, 8, QKV_WIDTH), F32),
            pltpu.SemaphoreType.DMA((n_sems,)), pltpu.SemaphoreType.DMA((n_sems,)),
            pltpu.SemaphoreType.DMA((64,)),
        ],
        compiler_params=pltpu.CompilerParams(
            collective_id=1, has_side_effects=True, vmem_limit_bytes=63 << 20
        ),
        name="back",
    )(
        grad_d, near_d, grad_g, grad_u, group_t, normed_terms, out_terms, middle, cotangent, own_in,
        wqkv, wout, normed, queries, kv_rows, probs, attended, vectors, cosine, sine,
    )


def finish(arrays, types):
    def spec(v):
        if v.shape[0] % 64 == 0:
            return pl.BlockSpec((v.shape[0] // 4,) + v.shape[1:], lambda i: (i,) + (0,) * (v.ndim - 1))
        return pl.BlockSpec(v.shape, lambda i: (0,) * v.ndim)

    def kernel(*refs):
        for src, dst in zip(refs[: len(arrays)], refs[len(arrays) :]):
            dst[...] = src[...].astype(dst.dtype)

    return pl.pallas_call(
        kernel,
        grid=(4,),
        out_shape=[jax.ShapeDtypeStruct(v.shape, t) for v, t in zip(arrays, types)],
        in_specs=[spec(v) for v in arrays],
        out_specs=[spec(v) for v in arrays],
        name="finish",
    )(*arrays)


def ff(normed, cotangent, w_gate, w_up, w_down):
    gate = nn(normed, w_gate)
    up_part = nn(normed, w_up)
    sig = jax.nn.sigmoid(gate)
    act = gate * sig
    hidden = (act * up_part).astype(BF)
    grad_wdown = tn(cotangent, hidden).astype(BF)
    grad_hidden = nn(cotangent, w_down)
    grad_gate = (grad_hidden * up_part * sig * (1.0 + gate * (1.0 - sig))).astype(BF)
    grad_up = (grad_hidden * act).astype(BF)
    grad_wgate = tn(normed, grad_gate).astype(BF)
    grad_wup = tn(normed, grad_up).astype(BF)
    normed_term = (nt(grad_gate, w_gate) + nt(grad_up, w_up)).astype(BF)
    out_term = nt(hidden, w_down).astype(BF)
    return hidden, grad_gate, grad_up, grad_wdown, grad_wgate, grad_wup, out_term, normed_term


def small_rows(gain_one, gain_two, bias):
    row = jnp.concatenate([gain_one, gain_two, bias]).astype(F32)
    return jnp.broadcast_to(jnp.pad(row, (0, -row.shape[0] % 256))[None], (8, 256))


def shards(
    layer_in, lengths, w_qkv, b_qkv, w_out, norm1_gain, norm2_gain, w_gate, w_up, w_down, grad_out
):
    size = lax.axis_size
    ZH, ZL, Y, X, C = (size(a) for a in ("zh", "zl", "y", "x", "c"))
    zh, zl, y, x, c = (lax.axis_index(a) for a in ("zh", "zl", "y", "x", "c"))
    everyone = ("zh", "zl", "y", "x", "c")
    devices = ZH * ZL * Y * X * C
    rows, width = layer_in.shape[1:]
    part = w_qkv.shape[0]
    group = QUERY_HEADS // KEY_VALUE_HEADS
    heads = QUERY_HEADS // X
    kv_heads = max(1, heads // group)
    share = heads // kv_heads
    q_cols, kv_cols = heads * HEAD_WIDTH, kv_heads * HEAD_WIDTH
    scale = HEAD_WIDTH ** (-0.5)

    own_in = layer_in[0]
    cotangent = grad_out[0]
    own_rows = own_in.astype(F32)
    query_rows, pack_rows = X * rows, C * X * rows
    bias_part = b_qkv.shape[0]
    def row_index(cores):
        spans = [
            (((x + dx) % X) * C + (c + dc) % C) * rows + jnp.arange(rows, dtype=jnp.int32)
            for dc in range(cores)
            for dx in range(X)
        ]
        return jnp.concatenate(spans)

    doc_lengths = lengths[0]
    key_index = row_index(C)
    key_doc, key_pos = doc_layout(key_index, doc_lengths)
    query_index, query_doc = key_index[:query_rows], key_doc[:query_rows]
    key_cos, key_sin = angles(key_pos)
    query_cos, query_sin = key_cos[:query_rows], key_sin[:query_rows]

    def gather_columns(pieces):
        held = ordered(
            [pick(pieces, x)] + [fetch(pick(pieces, (x - d) % X), "x", d) for d in range(1, X)],
            "x",
        )
        whole = jnp.zeros((ZH, ZL, Y) + held.shape, held.dtype)
        for dh in range(ZH):
            for dl in range(ZL):
                along = held if dh == dl == 0 else fetch(held, ("zh", "zl"), (dh, dl))
                for dy in range(Y):
                    piece = along if dy == 0 else fetch(along, "y", dy)
                    whole = lax.dynamic_update_slice(
                        whole,
                        piece[None, None, None],
                        ((zh + dh) % ZH, (zl + dl) % ZL, (y + dy) % Y, 0, 0, 0),
                    )
        whole = whole.reshape((ZH * ZL * Y * X,) + whole.shape[4:])
        both = ordered([whole] + [fetch(whole, "c", d) for d in range(1, C)], "c")
        return jnp.moveaxis(both, 0, 1).reshape(width, whole.shape[-1])

    def scatter_columns(grad):
        n = grad.shape[-1]
        grad = grad.astype(BF).reshape(ZH * ZL * Y * X, C, part, n)
        held = pick(grad, c, 1).astype(F32)
        for d in range(1, C):
            held = held + send(pick(grad, (c + d) % C, 1), "c", d)
        held = held.astype(BF).reshape(ZH, ZL, Y, X * part, n)
        kept = pick(held, y, 2).astype(F32)
        for d in range(1, Y):
            kept = kept + send(pick(held, (y + d) % Y, 2), "y", d)
        low = kept.astype(BF)
        total = 0.0
        for dh in range(ZH):
            for dl in range(ZL):
                if dh == dl == 0:
                    total = total + pick(pick(kept, zh), zl)
                else:
                    piece = pick(pick(low, (zh + dh) % ZH), (zl + dl) % ZL)
                    total = total + send(piece, ("zh", "zl"), (dh, dl)).astype(F32)
        total = total.reshape(X, part, n)
        lower = total.astype(BF)
        return ordered(
            [pick(total, x)]
            + [fetch(pick(lower, (x - d) % X), "x", d).astype(F32) for d in range(1, X)],
            "x",
        )

    def qkv_columns(array):
        blocks = []
        for at in range(X):
            kv = (at * heads) // group * HEAD_WIDTH
            key_at = QUERY_HEADS * HEAD_WIDTH + kv
            value_at = key_at + KEY_VALUE_HEADS * HEAD_WIDTH
            blocks.append(
                jnp.concatenate(
                    [
                        array[..., at * q_cols : (at + 1) * q_cols],
                        array[..., key_at : key_at + kv_cols],
                        array[..., value_at : value_at + kv_cols],
                    ],
                    axis=-1,
                )
            )
        return jnp.stack(blocks)

    def qkv_whole(blocks):
        queries = [blocks[at, ..., :q_cols] for at in range(X)]
        keys, values = [0.0] * KEY_VALUE_HEADS, [0.0] * KEY_VALUE_HEADS
        for at in range(X):
            for j in range(kv_heads):
                head = (at * heads) // group + j
                start = q_cols + j * HEAD_WIDTH
                keys[head] = keys[head] + blocks[at, ..., start : start + HEAD_WIDTH]
                start = start + kv_cols
                values[head] = values[head] + blocks[at, ..., start : start + HEAD_WIDTH]
        return jnp.concatenate(queries + keys + values, axis=-1)

    depth, units = w_gate.shape[0], w_gate.shape[1] // ZH

    def gather_units(weight):
        halves = weight.reshape(depth, ZH, units).transpose(1, 0, 2)
        whole = jnp.zeros((ZH, ZL, Y, depth, units), weight.dtype)
        for dh in range(ZH):
            first = pick(halves, zh) if dh == 0 else fetch(pick(halves, (zh - dh) % ZH), "zh", dh)
            for dl in range(ZL):
                second = first if dl == 0 else fetch(first, "zl", dl)
                for dy in range(Y):
                    third = second if dy == 0 else fetch(second, "y", dy)
                    whole = lax.dynamic_update_slice(
                        whole,
                        third[None, None, None],
                        ((zh + dh) % ZH, (zl + dl) % ZL, (y + dy) % Y, 0, 0),
                    )
        return whole.reshape(width, units)

    def scatter_units(grad):
        grad = grad.astype(BF).reshape(ZH, ZL, Y, depth, units)
        done = [None] * ZH
        for dh in reversed(range(ZH)):
            mine = pick(grad, (zh + dh) % ZH)
            kept = pick(mine, y, 1).astype(F32)
            for d in range(1, Y):
                kept = kept + send(pick(mine, (y + d) % Y, 1), "y", d).astype(F32)
            low = kept.astype(BF)
            total = pick(kept, zl)
            for d in range(1, ZL):
                total = total + send(pick(low, (zl + d) % ZL), "zl", d).astype(F32)
            done[dh] = total
        halves = [done[0]] + [
            send(done[dh].astype(BF), "zh", dh).astype(F32) for dh in range(1, ZH)
        ]
        halves = [halves[0]] + halves[:0:-1]
        return jnp.moveaxis(ordered(halves, "zh"), 0, 1).reshape(depth, ZH * units)

    near = [(dh, dx) for dh in range(ZH) for dx in range(X)]

    def gather_rows(own):
        held = jnp.concatenate([own if k == (0, 0) else fetch(own, ("zh", "x"), k) for k in near])
        return jnp.concatenate([held] + [fetch(held, "c", d) for d in range(1, C)])

    def scatter_rows(term):
        term = term.reshape(C, len(near), rows, width)
        held = term[0].astype(F32)
        for d in range(1, C):
            held = held + send(term[d].astype(BF), "c", d).astype(F32)
        total = held[0]
        for at, k in enumerate(near):
            if k != (0, 0):
                total = total + send(held[at].astype(BF), ("zh", "x"), k).astype(F32)
        return total

    def scatter_x(term):
        term = term.reshape(X, rows, width)
        total = term[0]
        for d in range(1, X):
            total = total + send(term[d].astype(BF), "x", d).astype(F32)
        return total

    if part % 16 == 0 and depth % 64 == 0 and heads % 2 == 0 and X > 1 and ZH == ZL == Y == 2:
        (
            wqkv_mine, wout_mine, normed_t, group_normed_t, queries, kv_low, probs_low,
            attended_low, middle, group_normed, group_cotangent, wgate_mine, wup_mine,
            wdown_part, vectors, cosine, sine, _,
        ) = front(
            own_in,
            cotangent,
            lengths,
            w_qkv,
            w_out.T,
            small_rows(norm1_gain, norm2_gain, b_qkv),
            w_gate,
            w_up,
            w_down.T,
            qkv_columns,
        )
        grad_gate, grad_up, grad_wdown, near_d, normed_term, out_term = forward_backward(
            group_normed.reshape(-1, width),
            group_cotangent.reshape(-1, width),
            wgate_mine.reshape(width, units),
            wup_mine.reshape(width, units),
            wdown_part,
        )
        whole = (ZH, ZL, Y, depth, units)
        terms = (C, ZH * X, rows, width)
        layer_out, grad_input, sum_wqkv, sum_wout, small, sum_wdown, sum_wgate, sum_wup, _ = back(
            grad_wdown.reshape(whole),
            near_d,
            grad_gate,
            grad_up,
            group_normed_t,
            normed_term.reshape(terms),
            out_term.reshape(terms),
            middle,
            cotangent,
            own_in,
            wqkv_mine,
            wout_mine,
            normed_t,
            queries,
            kv_low,
            probs_low,
            attended_low,
            vectors,
            cosine,
            sine,
        )
        place = (((zh * ZL + zl) * Y + y) * X + x) * C + c
        layer_out, grad_input, sum_wqkv, sum_wout, sum_wgate, sum_wup, sum_wdown = finish(
            (layer_out, grad_input, sum_wqkv, sum_wout, sum_wgate, sum_wup, sum_wdown),
            (BF,) + (F32,) * 6,
        )
        return (
            layer_out[None],
            grad_input[None],
            sum_wqkv,
            lax.dynamic_slice(small, (2, place * bias_part), (1, bias_part))[0],
            sum_wout.T,
            lax.dynamic_slice(small, (0, place * part), (1, part))[0],
            lax.dynamic_slice(small, (1, place * part), (1, part))[0],
            sum_wgate,
            sum_wup,
            sum_wdown.T,
        )

    small = jnp.concatenate([norm1_gain, norm2_gain, b_qkv])
    small = jnp.pad(small, (0, -small.shape[0] % 256))[None]
    small = lax.all_to_all(
        jnp.broadcast_to(small[None], (devices,) + small.shape), everyone, 0, 0, tiled=True
    )[:, 0].astype(F32)
    gain_one = small[:, :part].reshape(1, width)
    gain_two = small[:, part : 2 * part].reshape(1, width)
    bias = small[:, 2 * part : 2 * part + bias_part].reshape(-1)

    query_in = jnp.concatenate([own_in] + [fetch(own_in, "x", d) for d in range(1, X)])
    pack_in = jnp.concatenate([query_in] + [fetch(query_in, "c", d) for d in range(1, C)])

    wqkv_mine = gather_columns(qkv_columns(w_qkv))
    wout_t = w_out.T
    wout_mine = gather_columns(
        jnp.stack([wout_t[:, at * q_cols : (at + 1) * q_cols] for at in range(X)])
    )
    bias_mine = pick(qkv_columns(bias), x)

    wgate_mine, wup_mine = gather_units(w_gate), gather_units(w_up)
    wdown_mine = gather_units(w_down.T)

    group_cotangent = gather_rows(cotangent)

    pack_in = pack_in.astype(F32)
    normed_one = (pack_in * rms_parts(pack_in) * gain_one).astype(BF)
    query_normed = normed_one[:query_rows]
    pre_query = nn(query_normed, wqkv_mine[:, :q_cols]) + bias_mine[:q_cols]
    pre_kv = nn(normed_one, wqkv_mine[:, q_cols:]) + bias_mine[q_cols:]
    queries = rotate(
        pre_query.reshape(query_rows, heads, HEAD_WIDTH), query_cos, query_sin
    ).astype(BF)
    queries = queries.reshape(query_rows, kv_heads, share, HEAD_WIDTH)
    keys = rotate(
        pre_kv[:, :kv_cols].reshape(pack_rows, kv_heads, HEAD_WIDTH), key_cos, key_sin
    ).astype(BF)
    values = pre_kv[:, kv_cols:].reshape(pack_rows, kv_heads, HEAD_WIDTH).astype(BF)
    scores = jnp.einsum("tkgd,skd->kgts", queries, keys, preferred_element_type=F32) * scale
    allowed = (query_doc[:, None] == key_doc[None, :]) & (
        key_index[None, :] <= query_index[:, None]
    )
    masked = jnp.where(allowed, scores, NEGATIVE_BIG)
    top = jnp.max(masked, axis=-1, keepdims=True)
    weights = jnp.where(allowed, jnp.exp(masked - top), 0.0)
    probs = weights / jnp.sum(weights, axis=-1, keepdims=True)
    probs_low = probs.astype(BF)
    attended = jnp.einsum("kgts,skd->tkgd", probs_low, values, preferred_element_type=F32)
    attended_low = attended.reshape(query_rows, q_cols).astype(BF)
    middle = own_rows + scatter_x(nt(attended_low, wout_mine))
    normed_two = (middle * rms_parts(middle) * gain_two).astype(BF)

    group_normed = gather_rows(normed_two)

    hidden, grad_gate, grad_up, grad_wdown, grad_wgate, grad_wup, out_term, normed_term = ff(
        group_normed, group_cotangent, wgate_mine, wup_mine, wdown_mine
    )
    grad_normed_two = scatter_rows(normed_term)
    layer_out = (middle + scatter_rows(out_term)).astype(BF)
    sum_wdown = scatter_units(grad_wdown).T
    sum_wgate = scatter_units(grad_wgate)
    sum_wup = scatter_units(grad_wup)

    back_two, grad_gain_two = rms_back(middle, gain_two, grad_normed_two)
    grad_middle = cotangent.astype(F32) + back_two
    grad_att = grad_middle.astype(BF)
    query_grad_att = jnp.concatenate([grad_att] + [fetch(grad_att, "x", d) for d in range(1, X)])
    sum_wout = scatter_columns(tn(query_grad_att, attended_low))
    head_grads = nn(query_grad_att, wout_mine).astype(BF)
    head_grads = head_grads.reshape(query_rows, kv_heads, share, HEAD_WIDTH)
    grad_probs = jnp.einsum("tkgd,skd->kgts", head_grads, values, preferred_element_type=F32)
    probs = probs_low.astype(F32)
    delta = jnp.sum(probs * grad_probs, axis=-1, keepdims=True)
    grad_scores = (probs * (grad_probs - delta)).astype(BF)
    grad_query = (
        jnp.einsum("kgts,skd->tkgd", grad_scores, keys, preferred_element_type=F32) * scale
    )
    grad_key = jnp.einsum("kgts,tkgd->skd", grad_scores, queries, preferred_element_type=F32)
    grad_key = rotate(grad_key * scale, key_cos, -key_sin)
    grad_value = jnp.einsum("kgts,tkgd->skd", probs_low, head_grads, preferred_element_type=F32)
    grad_kv = jnp.concatenate(
        [grad_key.reshape(pack_rows, kv_cols), grad_value.reshape(pack_rows, kv_cols)], axis=1
    ).reshape(C, query_rows, 2 * kv_cols)
    kv_total = grad_kv[0]
    for d in range(1, C):
        kv_total = kv_total + send(grad_kv[d].astype(BF), "c", d).astype(F32)
    grad_query = rotate(
        grad_query.reshape(query_rows, heads, HEAD_WIDTH), query_cos, -query_sin
    ).reshape(query_rows, q_cols)
    grad_pre = jnp.concatenate([grad_query, kv_total], axis=1).astype(BF)
    sum_wqkv = qkv_whole(scatter_columns(tn(query_normed, grad_pre)))
    grad_bias = jnp.sum(grad_pre.astype(F32), axis=0)
    grad_normed_one = scatter_x(nt(grad_pre, wqkv_mine))
    back_one, grad_gain_one = rms_back(own_rows, gain_one, grad_normed_one)
    grad_input = grad_middle + back_one

    bias_blocks = jnp.where(
        jnp.arange(X, dtype=jnp.int32)[:, None] == x, grad_bias[None, :], 0.0
    )
    bias_whole = qkv_whole(bias_blocks)
    piece = jnp.concatenate(
        [
            grad_gain_one.reshape(devices, part),
            grad_gain_two.reshape(devices, part),
            bias_whole.reshape(devices, bias_part),
        ],
        axis=1,
    )
    piece = jnp.pad(piece, ((0, 0), (0, -piece.shape[1] % 256)))
    piece = jnp.sum(lax.all_to_all(piece[:, None], everyone, 0, 0, tiled=True)[:, 0], axis=0)
    return (
        layer_out[None],
        grad_input[None],
        sum_wqkv,
        piece[2 * part : 2 * part + bias_part],
        jnp.moveaxis(sum_wout, 0, 1).reshape(part, -1).T,
        piece[:part],
        piece[part : 2 * part],
        sum_wgate,
        sum_wup,
        sum_wdown,
    )


def solution(mesh):
    wide, narrow = mesh.shape["wide"], mesh.shape["narrow"]
    cores = 2 if narrow % 2 == 0 else 1
    along_x = narrow // cores
    along_y = along_x if wide % along_x == 0 else 1
    along_z = wide // along_y
    far = 2 if along_z % 2 == 0 else 1
    split = Mesh(
        mesh.devices.reshape(far, along_z // far, along_y, along_x, cores),
        ("zh", "zl", "y", "x", "c"),
    )
    w, n = ("zh", "zl", "y"), ("x", "c")
    placed = (
        P(w, n, None),
        P(w, None),
        P(w + n, None),
        P(w + n),
        P(None, w + n),
        P(w + n),
        P(w + n),
        P(w, n),
        P(w, n),
        P(n, w),
        P(w, n, None),
    )
    return jax.shard_map(
        shards,
        mesh=split,
        in_specs=placed,
        out_specs=(
            P(w, n, None),
            P(w, n, None),
            P(w + n, None),
            P(w + n),
            P(None, w + n),
            P(w + n),
            P(w + n),
            P(w, n),
            P(w, n),
            P(n, w),
        ),
        check_vma=False,
    )
```

```python
import math

import jax
import jax.numpy as jnp
from jax import lax
from jax.experimental import pallas as pl
from jax.experimental.pallas import tpu as pltpu
from jax.sharding import Mesh
from jax.sharding import PartitionSpec as P

QUERY_HEADS = 12
KEY_VALUE_HEADS = 2
HEAD_WIDTH = 128

EPSILON = 1e-06
ROPE_BASE = 10000.0
NEGATIVE_BIG = -1e30
HIGHEST = lax.Precision.HIGHEST


BF = jnp.bfloat16
F32 = jnp.float32
AXES = ("zh", "zl", "y", "x", "c")
MESH_ID = pl.DeviceIdType.MESH
QKV_WIDTH = (QUERY_HEADS + 2 * KEY_VALUE_HEADS) * HEAD_WIDTH


def fetch(value, axes, offsets):
    axes = (axes,) if isinstance(axes, str) else tuple(axes)
    offsets = (offsets,) if isinstance(offsets, int) else tuple(offsets)
    sizes = [lax.axis_size(a) for a in axes]
    total = math.prod(sizes)
    pairs = []
    for flat in range(total):
        rest, place = flat, []
        for size in reversed(sizes):
            place.append(rest % size)
            rest //= size
        place = place[::-1]
        source = 0
        for spot, off, size in zip(place, offsets, sizes):
            source = source * size + (spot + off) % size
        pairs.append((source, flat))
    return lax.ppermute(value, axes if len(axes) > 1 else axes[0], pairs)


def send(value, axes, offsets):
    offsets = (offsets,) if isinstance(offsets, int) else tuple(offsets)
    return fetch(value, axes, tuple(-o for o in offsets))


def pick(stack, place, axis=0):
    return lax.dynamic_index_in_dim(stack, place, axis, keepdims=False)


def nn(left, right):
    return lax.dot_general(left, right, (((1,), (0,)), ((), ())), preferred_element_type=F32)


def nt(left, right):
    return lax.dot_general(left, right, (((1,), (1,)), ((), ())), preferred_element_type=F32)


def tn(left, right):
    return lax.dot_general(left, right, (((0,), (0,)), ((), ())), preferred_element_type=F32)


def rms_parts(rows):
    return lax.rsqrt(jnp.mean(rows * rows, axis=-1, keepdims=True) + EPSILON)


def rms_back(rows, gain, grad):
    r = rms_parts(rows)
    scaled = gain * grad
    return (
        r * scaled - rows * (r * r * r) * jnp.mean(scaled * rows, axis=-1, keepdims=True),
        jnp.sum(grad * rows * r, axis=0),
    )


def doc_layout(index, doc_lengths):
    ends = jnp.cumsum(doc_lengths)
    starts = ends - doc_lengths
    document_index = jnp.sum((index[:, None] >= ends[None, :]).astype(jnp.int32), axis=1)
    onehot = (
        document_index[:, None] == jnp.arange(doc_lengths.shape[0], dtype=jnp.int32)[None, :]
    ).astype(jnp.int32)
    token_position = index - jnp.sum(onehot * starts[None, :], axis=1)
    return document_index, token_position.astype(F32)


def angles(position):
    half = HEAD_WIDTH // 2
    freq = jnp.exp(jnp.arange(half, dtype=F32) * (-2.0 * math.log(ROPE_BASE) / HEAD_WIDTH))
    angle = position[:, None] * freq[None, :]
    return jnp.cos(angle)[:, None, :], jnp.sin(angle)[:, None, :]


def rotate(rows, cosine, sine):
    half = HEAD_WIDTH // 2
    first, second = rows[..., :half], rows[..., half:]
    return jnp.concatenate(
        [first * cosine - second * sine, second * cosine + first * sine], axis=-1
    )


def ordered(pieces, axis):
    count, here = len(pieces), lax.axis_index(axis)
    if count == 1:
        return pieces[0][None]
    if count == 2:
        return jnp.where(here == 0, jnp.stack(pieces), jnp.stack(pieces[::-1]))
    whole = jnp.zeros((count,) + pieces[0].shape, pieces[0].dtype)
    for distance, piece in enumerate(pieces):
        whole = lax.dynamic_update_index_in_dim(whole, piece, (here + distance) % count, 0)
    return whole


def front(own_in, cotangent, lengths, w_qkv, w_out, small, w_gate, w_up, w_down, qkv_columns):
    size = lax.axis_size
    ZH, ZL, Y, X, C = (size(a) for a in AXES)
    rows, width = own_in.shape
    part = w_qkv.shape[0]
    q_cols = w_out.shape[1] // X
    qkv_n = qkv_columns(w_qkv).shape[-1]
    heads = q_cols // HEAD_WIDTH
    kv_cols = (qkv_n - q_cols) // 2
    kv_heads = kv_cols // HEAD_WIDTH
    share = heads // kv_heads
    query_rows, pack_rows = X * rows, C * X * rows
    depth = w_gate.shape[0]
    units = w_gate.shape[1] // ZH
    near = [(dh, dx) for dh in range(ZH) for dx in range(X)]
    far = [(dh, dl) for dh in range(ZH) for dl in range(ZL)]
    devices = ZH * ZL * Y * X * C
    bias_part = QKV_WIDTH // devices
    scale = HEAD_WIDTH ** (-0.5)
    docs = lengths.shape[-1]
    n_sems = 400

    def kernel(
        own_ref, cot_ref, len_ref, qkv_ref, out_ref, small_ref, g_ref, u_ref, d_ref,
        wqkv_o, wout_o, n1_o, n2t_o, q_o, kv_o, p_o, att_o, h_o, nr_o, go_o, wg_o, wu_o, wd_o, vec_o, cos_o, sin_o, relay,
        xr, w1, wo, sm, n1, qs, kv, ob, part_send, part_recv, n2s, hs,
        cos_s, sin_s, mask_s, rows_s, ps, raw, half, wq_raw, wq_cut, n1t, n2t, nr_v, go_v,
        send_sem, recv_sem, local_sem,
    ):
        zh, zl, y, x, c = (lax.axis_index(a) for a in AXES)
        sizes = dict(zip(AXES, (ZH, ZL, Y, X, C)))
        here = dict(zip(AXES, (zh, zl, y, x, c)))

        def device(**off):
            return tuple(
                lax.rem(here[a] + off[a], sizes[a]) if off.get(a, 0) % sizes[a] else here[a]
                for a in AXES
            )

        def at(a, d):
            d = d % sizes[a]
            return lax.rem(here[a] + d, sizes[a]) if d else here[a]

        peers = set()
        for d in range(1, C):
            peers.add((0, 0, 0, 0, d))
        for dh, dx in near[1:]:
            peers.add((dh, 0, 0, dx, 0))
        for dh, dl in far[1:]:
            peers.add((dh, dl, 0, 0, 0))
        for d in range(1, Y):
            peers.add((0, 0, d, 0, 0))
        peers = sorted(peers)
        barrier = pltpu.get_barrier_semaphore()
        for peer in peers:
            pl.semaphore_signal(
                barrier, inc=1, device_id=device(**dict(zip(AXES, peer))), device_id_type=MESH_ID
            )
        pl.semaphore_wait(barrier, len(peers))

        count = [0, 0]
        sent, local = [], []

        def put(src, dst, **off):
            k = count[0]
            count[0] += 1
            copy = pltpu.make_async_remote_copy(
                src_ref=src, dst_ref=dst, send_sem=send_sem.at[k], recv_sem=recv_sem.at[k],
                device_id=device(**off), device_id_type=MESH_ID,
            )
            copy.start()
            sent.append(copy)
            return copy

        def move(src, dst):
            k = count[1]
            count[1] += 1
            copy = pltpu.make_async_copy(src, dst, local_sem.at[k])
            copy.start()
            return copy

        inner = zh + zl == 1

        class Far:
            def __init__(self, src, dst, relay, onward):
                k = count[0]
                count[0] += 3
                self.relay, self.k = relay, k
                self.main = self.copy(src, dst, k, k, device(zh=1))
                self.step = self.copy(src, relay, k, k + 1, device(zl=1))
                self.onward = self.copy(relay, onward, k + 2, k, device(zh=1, zl=1))
                pl.when(inner)(self.main.start)
                pl.when(jnp.logical_not(inner))(self.step.start)
                sent.append(self)

            def copy(self, src, dst, k, r, to):
                return pltpu.make_async_remote_copy(
                    src_ref=src, dst_ref=dst, send_sem=send_sem.at[k], recv_sem=recv_sem.at[r],
                    device_id=to, device_id_type=MESH_ID,
                )

            def forward(self):
                @pl.when(inner)
                def _():
                    self.step.wait_recv()
                    self.onward.start()

            def wait_recv(self):
                self.main.wait_recv()

            def wait_send(self):
                self.main.wait_send()
                pl.when(inner)(self.onward.wait_send)

        class Gather:
            def __init__(self, buf, block, pieces):
                self.buf, self.block, self.pieces = buf, block, pieces

            def slot(self, dh, dl, dy, dx, dc):
                place = at("zh", dh)
                for a, d in (("zl", dl), ("y", dy), ("x", dx), ("c", dc)):
                    place = place * sizes[a] + at(a, d)
                start = pl.multiple_of(place * self.block, self.block)
                return self.buf.at[pl.ds(start, self.block)]

            def begin(self):
                self.own = move(self.pieces(x), self.slot(0, 0, 0, 0, 0))
                self.by_x = {
                    d: put(self.pieces(at("x", d)), self.slot(0, 0, 0, 0, 0), x=d)
                    for d in range(1, X)
                }

            def along_z(self):
                self.own.wait()
                for d in self.by_x:
                    self.by_x[d].wait_recv()
                self.by_h, self.by_l, self.by_y, self.by_c = {}, {}, {}, {}
                for dx in range(X):
                    s = self.slot(0, 0, 0, dx, 0)
                    for d in range(1, ZH):
                        self.by_h[d, dx] = put(s, s, zh=d)
                for dx in range(X):
                    self.along_l(0, dx)
                for dx in range(X):
                    self.spread(0, 0, dx)

            def along_l(self, dh, dx):
                s = self.slot(-dh, 0, 0, dx, 0)
                for d in range(1, ZL):
                    self.by_l[dh, d, dx] = put(s, s, zl=d)

            def spread(self, dh, dl, dx):
                s = self.slot(-dh, -dl, 0, dx, 0)
                for d in range(1, Y):
                    self.by_y[dh, dl, d, dx] = put(s, s, y=d)
                self.to_core(dh, dl, 0, dx)

            def to_core(self, dh, dl, dy, dx):
                s = self.slot(-dh, -dl, -dy, dx, 0)
                for d in range(1, C):
                    self.by_c[dh, dl, dy, d, dx] = put(s, s, c=d)

            def along_h(self):
                for d, dx in self.by_h:
                    self.by_h[d, dx].wait_recv()
                    self.along_l(d, dx)
                    self.spread(d, 0, dx)

            def along_y(self):
                for dh, dl, dx in self.by_l:
                    self.by_l[dh, dl, dx].wait_recv()
                    self.spread(dh, dl, dx)

            def along_c(self):
                for dh, dl in far:
                    for d in range(1, Y):
                        for dx in range(X):
                            self.by_y[dh, dl, d, dx].wait_recv()
                            self.to_core(dh, dl, d, dx)

            def end(self):
                for copy in self.by_c.values():
                    copy.wait_recv()

        class Units:
            def __init__(self, at_m, buf):
                self.m, self.buf = at_m, buf

            def slot(self, dh, dl, dy):
                return self.buf.at[at("zh", dh), at("zl", dl), at("y", dy)]

            def begin(self):
                mine = half.at[self.m, zh]
                s = self.slot(0, 0, 0)
                self.own = move(mine, s)
                self.by_h = {
                    1: Far(half.at[self.m, at("zh", 1)], s, relay.at[self.m], self.slot(0, 1, 0))
                }

            def own_l(self):
                self.by_l = {
                    (0, d): put(half.at[self.m, zh], self.slot(0, 0, 0), zl=d)
                    for d in range(1, ZL)
                }

            def own_y(self):
                self.by_y = {
                    (0, 0, d): put(half.at[self.m, zh], self.slot(0, 0, 0), y=d)
                    for d in range(1, Y)
                }

            def middle(self):
                for dh in self.by_h:
                    self.by_h[dh].wait_recv()
                    s = self.slot(-dh, 0, 0)
                    for d in range(1, ZL):
                        self.by_l[dh, d] = put(s, s, zl=d)
                    for d in range(1, Y):
                        self.by_y[dh, 0, d] = put(s, s, y=d)

            def last(self, dh, spread=True):
                for dl in range(1, ZL):
                    self.by_l[dh, dl].wait_recv()
                    s = self.slot(-dh, -dl, 0)
                    for d in range(1, Y) if spread else ():
                        self.by_y[dh, dl, d] = put(s, s, y=d)

            def end(self):
                self.own.wait()
                for copy in self.by_y.values():
                    copy.wait_recv()

        class Rows:
            def __init__(self, buf):
                self.buf = buf

            def begin(self, src):
                self.own = move(src, self.buf.at[0, 0, 0])
                self.by_h = {d: put(src, self.buf.at[0, -d % ZH, 0], zh=d) for d in range(1, ZH)}
                self.by_x = {(0, d): put(src, self.buf.at[0, 0, -d % X], x=d) for d in range(1, X)}
                self.by_c = [put(src, self.buf.at[-d % C, 0, 0], c=d) for d in range(1, C)]

            def spread(self, a, b):
                for d in range(1, C):
                    self.by_c.append(put(self.buf.at[0, a, b], self.buf.at[-d % C, a, b], c=d))

            def along_x(self):
                for dh in self.by_h:
                    self.by_h[dh].wait_recv()
                    a = -dh % ZH
                    for d in range(1, X):
                        self.by_x[dh, d] = put(self.buf.at[0, a, 0], self.buf.at[0, a, -d % X], x=d)
                    self.spread(a, 0)

            def to_core(self):
                for dh, d in self.by_x:
                    self.by_x[dh, d].wait_recv()
                    self.spread(-dh % ZH, -d % X)

            def end(self):
                self.own.wait()
                for copy in self.by_c:
                    copy.wait_recv()

        raws = [move(qkv_ref, wq_raw), move(g_ref, raw.at[0]), move(u_ref, raw.at[1])]
        raws.append(move(d_ref, raw.at[2]))

        def out_piece(to):
            return out_ref.at[:, pl.ds(pl.multiple_of(to * q_cols, 128), q_cols)]

        wq_g = Gather(w1, part, lambda to: wq_cut.at[to])
        wo_g = Gather(wo, part, out_piece)
        sm_g = Gather(sm, 8, lambda to: small_ref)
        raws[0].wait()
        cut = qkv_columns(wq_raw)
        for k in range(X):
            wq_cut[k] = cut[k]
        wq_g.begin()
        sm_g.begin()
        xr_own = move(own_ref, xr.at[0, 0])
        xr_x = {d: put(own_ref, xr.at[0, -d % X], x=d) for d in range(1, X)}
        wo_g.begin()
        wu, wgt, wdn = Units(1, wu_o), Units(0, wg_o), Units(2, wd_o)
        for m, unit in ((0, wgt), (1, wu), (2, wdn)):
            raws[m + 1].wait()
            @pl.loop(0, depth // 32)
            def _(i, m=m):
                r = pl.ds(pl.multiple_of(i * 32, 32), 32)
                for h in range(ZH):
                    half[m, h, r] = raw[m, r, h * units : (h + 1) * units]

            if m < 2:
                unit.own_y()
        wgt.own_l()
        sm_g.along_z()
        wq_g.along_z()

        lens = [len_ref[0, j] for j in range(docs)]
        ends = []
        for j in range(docs):
            ends.append(lens[j] if j == 0 else ends[-1] + lens[j])

        def slot_base(dc, dx):
            return (at("x", dx) * C + at("c", dc)) * rows

        def doc_of(index):
            doc = jnp.zeros(index.shape, jnp.int32)
            first = jnp.zeros(index.shape, jnp.int32)
            for j in range(docs):
                past = (index >= ends[j]).astype(jnp.int32)
                doc = doc + past
                first = first + past * lens[j]
            return doc, index - first

        lane = lax.broadcasted_iota(jnp.int32, (rows, HEAD_WIDTH), 1)
        folded = jnp.where(lane >= HEAD_WIDTH // 2, lane - HEAD_WIDTH // 2, lane)
        freq = jnp.exp(folded.astype(F32) * (-2.0 * math.log(ROPE_BASE) / HEAD_WIDTH))
        sign = jnp.where(lane >= HEAD_WIDTH // 2, 1.0, -1.0)
        slots = [(dc, dx) for dc in range(C) for dx in range(X)]
        def slot_of(k):
            there = lax.rem(x + lax.rem(k, X), X) * C + lax.rem(c + lax.div(k, X), C)
            return there * rows

        @pl.loop(0, C * X)
        def _(k):
            r = pl.ds(pl.multiple_of(k * rows, rows), rows)
            index = slot_of(k) + lax.broadcasted_iota(jnp.int32, (rows, HEAD_WIDTH), 0)
            angle = doc_of(index)[1].astype(F32) * freq
            cos_s[r] = jnp.cos(angle)
            sin_s[r] = jnp.sin(angle) * sign
            k_index = slot_of(k) + lax.broadcasted_iota(jnp.int32, (rows, rows), 1)
            k_doc = doc_of(k_index)[0]
            for a in range(X):
                q_index = slot_base(0, a) + lax.broadcasted_iota(jnp.int32, (rows, rows), 0)
                q_doc = doc_of(q_index)[0]
                allowed = (q_doc == k_doc) & (k_index <= q_index)
                mask_s[a * rows : (a + 1) * rows, r] = jnp.where(allowed, 0.0, NEGATIVE_BIG)

        xr_own.wait()
        for d in xr_x:
            xr_x[d].wait_recv()
        xr_c = [
            put(xr.at[0, k], xr.at[-d % C, k], c=d) for d in range(1, C) for k in range(X)
        ]
        sm_g.along_h()
        wq_g.along_h()
        wo_g.along_z()
        wgt.begin()
        wu.begin()
        sm_g.along_y()
        wq_g.along_y()
        sm_g.along_c()
        wo_g.along_h()
        wdn.own_y()
        wgt.by_h[1].forward()
        wu.own_l()
        wq_g.along_c()
        sm_g.end()
        wu.by_h[1].forward()

        def spread_row(first, block, total):
            pieces = sm[...].reshape(devices, 8, 256)[:, 0, :].astype(BF)
            left = lax.broadcasted_iota(jnp.int32, (256, total), 0)
            right = lax.broadcasted_iota(jnp.int32, (256, total), 1)
            select = (lax.rem(right, block) + first == left).astype(BF)
            wide = nn(pieces, select)
            owner = lax.broadcasted_iota(jnp.int32, (devices, total), 0)
            place = lax.broadcasted_iota(jnp.int32, (devices, total), 1)
            inside = (place >= owner * block) & (place < (owner + 1) * block)
            return jnp.sum(jnp.where(inside, wide, 0.0), axis=0, keepdims=True)

        rows_s[0:1, :width] = spread_row(0, part, width)
        rows_s[1:2, :width] = spread_row(part, part, width)
        rows_s[2:3, :] = spread_row(2 * part, bias_part, QKV_WIDTH)

        for copy in xr_c:
            copy.wait_recv()
        gain_one = rows_s[0:1, :width]
        for k, (dc, dx) in enumerate(slots):
            @pl.loop(0, rows // 32)
            def _(i, k=k, dc=dc, dx=dx):
                v = xr[dc, dx, pl.ds(pl.multiple_of(i * 32, 32), 32)].astype(F32)
                r = lax.rsqrt(jnp.mean(v * v, axis=-1, keepdims=True) + EPSILON)
                to = pl.ds(pl.multiple_of(k * rows + i * 32, 32), 32)
                n1[to] = (v * r * gain_one).astype(BF)

        eye = (
            lax.broadcasted_iota(jnp.int32, (128, 128), 0)
            == lax.broadcasted_iota(jnp.int32, (128, 128), 1)
        ).astype(BF)

        def flip(read, dst, amount):
            @pl.loop(0, width // 128)
            def _(j):
                cols = pl.ds(pl.multiple_of(j * 128, 128), 128)
                dst[cols] = nt(eye, read(cols)).astype(BF)

        wq_g.end()
        outs = [move(w1, wqkv_o), move(rows_s, vec_o), move(cos_s, cos_o), move(sin_s, sin_o)]
        kv_at = lax.div(x * heads, QUERY_HEADS // KEY_VALUE_HEADS) * HEAD_WIDTH
        k_off = QUERY_HEADS * HEAD_WIDTH + kv_at
        v_off = k_off + KEY_VALUE_HEADS * HEAD_WIDTH
        def turn(v, first, amount):
            return v * cos_s[first : first + amount] + pltpu.roll(
                v, HEAD_WIDTH // 2, 1
            ) * sin_s[first : first + amount]

        def bias_at(start, amount):
            return rows_s[2:3, pl.ds(pl.multiple_of(start, 128), amount)]

        @pl.loop(0, heads)
        def _(h):
            cols = pl.ds(pl.multiple_of(h * HEAD_WIDTH, HEAD_WIDTH), HEAD_WIDTH)
            v = nn(n1[0:query_rows], w1[:, cols])
            v = v + bias_at(x * q_cols + h * HEAD_WIDTH, HEAD_WIDTH)
            qs[:, cols] = turn(v, 0, query_rows).astype(BF)

        for j in range(kv_heads):
            at_k = q_cols + j * HEAD_WIDTH
            v = nn(n1[...], w1[:, at_k : at_k + HEAD_WIDTH]) + bias_at(k_off, kv_cols)[
                :, j * HEAD_WIDTH : (j + 1) * HEAD_WIDTH
            ]
            kv[:, j * HEAD_WIDTH : (j + 1) * HEAD_WIDTH] = turn(v, 0, pack_rows).astype(BF)
        v = nn(n1[...], w1[:, q_cols + kv_cols :]) + bias_at(v_off, kv_cols)
        kv[:, kv_cols:] = v.astype(BF)
        outs += [move(qs, q_o), move(kv, kv_o)]
        wo_g.along_y()
        wgt.last(0)
        wgt.middle()
        wdn.begin()
        wdn.own_l()

        @pl.loop(0, heads)
        def _(h):
            cols = pl.ds(pl.multiple_of(h * HEAD_WIDTH, HEAD_WIDTH), HEAD_WIDTH)
            g = lax.div(h, share)
            k_h = kv[:, pl.ds(pl.multiple_of(g * HEAD_WIDTH, HEAD_WIDTH), HEAD_WIDTH)]
            v_h = kv[:, pl.ds(pl.multiple_of(kv_cols + g * HEAD_WIDTH, HEAD_WIDTH), HEAD_WIDTH)]
            s = nt(qs[:, cols], k_h) * scale + mask_s[...]
            e = jnp.exp(s - jnp.max(s, axis=-1, keepdims=True))
            p = (e / jnp.sum(e, axis=-1, keepdims=True)).astype(BF)
            ps[h] = p
            ob[:, cols] = nn(p, v_h).astype(BF)

        outs += [move(ps, p_o), move(ob, att_o)]
        wo_g.along_c()
        wo_g.end()
        outs.append(move(wo, wout_o))
        block = 256
        for d in list(range(1, X)) + [0]:
            @pl.loop(0, width // block)
            def _(j, d=d):
                cols = pl.ds(pl.multiple_of(j * block, block), block)
                v = nt(ob[d * rows : (d + 1) * rows], wo[cols])
                if d:
                    part_send[d - 1, :, cols] = v.astype(BF)
                else:
                    hs[:, cols] = v

            if d:
                part_recv_copy = put(part_send.at[d - 1], part_recv.at[d - 1], x=d)
                parts = [part_recv_copy] if d == 1 else parts + [part_recv_copy]
        wu.last(0)
        go_rows = Rows(go_v)
        go_rows.begin(cot_ref)
        for d in range(1, X):
            parts[d - 1].wait_recv()
        gain_two = rows_s[1:2, :width]

        @pl.loop(0, rows // 32)
        def _(i):
            r = pl.ds(pl.multiple_of(i * 32, 32), 32)
            h = hs[r] + xr[0, 0, r].astype(F32)
            for d in range(1, X):
                h = h + part_recv[d - 1, r].astype(F32)
            hs[r] = h
            inv = lax.rsqrt(jnp.mean(h * h, axis=-1, keepdims=True) + EPSILON)
            n2s[r] = (h * inv * gain_two).astype(BF)

        nr_rows = Rows(nr_v)
        nr_rows.begin(n2s)
        outs.append(move(hs, h_o))
        flip(lambda cols: n1[0:query_rows, cols], n1t, query_rows)
        outs.append(move(n1t, n1_o))
        wdn.by_h[1].forward()
        wgt.last(1)
        wu.middle()
        wu.last(1)
        nr_rows.along_x()
        go_rows.along_x()
        wdn.last(0, False)
        wdn.middle()
        nr_rows.to_core()
        nr_rows.end()
        outs.append(move(nr_v, nr_o))
        group_rows = C * ZH * X * rows
        flip(lambda cols: nr_v[:, :, :, :, cols].reshape(group_rows, 128), n2t, group_rows)
        outs.append(move(n2t, n2t_o))
        go_rows.to_core()
        wdn.last(1, False)
        go_rows.end()
        outs.append(move(go_v, go_o))
        wgt.end()
        wu.end()
        wdn.end()
        for copy in outs:
            copy.wait()
        for copy in sent:
            copy.wait_send()
        assert count[0] <= n_sems, count

    any_spec = pl.BlockSpec(memory_space=pl.ANY)
    whole = (ZH, ZL, Y, depth, units)
    group = (C, ZH, X, rows, width)
    sds = jax.ShapeDtypeStruct
    return pl.pallas_call(
        kernel,
        out_shape=[
            sds((width, qkv_n), BF), sds((width, q_cols), BF), sds((width, query_rows), BF),
            sds((width, C * ZH * X * rows), BF),
            sds((query_rows, q_cols), BF), sds((pack_rows, 2 * kv_cols), BF),
            sds((heads, query_rows, pack_rows), BF), sds((query_rows, q_cols), BF),
            sds((rows, width), F32), sds(group, BF), sds(group, BF),
            sds(whole, BF), sds(whole, BF), sds(whole, BF),
            sds((8, QKV_WIDTH), F32),
            sds((pack_rows, HEAD_WIDTH), F32), sds((pack_rows, HEAD_WIDTH), F32),
            sds((3, depth, units), BF),
        ],
        in_specs=[any_spec, any_spec, pl.BlockSpec(memory_space=pltpu.SMEM)] + [any_spec] * 6,
        out_specs=[any_spec] * 18,
        scratch_shapes=[
            pltpu.VMEM((C, X, rows, width), BF),
            pltpu.VMEM((width, qkv_n), BF),
            pltpu.VMEM((width, q_cols), BF),
            pltpu.VMEM((devices * 8, 256), F32),
            pltpu.VMEM((pack_rows, width), BF),
            pltpu.VMEM((query_rows, q_cols), BF),
            pltpu.VMEM((pack_rows, 2 * kv_cols), BF),
            pltpu.VMEM((query_rows, q_cols), BF),
            pltpu.VMEM((max(X - 1, 1), rows, width), BF),
            pltpu.VMEM((max(X - 1, 1), rows, width), BF),
            pltpu.VMEM((rows, width), BF),
            pltpu.VMEM((rows, width), F32),
            pltpu.VMEM((pack_rows, HEAD_WIDTH), F32),
            pltpu.VMEM((pack_rows, HEAD_WIDTH), F32),
            pltpu.VMEM((query_rows, pack_rows), F32),
            pltpu.VMEM((8, QKV_WIDTH), F32),
            pltpu.VMEM((heads, query_rows, pack_rows), BF),
            pltpu.VMEM((3,) + w_gate.shape, BF),
            pltpu.VMEM((3, ZH, depth, units), BF),
            pltpu.VMEM(w_qkv.shape, BF),
            pltpu.VMEM((X, part, qkv_n), BF),
            pltpu.VMEM((width, query_rows), BF),
            pltpu.VMEM((width, C * ZH * X * rows), BF),
            pltpu.VMEM(group, BF),
            pltpu.VMEM(group, BF),
            pltpu.SemaphoreType.DMA((n_sems,)),
            pltpu.SemaphoreType.DMA((n_sems,)),
            pltpu.SemaphoreType.DMA((32,)),
        ],
        compiler_params=pltpu.CompilerParams(
            collective_id=0, has_side_effects=True, vmem_limit_bytes=60 << 20
        ),
        name="front",
    )(own_in, cotangent, lengths, w_qkv, w_out, small, w_gate, w_up, w_down)


def forward_backward(normed, cotangent, w_gate, w_up, w_down):
    size = lax.axis_size
    ZH, ZL, Y, X, C = (size(a) for a in AXES)
    total, width = normed.shape
    depth, units = w_down.shape[-2:]
    step = 256

    def kernel(
        n_ref, g_ref, wg_ref, wu_ref, wd_ref,
        dg_o, du_o, dw_o, near_o, nt_o, ot_o,
        n_s, g_s, turned, wg, wu, wd, gates, ups, hidden, dg, du, dw, nt_s, ot_s,
        send_sem, recv_sem, local_sem, out_sem,
    ):
        here = dict(zip(AXES, (lax.axis_index(a) for a in AXES)))
        sizes = dict(zip(AXES, (ZH, ZL, Y, X, C)))

        def at(a, d):
            d = d % sizes[a]
            return lax.rem(here[a] + d, sizes[a]) if d else here[a]

        other = tuple(at(a, 1) if a == "y" else here[a] for a in AXES)
        barrier = pltpu.get_barrier_semaphore()
        pl.semaphore_signal(barrier, inc=1, device_id=other, device_id_type=MESH_ID)
        pl.semaphore_wait(barrier, 1)
        sent = []

        def put(src, dst):
            k = len(sent)
            copy = pltpu.make_async_remote_copy(
                src_ref=src, dst_ref=dst, send_sem=send_sem.at[k], recv_sem=recv_sem.at[k],
                device_id=other, device_id_type=MESH_ID,
            )
            copy.start()
            sent.append(copy)
            return copy

        count = [0]

        def move(src, dst):
            k = count[0]
            count[0] += 1
            copy = pltpu.make_async_copy(src, dst, local_sem.at[k])
            copy.start()
            return copy

        def row(a, b, e):
            start = pl.multiple_of(((a * ZL + b) * Y + e) * depth, depth)
            return pl.ds(start, depth)

        def at_rows(t):
            return pl.ds(pl.multiple_of(t * step, step), step)

        zh, zl, y = here["zh"], here["zl"], here["y"]
        loads = [move(n_ref, n_s), move(wg_ref, wg), move(wu_ref, wu), move(g_ref, g_s)]
        down = []
        for d in range(ZH):
            a = at("zh", d)
            for e in range(1, ZL):
                b = at("zl", e)
                down.append(put(wd_ref.at[a, b, y], wd.at[row(a, b, y)]))
                loads.append(move(wd_ref.at[a, b, y], wd.at[row(a, b, y)]))
            for e in range(Y):
                loads.append(move(wd_ref.at[a, zl, e], wd.at[row(a, zl, e)]))
        for copy in loads[:2]:
            copy.wait()

        @pl.loop(0, total // step)
        def _(t):
            r = at_rows(t)
            gates[r] = nn(n_s[r], wg[...])

        loads[2].wait()

        @pl.loop(0, total // step)
        def _(t):
            r = at_rows(t)
            up = nn(n_s[r], wu[...])
            gate = gates[r]
            ups[r] = up
            hidden[r] = (gate * jax.nn.sigmoid(gate) * up).astype(BF)

        loads[3].wait()
        eye = (
            lax.broadcasted_iota(jnp.int32, (128, 128), 0)
            == lax.broadcasted_iota(jnp.int32, (128, 128), 1)
        ).astype(BF)

        @pl.loop(0, width // 128)
        def _(j):
            cols = pl.ds(pl.multiple_of(j * 128, 128), 128)
            turned[cols] = nt(eye, g_s[:, cols]).astype(BF)

        def blocks(first, last):
            @pl.loop(first, last)
            def _(k):
                a = lax.rem(zh + lax.rem(k + 2, 4) // ZL, ZH)
                b = lax.rem(zl + lax.rem(k, ZL), ZL)
                e = lax.rem(y + 1 + k // 4, Y)
                at_block = row(a, b, e)
                dw[at_block] = nn(turned[at_block], hidden[...]).astype(BF)

        blocks(0, 2)
        for k in range(ZL):
            put(dw.at[row(at("zh", 1), at("zl", k), at("y", 1))], near_o.at[k])
        blocks(2, 8)
        outs = [move(dw, dw_o)]
        for copy in loads[4:]:
            copy.wait()
        for copy in down:
            copy.wait_recv()

        def stream(k, src, dst, r):
            pltpu.make_async_copy(src.at[r], dst.at[r], out_sem.at[k]).start()

        results = ((dg, dg_o), (du, du_o), (nt_s, nt_o), (ot_s, ot_o))

        @pl.loop(0, total // step)
        def _(t):
            r = at_rows(t)
            grad = nn(g_s[r], wd[...])
            ot_s[r] = nt(hidden[r], wd[...]).astype(BF)
            gate, up = gates[r], ups[r]
            sig = jax.nn.sigmoid(gate)
            low_g = (grad * up * sig * (1.0 + gate * (1.0 - sig))).astype(BF)
            low_u = (grad * gate * sig).astype(BF)
            dg[r] = low_g
            du[r] = low_u
            nt_s[r] = (nt(low_g, wg[...]) + nt(low_u, wu[...])).astype(BF)
            for k, (src, dst) in enumerate(results):
                stream(k, src, dst, r)

        for k, (src, dst) in enumerate(results):
            pltpu.make_async_copy(src, dst, out_sem.at[k]).wait()
        for copy in outs:
            copy.wait()
        for copy in sent[len(down) :]:
            copy.wait_recv()
        for copy in sent:
            copy.wait_send()

    any_spec = pl.BlockSpec(memory_space=pl.ANY)
    sds, vm = jax.ShapeDtypeStruct, pltpu.VMEM
    return pl.pallas_call(
        kernel,
        out_shape=[
            sds((total, units), BF), sds((total, units), BF), sds((width, units), BF),
            sds((ZL, depth, units), BF), sds((total, width), BF), sds((total, width), BF),
        ],
        in_specs=[any_spec] * 5,
        out_specs=[any_spec] * 6,
        scratch_shapes=[
            vm((total, width), BF), vm((total, width), BF), vm((width, total), BF),
            vm((width, units), BF), vm((width, units), BF), vm((width, units), BF),
            vm((total, units), F32), vm((total, units), F32), vm((total, units), BF),
            vm((total, units), BF), vm((total, units), BF), vm((width, units), BF),
            vm((total, width), BF), vm((total, width), BF),
            pltpu.SemaphoreType.DMA((8,)), pltpu.SemaphoreType.DMA((8,)),
            pltpu.SemaphoreType.DMA((16,)), pltpu.SemaphoreType.DMA((4,)),
        ],
        compiler_params=pltpu.CompilerParams(
            collective_id=2, has_side_effects=True, vmem_limit_bytes=62 << 20
        ),
        name="forward_backward",
    )(normed, cotangent, w_gate, w_up, w_down)


def back(
    grad_d, near_d, grad_g, grad_u, group_t, normed_terms, out_terms, middle, cotangent, own_in,
    wqkv, wout, normed, queries, kv_rows, probs, attended, vectors, cosine, sine,
):
    size = lax.axis_size
    ZH, ZL, Y, X, C = (size(a) for a in AXES)
    rows, width = own_in.shape
    qkv_n, q_cols = wqkv.shape[1], wout.shape[1]
    heads = q_cols // HEAD_WIDTH
    kv_cols = (qkv_n - q_cols) // 2
    kv_heads = kv_cols // HEAD_WIDTH
    share = heads // kv_heads
    query_rows, pack_rows = X * rows, C * X * rows
    depth, units = grad_d.shape[-2:]
    group_rows = group_t.shape[1]
    near = [(dh, dx) for dh in range(ZH) for dx in range(X)]
    far = [(dh, dl) for dh in range(ZH) for dl in range(ZL)]
    devices = ZH * ZL * Y * X * C
    part = width // devices
    zs = ZH * ZL
    scale = HEAD_WIDTH ** (-0.5)
    n_sems = 200

    blocks = {}
    for dx in range(X):
        for h in range(heads):
            blocks.setdefault(dx * heads + h, []).append((dx, h * HEAD_WIDTH))
        for j in range(kv_heads):
            head = dx * heads // (QUERY_HEADS // KEY_VALUE_HEADS) + j
            for at_kv, start in ((0, q_cols), (KEY_VALUE_HEADS, q_cols + kv_cols)):
                blocks.setdefault(QUERY_HEADS + at_kv + head, []).append(
                    (dx, start + j * HEAD_WIDTH)
                )
    qkv_layout = [(k * HEAD_WIDTH, b) for k, b in sorted(blocks.items())]
    out_layout = [(k * HEAD_WIDTH, b) for k, b in sorted(blocks.items()) if k < QUERY_HEADS]
    def kernel(
        gd_ref, dd_ref, gg_ref, gu_ref, gt_ref, nt_ref, ot_ref, mid_ref, cot_ref, in_ref,
        w1_ref, wo_ref, n1_ref, q_ref, kv_ref, p_ref, att_ref, vec_ref, cos_ref, sin_ref,
        lo_o, gi_o, dqkv_o, dout_o, vec_out, od_o, og_o, ou_o, relay,
        own_g, from_y, from_l, from_h, out_w, turned, units_t,
        half_n, half_o, from_c, from_n, hs, cots, ins, w1, wo, n1t, qs, kv, ps,
        atts, vec, cos_s, sin_s, da, dat, dos, dpre, dkv, dkv_low, dkv_in, dh_s,
        d_qkv, c_qkv, y_qkv, z_qkv, t_qkv, b_qkv, x_qkv,
        d_out, c_out, y_out, z_out, t_out, b_out, x_out, w_qkv_s, w_out_s,
        n_send, n_recv, lo_s, gi_s, vs, v_in, v_send,
        send_sem, recv_sem, local_sem,
    ):
        zh, zl, y, x, c = (lax.axis_index(a) for a in AXES)
        sizes = dict(zip(AXES, (ZH, ZL, Y, X, C)))
        here = dict(zip(AXES, (zh, zl, y, x, c)))

        def at(a, d):
            d = d % sizes[a]
            return lax.rem(here[a] + d, sizes[a]) if d else here[a]

        def device(**off):
            return tuple(at(a, off.get(a, 0)) for a in AXES)

        peers = set()
        for d in range(1, C):
            peers.add((0, 0, 0, 0, d))
        for dh, dx in near[1:]:
            peers.add((dh, 0, 0, dx, 0))
        for dh, dl in far[1:]:
            peers.add((dh, dl, 0, 0, 0))
        for d in range(1, Y):
            peers.add((0, 0, d, 0, 0))
        peers = sorted(peers)
        barrier = pltpu.get_barrier_semaphore()
        for peer in peers:
            pl.semaphore_signal(
                barrier, inc=1, device_id=device(**dict(zip(AXES, peer))), device_id_type=MESH_ID
            )
        pl.semaphore_wait(barrier, len(peers))

        count = [0, 0]
        sent = []

        def put(src, dst, **off):
            k = count[0]
            count[0] += 1
            copy = pltpu.make_async_remote_copy(
                src_ref=src, dst_ref=dst, send_sem=send_sem.at[k], recv_sem=recv_sem.at[k],
                device_id=device(**off), device_id_type=MESH_ID,
            )
            copy.start()
            sent.append(copy)
            return copy

        def move(src, dst):
            k = count[1]
            count[1] += 1
            copy = pltpu.make_async_copy(src, dst, local_sem.at[k])
            copy.start()
            return copy

        def by_rows(total, step, body):
            @pl.loop(0, total // step)
            def _(i):
                body(pl.ds(pl.multiple_of(i * step, step), step))

        inner = zh + zl == 1

        class Far:
            def __init__(self, src, dst, relay, onward):
                k = count[0]
                count[0] += 3
                self.relay, self.k = relay, k
                self.main = self.copy(src, dst, k, k, device(zh=1))
                self.step = self.copy(src, relay, k, k + 1, device(zl=1))
                self.onward = self.copy(relay, onward, k + 2, k, device(zh=1, zl=1))
                pl.when(inner)(self.main.start)
                pl.when(jnp.logical_not(inner))(self.step.start)
                sent.append(self)

            def copy(self, src, dst, k, r, to):
                return pltpu.make_async_remote_copy(
                    src_ref=src, dst_ref=dst, send_sem=send_sem.at[k], recv_sem=recv_sem.at[r],
                    device_id=to, device_id_type=MESH_ID,
                )

            def forward(self):
                @pl.when(inner)
                def _():
                    self.step.wait_recv()
                    self.onward.start()

            def wait_recv(self):
                self.main.wait_recv()

            def wait_send(self):
                self.main.wait_send()
                pl.when(inner)(self.onward.wait_send)

        class Units:
            def __init__(self, m, src):
                self.m, self.src = m, src
                self.by_y, self.own, self.by_l, self.by_h = {}, {}, {}, {}

            def begin(self, blocks, arrived=()):
                for dh, dl in blocks:
                    k = dh * ZL + dl
                    a, b = at("zh", dh), at("zl", dl)
                    if (dh, dl) in arrived:
                        self.by_y[dh, dl] = [move(dd_ref.at[arrived.index((dh, dl))], from_y.at[self.m, k, 0])]
                    else:
                        self.by_y[dh, dl] = [
                            put(self.src.at[a, b, at("y", d)], from_y.at[self.m, k, d - 1], y=d)
                            for d in range(1, Y)
                        ]
                    self.own[dh, dl] = move(self.src.at[a, b, y], own_g.at[self.m, k])

            def add_y(self, blocks):
                m = self.m
                for dh, dl in blocks:
                    k = dh * ZL + dl
                    self.own[dh, dl].wait()
                    for copy in self.by_y[dh, dl]:
                        if any(copy is other for other in sent):
                            copy.wait_recv()
                        else:
                            copy.wait()

                    def body(r, k=k):
                        v = own_g[m, k, r].astype(F32)
                        for d in range(1, Y):
                            v = v + from_y[m, k, d - 1, r].astype(F32)
                        own_g[m, k, r] = v.astype(BF)

                    by_rows(depth, 64, body)
                    if dl:
                        self.by_l[dh, dl] = put(
                            own_g.at[m, k], from_l.at[m, dh, dl - 1], zl=dl
                        )

            def add_l(self, far):
                m = self.m
                for dh in range(ZH - 1, 0, -1) if far else (0,):
                    for d in range(1, ZL):
                        self.by_l[dh, d].wait_recv()
                    if dh:
                        def body(r, dh=dh):
                            v = own_g[m, dh * ZL, r].astype(F32)
                            for d in range(1, ZL):
                                v = v + from_l[m, dh, d - 1, r].astype(F32)
                            own_g[m, dh * ZL, r] = v.astype(BF)

                        by_rows(depth, 64, body)
                        to = from_h.at[m, dh - 1]
                        self.by_h[dh] = Far(own_g.at[m, dh * ZL], to, relay.at[m], to)

            def half(self, h, r, cols=slice(None)):
                m = self.m
                v = own_g[m, 0, r, cols].astype(F32)
                for d in range(1, ZL):
                    v = v + from_l[m, 0, d - 1, r, cols].astype(F32)
                for d in range(1, ZH):
                    other = from_h[m, d - 1, r, cols].astype(F32)
                    v = jnp.where(lax.rem(zh + ZH - d, ZH) == h, other, v)
                return v

            def wait_h(self):
                for copy in self.by_h.values():
                    copy.wait_recv()

        def block(m, k, place_y):
            a = lax.rem(zh + k // ZL, ZH)
            b = lax.rem(zl + k % ZL, ZL)
            start = pl.multiple_of(((a * ZL + b) * Y + place_y) * depth, depth)
            return nn(turned[pl.ds(start, depth)], units_t[m])

        def compute_other(first, last):
            @pl.loop(2 * first, 2 * last)
            def _(i):
                m, k = lax.rem(i, 2), zs - 1 - lax.div(i, 2)
                a = lax.rem(zh + lax.div(k, ZL), ZH)
                b = lax.rem(zl + lax.rem(k, ZL), ZL)
                start = pl.multiple_of(((a * ZL + b) * Y + at("y", 1)) * depth, depth)
                own_g[m + 1, k] = nn(turned[pl.ds(start, depth)], units_t[m]).astype(BF)

        def send_block(u, k):
            u.by_y[k] = put(own_g.at[u.m, k], from_y.at[u.m, k, 0], y=1)

        def add_block(u, k):
            u.by_y[k].wait()
            sent[:] = [other for other in sent if other is not u.by_y[k]]
            v = block(u.m - 1, k, y) + from_y[u.m, k, 0].astype(F32)
            own_g[u.m, k] = v.astype(BF)
            if k % ZL:
                u.by_l[k // ZL, k % ZL] = put(
                    own_g.at[u.m, k], from_l.at[u.m, k // ZL, k % ZL - 1], zl=k % ZL
                )

        class Scatter:
            def __init__(self, dd, in_c, in_y, in_z, tt, tb, in_x, whole, out, layout):
                self.r = (dd, in_c, in_y, in_z, tt, tb, in_x)
                self.whole, self.out, self.layout = whole, out, layout

            def fill(self, left, right):
                dd = self.r[0]
                span = X * C * part

                @pl.loop(0, zs)
                def _(z):
                    for b in range(Y):
                        start = pl.multiple_of((z * Y + b) * span, span)
                        v = nn(left[pl.ds(start, span)], right[...]).astype(BF)
                        for dx in range(X):
                            for dc in range(C):
                                first = (dx * C + dc) * part
                                dd[dc, b, z, dx * part : (dx + 1) * part] = v[
                                    first : first + part
                                ]

            def to_c(self):
                dd, in_c = self.r[:2]
                self.by_c = {
                    (f, d): put(dd.at[at("c", d), at("y", f)], in_c.at[f, d - 1], c=d)
                    for f in list(range(1, Y)) + [0]
                    for d in range(1, C)
                }

            def to_y(self):
                dd, in_c, in_y = self.r[:3]
                self.by_y = []
                for f in list(range(1, Y)) + [0]:
                    for d in range(1, C):
                        self.by_c[f, d].wait_recv()
                    b = at("y", f)

                    @pl.loop(0, zs)
                    def _(z):
                        v = dd[c, b, z].astype(F32)
                        for d in range(1, C):
                            v = v + in_c[f, d - 1, z].astype(F32)
                        dd[c, b, z] = v.astype(BF)

                    if f:
                        self.by_y.append(put(dd.at[c, b], in_y.at[f - 1], y=f))

            def to_z(self):
                dd, in_c, in_y, in_z = self.r[:4]
                for copy in self.by_y:
                    copy.wait_recv()

                @pl.loop(0, zs)
                def _(z):
                    v = dd[c, y, z].astype(F32)
                    for f in range(1, Y):
                        v = v + in_y[f - 1, z].astype(F32)
                    dd[c, y, z] = v.astype(BF)

                self.by_l = {
                    (dh, d): put(
                        dd.at[c, y, at("zh", dh) * ZL + at("zl", d)],
                        in_z.at[dh * (ZL - 1) + d - 1],
                        zl=d,
                    )
                    for dh in range(ZH - 1, -1, -1)
                    for d in range(1, ZL)
                }

            def summed_l(self, dh):
                dd, in_z = self.r[0], self.r[3]
                v = dd[c, y, at("zh", dh) * ZL + zl].astype(F32)
                for d in range(1, ZL):
                    v = v + in_z[dh * (ZL - 1) + d - 1].astype(F32)
                return v

            def to_h(self):
                dd, in_z = self.r[0], self.r[3]
                for copy in self.by_l.values():
                    copy.wait_recv()
                self.by_h = []
                for dh in range(1, ZH):
                    place = at("zh", dh) * ZL + zl
                    dd[c, y, place] = self.summed_l(dh).astype(BF)
                    self.by_h.append(
                        put(dd.at[c, y, place], in_z.at[ZH * (ZL - 1) + dh - 1], zh=dh)
                    )

            def to_x(self):
                dd, in_c, in_y, in_z, tt, tb, in_x = self.r
                for copy in self.by_h:
                    copy.wait_recv()
                v = self.summed_l(0)
                for dh in range(1, ZH):
                    v = v + in_z[ZH * (ZL - 1) + dh - 1].astype(F32)
                for dx in range(X):
                    tt[dx] = v[dx * part : (dx + 1) * part]
                    tb[dx] = v[dx * part : (dx + 1) * part].astype(BF)
                self.by_x = [put(tb.at[at("x", d)], in_x.at[d - 1], x=d) for d in range(1, X)]

            def end(self):
                tt, in_x = self.r[4], self.r[6]
                for d in range(1, X):
                    self.by_x[d - 1].wait_recv()
                for d in range(1, X):
                    tt[at("x", -d)] = in_x[d - 1].astype(F32)
                for first, blocks in self.layout:
                    v = 0.0
                    for dx, start in blocks:
                        v = v + tt[dx, :, start : start + HEAD_WIDTH]
                    self.whole[:, first : first + HEAD_WIDTH] = v
                return move(self.whole, self.out)

        class Rows:
            def __init__(self, m, src, mine):
                self.m, self.mine = m, mine
                order = list(range(1, len(near))) + [0]
                self.by_c = {
                    (k, d): put(src.at[d, k], from_c.at[m, k, d - 1], c=d)
                    for k in order
                    for d in range(1, C)
                }
                self.own = move(src.at[0], mine)

            def summed(self, k, r):
                v = self.mine[k, r].astype(F32)
                for d in range(1, C):
                    v = v + from_c[self.m, k, d - 1, r].astype(F32)
                return v

            def spread(self):
                self.own.wait()
                self.by_n = []
                for k, (dh, dx) in enumerate(near):
                    for d in range(1, C):
                        if k:
                            self.by_c[k, d].wait_recv()
                    if k:
                        def body(r, k=k):
                            self.mine[k, r] = self.summed(k, r).astype(BF)

                        by_rows(rows, 32, body)
                        self.by_n.append(
                            put(self.mine.at[k], from_n.at[self.m, k - 1], zh=dh, x=dx)
                        )
                for d in range(1, C):
                    self.by_c[0, d].wait_recv()

            def spread_x(self):
                self.own.wait()
                self.by_n = {}
                for dh in reversed(range(ZH)):
                    for dx in range(1, X):
                        k = dh * X + dx
                        for d in range(1, C):
                            self.by_c[k, d].wait_recv()

                        def body(r, k=k):
                            self.mine[k, r] = self.summed(k, r).astype(BF)

                        by_rows(rows, 32, body)
                        to = from_n.at[self.m, dh * (X - 1) + dx - 1]
                        self.by_n[dh, dx] = put(self.mine.at[k], to, x=dx)

            def came_x(self, dh, r):
                v = self.summed(dh * X, r)
                for dx in range(1, X):
                    v = v + from_n[self.m, dh * (X - 1) + dx - 1, r].astype(F32)
                return v

            def relay(self):
                for dh in reversed(range(ZH)):
                    for d in range(1, C):
                        self.by_c[dh * X, d].wait_recv()
                    for dx in range(1, X):
                        self.by_n[dh, dx].wait_recv()
                    if dh:
                        def body(r, dh=dh):
                            self.mine[dh * X, r] = self.came_x(dh, r).astype(BF)

                        by_rows(rows, 32, body)
                        to = from_n.at[self.m, ZH * (X - 1) + dh - 1]
                        self.by_n[dh, 0] = put(self.mine.at[dh * X], to, zh=dh)

            def landed(self):
                for dh in range(1, ZH):
                    self.by_n[dh, 0].wait_recv()

            def final(self, r):
                v = self.came_x(0, r)
                for dh in range(1, ZH):
                    v = v + from_n[self.m, ZH * (X - 1) + dh - 1, r].astype(F32)
                return v

            def arrive(self):
                for copy in self.by_n:
                    copy.wait_recv()

            def total(self, r):
                v = self.summed(0, r)
                for k in range(1, len(near)):
                    v = v + from_n[self.m, k - 1, r].astype(F32)
                return v

        terms = Rows(0, nt_ref, half_n)
        loads = {
            "turned": move(gt_ref, turned),
            "g": move(gg_ref, units_t.at[0]),
            "u": move(gu_ref, units_t.at[1]),
        }
        for name, src, dst in (
            ("mid", mid_ref, hs), ("cot", cot_ref, cots), ("vec", vec_ref, vec),
            ("n1", n1_ref, n1t), ("wo", wo_ref, wo), ("kv", kv_ref, kv), ("p", p_ref, ps),
            ("att", att_ref, atts), ("q", q_ref, qs), ("cos", cos_ref, cos_s),
            ("sin", sin_ref, sin_s), ("w1", w1_ref, w1), ("in", in_ref, ins),
        ):
            loads[name] = move(src, dst)
        ud, ug, uu = Units(0, gd_ref), Units(1, None), Units(2, None)
        arrived = [(dh, dl) for dh, dl in far if dh]
        ud.begin(arrived[::-1] + [(0, 1)], arrived)
        outs_terms = Rows(1, ot_ref, half_o)

        eye = (
            lax.broadcasted_iota(jnp.int32, (128, 128), 0)
            == lax.broadcasted_iota(jnp.int32, (128, 128), 1)
        ).astype(BF)

        terms.spread_x()
        for name in ("turned", "g", "u", "n1"):
            loads[name].wait()
        compute_other(0, 2)
        for u in (ug, uu):
            for k in (3, 2):
                send_block(u, k)
        ud.add_y(arrived[::-1])
        compute_other(2, 4)
        terms.relay()
        add_block(ug, 3)
        ud.add_l(far=True)
        add_block(ug, 2)
        for name in ("mid", "cot", "vec"):
            loads[name].wait()
        gain_one, gain_two = vec[0:1, :width], vec[1:2, :width]
        terms.landed()
        vs[...] = jnp.zeros_like(vs)

        @pl.loop(0, rows // 32)
        def _(i):
            r = pl.ds(pl.multiple_of(i * 32, 32), 32)
            grad, h = terms.final(r), hs[r]
            inv = lax.rsqrt(jnp.mean(h * h, axis=-1, keepdims=True) + EPSILON)
            scaled = gain_two * grad
            v = (
                cots[r].astype(F32)
                + inv * scaled
                - h * (inv * inv * inv) * jnp.mean(scaled * h, axis=-1, keepdims=True)
            )
            dh_s[r] = v
            da[0, r] = v.astype(BF)
            vs[1:2, :width] = vs[1:2, :width] + jnp.sum(grad * h * inv, axis=0, keepdims=True)

        da_x = [put(da.at[0], da.at[-d % X], x=d) for d in range(1, X)]
        ud.by_h[1].forward()
        outs_terms.spread_x()
        add_block(uu, 3)
        loads["wo"].wait()
        loads["att"].wait()
        for copy in da_x:
            copy.wait_recv()

        @pl.loop(0, heads // 2)
        def _(j):
            cols = pl.ds(pl.multiple_of(j * 256, 256), 256)
            for k in range(X):
                dos[k * rows : (k + 1) * rows, cols] = nn(da[k], wo[:, cols]).astype(BF)

        for k in range(X):
            for j in range(width // 128):
                cols = slice(j * 128, (j + 1) * 128)
                dat[cols, k * rows : (k + 1) * rows] = nt(eye, da[k, :, cols]).astype(BF)
        s_out = Scatter(d_out, c_out, y_out, z_out, t_out, b_out, x_out, w_out_s, dout_o, out_layout)
        s_out.fill(dat, atts)
        s_out.to_c()
        ug.add_l(far=True)
        add_block(uu, 2)
        ud.add_y([(0, 1)])
        for name in ("kv", "p", "q", "cos", "sin", "w1", "in"):
            loads[name].wait()
        dkv[...] = jnp.zeros_like(dkv)

        @pl.loop(0, heads)
        def _(h):
            cols = pl.ds(pl.multiple_of(h * HEAD_WIDTH, HEAD_WIDTH), HEAD_WIDTH)
            g = lax.div(h, share)
            k_at = pl.ds(pl.multiple_of(g * HEAD_WIDTH, HEAD_WIDTH), HEAD_WIDTH)
            v_at = pl.ds(pl.multiple_of(kv_cols + g * HEAD_WIDTH, HEAD_WIDTH), HEAD_WIDTH)
            p_low, do_h = ps[h], dos[:, cols]
            p = p_low.astype(F32)
            dp = nt(do_h, kv[:, v_at])
            delta = jnp.sum(p * dp, axis=-1, keepdims=True)
            ds = (p * (dp - delta)).astype(BF)
            dq = nn(ds, kv[:, k_at]) * scale
            dq = dq * cos_s[:query_rows] - pltpu.roll(dq, HEAD_WIDTH // 2, 1) * sin_s[:query_rows]
            dpre[:, cols] = dq.astype(BF)
            dkv[:, k_at] += tn(ds, qs[:, cols]) * scale
            dkv[:, v_at] += tn(p_low, do_h)

        kv_c = []
        for d in range(1, C):
            dkv_low[d - 1] = dkv[d * query_rows : (d + 1) * query_rows].astype(BF)
            kv_c.append(put(dkv_low.at[d - 1], dkv_in.at[d - 1], c=d))
        s_out.to_y()
        for copy in kv_c:
            copy.wait_recv()
        total = dkv[:query_rows]
        for d in range(1, C):
            total = total + dkv_in[d - 1].astype(F32)
        for j in range(kv_heads):
            cols = slice(j * HEAD_WIDTH, (j + 1) * HEAD_WIDTH)
            v = total[:, cols]
            v = v * cos_s[:query_rows] - pltpu.roll(v, HEAD_WIDTH // 2, 1) * sin_s[:query_rows]
            dpre[:, q_cols + j * HEAD_WIDTH : q_cols + (j + 1) * HEAD_WIDTH] = v.astype(BF)
        dpre[:, q_cols + kv_cols :] = total[:, kv_cols:].astype(BF)
        s_qkv = Scatter(d_qkv, c_qkv, y_qkv, z_qkv, t_qkv, b_qkv, x_qkv, w_qkv_s, dqkv_o, qkv_layout)
        s_qkv.fill(n1t, dpre)
        s_qkv.to_c()

        for k in list(range(1, X)) + [0]:
            @pl.loop(0, width // 256)
            def _(j, k=k):
                cols = pl.ds(pl.multiple_of(j * 256, 256), 256)
                v = nt(dpre[k * rows : (k + 1) * rows], w1[cols])
                if k:
                    n_send[k - 1, :, cols] = v.astype(BF)
                else:
                    gi_s[:, cols] = v

            if k:
                copy = put(n_send.at[k - 1], n_recv.at[k - 1], x=k)
                n_x = [copy] if k == 1 else n_x + [copy]
        kv_at = lax.div(x * heads, QUERY_HEADS // KEY_VALUE_HEADS) * HEAD_WIDTH
        k_off = QUERY_HEADS * HEAD_WIDTH + kv_at
        v_off = k_off + KEY_VALUE_HEADS * HEAD_WIDTH
        sums = jnp.sum(dpre[...].astype(F32), axis=0, keepdims=True)

        def place(start, first, amount):
            vs[2:3, pl.ds(pl.multiple_of(start, 128), amount)] = sums[:, first : first + amount]

        place(x * q_cols, 0, q_cols)
        place(k_off, q_cols, kv_cols)
        place(v_off, q_cols + kv_cols, kv_cols)
        s_qkv.to_y()
        send_block(ug, 1)
        ug.by_h[1].forward()
        s_out.to_z()
        outs_terms.relay()
        for copy in n_x:
            copy.wait_recv()

        @pl.loop(0, rows // 32)
        def _(i):
            r = pl.ds(pl.multiple_of(i * 32, 32), 32)
            grad, h = gi_s[r], ins[r].astype(F32)
            for d in range(1, X):
                grad = grad + n_recv[d - 1, r].astype(F32)
            inv = lax.rsqrt(jnp.mean(h * h, axis=-1, keepdims=True) + EPSILON)
            scaled = gain_one * grad
            gi_s[r] = (
                dh_s[r]
                + inv * scaled
                - h * (inv * inv * inv) * jnp.mean(scaled * h, axis=-1, keepdims=True)
            )
            vs[0:1, :width] = vs[0:1, :width] + jnp.sum(grad * h * inv, axis=0, keepdims=True)

        done = [move(gi_s, gi_o)]

        def put_far(u):
            u.wait_h()

            def body(r):
                v = from_h[u.m, 0, r]

                @pl.when(zh == 0)
                def _():
                    out_w[u.m, r, units:] = v

                @pl.when(zh != 0)
                def _():
                    out_w[u.m, r, :units] = v

            by_rows(depth, 64, body)

        def put_near(u, out):
            def body(r):
                v = own_g[u.m, 0, r].astype(F32)
                for d in range(1, ZL):
                    v = v + from_l[u.m, 0, d - 1, r].astype(F32)
                v = v.astype(BF)

                @pl.when(zh == 0)
                def _():
                    out_w[u.m, r, :units] = v

                @pl.when(zh != 0)
                def _():
                    out_w[u.m, r, units:] = v

            by_rows(depth, 64, body)
            done.append(move(out_w.at[u.m], out))

        places = iter(range(V_IN))
        stages = iter(range(4))

        def small_stage(offsets):
            k = next(stages)
            v_send[k] = vs[...]
            return [(p, put(v_send.at[k], v_in.at[p], **off)) for off, p in zip(offsets, places)]

        def small_finish(copies):
            for p, copy in copies:
                copy.wait_recv()
                vs[...] = vs[...] + v_in[p]

        state = small_stage([dict(y=d) for d in range(1, Y)])
        send_block(uu, 1)
        send_block(ug, 0)
        send_block(uu, 0)
        ud.begin([(0, 0)])
        uu.add_l(far=True)
        s_qkv.to_z()
        s_out.to_h()
        small_finish(state)
        state = small_stage([dict(zh=dh, zl=dl) for dh, dl in far[1:]])
        uu.by_h[1].forward()
        add_block(ug, 1)
        s_qkv.to_h()
        add_block(uu, 1)
        s_out.to_x()
        small_finish(state)
        state = small_stage([dict(x=d) for d in range(1, X)])
        outs_terms.landed()

        def finish(r):
            lo_s[r] = (hs[r] + outs_terms.final(r)).astype(BF)

        by_rows(rows, 32, finish)
        done.append(move(lo_s, lo_o))
        small_finish(state)
        state = small_stage([dict(c=d) for d in range(1, C)])
        done.append(s_out.end())
        ud.add_l(far=False)
        ug.add_l(far=False)
        for u in (ud, ug, uu):
            put_far(u)
        add_block(ug, 0)
        put_near(ug, og_o)
        s_qkv.to_x()
        add_block(uu, 0)
        ud.add_y([(0, 0)])
        put_near(ud, od_o)
        small_finish(state)
        done.append(move(vs, vec_out))
        done.append(s_qkv.end())
        uu.add_l(far=False)
        put_near(uu, ou_o)
        for copy in done:
            copy.wait()
        for copy in sent:
            copy.wait_send()
        assert count[0] <= n_sems and count[1] <= 64, count

    V_IN = (C - 1) + (X - 1) + (Y - 1) + (zs - 1)
    any_spec = pl.BlockSpec(memory_space=pl.ANY)
    sds = jax.ShapeDtypeStruct
    vm = pltpu.VMEM

    def scatter_scratch(n):
        return [
            vm((C, Y, zs, X * part, n), BF), vm((Y, max(C - 1, 1), zs, X * part, n), BF),
            vm((max(Y - 1, 1), zs, X * part, n), BF), vm((max(zs - 1, 1), X * part, n), BF),
            vm((X, part, n), F32), vm((X, part, n), BF), vm((max(X - 1, 1), part, n), BF),
        ]

    nk = len(near)
    return pl.pallas_call(
        kernel,
        out_shape=[
            sds((rows, width), BF), sds((rows, width), F32), sds((part, QKV_WIDTH), F32),
            sds((part, X * q_cols), F32), sds((8, QKV_WIDTH), F32),
            sds((depth, ZH * units), BF), sds((depth, ZH * units), BF),
            sds((depth, ZH * units), BF), sds((3, depth, units), BF),
        ],
        in_specs=[any_spec] * 20,
        out_specs=[any_spec] * 9,
        scratch_shapes=[
            vm((3, zs, depth, units), BF), vm((3, zs, max(Y - 1, 1), depth, units), BF),
            vm((3, ZH, max(ZL - 1, 1), depth, units), BF), vm((3, max(ZH - 1, 1), depth, units), BF),
            vm((3, depth, ZH * units), BF), vm((width, group_rows), BF), vm((2, group_rows, units), BF),
            vm((nk, rows, width), BF), vm((nk, rows, width), BF),
            vm((2, nk, max(C - 1, 1), rows, width), BF), vm((2, max(nk - 1, 1), rows, width), BF),
            vm((rows, width), F32), vm((rows, width), BF), vm((rows, width), BF),
            vm((width, qkv_n), BF), vm((width, q_cols), BF),
            vm((width, query_rows), BF), vm((query_rows, q_cols), BF),
            vm((pack_rows, 2 * kv_cols), BF), vm((heads, query_rows, pack_rows), BF),
            vm((query_rows, q_cols), BF), vm((8, QKV_WIDTH), F32),
            vm((pack_rows, HEAD_WIDTH), F32), vm((pack_rows, HEAD_WIDTH), F32),
            vm((X, rows, width), BF), vm((width, query_rows), BF), vm((query_rows, q_cols), BF),
            vm((query_rows, qkv_n), BF), vm((pack_rows, 2 * kv_cols), F32),
            vm((max(C - 1, 1), query_rows, 2 * kv_cols), BF),
            vm((max(C - 1, 1), query_rows, 2 * kv_cols), BF),
            vm((rows, width), F32),
        ]
        + scatter_scratch(qkv_n)
        + scatter_scratch(q_cols)
        + [
            vm((part, QKV_WIDTH), F32), vm((part, X * q_cols), F32),
            vm((max(X - 1, 1), rows, width), BF), vm((max(X - 1, 1), rows, width), BF),
            vm((rows, width), BF), vm((rows, width), F32), vm((8, QKV_WIDTH), F32),
            vm((max(V_IN, 1), 8, QKV_WIDTH), F32), vm((4, 8, QKV_WIDTH), F32),
            pltpu.SemaphoreType.DMA((n_sems,)), pltpu.SemaphoreType.DMA((n_sems,)),
            pltpu.SemaphoreType.DMA((64,)),
        ],
        compiler_params=pltpu.CompilerParams(
            collective_id=1, has_side_effects=True, vmem_limit_bytes=63 << 20
        ),
        name="back",
    )(
        grad_d, near_d, grad_g, grad_u, group_t, normed_terms, out_terms, middle, cotangent, own_in,
        wqkv, wout, normed, queries, kv_rows, probs, attended, vectors, cosine, sine,
    )


def finish(arrays, types):
    def spec(v):
        if v.shape[0] % 64 == 0:
            return pl.BlockSpec((v.shape[0] // 4,) + v.shape[1:], lambda i: (i,) + (0,) * (v.ndim - 1))
        return pl.BlockSpec(v.shape, lambda i: (0,) * v.ndim)

    def kernel(*refs):
        for src, dst in zip(refs[: len(arrays)], refs[len(arrays) :]):
            dst[...] = src[...].astype(dst.dtype)

    return pl.pallas_call(
        kernel,
        grid=(4,),
        out_shape=[jax.ShapeDtypeStruct(v.shape, t) for v, t in zip(arrays, types)],
        in_specs=[spec(v) for v in arrays],
        out_specs=[spec(v) for v in arrays],
        name="finish",
    )(*arrays)


def ff(normed, cotangent, w_gate, w_up, w_down):
    gate = nn(normed, w_gate)
    up_part = nn(normed, w_up)
    sig = jax.nn.sigmoid(gate)
    act = gate * sig
    hidden = (act * up_part).astype(BF)
    grad_wdown = tn(cotangent, hidden).astype(BF)
    grad_hidden = nn(cotangent, w_down)
    grad_gate = (grad_hidden * up_part * sig * (1.0 + gate * (1.0 - sig))).astype(BF)
    grad_up = (grad_hidden * act).astype(BF)
    grad_wgate = tn(normed, grad_gate).astype(BF)
    grad_wup = tn(normed, grad_up).astype(BF)
    normed_term = (nt(grad_gate, w_gate) + nt(grad_up, w_up)).astype(BF)
    out_term = nt(hidden, w_down).astype(BF)
    return hidden, grad_gate, grad_up, grad_wdown, grad_wgate, grad_wup, out_term, normed_term


def small_rows(gain_one, gain_two, bias):
    row = jnp.concatenate([gain_one, gain_two, bias]).astype(F32)
    return jnp.broadcast_to(jnp.pad(row, (0, -row.shape[0] % 256))[None], (8, 256))


def shards(
    layer_in, lengths, w_qkv, b_qkv, w_out, norm1_gain, norm2_gain, w_gate, w_up, w_down, grad_out
):
    size = lax.axis_size
    ZH, ZL, Y, X, C = (size(a) for a in ("zh", "zl", "y", "x", "c"))
    zh, zl, y, x, c = (lax.axis_index(a) for a in ("zh", "zl", "y", "x", "c"))
    everyone = ("zh", "zl", "y", "x", "c")
    devices = ZH * ZL * Y * X * C
    rows, width = layer_in.shape[1:]
    part = w_qkv.shape[0]
    group = QUERY_HEADS // KEY_VALUE_HEADS
    heads = QUERY_HEADS // X
    kv_heads = max(1, heads // group)
    share = heads // kv_heads
    q_cols, kv_cols = heads * HEAD_WIDTH, kv_heads * HEAD_WIDTH
    scale = HEAD_WIDTH ** (-0.5)

    own_in = layer_in[0]
    cotangent = grad_out[0]
    own_rows = own_in.astype(F32)
    query_rows, pack_rows = X * rows, C * X * rows
    bias_part = b_qkv.shape[0]
    def row_index(cores):
        spans = [
            (((x + dx) % X) * C + (c + dc) % C) * rows + jnp.arange(rows, dtype=jnp.int32)
            for dc in range(cores)
            for dx in range(X)
        ]
        return jnp.concatenate(spans)

    doc_lengths = lengths[0]
    key_index = row_index(C)
    key_doc, key_pos = doc_layout(key_index, doc_lengths)
    query_index, query_doc = key_index[:query_rows], key_doc[:query_rows]
    key_cos, key_sin = angles(key_pos)
    query_cos, query_sin = key_cos[:query_rows], key_sin[:query_rows]

    def gather_columns(pieces):
        held = ordered(
            [pick(pieces, x)] + [fetch(pick(pieces, (x - d) % X), "x", d) for d in range(1, X)],
            "x",
        )
        whole = jnp.zeros((ZH, ZL, Y) + held.shape, held.dtype)
        for dh in range(ZH):
            for dl in range(ZL):
                along = held if dh == dl == 0 else fetch(held, ("zh", "zl"), (dh, dl))
                for dy in range(Y):
                    piece = along if dy == 0 else fetch(along, "y", dy)
                    whole = lax.dynamic_update_slice(
                        whole,
                        piece[None, None, None],
                        ((zh + dh) % ZH, (zl + dl) % ZL, (y + dy) % Y, 0, 0, 0),
                    )
        whole = whole.reshape((ZH * ZL * Y * X,) + whole.shape[4:])
        both = ordered([whole] + [fetch(whole, "c", d) for d in range(1, C)], "c")
        return jnp.moveaxis(both, 0, 1).reshape(width, whole.shape[-1])

    def scatter_columns(grad):
        n = grad.shape[-1]
        grad = grad.astype(BF).reshape(ZH * ZL * Y * X, C, part, n)
        held = pick(grad, c, 1).astype(F32)
        for d in range(1, C):
            held = held + send(pick(grad, (c + d) % C, 1), "c", d)
        held = held.astype(BF).reshape(ZH, ZL, Y, X * part, n)
        kept = pick(held, y, 2).astype(F32)
        for d in range(1, Y):
            kept = kept + send(pick(held, (y + d) % Y, 2), "y", d)
        low = kept.astype(BF)
        total = 0.0
        for dh in range(ZH):
            for dl in range(ZL):
                if dh == dl == 0:
                    total = total + pick(pick(kept, zh), zl)
                else:
                    piece = pick(pick(low, (zh + dh) % ZH), (zl + dl) % ZL)
                    total = total + send(piece, ("zh", "zl"), (dh, dl)).astype(F32)
        total = total.reshape(X, part, n)
        lower = total.astype(BF)
        return ordered(
            [pick(total, x)]
            + [fetch(pick(lower, (x - d) % X), "x", d).astype(F32) for d in range(1, X)],
            "x",
        )

    def qkv_columns(array):
        blocks = []
        for at in range(X):
            kv = (at * heads) // group * HEAD_WIDTH
            key_at = QUERY_HEADS * HEAD_WIDTH + kv
            value_at = key_at + KEY_VALUE_HEADS * HEAD_WIDTH
            blocks.append(
                jnp.concatenate(
                    [
                        array[..., at * q_cols : (at + 1) * q_cols],
                        array[..., key_at : key_at + kv_cols],
                        array[..., value_at : value_at + kv_cols],
                    ],
                    axis=-1,
                )
            )
        return jnp.stack(blocks)

    def qkv_whole(blocks):
        queries = [blocks[at, ..., :q_cols] for at in range(X)]
        keys, values = [0.0] * KEY_VALUE_HEADS, [0.0] * KEY_VALUE_HEADS
        for at in range(X):
            for j in range(kv_heads):
                head = (at * heads) // group + j
                start = q_cols + j * HEAD_WIDTH
                keys[head] = keys[head] + blocks[at, ..., start : start + HEAD_WIDTH]
                start = start + kv_cols
                values[head] = values[head] + blocks[at, ..., start : start + HEAD_WIDTH]
        return jnp.concatenate(queries + keys + values, axis=-1)

    depth, units = w_gate.shape[0], w_gate.shape[1] // ZH

    def gather_units(weight):
        halves = weight.reshape(depth, ZH, units).transpose(1, 0, 2)
        whole = jnp.zeros((ZH, ZL, Y, depth, units), weight.dtype)
        for dh in range(ZH):
            first = pick(halves, zh) if dh == 0 else fetch(pick(halves, (zh - dh) % ZH), "zh", dh)
            for dl in range(ZL):
                second = first if dl == 0 else fetch(first, "zl", dl)
                for dy in range(Y):
                    third = second if dy == 0 else fetch(second, "y", dy)
                    whole = lax.dynamic_update_slice(
                        whole,
                        third[None, None, None],
                        ((zh + dh) % ZH, (zl + dl) % ZL, (y + dy) % Y, 0, 0),
                    )
        return whole.reshape(width, units)

    def scatter_units(grad):
        grad = grad.astype(BF).reshape(ZH, ZL, Y, depth, units)
        done = [None] * ZH
        for dh in reversed(range(ZH)):
            mine = pick(grad, (zh + dh) % ZH)
            kept = pick(mine, y, 1).astype(F32)
            for d in range(1, Y):
                kept = kept + send(pick(mine, (y + d) % Y, 1), "y", d).astype(F32)
            low = kept.astype(BF)
            total = pick(kept, zl)
            for d in range(1, ZL):
                total = total + send(pick(low, (zl + d) % ZL), "zl", d).astype(F32)
            done[dh] = total
        halves = [done[0]] + [
            send(done[dh].astype(BF), "zh", dh).astype(F32) for dh in range(1, ZH)
        ]
        halves = [halves[0]] + halves[:0:-1]
        return jnp.moveaxis(ordered(halves, "zh"), 0, 1).reshape(depth, ZH * units)

    near = [(dh, dx) for dh in range(ZH) for dx in range(X)]

    def gather_rows(own):
        held = jnp.concatenate([own if k == (0, 0) else fetch(own, ("zh", "x"), k) for k in near])
        return jnp.concatenate([held] + [fetch(held, "c", d) for d in range(1, C)])

    def scatter_rows(term):
        term = term.reshape(C, len(near), rows, width)
        held = term[0].astype(F32)
        for d in range(1, C):
            held = held + send(term[d].astype(BF), "c", d).astype(F32)
        total = held[0]
        for at, k in enumerate(near):
            if k != (0, 0):
                total = total + send(held[at].astype(BF), ("zh", "x"), k).astype(F32)
        return total

    def scatter_x(term):
        term = term.reshape(X, rows, width)
        total = term[0]
        for d in range(1, X):
            total = total + send(term[d].astype(BF), "x", d).astype(F32)
        return total

    if part % 16 == 0 and depth % 64 == 0 and heads % 2 == 0 and X > 1 and ZH == ZL == Y == 2:
        (
            wqkv_mine, wout_mine, normed_t, group_normed_t, queries, kv_low, probs_low,
            attended_low, middle, group_normed, group_cotangent, wgate_mine, wup_mine,
            wdown_part, vectors, cosine, sine, _,
        ) = front(
            own_in,
            cotangent,
            lengths,
            w_qkv,
            w_out.T,
            small_rows(norm1_gain, norm2_gain, b_qkv),
            w_gate,
            w_up,
            w_down.T,
            qkv_columns,
        )
        grad_gate, grad_up, grad_wdown, near_d, normed_term, out_term = forward_backward(
            group_normed.reshape(-1, width),
            group_cotangent.reshape(-1, width),
            wgate_mine.reshape(width, units),
            wup_mine.reshape(width, units),
            wdown_part,
        )
        whole = (ZH, ZL, Y, depth, units)
        terms = (C, ZH * X, rows, width)
        layer_out, grad_input, sum_wqkv, sum_wout, small, sum_wdown, sum_wgate, sum_wup, _ = back(
            grad_wdown.reshape(whole),
            near_d,
            grad_gate,
            grad_up,
            group_normed_t,
            normed_term.reshape(terms),
            out_term.reshape(terms),
            middle,
            cotangent,
            own_in,
            wqkv_mine,
            wout_mine,
            normed_t,
            queries,
            kv_low,
            probs_low,
            attended_low,
            vectors,
            cosine,
            sine,
        )
        place = (((zh * ZL + zl) * Y + y) * X + x) * C + c
        layer_out, grad_input, sum_wqkv, sum_wout, sum_wgate, sum_wup, sum_wdown = finish(
            (layer_out, grad_input, sum_wqkv, sum_wout, sum_wgate, sum_wup, sum_wdown),
            (BF,) + (F32,) * 6,
        )
        return (
            layer_out[None],
            grad_input[None],
            sum_wqkv,
            lax.dynamic_slice(small, (2, place * bias_part), (1, bias_part))[0],
            sum_wout.T,
            lax.dynamic_slice(small, (0, place * part), (1, part))[0],
            lax.dynamic_slice(small, (1, place * part), (1, part))[0],
            sum_wgate,
            sum_wup,
            sum_wdown.T,
        )

    small = jnp.concatenate([norm1_gain, norm2_gain, b_qkv])
    small = jnp.pad(small, (0, -small.shape[0] % 256))[None]
    small = lax.all_to_all(
        jnp.broadcast_to(small[None], (devices,) + small.shape), everyone, 0, 0, tiled=True
    )[:, 0].astype(F32)
    gain_one = small[:, :part].reshape(1, width)
    gain_two = small[:, part : 2 * part].reshape(1, width)
    bias = small[:, 2 * part : 2 * part + bias_part].reshape(-1)

    query_in = jnp.concatenate([own_in] + [fetch(own_in, "x", d) for d in range(1, X)])
    pack_in = jnp.concatenate([query_in] + [fetch(query_in, "c", d) for d in range(1, C)])

    wqkv_mine = gather_columns(qkv_columns(w_qkv))
    wout_t = w_out.T
    wout_mine = gather_columns(
        jnp.stack([wout_t[:, at * q_cols : (at + 1) * q_cols] for at in range(X)])
    )
    bias_mine = pick(qkv_columns(bias), x)

    wgate_mine, wup_mine = gather_units(w_gate), gather_units(w_up)
    wdown_mine = gather_units(w_down.T)

    group_cotangent = gather_rows(cotangent)

    pack_in = pack_in.astype(F32)
    normed_one = (pack_in * rms_parts(pack_in) * gain_one).astype(BF)
    query_normed = normed_one[:query_rows]
    pre_query = nn(query_normed, wqkv_mine[:, :q_cols]) + bias_mine[:q_cols]
    pre_kv = nn(normed_one, wqkv_mine[:, q_cols:]) + bias_mine[q_cols:]
    queries = rotate(
        pre_query.reshape(query_rows, heads, HEAD_WIDTH), query_cos, query_sin
    ).astype(BF)
    queries = queries.reshape(query_rows, kv_heads, share, HEAD_WIDTH)
    keys = rotate(
        pre_kv[:, :kv_cols].reshape(pack_rows, kv_heads, HEAD_WIDTH), key_cos, key_sin
    ).astype(BF)
    values = pre_kv[:, kv_cols:].reshape(pack_rows, kv_heads, HEAD_WIDTH).astype(BF)
    scores = jnp.einsum("tkgd,skd->kgts", queries, keys, preferred_element_type=F32) * scale
    allowed = (query_doc[:, None] == key_doc[None, :]) & (
        key_index[None, :] <= query_index[:, None]
    )
    masked = jnp.where(allowed, scores, NEGATIVE_BIG)
    top = jnp.max(masked, axis=-1, keepdims=True)
    weights = jnp.where(allowed, jnp.exp(masked - top), 0.0)
    probs = weights / jnp.sum(weights, axis=-1, keepdims=True)
    probs_low = probs.astype(BF)
    attended = jnp.einsum("kgts,skd->tkgd", probs_low, values, preferred_element_type=F32)
    attended_low = attended.reshape(query_rows, q_cols).astype(BF)
    middle = own_rows + scatter_x(nt(attended_low, wout_mine))
    normed_two = (middle * rms_parts(middle) * gain_two).astype(BF)

    group_normed = gather_rows(normed_two)

    hidden, grad_gate, grad_up, grad_wdown, grad_wgate, grad_wup, out_term, normed_term = ff(
        group_normed, group_cotangent, wgate_mine, wup_mine, wdown_mine
    )
    grad_normed_two = scatter_rows(normed_term)
    layer_out = (middle + scatter_rows(out_term)).astype(BF)
    sum_wdown = scatter_units(grad_wdown).T
    sum_wgate = scatter_units(grad_wgate)
    sum_wup = scatter_units(grad_wup)

    back_two, grad_gain_two = rms_back(middle, gain_two, grad_normed_two)
    grad_middle = cotangent.astype(F32) + back_two
    grad_att = grad_middle.astype(BF)
    query_grad_att = jnp.concatenate([grad_att] + [fetch(grad_att, "x", d) for d in range(1, X)])
    sum_wout = scatter_columns(tn(query_grad_att, attended_low))
    head_grads = nn(query_grad_att, wout_mine).astype(BF)
    head_grads = head_grads.reshape(query_rows, kv_heads, share, HEAD_WIDTH)
    grad_probs = jnp.einsum("tkgd,skd->kgts", head_grads, values, preferred_element_type=F32)
    probs = probs_low.astype(F32)
    delta = jnp.sum(probs * grad_probs, axis=-1, keepdims=True)
    grad_scores = (probs * (grad_probs - delta)).astype(BF)
    grad_query = (
        jnp.einsum("kgts,skd->tkgd", grad_scores, keys, preferred_element_type=F32) * scale
    )
    grad_key = jnp.einsum("kgts,tkgd->skd", grad_scores, queries, preferred_element_type=F32)
    grad_key = rotate(grad_key * scale, key_cos, -key_sin)
    grad_value = jnp.einsum("kgts,tkgd->skd", probs_low, head_grads, preferred_element_type=F32)
    grad_kv = jnp.concatenate(
        [grad_key.reshape(pack_rows, kv_cols), grad_value.reshape(pack_rows, kv_cols)], axis=1
    ).reshape(C, query_rows, 2 * kv_cols)
    kv_total = grad_kv[0]
    for d in range(1, C):
        kv_total = kv_total + send(grad_kv[d].astype(BF), "c", d).astype(F32)
    grad_query = rotate(
        grad_query.reshape(query_rows, heads, HEAD_WIDTH), query_cos, -query_sin
    ).reshape(query_rows, q_cols)
    grad_pre = jnp.concatenate([grad_query, kv_total], axis=1).astype(BF)
    sum_wqkv = qkv_whole(scatter_columns(tn(query_normed, grad_pre)))
    grad_bias = jnp.sum(grad_pre.astype(F32), axis=0)
    grad_normed_one = scatter_x(nt(grad_pre, wqkv_mine))
    back_one, grad_gain_one = rms_back(own_rows, gain_one, grad_normed_one)
    grad_input = grad_middle + back_one

    bias_blocks = jnp.where(
        jnp.arange(X, dtype=jnp.int32)[:, None] == x, grad_bias[None, :], 0.0
    )
    bias_whole = qkv_whole(bias_blocks)
    piece = jnp.concatenate(
        [
            grad_gain_one.reshape(devices, part),
            grad_gain_two.reshape(devices, part),
            bias_whole.reshape(devices, bias_part),
        ],
        axis=1,
    )
    piece = jnp.pad(piece, ((0, 0), (0, -piece.shape[1] % 256)))
    piece = jnp.sum(lax.all_to_all(piece[:, None], everyone, 0, 0, tiled=True)[:, 0], axis=0)
    return (
        layer_out[None],
        grad_input[None],
        sum_wqkv,
        piece[2 * part : 2 * part + bias_part],
        jnp.moveaxis(sum_wout, 0, 1).reshape(part, -1).T,
        piece[:part],
        piece[part : 2 * part],
        sum_wgate,
        sum_wup,
        sum_wdown,
    )


def solution(mesh):
    wide, narrow = mesh.shape["wide"], mesh.shape["narrow"]
    cores = 2 if narrow % 2 == 0 else 1
    along_x = narrow // cores
    along_y = along_x if wide % along_x == 0 else 1
    along_z = wide // along_y
    far = 2 if along_z % 2 == 0 else 1
    split = Mesh(
        mesh.devices.reshape(far, along_z // far, along_y, along_x, cores),
        ("zh", "zl", "y", "x", "c"),
    )
    w, n = ("zh", "zl", "y"), ("x", "c")
    placed = (
        P(w, n, None),
        P(w, None),
        P(w + n, None),
        P(w + n),
        P(None, w + n),
        P(w + n),
        P(w + n),
        P(w, n),
        P(w, n),
        P(n, w),
        P(w, n, None),
    )
    return jax.shard_map(
        shards,
        mesh=split,
        in_specs=placed,
        out_specs=(
            P(w, n, None),
            P(w, n, None),
            P(w + n, None),
            P(w + n),
            P(None, w + n),
            P(w + n),
            P(w + n),
            P(w, n),
            P(w, n),
            P(n, w),
        ),
        check_vma=False,
    )
```

```python
import math

import jax
import jax.numpy as jnp
from jax import lax
from jax.experimental import pallas as pl
from jax.experimental.pallas import tpu as pltpu
from jax.sharding import Mesh
from jax.sharding import PartitionSpec as P

QUERY_HEADS = 12
KEY_VALUE_HEADS = 2
HEAD_WIDTH = 128

EPSILON = 1e-06
ROPE_BASE = 10000.0
NEGATIVE_BIG = -1e30
HIGHEST = lax.Precision.HIGHEST


BF = jnp.bfloat16
F32 = jnp.float32
AXES = ("zh", "zl", "y", "x", "c")
MESH_ID = pl.DeviceIdType.MESH
QKV_WIDTH = (QUERY_HEADS + 2 * KEY_VALUE_HEADS) * HEAD_WIDTH


def fetch(value, axes, offsets):
    axes = (axes,) if isinstance(axes, str) else tuple(axes)
    offsets = (offsets,) if isinstance(offsets, int) else tuple(offsets)
    sizes = [lax.axis_size(a) for a in axes]
    total = math.prod(sizes)
    pairs = []
    for flat in range(total):
        rest, place = flat, []
        for size in reversed(sizes):
            place.append(rest % size)
            rest //= size
        place = place[::-1]
        source = 0
        for spot, off, size in zip(place, offsets, sizes):
            source = source * size + (spot + off) % size
        pairs.append((source, flat))
    return lax.ppermute(value, axes if len(axes) > 1 else axes[0], pairs)


def send(value, axes, offsets):
    offsets = (offsets,) if isinstance(offsets, int) else tuple(offsets)
    return fetch(value, axes, tuple(-o for o in offsets))


def pick(stack, place, axis=0):
    return lax.dynamic_index_in_dim(stack, place, axis, keepdims=False)


def nn(left, right):
    return lax.dot_general(left, right, (((1,), (0,)), ((), ())), preferred_element_type=F32)


def nt(left, right):
    return lax.dot_general(left, right, (((1,), (1,)), ((), ())), preferred_element_type=F32)


def tn(left, right):
    return lax.dot_general(left, right, (((0,), (0,)), ((), ())), preferred_element_type=F32)


def rms_parts(rows):
    return lax.rsqrt(jnp.mean(rows * rows, axis=-1, keepdims=True) + EPSILON)


def rms_back(rows, gain, grad):
    r = rms_parts(rows)
    scaled = gain * grad
    return (
        r * scaled - rows * (r * r * r) * jnp.mean(scaled * rows, axis=-1, keepdims=True),
        jnp.sum(grad * rows * r, axis=0),
    )


def doc_layout(index, doc_lengths):
    ends = jnp.cumsum(doc_lengths)
    starts = ends - doc_lengths
    document_index = jnp.sum((index[:, None] >= ends[None, :]).astype(jnp.int32), axis=1)
    onehot = (
        document_index[:, None] == jnp.arange(doc_lengths.shape[0], dtype=jnp.int32)[None, :]
    ).astype(jnp.int32)
    token_position = index - jnp.sum(onehot * starts[None, :], axis=1)
    return document_index, token_position.astype(F32)


def angles(position):
    half = HEAD_WIDTH // 2
    freq = jnp.exp(jnp.arange(half, dtype=F32) * (-2.0 * math.log(ROPE_BASE) / HEAD_WIDTH))
    angle = position[:, None] * freq[None, :]
    return jnp.cos(angle)[:, None, :], jnp.sin(angle)[:, None, :]


def rotate(rows, cosine, sine):
    half = HEAD_WIDTH // 2
    first, second = rows[..., :half], rows[..., half:]
    return jnp.concatenate(
        [first * cosine - second * sine, second * cosine + first * sine], axis=-1
    )


def ordered(pieces, axis):
    count, here = len(pieces), lax.axis_index(axis)
    if count == 1:
        return pieces[0][None]
    if count == 2:
        return jnp.where(here == 0, jnp.stack(pieces), jnp.stack(pieces[::-1]))
    whole = jnp.zeros((count,) + pieces[0].shape, pieces[0].dtype)
    for distance, piece in enumerate(pieces):
        whole = lax.dynamic_update_index_in_dim(whole, piece, (here + distance) % count, 0)
    return whole


def front(own_in, cotangent, lengths, w_qkv, w_out, small, w_gate, w_up, w_down, qkv_columns):
    size = lax.axis_size
    ZH, ZL, Y, X, C = (size(a) for a in AXES)
    rows, width = own_in.shape
    part = w_qkv.shape[0]
    q_cols = w_out.shape[1] // X
    qkv_n = qkv_columns(w_qkv).shape[-1]
    heads = q_cols // HEAD_WIDTH
    kv_cols = (qkv_n - q_cols) // 2
    kv_heads = kv_cols // HEAD_WIDTH
    share = heads // kv_heads
    query_rows, pack_rows = X * rows, C * X * rows
    depth = w_gate.shape[0]
    units = w_gate.shape[1] // ZH
    near = [(dh, dx) for dh in range(ZH) for dx in range(X)]
    far = [(dh, dl) for dh in range(ZH) for dl in range(ZL)]
    devices = ZH * ZL * Y * X * C
    bias_part = QKV_WIDTH // devices
    scale = HEAD_WIDTH ** (-0.5)
    docs = lengths.shape[-1]
    n_sems = 400

    def kernel(
        own_ref, cot_ref, len_ref, qkv_ref, out_ref, small_ref, g_ref, u_ref, d_ref,
        wqkv_o, wout_o, n1_o, n2t_o, q_o, kv_o, p_o, att_o, h_o, nr_o, go_o, wg_o, wu_o, wd_o, vec_o, cos_o, sin_o, relay, got_o,
        xr, w1, wo, sm, n1, qs, kv, ob, part_send, part_recv, n2s, hs,
        cos_s, sin_s, mask_s, rows_s, ps, raw, half, wq_raw, wq_cut, n1t, n2t, nr_v, go_v, got,
        send_sem, recv_sem, local_sem,
    ):
        zh, zl, y, x, c = (lax.axis_index(a) for a in AXES)
        sizes = dict(zip(AXES, (ZH, ZL, Y, X, C)))
        here = dict(zip(AXES, (zh, zl, y, x, c)))

        def device(**off):
            return tuple(
                lax.rem(here[a] + off[a], sizes[a]) if off.get(a, 0) % sizes[a] else here[a]
                for a in AXES
            )

        def at(a, d):
            d = d % sizes[a]
            return lax.rem(here[a] + d, sizes[a]) if d else here[a]

        peers = set()
        for d in range(1, C):
            peers.add((0, 0, 0, 0, d))
        for dh, dx in near[1:]:
            peers.add((dh, 0, 0, dx, 0))
        for dh, dl in far[1:]:
            peers.add((dh, dl, 0, 0, 0))
        for d in range(1, Y):
            peers.add((0, 0, d, 0, 0))
        peers = sorted(peers)
        barrier = pltpu.get_barrier_semaphore()
        for peer in peers:
            pl.semaphore_signal(
                barrier, inc=1, device_id=device(**dict(zip(AXES, peer))), device_id_type=MESH_ID
            )
        pl.semaphore_wait(barrier, len(peers))

        count = [0, 0]
        sent, local = [], []

        def put(src, dst, **off):
            k = count[0]
            count[0] += 1
            copy = pltpu.make_async_remote_copy(
                src_ref=src, dst_ref=dst, send_sem=send_sem.at[k], recv_sem=recv_sem.at[k],
                device_id=device(**off), device_id_type=MESH_ID,
            )
            copy.start()
            sent.append(copy)
            return copy

        def move(src, dst):
            k = count[1]
            count[1] += 1
            copy = pltpu.make_async_copy(src, dst, local_sem.at[k])
            copy.start()
            return copy

        inner = zh + zl == 1

        class Far:
            def __init__(self, src, dst, relay, onward):
                k = count[0]
                count[0] += 3
                self.relay, self.k = relay, k
                self.main = self.copy(src, dst, k, k, device(zh=1))
                self.step = self.copy(src, relay, k, k + 1, device(zl=1))
                self.onward = self.copy(relay, onward, k + 2, k, device(zh=1, zl=1))
                pl.when(inner)(self.main.start)
                pl.when(jnp.logical_not(inner))(self.step.start)
                sent.append(self)

            def copy(self, src, dst, k, r, to):
                return pltpu.make_async_remote_copy(
                    src_ref=src, dst_ref=dst, send_sem=send_sem.at[k], recv_sem=recv_sem.at[r],
                    device_id=to, device_id_type=MESH_ID,
                )

            def forward(self):
                @pl.when(inner)
                def _():
                    self.step.wait_recv()
                    self.onward.start()

            def wait_recv(self):
                self.main.wait_recv()

            def wait_send(self):
                self.main.wait_send()
                pl.when(inner)(self.onward.wait_send)

        class Gather:
            def __init__(self, buf, block, pieces):
                self.buf, self.block, self.pieces = buf, block, pieces

            def slot(self, dh, dl, dy, dx, dc):
                place = at("zh", dh)
                for a, d in (("zl", dl), ("y", dy), ("x", dx), ("c", dc)):
                    place = place * sizes[a] + at(a, d)
                start = pl.multiple_of(place * self.block, self.block)
                return self.buf.at[pl.ds(start, self.block)]

            def begin(self):
                self.own = move(self.pieces(x), self.slot(0, 0, 0, 0, 0))
                self.by_x = {
                    d: put(self.pieces(at("x", d)), self.slot(0, 0, 0, 0, 0), x=d)
                    for d in range(1, X)
                }

            def along_z(self):
                self.own.wait()
                for d in self.by_x:
                    self.by_x[d].wait_recv()
                self.by_h, self.by_l, self.by_y, self.by_c = {}, {}, {}, {}
                for dx in range(X):
                    s = self.slot(0, 0, 0, dx, 0)
                    for d in range(1, ZH):
                        self.by_h[d, dx] = put(s, s, zh=d)
                for dx in range(X):
                    self.along_l(0, dx)
                for dx in range(X):
                    self.spread(0, 0, dx)

            def along_l(self, dh, dx):
                s = self.slot(-dh, 0, 0, dx, 0)
                for d in range(1, ZL):
                    self.by_l[dh, d, dx] = put(s, s, zl=d)

            def spread(self, dh, dl, dx):
                s = self.slot(-dh, -dl, 0, dx, 0)
                for d in range(1, Y):
                    self.by_y[dh, dl, d, dx] = put(s, s, y=d)
                self.to_core(dh, dl, 0, dx)

            def to_core(self, dh, dl, dy, dx):
                s = self.slot(-dh, -dl, -dy, dx, 0)
                for d in range(1, C):
                    self.by_c[dh, dl, dy, d, dx] = put(s, s, c=d)

            def along_h(self):
                for d, dx in self.by_h:
                    self.by_h[d, dx].wait_recv()
                    self.along_l(d, dx)
                    self.spread(d, 0, dx)

            def along_y(self):
                for dh, dl, dx in self.by_l:
                    self.by_l[dh, dl, dx].wait_recv()
                    self.spread(dh, dl, dx)

            def along_c(self):
                for dh, dl in far:
                    for d in range(1, Y):
                        for dx in range(X):
                            self.by_y[dh, dl, d, dx].wait_recv()
                            self.to_core(dh, dl, d, dx)

            def end(self):
                for copy in self.by_c.values():
                    copy.wait_recv()

        class Units:
            def __init__(self, at_m, buf):
                self.m, self.buf = at_m, buf

            def slot(self, dh, dl, dy):
                return self.buf.at[at("zh", dh), at("zl", dl), at("y", dy)]

            def begin(self):
                mine = half.at[self.m, zh]
                s = self.slot(0, 0, 0)
                self.own = move(mine, s)
                self.by_h = {
                    1: Far(half.at[self.m, at("zh", 1)], s, relay.at[self.m], self.slot(0, 1, 0))
                }

            def own_l(self):
                self.by_l = {
                    (0, d): put(half.at[self.m, zh], self.slot(0, 0, 0), zl=d)
                    for d in range(1, ZL)
                }

            def own_y(self):
                self.by_y = {
                    (0, 0, d): put(half.at[self.m, zh], self.slot(0, 0, 0), y=d)
                    for d in range(1, Y)
                }

            def middle(self):
                for dh in self.by_h:
                    self.by_h[dh].wait_recv()
                    s = self.slot(-dh, 0, 0)
                    for d in range(1, ZL):
                        self.by_l[dh, d] = put(s, s, zl=d)
                    for d in range(1, Y):
                        self.by_y[dh, 0, d] = put(s, s, y=d)

            def last(self, dh, spread=True):
                for dl in range(1, ZL):
                    self.by_l[dh, dl].wait_recv()
                    s = self.slot(-dh, -dl, 0)
                    for d in range(1, Y) if spread else ():
                        self.by_y[dh, dl, d] = put(s, s, y=d)

            def end(self):
                self.own.wait()
                for copy in self.by_y.values():
                    copy.wait_recv()

        class Rows:
            def __init__(self, buf):
                self.buf = buf

            def begin(self, src):
                self.own = move(src, self.buf.at[0, 0, 0])
                self.by_h = {d: put(src, self.buf.at[0, -d % ZH, 0], zh=d) for d in range(1, ZH)}
                self.by_x = {(0, d): put(src, self.buf.at[0, 0, -d % X], x=d) for d in range(1, X)}
                self.by_c = [put(src, self.buf.at[-d % C, 0, 0], c=d) for d in range(1, C)]

            def spread(self, a, b):
                for d in range(1, C):
                    self.by_c.append(put(self.buf.at[0, a, b], self.buf.at[-d % C, a, b], c=d))

            def along_x(self):
                for dh in self.by_h:
                    self.by_h[dh].wait_recv()
                    a = -dh % ZH
                    for d in range(1, X):
                        self.by_x[dh, d] = put(self.buf.at[0, a, 0], self.buf.at[0, a, -d % X], x=d)
                    self.spread(a, 0)

            def to_core(self):
                for dh, d in self.by_x:
                    self.by_x[dh, d].wait_recv()
                    self.spread(-dh % ZH, -d % X)

            def end(self):
                self.own.wait()
                for copy in self.by_c:
                    copy.wait_recv()

        raws = [move(qkv_ref, wq_raw), move(g_ref, raw.at[0]), move(u_ref, raw.at[1])]
        raws.append(move(d_ref, raw.at[2]))

        def out_piece(to):
            return out_ref.at[:, pl.ds(pl.multiple_of(to * q_cols, 128), q_cols)]

        wq_g = Gather(w1, part, lambda to: wq_cut.at[to])
        wo_g = Gather(wo, part, out_piece)
        sm_g = Gather(sm, 8, lambda to: small_ref)
        raws[0].wait()
        cut = qkv_columns(wq_raw)
        for k in range(X):
            wq_cut[k] = cut[k]
        wq_g.begin()
        sm_g.begin()
        xr_own = move(own_ref, xr.at[0, 0])
        xr_x = {d: put(own_ref, xr.at[0, -d % X], x=d) for d in range(1, X)}
        wo_g.begin()
        wu, wgt, wdn = Units(1, wu_o), Units(0, wg_o), Units(2, wd_o)
        for m, unit in ((0, wgt), (1, wu), (2, wdn)):
            raws[m + 1].wait()
            @pl.loop(0, depth // 32)
            def _(i, m=m):
                r = pl.ds(pl.multiple_of(i * 32, 32), 32)
                for h in range(ZH):
                    half[m, h, r] = raw[m, r, h * units : (h + 1) * units]

            if m < 2:
                unit.own_y()
        wgt.own_l()
        sm_g.along_z()
        wq_g.along_z()

        lens = [len_ref[0, j] for j in range(docs)]
        ends = []
        for j in range(docs):
            ends.append(lens[j] if j == 0 else ends[-1] + lens[j])

        def slot_base(dc, dx):
            return (at("x", dx) * C + at("c", dc)) * rows

        def doc_of(index):
            doc = jnp.zeros(index.shape, jnp.int32)
            first = jnp.zeros(index.shape, jnp.int32)
            for j in range(docs):
                past = (index >= ends[j]).astype(jnp.int32)
                doc = doc + past
                first = first + past * lens[j]
            return doc, index - first

        lane = lax.broadcasted_iota(jnp.int32, (rows, HEAD_WIDTH), 1)
        folded = jnp.where(lane >= HEAD_WIDTH // 2, lane - HEAD_WIDTH // 2, lane)
        freq = jnp.exp(folded.astype(F32) * (-2.0 * math.log(ROPE_BASE) / HEAD_WIDTH))
        sign = jnp.where(lane >= HEAD_WIDTH // 2, 1.0, -1.0)
        slots = [(dc, dx) for dc in range(C) for dx in range(X)]
        def slot_of(k):
            there = lax.rem(x + lax.rem(k, X), X) * C + lax.rem(c + lax.div(k, X), C)
            return there * rows

        @pl.loop(0, C * X)
        def _(k):
            r = pl.ds(pl.multiple_of(k * rows, rows), rows)
            index = slot_of(k) + lax.broadcasted_iota(jnp.int32, (rows, HEAD_WIDTH), 0)
            angle = doc_of(index)[1].astype(F32) * freq
            cos_s[r] = jnp.cos(angle)
            sin_s[r] = jnp.sin(angle) * sign
            k_index = slot_of(k) + lax.broadcasted_iota(jnp.int32, (rows, rows), 1)
            k_doc = doc_of(k_index)[0]
            for a in range(X):
                q_index = slot_base(0, a) + lax.broadcasted_iota(jnp.int32, (rows, rows), 0)
                q_doc = doc_of(q_index)[0]
                allowed = (q_doc == k_doc) & (k_index <= q_index)
                mask_s[a * rows : (a + 1) * rows, r] = jnp.where(allowed, 0.0, NEGATIVE_BIG)

        xr_own.wait()
        for d in xr_x:
            xr_x[d].wait_recv()
        xr_c = [
            put(xr.at[0, k], xr.at[-d % C, k], c=d) for d in range(1, C) for k in range(X)
        ]
        sm_g.along_h()
        wq_g.along_h()
        wo_g.along_z()
        wgt.begin()
        wu.begin()
        sm_g.along_y()
        wq_g.along_y()
        sm_g.along_c()
        wo_g.along_h()
        wdn.own_y()
        wgt.by_h[1].forward()
        wu.own_l()
        wq_g.along_c()
        sm_g.end()
        wu.by_h[1].forward()

        def spread_row(first, block, total):
            pieces = sm[...].reshape(devices, 8, 256)[:, 0, :].astype(BF)
            left = lax.broadcasted_iota(jnp.int32, (256, total), 0)
            right = lax.broadcasted_iota(jnp.int32, (256, total), 1)
            select = (lax.rem(right, block) + first == left).astype(BF)
            wide = nn(pieces, select)
            owner = lax.broadcasted_iota(jnp.int32, (devices, total), 0)
            place = lax.broadcasted_iota(jnp.int32, (devices, total), 1)
            inside = (place >= owner * block) & (place < (owner + 1) * block)
            return jnp.sum(jnp.where(inside, wide, 0.0), axis=0, keepdims=True)

        rows_s[0:1, :width] = spread_row(0, part, width)
        rows_s[1:2, :width] = spread_row(part, part, width)
        rows_s[2:3, :] = spread_row(2 * part, bias_part, QKV_WIDTH)

        for copy in xr_c:
            copy.wait_recv()
        gain_one = rows_s[0:1, :width]
        for k, (dc, dx) in enumerate(slots):
            @pl.loop(0, rows // 32)
            def _(i, k=k, dc=dc, dx=dx):
                v = xr[dc, dx, pl.ds(pl.multiple_of(i * 32, 32), 32)].astype(F32)
                r = lax.rsqrt(jnp.mean(v * v, axis=-1, keepdims=True) + EPSILON)
                to = pl.ds(pl.multiple_of(k * rows + i * 32, 32), 32)
                n1[to] = (v * r * gain_one).astype(BF)

        eye = (
            lax.broadcasted_iota(jnp.int32, (128, 128), 0)
            == lax.broadcasted_iota(jnp.int32, (128, 128), 1)
        ).astype(BF)

        def flip(read, dst, amount):
            @pl.loop(0, width // 128)
            def _(j):
                cols = pl.ds(pl.multiple_of(j * 128, 128), 128)
                dst[cols] = nt(eye, read(cols)).astype(BF)

        wq_g.end()
        outs = [move(w1, wqkv_o), move(rows_s, vec_o), move(cos_s, cos_o), move(sin_s, sin_o)]
        kv_at = lax.div(x * heads, QUERY_HEADS // KEY_VALUE_HEADS) * HEAD_WIDTH
        k_off = QUERY_HEADS * HEAD_WIDTH + kv_at
        v_off = k_off + KEY_VALUE_HEADS * HEAD_WIDTH
        def turn(v, first, amount):
            return v * cos_s[first : first + amount] + pltpu.roll(
                v, HEAD_WIDTH // 2, 1
            ) * sin_s[first : first + amount]

        def bias_at(start, amount):
            return rows_s[2:3, pl.ds(pl.multiple_of(start, 128), amount)]

        @pl.loop(0, heads)
        def _(h):
            cols = pl.ds(pl.multiple_of(h * HEAD_WIDTH, HEAD_WIDTH), HEAD_WIDTH)
            v = nn(n1[0:query_rows], w1[:, cols])
            v = v + bias_at(x * q_cols + h * HEAD_WIDTH, HEAD_WIDTH)
            qs[:, cols] = turn(v, 0, query_rows).astype(BF)

        for j in range(kv_heads):
            at_k = q_cols + j * HEAD_WIDTH
            v = nn(n1[...], w1[:, at_k : at_k + HEAD_WIDTH]) + bias_at(k_off, kv_cols)[
                :, j * HEAD_WIDTH : (j + 1) * HEAD_WIDTH
            ]
            kv[:, j * HEAD_WIDTH : (j + 1) * HEAD_WIDTH] = turn(v, 0, pack_rows).astype(BF)
        v = nn(n1[...], w1[:, q_cols + kv_cols :]) + bias_at(v_off, kv_cols)
        kv[:, kv_cols:] = v.astype(BF)
        outs += [move(qs, q_o), move(kv, kv_o)]
        wo_g.along_y()
        wgt.last(0)
        wgt.middle()
        wdn.begin()
        wdn.own_l()

        @pl.loop(0, heads)
        def _(h):
            cols = pl.ds(pl.multiple_of(h * HEAD_WIDTH, HEAD_WIDTH), HEAD_WIDTH)
            g = lax.div(h, share)
            k_h = kv[:, pl.ds(pl.multiple_of(g * HEAD_WIDTH, HEAD_WIDTH), HEAD_WIDTH)]
            v_h = kv[:, pl.ds(pl.multiple_of(kv_cols + g * HEAD_WIDTH, HEAD_WIDTH), HEAD_WIDTH)]
            s = nt(qs[:, cols], k_h) * scale + mask_s[...]
            e = jnp.exp(s - jnp.max(s, axis=-1, keepdims=True))
            p = (e / jnp.sum(e, axis=-1, keepdims=True)).astype(BF)
            ps[h] = p
            ob[:, cols] = nn(p, v_h).astype(BF)

        outs += [move(ps, p_o), move(ob, att_o)]
        wo_g.along_c()
        wo_g.end()
        outs.append(move(wo, wout_o))
        block = 256
        for d in list(range(1, X)) + [0]:
            @pl.loop(0, width // block)
            def _(j, d=d):
                cols = pl.ds(pl.multiple_of(j * block, block), block)
                v = nt(ob[d * rows : (d + 1) * rows], wo[cols])
                if d:
                    part_send[d - 1, :, cols] = v.astype(BF)
                else:
                    hs[:, cols] = v

            if d:
                part_recv_copy = put(part_send.at[d - 1], part_recv.at[d - 1], x=d)
                parts = [part_recv_copy] if d == 1 else parts + [part_recv_copy]
        wu.last(0)
        go_rows = Rows(go_v)
        go_rows.begin(cot_ref)
        for d in range(1, X):
            parts[d - 1].wait_recv()
        gain_two = rows_s[1:2, :width]

        @pl.loop(0, rows // 32)
        def _(i):
            r = pl.ds(pl.multiple_of(i * 32, 32), 32)
            h = hs[r] + xr[0, 0, r].astype(F32)
            for d in range(1, X):
                h = h + part_recv[d - 1, r].astype(F32)
            hs[r] = h
            inv = lax.rsqrt(jnp.mean(h * h, axis=-1, keepdims=True) + EPSILON)
            n2s[r] = (h * inv * gain_two).astype(BF)

        nr_rows = Rows(nr_v)
        nr_rows.begin(n2s)
        outs.append(move(hs, h_o))
        flip(lambda cols: n1[0:query_rows, cols], n1t, query_rows)
        outs.append(move(n1t, n1_o))
        wdn.by_h[1].forward()
        wgt.last(1)
        wu.middle()
        wu.last(1)
        nr_rows.along_x()
        go_rows.along_x()
        wdn.last(0, False)
        wdn.middle()
        nr_rows.to_core()
        nr_rows.end()
        outs.append(move(nr_v, nr_o))
        group_rows = C * ZH * X * rows
        flip(lambda cols: nr_v[:, :, :, :, cols].reshape(group_rows, 128), n2t, group_rows)
        outs.append(move(n2t, n2t_o))
        go_rows.to_core()
        wdn.last(1, False)
        go_rows.end()
        outs.append(move(go_v, go_o))
        flip(lambda cols: go_v[:, :, :, :, cols].reshape(group_rows, 128), got, group_rows)
        outs.append(move(got, got_o))
        wgt.end()
        wu.end()
        wdn.end()
        for copy in outs:
            copy.wait()
        for copy in sent:
            copy.wait_send()
        assert count[0] <= n_sems, count

    any_spec = pl.BlockSpec(memory_space=pl.ANY)
    whole = (ZH, ZL, Y, depth, units)
    group = (C, ZH, X, rows, width)
    sds = jax.ShapeDtypeStruct
    return pl.pallas_call(
        kernel,
        out_shape=[
            sds((width, qkv_n), BF), sds((width, q_cols), BF), sds((width, query_rows), BF),
            sds((width, C * ZH * X * rows), BF),
            sds((query_rows, q_cols), BF), sds((pack_rows, 2 * kv_cols), BF),
            sds((heads, query_rows, pack_rows), BF), sds((query_rows, q_cols), BF),
            sds((rows, width), F32), sds(group, BF), sds(group, BF),
            sds(whole, BF), sds(whole, BF), sds(whole, BF),
            sds((8, QKV_WIDTH), F32),
            sds((pack_rows, HEAD_WIDTH), F32), sds((pack_rows, HEAD_WIDTH), F32),
            sds((3, depth, units), BF), sds((width, C * ZH * X * rows), BF),
        ],
        in_specs=[any_spec, any_spec, pl.BlockSpec(memory_space=pltpu.SMEM)] + [any_spec] * 6,
        out_specs=[any_spec] * 19,
        scratch_shapes=[
            pltpu.VMEM((C, X, rows, width), BF),
            pltpu.VMEM((width, qkv_n), BF),
            pltpu.VMEM((width, q_cols), BF),
            pltpu.VMEM((devices * 8, 256), F32),
            pltpu.VMEM((pack_rows, width), BF),
            pltpu.VMEM((query_rows, q_cols), BF),
            pltpu.VMEM((pack_rows, 2 * kv_cols), BF),
            pltpu.VMEM((query_rows, q_cols), BF),
            pltpu.VMEM((max(X - 1, 1), rows, width), BF),
            pltpu.VMEM((max(X - 1, 1), rows, width), BF),
            pltpu.VMEM((rows, width), BF),
            pltpu.VMEM((rows, width), F32),
            pltpu.VMEM((pack_rows, HEAD_WIDTH), F32),
            pltpu.VMEM((pack_rows, HEAD_WIDTH), F32),
            pltpu.VMEM((query_rows, pack_rows), F32),
            pltpu.VMEM((8, QKV_WIDTH), F32),
            pltpu.VMEM((heads, query_rows, pack_rows), BF),
            pltpu.VMEM((3,) + w_gate.shape, BF),
            pltpu.VMEM((3, ZH, depth, units), BF),
            pltpu.VMEM(w_qkv.shape, BF),
            pltpu.VMEM((X, part, qkv_n), BF),
            pltpu.VMEM((width, query_rows), BF),
            pltpu.VMEM((width, C * ZH * X * rows), BF),
            pltpu.VMEM(group, BF),
            pltpu.VMEM(group, BF),
            pltpu.VMEM((width, C * ZH * X * rows), BF),
            pltpu.SemaphoreType.DMA((n_sems,)),
            pltpu.SemaphoreType.DMA((n_sems,)),
            pltpu.SemaphoreType.DMA((32,)),
        ],
        compiler_params=pltpu.CompilerParams(
            collective_id=0, has_side_effects=True, vmem_limit_bytes=60 << 20
        ),
        name="front",
    )(own_in, cotangent, lengths, w_qkv, w_out, small, w_gate, w_up, w_down)


def forward_backward(normed, cotangent, cotangent_t, w_gate, w_up, w_down):
    size = lax.axis_size
    ZH, ZL, Y, X, C = (size(a) for a in AXES)
    total, width = normed.shape
    depth, units = w_down.shape[-2:]
    step = 256

    def kernel(
        n_ref, g_ref, t_ref, wg_ref, wu_ref, wd_ref,
        dg_o, du_o, dw_o, near_o, nt_o, ot_o,
        n_s, g_s, turned, wg, wu, wd, gates, ups, hidden, dg, du, dw, nt_s, ot_s,
        send_sem, recv_sem, local_sem, out_sem,
    ):
        here = dict(zip(AXES, (lax.axis_index(a) for a in AXES)))
        sizes = dict(zip(AXES, (ZH, ZL, Y, X, C)))

        def at(a, d):
            d = d % sizes[a]
            return lax.rem(here[a] + d, sizes[a]) if d else here[a]

        other = tuple(at(a, 1) if a == "y" else here[a] for a in AXES)
        barrier = pltpu.get_barrier_semaphore()
        pl.semaphore_signal(barrier, inc=1, device_id=other, device_id_type=MESH_ID)
        pl.semaphore_wait(barrier, 1)
        sent = []

        def put(src, dst):
            k = len(sent)
            copy = pltpu.make_async_remote_copy(
                src_ref=src, dst_ref=dst, send_sem=send_sem.at[k], recv_sem=recv_sem.at[k],
                device_id=other, device_id_type=MESH_ID,
            )
            copy.start()
            sent.append(copy)
            return copy

        count = [0]

        def move(src, dst):
            k = count[0]
            count[0] += 1
            copy = pltpu.make_async_copy(src, dst, local_sem.at[k])
            copy.start()
            return copy

        def row(a, b, e):
            start = pl.multiple_of(((a * ZL + b) * Y + e) * depth, depth)
            return pl.ds(start, depth)

        def at_rows(t):
            return pl.ds(pl.multiple_of(t * step, step), step)

        zh, zl, y = here["zh"], here["zl"], here["y"]
        loads = [move(n_ref, n_s), move(wg_ref, wg), move(wu_ref, wu), move(t_ref, turned)]
        loads.append(move(g_ref, g_s))
        down = []
        for d in range(ZH):
            a = at("zh", d)
            for e in range(1, ZL):
                b = at("zl", e)
                down.append(put(wd_ref.at[a, b, y], wd.at[row(a, b, y)]))
                loads.append(move(wd_ref.at[a, b, y], wd.at[row(a, b, y)]))
            for e in range(Y):
                loads.append(move(wd_ref.at[a, zl, e], wd.at[row(a, zl, e)]))
        for copy in loads[:2]:
            copy.wait()

        @pl.loop(0, total // step)
        def _(t):
            r = at_rows(t)
            gates[r] = nn(n_s[r], wg[...])

        loads[2].wait()

        @pl.loop(0, total // step)
        def _(t):
            r = at_rows(t)
            up = nn(n_s[r], wu[...])
            gate = gates[r]
            ups[r] = up
            hidden[r] = (gate * jax.nn.sigmoid(gate) * up).astype(BF)

        loads[3].wait()
        def blocks(first, last):
            @pl.loop(first, last)
            def _(k):
                a = lax.rem(zh + lax.rem(k + 2, 4) // ZL, ZH)
                b = lax.rem(zl + lax.rem(k, ZL), ZL)
                e = lax.rem(y + 1 + k // 4, Y)
                at_block = row(a, b, e)
                dw[at_block] = nn(turned[at_block], hidden[...]).astype(BF)

        blocks(0, 2)
        for k in range(ZL):
            put(dw.at[row(at("zh", 1), at("zl", k), at("y", 1))], near_o.at[k])
        blocks(2, 8)
        outs = [move(dw, dw_o)]
        for copy in loads[4:]:
            copy.wait()
        for copy in down:
            copy.wait_recv()

        def stream(k, src, dst, r):
            pltpu.make_async_copy(src.at[r], dst.at[r], out_sem.at[k]).start()

        results = ((dg, dg_o), (du, du_o), (nt_s, nt_o), (ot_s, ot_o))

        @pl.loop(0, total // step)
        def _(t):
            r = at_rows(t)
            grad = nn(g_s[r], wd[...])
            ot_s[r] = nt(hidden[r], wd[...]).astype(BF)
            gate, up = gates[r], ups[r]
            sig = jax.nn.sigmoid(gate)
            low_g = (grad * up * sig * (1.0 + gate * (1.0 - sig))).astype(BF)
            low_u = (grad * gate * sig).astype(BF)
            dg[r] = low_g
            du[r] = low_u
            nt_s[r] = (nt(low_g, wg[...]) + nt(low_u, wu[...])).astype(BF)
            for k, (src, dst) in enumerate(results):
                stream(k, src, dst, r)

        for k, (src, dst) in enumerate(results):
            pltpu.make_async_copy(src, dst, out_sem.at[k]).wait()
        for copy in outs:
            copy.wait()
        for copy in sent[len(down) :]:
            copy.wait_recv()
        for copy in sent:
            copy.wait_send()

    any_spec = pl.BlockSpec(memory_space=pl.ANY)
    sds, vm = jax.ShapeDtypeStruct, pltpu.VMEM
    return pl.pallas_call(
        kernel,
        out_shape=[
            sds((total, units), BF), sds((total, units), BF), sds((width, units), BF),
            sds((ZL, depth, units), BF), sds((total, width), BF), sds((total, width), BF),
        ],
        in_specs=[any_spec] * 6,
        out_specs=[any_spec] * 6,
        scratch_shapes=[
            vm((total, width), BF), vm((total, width), BF), vm((width, total), BF),
            vm((width, units), BF), vm((width, units), BF), vm((width, units), BF),
            vm((total, units), F32), vm((total, units), F32), vm((total, units), BF),
            vm((total, units), BF), vm((total, units), BF), vm((width, units), BF),
            vm((total, width), BF), vm((total, width), BF),
            pltpu.SemaphoreType.DMA((8,)), pltpu.SemaphoreType.DMA((8,)),
            pltpu.SemaphoreType.DMA((16,)), pltpu.SemaphoreType.DMA((4,)),
        ],
        compiler_params=pltpu.CompilerParams(
            collective_id=2, has_side_effects=True, vmem_limit_bytes=62 << 20
        ),
        name="forward_backward",
    )(normed, cotangent, cotangent_t, w_gate, w_up, w_down)


def back(
    grad_d, near_d, grad_g, grad_u, group_t, normed_terms, out_terms, middle, cotangent, own_in,
    wqkv, wout, normed, queries, kv_rows, probs, attended, vectors, cosine, sine,
):
    size = lax.axis_size
    ZH, ZL, Y, X, C = (size(a) for a in AXES)
    rows, width = own_in.shape
    qkv_n, q_cols = wqkv.shape[1], wout.shape[1]
    heads = q_cols // HEAD_WIDTH
    kv_cols = (qkv_n - q_cols) // 2
    kv_heads = kv_cols // HEAD_WIDTH
    share = heads // kv_heads
    query_rows, pack_rows = X * rows, C * X * rows
    depth, units = grad_d.shape[-2:]
    group_rows = group_t.shape[1]
    near = [(dh, dx) for dh in range(ZH) for dx in range(X)]
    far = [(dh, dl) for dh in range(ZH) for dl in range(ZL)]
    devices = ZH * ZL * Y * X * C
    part = width // devices
    zs = ZH * ZL
    scale = HEAD_WIDTH ** (-0.5)
    n_sems = 200

    blocks = {}
    for dx in range(X):
        for h in range(heads):
            blocks.setdefault(dx * heads + h, []).append((dx, h * HEAD_WIDTH))
        for j in range(kv_heads):
            head = dx * heads // (QUERY_HEADS // KEY_VALUE_HEADS) + j
            for at_kv, start in ((0, q_cols), (KEY_VALUE_HEADS, q_cols + kv_cols)):
                blocks.setdefault(QUERY_HEADS + at_kv + head, []).append(
                    (dx, start + j * HEAD_WIDTH)
                )
    qkv_layout = [(k * HEAD_WIDTH, b) for k, b in sorted(blocks.items())]
    out_layout = [(k * HEAD_WIDTH, b) for k, b in sorted(blocks.items()) if k < QUERY_HEADS]
    def kernel(
        gd_ref, dd_ref, gg_ref, gu_ref, gt_ref, nt_ref, ot_ref, mid_ref, cot_ref, in_ref,
        w1_ref, wo_ref, n1_ref, q_ref, kv_ref, p_ref, att_ref, vec_ref, cos_ref, sin_ref,
        lo_o, gi_o, dqkv_o, dout_o, vec_out, od_o, og_o, ou_o, relay,
        own_g, from_y, from_l, from_h, out_w, turned, units_t,
        half_n, half_o, from_c, from_n, hs, cots, ins, w1, wo, n1t, qs, kv, ps,
        atts, vec, cos_s, sin_s, da, dat, dos, dpre, dkv, dkv_low, dkv_in, dh_s,
        d_qkv, c_qkv, y_qkv, z_qkv, t_qkv, b_qkv, x_qkv,
        d_out, c_out, y_out, z_out, t_out, b_out, x_out, w_qkv_s, w_out_s,
        n_send, n_recv, lo_s, gi_s, vs, v_in, v_send,
        send_sem, recv_sem, local_sem,
    ):
        zh, zl, y, x, c = (lax.axis_index(a) for a in AXES)
        sizes = dict(zip(AXES, (ZH, ZL, Y, X, C)))
        here = dict(zip(AXES, (zh, zl, y, x, c)))

        def at(a, d):
            d = d % sizes[a]
            return lax.rem(here[a] + d, sizes[a]) if d else here[a]

        def device(**off):
            return tuple(at(a, off.get(a, 0)) for a in AXES)

        peers = set()
        for d in range(1, C):
            peers.add((0, 0, 0, 0, d))
        for dh, dx in near[1:]:
            peers.add((dh, 0, 0, dx, 0))
        for dh, dl in far[1:]:
            peers.add((dh, dl, 0, 0, 0))
        for d in range(1, Y):
            peers.add((0, 0, d, 0, 0))
        peers = sorted(peers)
        barrier = pltpu.get_barrier_semaphore()
        for peer in peers:
            pl.semaphore_signal(
                barrier, inc=1, device_id=device(**dict(zip(AXES, peer))), device_id_type=MESH_ID
            )
        pl.semaphore_wait(barrier, len(peers))

        count = [0, 0]
        sent = []

        def put(src, dst, **off):
            k = count[0]
            count[0] += 1
            copy = pltpu.make_async_remote_copy(
                src_ref=src, dst_ref=dst, send_sem=send_sem.at[k], recv_sem=recv_sem.at[k],
                device_id=device(**off), device_id_type=MESH_ID,
            )
            copy.start()
            sent.append(copy)
            return copy

        def move(src, dst):
            k = count[1]
            count[1] += 1
            copy = pltpu.make_async_copy(src, dst, local_sem.at[k])
            copy.start()
            return copy

        def by_rows(total, step, body):
            @pl.loop(0, total // step)
            def _(i):
                body(pl.ds(pl.multiple_of(i * step, step), step))

        inner = zh + zl == 1

        class Far:
            def __init__(self, src, dst, relay, onward):
                k = count[0]
                count[0] += 3
                self.relay, self.k = relay, k
                self.main = self.copy(src, dst, k, k, device(zh=1))
                self.step = self.copy(src, relay, k, k + 1, device(zl=1))
                self.onward = self.copy(relay, onward, k + 2, k, device(zh=1, zl=1))
                pl.when(inner)(self.main.start)
                pl.when(jnp.logical_not(inner))(self.step.start)
                sent.append(self)

            def copy(self, src, dst, k, r, to):
                return pltpu.make_async_remote_copy(
                    src_ref=src, dst_ref=dst, send_sem=send_sem.at[k], recv_sem=recv_sem.at[r],
                    device_id=to, device_id_type=MESH_ID,
                )

            def forward(self):
                @pl.when(inner)
                def _():
                    self.step.wait_recv()
                    self.onward.start()

            def wait_recv(self):
                self.main.wait_recv()

            def wait_send(self):
                self.main.wait_send()
                pl.when(inner)(self.onward.wait_send)

        class Units:
            def __init__(self, m, src):
                self.m, self.src = m, src
                self.by_y, self.own, self.by_l, self.by_h = {}, {}, {}, {}

            def begin(self, blocks, arrived=()):
                for dh, dl in blocks:
                    k = dh * ZL + dl
                    a, b = at("zh", dh), at("zl", dl)
                    if (dh, dl) in arrived:
                        self.by_y[dh, dl] = [move(dd_ref.at[arrived.index((dh, dl))], from_y.at[self.m, k, 0])]
                    else:
                        self.by_y[dh, dl] = [
                            put(self.src.at[a, b, at("y", d)], from_y.at[self.m, k, d - 1], y=d)
                            for d in range(1, Y)
                        ]
                    self.own[dh, dl] = move(self.src.at[a, b, y], own_g.at[self.m, k])

            def add_y(self, blocks):
                m = self.m
                for dh, dl in blocks:
                    k = dh * ZL + dl
                    self.own[dh, dl].wait()
                    for copy in self.by_y[dh, dl]:
                        if any(copy is other for other in sent):
                            copy.wait_recv()
                        else:
                            copy.wait()

                    def body(r, k=k):
                        v = own_g[m, k, r].astype(F32)
                        for d in range(1, Y):
                            v = v + from_y[m, k, d - 1, r].astype(F32)
                        own_g[m, k, r] = v.astype(BF)

                    by_rows(depth, 64, body)
                    if dl:
                        self.by_l[dh, dl] = put(
                            own_g.at[m, k], from_l.at[m, dh, dl - 1], zl=dl
                        )

            def add_l(self, far):
                m = self.m
                for dh in range(ZH - 1, 0, -1) if far else (0,):
                    for d in range(1, ZL):
                        self.by_l[dh, d].wait_recv()
                    if dh:
                        def body(r, dh=dh):
                            v = own_g[m, dh * ZL, r].astype(F32)
                            for d in range(1, ZL):
                                v = v + from_l[m, dh, d - 1, r].astype(F32)
                            own_g[m, dh * ZL, r] = v.astype(BF)

                        by_rows(depth, 64, body)
                        to = from_h.at[m, dh - 1]
                        self.by_h[dh] = Far(own_g.at[m, dh * ZL], to, relay.at[m], to)

            def half(self, h, r, cols=slice(None)):
                m = self.m
                v = own_g[m, 0, r, cols].astype(F32)
                for d in range(1, ZL):
                    v = v + from_l[m, 0, d - 1, r, cols].astype(F32)
                for d in range(1, ZH):
                    other = from_h[m, d - 1, r, cols].astype(F32)
                    v = jnp.where(lax.rem(zh + ZH - d, ZH) == h, other, v)
                return v

            def wait_h(self):
                for copy in self.by_h.values():
                    copy.wait_recv()

        def block(m, k, place_y):
            a = lax.rem(zh + k // ZL, ZH)
            b = lax.rem(zl + k % ZL, ZL)
            start = pl.multiple_of(((a * ZL + b) * Y + place_y) * depth, depth)
            return nn(turned[pl.ds(start, depth)], units_t[m])

        def compute_other(first, last):
            @pl.loop(2 * first, 2 * last)
            def _(i):
                m, k = lax.rem(i, 2), zs - 1 - lax.div(i, 2)
                a = lax.rem(zh + lax.div(k, ZL), ZH)
                b = lax.rem(zl + lax.rem(k, ZL), ZL)
                start = pl.multiple_of(((a * ZL + b) * Y + at("y", 1)) * depth, depth)
                own_g[m + 1, k] = nn(turned[pl.ds(start, depth)], units_t[m]).astype(BF)

        def send_block(u, k):
            u.by_y[k] = put(own_g.at[u.m, k], from_y.at[u.m, k, 0], y=1)

        def add_block(u, k):
            u.by_y[k].wait()
            sent[:] = [other for other in sent if other is not u.by_y[k]]
            v = block(u.m - 1, k, y) + from_y[u.m, k, 0].astype(F32)
            own_g[u.m, k] = v.astype(BF)
            if k % ZL:
                u.by_l[k // ZL, k % ZL] = put(
                    own_g.at[u.m, k], from_l.at[u.m, k // ZL, k % ZL - 1], zl=k % ZL
                )

        class Scatter:
            def __init__(self, dd, in_c, in_y, in_z, tt, tb, in_x, whole, out, layout):
                self.r = (dd, in_c, in_y, in_z, tt, tb, in_x)
                self.whole, self.out, self.layout = whole, out, layout

            def fill(self, left, right):
                dd = self.r[0]
                span = X * C * part

                @pl.loop(0, zs)
                def _(z):
                    for b in range(Y):
                        start = pl.multiple_of((z * Y + b) * span, span)
                        v = nn(left[pl.ds(start, span)], right[...]).astype(BF)
                        for dx in range(X):
                            for dc in range(C):
                                first = (dx * C + dc) * part
                                dd[dc, b, z, dx * part : (dx + 1) * part] = v[
                                    first : first + part
                                ]

            def to_c(self):
                dd, in_c = self.r[:2]
                self.by_c = {
                    (f, d): put(dd.at[at("c", d), at("y", f)], in_c.at[f, d - 1], c=d)
                    for f in list(range(1, Y)) + [0]
                    for d in range(1, C)
                }

            def to_y(self):
                dd, in_c, in_y = self.r[:3]
                self.by_y = []
                for f in list(range(1, Y)) + [0]:
                    for d in range(1, C):
                        self.by_c[f, d].wait_recv()
                    b = at("y", f)

                    @pl.loop(0, zs)
                    def _(z):
                        v = dd[c, b, z].astype(F32)
                        for d in range(1, C):
                            v = v + in_c[f, d - 1, z].astype(F32)
                        dd[c, b, z] = v.astype(BF)

                    if f:
                        self.by_y.append(put(dd.at[c, b], in_y.at[f - 1], y=f))

            def to_z(self):
                dd, in_c, in_y, in_z = self.r[:4]
                for copy in self.by_y:
                    copy.wait_recv()

                @pl.loop(0, zs)
                def _(z):
                    v = dd[c, y, z].astype(F32)
                    for f in range(1, Y):
                        v = v + in_y[f - 1, z].astype(F32)
                    dd[c, y, z] = v.astype(BF)

                self.by_l = {
                    (dh, d): put(
                        dd.at[c, y, at("zh", dh) * ZL + at("zl", d)],
                        in_z.at[dh * (ZL - 1) + d - 1],
                        zl=d,
                    )
                    for dh in range(ZH - 1, -1, -1)
                    for d in range(1, ZL)
                }

            def summed_l(self, dh):
                dd, in_z = self.r[0], self.r[3]
                v = dd[c, y, at("zh", dh) * ZL + zl].astype(F32)
                for d in range(1, ZL):
                    v = v + in_z[dh * (ZL - 1) + d - 1].astype(F32)
                return v

            def to_h(self):
                dd, in_z = self.r[0], self.r[3]
                for copy in self.by_l.values():
                    copy.wait_recv()
                self.by_h = []
                for dh in range(1, ZH):
                    place = at("zh", dh) * ZL + zl
                    dd[c, y, place] = self.summed_l(dh).astype(BF)
                    self.by_h.append(
                        put(dd.at[c, y, place], in_z.at[ZH * (ZL - 1) + dh - 1], zh=dh)
                    )

            def to_x(self):
                dd, in_c, in_y, in_z, tt, tb, in_x = self.r
                for copy in self.by_h:
                    copy.wait_recv()
                v = self.summed_l(0)
                for dh in range(1, ZH):
                    v = v + in_z[ZH * (ZL - 1) + dh - 1].astype(F32)
                for dx in range(X):
                    tt[dx] = v[dx * part : (dx + 1) * part]
                    tb[dx] = v[dx * part : (dx + 1) * part].astype(BF)
                self.by_x = [put(tb.at[at("x", d)], in_x.at[d - 1], x=d) for d in range(1, X)]

            def end(self):
                tt, in_x = self.r[4], self.r[6]
                for d in range(1, X):
                    self.by_x[d - 1].wait_recv()
                for d in range(1, X):
                    tt[at("x", -d)] = in_x[d - 1].astype(F32)
                for first, blocks in self.layout:
                    v = 0.0
                    for dx, start in blocks:
                        v = v + tt[dx, :, start : start + HEAD_WIDTH]
                    self.whole[:, first : first + HEAD_WIDTH] = v
                return move(self.whole, self.out)

        class Rows:
            def __init__(self, m, src, mine):
                self.m, self.mine = m, mine
                order = list(range(1, len(near))) + [0]
                self.by_c = {
                    (k, d): put(src.at[d, k], from_c.at[m, k, d - 1], c=d)
                    for k in order
                    for d in range(1, C)
                }
                self.own = move(src.at[0], mine)

            def summed(self, k, r):
                v = self.mine[k, r].astype(F32)
                for d in range(1, C):
                    v = v + from_c[self.m, k, d - 1, r].astype(F32)
                return v

            def spread(self):
                self.own.wait()
                self.by_n = []
                for k, (dh, dx) in enumerate(near):
                    for d in range(1, C):
                        if k:
                            self.by_c[k, d].wait_recv()
                    if k:
                        def body(r, k=k):
                            self.mine[k, r] = self.summed(k, r).astype(BF)

                        by_rows(rows, 32, body)
                        self.by_n.append(
                            put(self.mine.at[k], from_n.at[self.m, k - 1], zh=dh, x=dx)
                        )
                for d in range(1, C):
                    self.by_c[0, d].wait_recv()

            def spread_x(self):
                self.own.wait()
                self.by_n = {}
                for dh in reversed(range(ZH)):
                    for dx in range(1, X):
                        k = dh * X + dx
                        for d in range(1, C):
                            self.by_c[k, d].wait_recv()

                        def body(r, k=k):
                            self.mine[k, r] = self.summed(k, r).astype(BF)

                        by_rows(rows, 32, body)
                        to = from_n.at[self.m, dh * (X - 1) + dx - 1]
                        self.by_n[dh, dx] = put(self.mine.at[k], to, x=dx)

            def came_x(self, dh, r):
                v = self.summed(dh * X, r)
                for dx in range(1, X):
                    v = v + from_n[self.m, dh * (X - 1) + dx - 1, r].astype(F32)
                return v

            def relay(self):
                for dh in reversed(range(ZH)):
                    for d in range(1, C):
                        self.by_c[dh * X, d].wait_recv()
                    for dx in range(1, X):
                        self.by_n[dh, dx].wait_recv()
                    if dh:
                        def body(r, dh=dh):
                            self.mine[dh * X, r] = self.came_x(dh, r).astype(BF)

                        by_rows(rows, 32, body)
                        to = from_n.at[self.m, ZH * (X - 1) + dh - 1]
                        self.by_n[dh, 0] = put(self.mine.at[dh * X], to, zh=dh)

            def landed(self):
                for dh in range(1, ZH):
                    self.by_n[dh, 0].wait_recv()

            def final(self, r):
                v = self.came_x(0, r)
                for dh in range(1, ZH):
                    v = v + from_n[self.m, ZH * (X - 1) + dh - 1, r].astype(F32)
                return v

            def arrive(self):
                for copy in self.by_n:
                    copy.wait_recv()

            def total(self, r):
                v = self.summed(0, r)
                for k in range(1, len(near)):
                    v = v + from_n[self.m, k - 1, r].astype(F32)
                return v

        terms = Rows(0, nt_ref, half_n)
        loads = {
            "turned": move(gt_ref, turned),
            "g": move(gg_ref, units_t.at[0]),
            "u": move(gu_ref, units_t.at[1]),
        }
        for name, src, dst in (
            ("mid", mid_ref, hs), ("cot", cot_ref, cots), ("vec", vec_ref, vec),
            ("n1", n1_ref, n1t), ("wo", wo_ref, wo), ("kv", kv_ref, kv), ("p", p_ref, ps),
            ("att", att_ref, atts), ("q", q_ref, qs), ("cos", cos_ref, cos_s),
            ("sin", sin_ref, sin_s), ("w1", w1_ref, w1), ("in", in_ref, ins),
        ):
            loads[name] = move(src, dst)
        ud, ug, uu = Units(0, gd_ref), Units(1, None), Units(2, None)
        arrived = [(dh, dl) for dh, dl in far if dh]
        ud.begin(arrived[::-1] + [(0, 1)], arrived)
        outs_terms = Rows(1, ot_ref, half_o)

        eye = (
            lax.broadcasted_iota(jnp.int32, (128, 128), 0)
            == lax.broadcasted_iota(jnp.int32, (128, 128), 1)
        ).astype(BF)

        terms.spread_x()
        for name in ("turned", "g", "u", "n1"):
            loads[name].wait()
        compute_other(0, 2)
        for u in (ug, uu):
            for k in (3, 2):
                send_block(u, k)
        ud.add_y(arrived[::-1])
        compute_other(2, 4)
        terms.relay()
        add_block(ug, 3)
        ud.add_l(far=True)
        add_block(ug, 2)
        for name in ("mid", "cot", "vec"):
            loads[name].wait()
        gain_one, gain_two = vec[0:1, :width], vec[1:2, :width]
        terms.landed()
        vs[...] = jnp.zeros_like(vs)

        @pl.loop(0, rows // 32)
        def _(i):
            r = pl.ds(pl.multiple_of(i * 32, 32), 32)
            grad, h = terms.final(r), hs[r]
            inv = lax.rsqrt(jnp.mean(h * h, axis=-1, keepdims=True) + EPSILON)
            scaled = gain_two * grad
            v = (
                cots[r].astype(F32)
                + inv * scaled
                - h * (inv * inv * inv) * jnp.mean(scaled * h, axis=-1, keepdims=True)
            )
            dh_s[r] = v
            da[0, r] = v.astype(BF)
            vs[1:2, :width] = vs[1:2, :width] + jnp.sum(grad * h * inv, axis=0, keepdims=True)

        da_x = [put(da.at[0], da.at[-d % X], x=d) for d in range(1, X)]
        ud.by_h[1].forward()
        outs_terms.spread_x()
        add_block(uu, 3)
        loads["wo"].wait()
        loads["att"].wait()
        for copy in da_x:
            copy.wait_recv()

        @pl.loop(0, heads // 2)
        def _(j):
            cols = pl.ds(pl.multiple_of(j * 256, 256), 256)
            for k in range(X):
                dos[k * rows : (k + 1) * rows, cols] = nn(da[k], wo[:, cols]).astype(BF)

        for k in range(X):
            for j in range(width // 128):
                cols = slice(j * 128, (j + 1) * 128)
                dat[cols, k * rows : (k + 1) * rows] = nt(eye, da[k, :, cols]).astype(BF)
        s_out = Scatter(d_out, c_out, y_out, z_out, t_out, b_out, x_out, w_out_s, dout_o, out_layout)
        s_out.fill(dat, atts)
        s_out.to_c()
        ug.add_l(far=True)
        add_block(uu, 2)
        ud.add_y([(0, 1)])
        for name in ("kv", "p", "q", "cos", "sin", "w1", "in"):
            loads[name].wait()
        dkv[...] = jnp.zeros_like(dkv)

        @pl.loop(0, heads)
        def _(h):
            cols = pl.ds(pl.multiple_of(h * HEAD_WIDTH, HEAD_WIDTH), HEAD_WIDTH)
            g = lax.div(h, share)
            k_at = pl.ds(pl.multiple_of(g * HEAD_WIDTH, HEAD_WIDTH), HEAD_WIDTH)
            v_at = pl.ds(pl.multiple_of(kv_cols + g * HEAD_WIDTH, HEAD_WIDTH), HEAD_WIDTH)
            p_low, do_h = ps[h], dos[:, cols]
            p = p_low.astype(F32)
            dp = nt(do_h, kv[:, v_at])
            delta = jnp.sum(p * dp, axis=-1, keepdims=True)
            ds = (p * (dp - delta)).astype(BF)
            dq = nn(ds, kv[:, k_at]) * scale
            dq = dq * cos_s[:query_rows] - pltpu.roll(dq, HEAD_WIDTH // 2, 1) * sin_s[:query_rows]
            dpre[:, cols] = dq.astype(BF)
            dkv[:, k_at] += tn(ds, qs[:, cols]) * scale
            dkv[:, v_at] += tn(p_low, do_h)

        kv_c = []
        for d in range(1, C):
            dkv_low[d - 1] = dkv[d * query_rows : (d + 1) * query_rows].astype(BF)
            kv_c.append(put(dkv_low.at[d - 1], dkv_in.at[d - 1], c=d))
        s_out.to_y()
        for copy in kv_c:
            copy.wait_recv()
        total = dkv[:query_rows]
        for d in range(1, C):
            total = total + dkv_in[d - 1].astype(F32)
        for j in range(kv_heads):
            cols = slice(j * HEAD_WIDTH, (j + 1) * HEAD_WIDTH)
            v = total[:, cols]
            v = v * cos_s[:query_rows] - pltpu.roll(v, HEAD_WIDTH // 2, 1) * sin_s[:query_rows]
            dpre[:, q_cols + j * HEAD_WIDTH : q_cols + (j + 1) * HEAD_WIDTH] = v.astype(BF)
        dpre[:, q_cols + kv_cols :] = total[:, kv_cols:].astype(BF)
        s_qkv = Scatter(d_qkv, c_qkv, y_qkv, z_qkv, t_qkv, b_qkv, x_qkv, w_qkv_s, dqkv_o, qkv_layout)
        s_qkv.fill(n1t, dpre)
        s_qkv.to_c()

        for k in list(range(1, X)) + [0]:
            @pl.loop(0, width // 256)
            def _(j, k=k):
                cols = pl.ds(pl.multiple_of(j * 256, 256), 256)
                v = nt(dpre[k * rows : (k + 1) * rows], w1[cols])
                if k:
                    n_send[k - 1, :, cols] = v.astype(BF)
                else:
                    gi_s[:, cols] = v

            if k:
                copy = put(n_send.at[k - 1], n_recv.at[k - 1], x=k)
                n_x = [copy] if k == 1 else n_x + [copy]
        kv_at = lax.div(x * heads, QUERY_HEADS // KEY_VALUE_HEADS) * HEAD_WIDTH
        k_off = QUERY_HEADS * HEAD_WIDTH + kv_at
        v_off = k_off + KEY_VALUE_HEADS * HEAD_WIDTH
        sums = jnp.sum(dpre[...].astype(F32), axis=0, keepdims=True)

        def place(start, first, amount):
            vs[2:3, pl.ds(pl.multiple_of(start, 128), amount)] = sums[:, first : first + amount]

        place(x * q_cols, 0, q_cols)
        place(k_off, q_cols, kv_cols)
        place(v_off, q_cols + kv_cols, kv_cols)
        s_qkv.to_y()
        send_block(ug, 1)
        ug.by_h[1].forward()
        s_out.to_z()
        outs_terms.relay()
        for copy in n_x:
            copy.wait_recv()

        @pl.loop(0, rows // 32)
        def _(i):
            r = pl.ds(pl.multiple_of(i * 32, 32), 32)
            grad, h = gi_s[r], ins[r].astype(F32)
            for d in range(1, X):
                grad = grad + n_recv[d - 1, r].astype(F32)
            inv = lax.rsqrt(jnp.mean(h * h, axis=-1, keepdims=True) + EPSILON)
            scaled = gain_one * grad
            gi_s[r] = (
                dh_s[r]
                + inv * scaled
                - h * (inv * inv * inv) * jnp.mean(scaled * h, axis=-1, keepdims=True)
            )
            vs[0:1, :width] = vs[0:1, :width] + jnp.sum(grad * h * inv, axis=0, keepdims=True)

        done = [move(gi_s, gi_o)]

        def put_far(u):
            u.wait_h()

            def body(r):
                v = from_h[u.m, 0, r]

                @pl.when(zh == 0)
                def _():
                    out_w[u.m, r, units:] = v

                @pl.when(zh != 0)
                def _():
                    out_w[u.m, r, :units] = v

            by_rows(depth, 64, body)

        def put_near(u, out):
            def body(r):
                v = own_g[u.m, 0, r].astype(F32)
                for d in range(1, ZL):
                    v = v + from_l[u.m, 0, d - 1, r].astype(F32)
                v = v.astype(BF)

                @pl.when(zh == 0)
                def _():
                    out_w[u.m, r, :units] = v

                @pl.when(zh != 0)
                def _():
                    out_w[u.m, r, units:] = v

            by_rows(depth, 64, body)
            done.append(move(out_w.at[u.m], out))

        places = iter(range(V_IN))
        stages = iter(range(4))

        def small_stage(offsets):
            k = next(stages)
            v_send[k] = vs[...]
            return [(p, put(v_send.at[k], v_in.at[p], **off)) for off, p in zip(offsets, places)]

        def small_finish(copies):
            for p, copy in copies:
                copy.wait_recv()
                vs[...] = vs[...] + v_in[p]

        state = small_stage([dict(y=d) for d in range(1, Y)])
        send_block(uu, 1)
        send_block(ug, 0)
        send_block(uu, 0)
        ud.begin([(0, 0)])
        uu.add_l(far=True)
        s_qkv.to_z()
        s_out.to_h()
        small_finish(state)
        state = small_stage([dict(zh=dh, zl=dl) for dh, dl in far[1:]])
        uu.by_h[1].forward()
        add_block(ug, 1)
        s_qkv.to_h()
        add_block(uu, 1)
        s_out.to_x()
        small_finish(state)
        state = small_stage([dict(x=d) for d in range(1, X)])
        outs_terms.landed()

        def finish(r):
            lo_s[r] = (hs[r] + outs_terms.final(r)).astype(BF)

        by_rows(rows, 32, finish)
        done.append(move(lo_s, lo_o))
        small_finish(state)
        state = small_stage([dict(c=d) for d in range(1, C)])
        done.append(s_out.end())
        ud.add_l(far=False)
        ug.add_l(far=False)
        for u in (ud, ug, uu):
            put_far(u)
        add_block(ug, 0)
        put_near(ug, og_o)
        s_qkv.to_x()
        add_block(uu, 0)
        ud.add_y([(0, 0)])
        put_near(ud, od_o)
        small_finish(state)
        done.append(move(vs, vec_out))
        done.append(s_qkv.end())
        uu.add_l(far=False)
        put_near(uu, ou_o)
        for copy in done:
            copy.wait()
        for copy in sent:
            copy.wait_send()
        assert count[0] <= n_sems and count[1] <= 64, count

    V_IN = (C - 1) + (X - 1) + (Y - 1) + (zs - 1)
    any_spec = pl.BlockSpec(memory_space=pl.ANY)
    sds = jax.ShapeDtypeStruct
    vm = pltpu.VMEM

    def scatter_scratch(n):
        return [
            vm((C, Y, zs, X * part, n), BF), vm((Y, max(C - 1, 1), zs, X * part, n), BF),
            vm((max(Y - 1, 1), zs, X * part, n), BF), vm((max(zs - 1, 1), X * part, n), BF),
            vm((X, part, n), F32), vm((X, part, n), BF), vm((max(X - 1, 1), part, n), BF),
        ]

    nk = len(near)
    return pl.pallas_call(
        kernel,
        out_shape=[
            sds((rows, width), BF), sds((rows, width), F32), sds((part, QKV_WIDTH), F32),
            sds((part, X * q_cols), F32), sds((8, QKV_WIDTH), F32),
            sds((depth, ZH * units), BF), sds((depth, ZH * units), BF),
            sds((depth, ZH * units), BF), sds((3, depth, units), BF),
        ],
        in_specs=[any_spec] * 20,
        out_specs=[any_spec] * 9,
        scratch_shapes=[
            vm((3, zs, depth, units), BF), vm((3, zs, max(Y - 1, 1), depth, units), BF),
            vm((3, ZH, max(ZL - 1, 1), depth, units), BF), vm((3, max(ZH - 1, 1), depth, units), BF),
            vm((3, depth, ZH * units), BF), vm((width, group_rows), BF), vm((2, group_rows, units), BF),
            vm((nk, rows, width), BF), vm((nk, rows, width), BF),
            vm((2, nk, max(C - 1, 1), rows, width), BF), vm((2, max(nk - 1, 1), rows, width), BF),
            vm((rows, width), F32), vm((rows, width), BF), vm((rows, width), BF),
            vm((width, qkv_n), BF), vm((width, q_cols), BF),
            vm((width, query_rows), BF), vm((query_rows, q_cols), BF),
            vm((pack_rows, 2 * kv_cols), BF), vm((heads, query_rows, pack_rows), BF),
            vm((query_rows, q_cols), BF), vm((8, QKV_WIDTH), F32),
            vm((pack_rows, HEAD_WIDTH), F32), vm((pack_rows, HEAD_WIDTH), F32),
            vm((X, rows, width), BF), vm((width, query_rows), BF), vm((query_rows, q_cols), BF),
            vm((query_rows, qkv_n), BF), vm((pack_rows, 2 * kv_cols), F32),
            vm((max(C - 1, 1), query_rows, 2 * kv_cols), BF),
            vm((max(C - 1, 1), query_rows, 2 * kv_cols), BF),
            vm((rows, width), F32),
        ]
        + scatter_scratch(qkv_n)
        + scatter_scratch(q_cols)
        + [
            vm((part, QKV_WIDTH), F32), vm((part, X * q_cols), F32),
            vm((max(X - 1, 1), rows, width), BF), vm((max(X - 1, 1), rows, width), BF),
            vm((rows, width), BF), vm((rows, width), F32), vm((8, QKV_WIDTH), F32),
            vm((max(V_IN, 1), 8, QKV_WIDTH), F32), vm((4, 8, QKV_WIDTH), F32),
            pltpu.SemaphoreType.DMA((n_sems,)), pltpu.SemaphoreType.DMA((n_sems,)),
            pltpu.SemaphoreType.DMA((64,)),
        ],
        compiler_params=pltpu.CompilerParams(
            collective_id=1, has_side_effects=True, vmem_limit_bytes=63 << 20
        ),
        name="back",
    )(
        grad_d, near_d, grad_g, grad_u, group_t, normed_terms, out_terms, middle, cotangent, own_in,
        wqkv, wout, normed, queries, kv_rows, probs, attended, vectors, cosine, sine,
    )


def finish(arrays, types):
    def spec(v):
        if v.shape[0] % 64 == 0:
            return pl.BlockSpec((v.shape[0] // 4,) + v.shape[1:], lambda i: (i,) + (0,) * (v.ndim - 1))
        return pl.BlockSpec(v.shape, lambda i: (0,) * v.ndim)

    def kernel(*refs):
        for src, dst in zip(refs[: len(arrays)], refs[len(arrays) :]):
            dst[...] = src[...].astype(dst.dtype)

    return pl.pallas_call(
        kernel,
        grid=(4,),
        out_shape=[jax.ShapeDtypeStruct(v.shape, t) for v, t in zip(arrays, types)],
        in_specs=[spec(v) for v in arrays],
        out_specs=[spec(v) for v in arrays],
        name="finish",
    )(*arrays)


def ff(normed, cotangent, w_gate, w_up, w_down):
    gate = nn(normed, w_gate)
    up_part = nn(normed, w_up)
    sig = jax.nn.sigmoid(gate)
    act = gate * sig
    hidden = (act * up_part).astype(BF)
    grad_wdown = tn(cotangent, hidden).astype(BF)
    grad_hidden = nn(cotangent, w_down)
    grad_gate = (grad_hidden * up_part * sig * (1.0 + gate * (1.0 - sig))).astype(BF)
    grad_up = (grad_hidden * act).astype(BF)
    grad_wgate = tn(normed, grad_gate).astype(BF)
    grad_wup = tn(normed, grad_up).astype(BF)
    normed_term = (nt(grad_gate, w_gate) + nt(grad_up, w_up)).astype(BF)
    out_term = nt(hidden, w_down).astype(BF)
    return hidden, grad_gate, grad_up, grad_wdown, grad_wgate, grad_wup, out_term, normed_term


def small_rows(gain_one, gain_two, bias):
    row = jnp.concatenate([gain_one, gain_two, bias]).astype(F32)
    return jnp.broadcast_to(jnp.pad(row, (0, -row.shape[0] % 256))[None], (8, 256))


def shards(
    layer_in, lengths, w_qkv, b_qkv, w_out, norm1_gain, norm2_gain, w_gate, w_up, w_down, grad_out
):
    size = lax.axis_size
    ZH, ZL, Y, X, C = (size(a) for a in ("zh", "zl", "y", "x", "c"))
    zh, zl, y, x, c = (lax.axis_index(a) for a in ("zh", "zl", "y", "x", "c"))
    everyone = ("zh", "zl", "y", "x", "c")
    devices = ZH * ZL * Y * X * C
    rows, width = layer_in.shape[1:]
    part = w_qkv.shape[0]
    group = QUERY_HEADS // KEY_VALUE_HEADS
    heads = QUERY_HEADS // X
    kv_heads = max(1, heads // group)
    share = heads // kv_heads
    q_cols, kv_cols = heads * HEAD_WIDTH, kv_heads * HEAD_WIDTH
    scale = HEAD_WIDTH ** (-0.5)

    own_in = layer_in[0]
    cotangent = grad_out[0]
    own_rows = own_in.astype(F32)
    query_rows, pack_rows = X * rows, C * X * rows
    bias_part = b_qkv.shape[0]
    def row_index(cores):
        spans = [
            (((x + dx) % X) * C + (c + dc) % C) * rows + jnp.arange(rows, dtype=jnp.int32)
            for dc in range(cores)
            for dx in range(X)
        ]
        return jnp.concatenate(spans)

    doc_lengths = lengths[0]
    key_index = row_index(C)
    key_doc, key_pos = doc_layout(key_index, doc_lengths)
    query_index, query_doc = key_index[:query_rows], key_doc[:query_rows]
    key_cos, key_sin = angles(key_pos)
    query_cos, query_sin = key_cos[:query_rows], key_sin[:query_rows]

    def gather_columns(pieces):
        held = ordered(
            [pick(pieces, x)] + [fetch(pick(pieces, (x - d) % X), "x", d) for d in range(1, X)],
            "x",
        )
        whole = jnp.zeros((ZH, ZL, Y) + held.shape, held.dtype)
        for dh in range(ZH):
            for dl in range(ZL):
                along = held if dh == dl == 0 else fetch(held, ("zh", "zl"), (dh, dl))
                for dy in range(Y):
                    piece = along if dy == 0 else fetch(along, "y", dy)
                    whole = lax.dynamic_update_slice(
                        whole,
                        piece[None, None, None],
                        ((zh + dh) % ZH, (zl + dl) % ZL, (y + dy) % Y, 0, 0, 0),
                    )
        whole = whole.reshape((ZH * ZL * Y * X,) + whole.shape[4:])
        both = ordered([whole] + [fetch(whole, "c", d) for d in range(1, C)], "c")
        return jnp.moveaxis(both, 0, 1).reshape(width, whole.shape[-1])

    def scatter_columns(grad):
        n = grad.shape[-1]
        grad = grad.astype(BF).reshape(ZH * ZL * Y * X, C, part, n)
        held = pick(grad, c, 1).astype(F32)
        for d in range(1, C):
            held = held + send(pick(grad, (c + d) % C, 1), "c", d)
        held = held.astype(BF).reshape(ZH, ZL, Y, X * part, n)
        kept = pick(held, y, 2).astype(F32)
        for d in range(1, Y):
            kept = kept + send(pick(held, (y + d) % Y, 2), "y", d)
        low = kept.astype(BF)
        total = 0.0
        for dh in range(ZH):
            for dl in range(ZL):
                if dh == dl == 0:
                    total = total + pick(pick(kept, zh), zl)
                else:
                    piece = pick(pick(low, (zh + dh) % ZH), (zl + dl) % ZL)
                    total = total + send(piece, ("zh", "zl"), (dh, dl)).astype(F32)
        total = total.reshape(X, part, n)
        lower = total.astype(BF)
        return ordered(
            [pick(total, x)]
            + [fetch(pick(lower, (x - d) % X), "x", d).astype(F32) for d in range(1, X)],
            "x",
        )

    def qkv_columns(array):
        blocks = []
        for at in range(X):
            kv = (at * heads) // group * HEAD_WIDTH
            key_at = QUERY_HEADS * HEAD_WIDTH + kv
            value_at = key_at + KEY_VALUE_HEADS * HEAD_WIDTH
            blocks.append(
                jnp.concatenate(
                    [
                        array[..., at * q_cols : (at + 1) * q_cols],
                        array[..., key_at : key_at + kv_cols],
                        array[..., value_at : value_at + kv_cols],
                    ],
                    axis=-1,
                )
            )
        return jnp.stack(blocks)

    def qkv_whole(blocks):
        queries = [blocks[at, ..., :q_cols] for at in range(X)]
        keys, values = [0.0] * KEY_VALUE_HEADS, [0.0] * KEY_VALUE_HEADS
        for at in range(X):
            for j in range(kv_heads):
                head = (at * heads) // group + j
                start = q_cols + j * HEAD_WIDTH
                keys[head] = keys[head] + blocks[at, ..., start : start + HEAD_WIDTH]
                start = start + kv_cols
                values[head] = values[head] + blocks[at, ..., start : start + HEAD_WIDTH]
        return jnp.concatenate(queries + keys + values, axis=-1)

    depth, units = w_gate.shape[0], w_gate.shape[1] // ZH

    def gather_units(weight):
        halves = weight.reshape(depth, ZH, units).transpose(1, 0, 2)
        whole = jnp.zeros((ZH, ZL, Y, depth, units), weight.dtype)
        for dh in range(ZH):
            first = pick(halves, zh) if dh == 0 else fetch(pick(halves, (zh - dh) % ZH), "zh", dh)
            for dl in range(ZL):
                second = first if dl == 0 else fetch(first, "zl", dl)
                for dy in range(Y):
                    third = second if dy == 0 else fetch(second, "y", dy)
                    whole = lax.dynamic_update_slice(
                        whole,
                        third[None, None, None],
                        ((zh + dh) % ZH, (zl + dl) % ZL, (y + dy) % Y, 0, 0),
                    )
        return whole.reshape(width, units)

    def scatter_units(grad):
        grad = grad.astype(BF).reshape(ZH, ZL, Y, depth, units)
        done = [None] * ZH
        for dh in reversed(range(ZH)):
            mine = pick(grad, (zh + dh) % ZH)
            kept = pick(mine, y, 1).astype(F32)
            for d in range(1, Y):
                kept = kept + send(pick(mine, (y + d) % Y, 1), "y", d).astype(F32)
            low = kept.astype(BF)
            total = pick(kept, zl)
            for d in range(1, ZL):
                total = total + send(pick(low, (zl + d) % ZL), "zl", d).astype(F32)
            done[dh] = total
        halves = [done[0]] + [
            send(done[dh].astype(BF), "zh", dh).astype(F32) for dh in range(1, ZH)
        ]
        halves = [halves[0]] + halves[:0:-1]
        return jnp.moveaxis(ordered(halves, "zh"), 0, 1).reshape(depth, ZH * units)

    near = [(dh, dx) for dh in range(ZH) for dx in range(X)]

    def gather_rows(own):
        held = jnp.concatenate([own if k == (0, 0) else fetch(own, ("zh", "x"), k) for k in near])
        return jnp.concatenate([held] + [fetch(held, "c", d) for d in range(1, C)])

    def scatter_rows(term):
        term = term.reshape(C, len(near), rows, width)
        held = term[0].astype(F32)
        for d in range(1, C):
            held = held + send(term[d].astype(BF), "c", d).astype(F32)
        total = held[0]
        for at, k in enumerate(near):
            if k != (0, 0):
                total = total + send(held[at].astype(BF), ("zh", "x"), k).astype(F32)
        return total

    def scatter_x(term):
        term = term.reshape(X, rows, width)
        total = term[0]
        for d in range(1, X):
            total = total + send(term[d].astype(BF), "x", d).astype(F32)
        return total

    if part % 16 == 0 and depth % 64 == 0 and heads % 2 == 0 and X > 1 and ZH == ZL == Y == 2:
        (
            wqkv_mine, wout_mine, normed_t, group_normed_t, queries, kv_low, probs_low,
            attended_low, middle, group_normed, group_cotangent, wgate_mine, wup_mine,
            wdown_part, vectors, cosine, sine, _, group_cotangent_t,
        ) = front(
            own_in,
            cotangent,
            lengths,
            w_qkv,
            w_out.T,
            small_rows(norm1_gain, norm2_gain, b_qkv),
            w_gate,
            w_up,
            w_down.T,
            qkv_columns,
        )
        grad_gate, grad_up, grad_wdown, near_d, normed_term, out_term = forward_backward(
            group_normed.reshape(-1, width),
            group_cotangent.reshape(-1, width),
            group_cotangent_t,
            wgate_mine.reshape(width, units),
            wup_mine.reshape(width, units),
            wdown_part,
        )
        whole = (ZH, ZL, Y, depth, units)
        terms = (C, ZH * X, rows, width)
        layer_out, grad_input, sum_wqkv, sum_wout, small, sum_wdown, sum_wgate, sum_wup, _ = back(
            grad_wdown.reshape(whole),
            near_d,
            grad_gate,
            grad_up,
            group_normed_t,
            normed_term.reshape(terms),
            out_term.reshape(terms),
            middle,
            cotangent,
            own_in,
            wqkv_mine,
            wout_mine,
            normed_t,
            queries,
            kv_low,
            probs_low,
            attended_low,
            vectors,
            cosine,
            sine,
        )
        place = (((zh * ZL + zl) * Y + y) * X + x) * C + c
        layer_out, grad_input, sum_wqkv, sum_wout, sum_wgate, sum_wup, sum_wdown = finish(
            (layer_out, grad_input, sum_wqkv, sum_wout, sum_wgate, sum_wup, sum_wdown),
            (BF,) + (F32,) * 6,
        )
        return (
            layer_out[None],
            grad_input[None],
            sum_wqkv,
            lax.dynamic_slice(small, (2, place * bias_part), (1, bias_part))[0],
            sum_wout.T,
            lax.dynamic_slice(small, (0, place * part), (1, part))[0],
            lax.dynamic_slice(small, (1, place * part), (1, part))[0],
            sum_wgate,
            sum_wup,
            sum_wdown.T,
        )

    small = jnp.concatenate([norm1_gain, norm2_gain, b_qkv])
    small = jnp.pad(small, (0, -small.shape[0] % 256))[None]
    small = lax.all_to_all(
        jnp.broadcast_to(small[None], (devices,) + small.shape), everyone, 0, 0, tiled=True
    )[:, 0].astype(F32)
    gain_one = small[:, :part].reshape(1, width)
    gain_two = small[:, part : 2 * part].reshape(1, width)
    bias = small[:, 2 * part : 2 * part + bias_part].reshape(-1)

    query_in = jnp.concatenate([own_in] + [fetch(own_in, "x", d) for d in range(1, X)])
    pack_in = jnp.concatenate([query_in] + [fetch(query_in, "c", d) for d in range(1, C)])

    wqkv_mine = gather_columns(qkv_columns(w_qkv))
    wout_t = w_out.T
    wout_mine = gather_columns(
        jnp.stack([wout_t[:, at * q_cols : (at + 1) * q_cols] for at in range(X)])
    )
    bias_mine = pick(qkv_columns(bias), x)

    wgate_mine, wup_mine = gather_units(w_gate), gather_units(w_up)
    wdown_mine = gather_units(w_down.T)

    group_cotangent = gather_rows(cotangent)

    pack_in = pack_in.astype(F32)
    normed_one = (pack_in * rms_parts(pack_in) * gain_one).astype(BF)
    query_normed = normed_one[:query_rows]
    pre_query = nn(query_normed, wqkv_mine[:, :q_cols]) + bias_mine[:q_cols]
    pre_kv = nn(normed_one, wqkv_mine[:, q_cols:]) + bias_mine[q_cols:]
    queries = rotate(
        pre_query.reshape(query_rows, heads, HEAD_WIDTH), query_cos, query_sin
    ).astype(BF)
    queries = queries.reshape(query_rows, kv_heads, share, HEAD_WIDTH)
    keys = rotate(
        pre_kv[:, :kv_cols].reshape(pack_rows, kv_heads, HEAD_WIDTH), key_cos, key_sin
    ).astype(BF)
    values = pre_kv[:, kv_cols:].reshape(pack_rows, kv_heads, HEAD_WIDTH).astype(BF)
    scores = jnp.einsum("tkgd,skd->kgts", queries, keys, preferred_element_type=F32) * scale
    allowed = (query_doc[:, None] == key_doc[None, :]) & (
        key_index[None, :] <= query_index[:, None]
    )
    masked = jnp.where(allowed, scores, NEGATIVE_BIG)
    top = jnp.max(masked, axis=-1, keepdims=True)
    weights = jnp.where(allowed, jnp.exp(masked - top), 0.0)
    probs = weights / jnp.sum(weights, axis=-1, keepdims=True)
    probs_low = probs.astype(BF)
    attended = jnp.einsum("kgts,skd->tkgd", probs_low, values, preferred_element_type=F32)
    attended_low = attended.reshape(query_rows, q_cols).astype(BF)
    middle = own_rows + scatter_x(nt(attended_low, wout_mine))
    normed_two = (middle * rms_parts(middle) * gain_two).astype(BF)

    group_normed = gather_rows(normed_two)

    hidden, grad_gate, grad_up, grad_wdown, grad_wgate, grad_wup, out_term, normed_term = ff(
        group_normed, group_cotangent, wgate_mine, wup_mine, wdown_mine
    )
    grad_normed_two = scatter_rows(normed_term)
    layer_out = (middle + scatter_rows(out_term)).astype(BF)
    sum_wdown = scatter_units(grad_wdown).T
    sum_wgate = scatter_units(grad_wgate)
    sum_wup = scatter_units(grad_wup)

    back_two, grad_gain_two = rms_back(middle, gain_two, grad_normed_two)
    grad_middle = cotangent.astype(F32) + back_two
    grad_att = grad_middle.astype(BF)
    query_grad_att = jnp.concatenate([grad_att] + [fetch(grad_att, "x", d) for d in range(1, X)])
    sum_wout = scatter_columns(tn(query_grad_att, attended_low))
    head_grads = nn(query_grad_att, wout_mine).astype(BF)
    head_grads = head_grads.reshape(query_rows, kv_heads, share, HEAD_WIDTH)
    grad_probs = jnp.einsum("tkgd,skd->kgts", head_grads, values, preferred_element_type=F32)
    probs = probs_low.astype(F32)
    delta = jnp.sum(probs * grad_probs, axis=-1, keepdims=True)
    grad_scores = (probs * (grad_probs - delta)).astype(BF)
    grad_query = (
        jnp.einsum("kgts,skd->tkgd", grad_scores, keys, preferred_element_type=F32) * scale
    )
    grad_key = jnp.einsum("kgts,tkgd->skd", grad_scores, queries, preferred_element_type=F32)
    grad_key = rotate(grad_key * scale, key_cos, -key_sin)
    grad_value = jnp.einsum("kgts,tkgd->skd", probs_low, head_grads, preferred_element_type=F32)
    grad_kv = jnp.concatenate(
        [grad_key.reshape(pack_rows, kv_cols), grad_value.reshape(pack_rows, kv_cols)], axis=1
    ).reshape(C, query_rows, 2 * kv_cols)
    kv_total = grad_kv[0]
    for d in range(1, C):
        kv_total = kv_total + send(grad_kv[d].astype(BF), "c", d).astype(F32)
    grad_query = rotate(
        grad_query.reshape(query_rows, heads, HEAD_WIDTH), query_cos, -query_sin
    ).reshape(query_rows, q_cols)
    grad_pre = jnp.concatenate([grad_query, kv_total], axis=1).astype(BF)
    sum_wqkv = qkv_whole(scatter_columns(tn(query_normed, grad_pre)))
    grad_bias = jnp.sum(grad_pre.astype(F32), axis=0)
    grad_normed_one = scatter_x(nt(grad_pre, wqkv_mine))
    back_one, grad_gain_one = rms_back(own_rows, gain_one, grad_normed_one)
    grad_input = grad_middle + back_one

    bias_blocks = jnp.where(
        jnp.arange(X, dtype=jnp.int32)[:, None] == x, grad_bias[None, :], 0.0
    )
    bias_whole = qkv_whole(bias_blocks)
    piece = jnp.concatenate(
        [
            grad_gain_one.reshape(devices, part),
            grad_gain_two.reshape(devices, part),
            bias_whole.reshape(devices, bias_part),
        ],
        axis=1,
    )
    piece = jnp.pad(piece, ((0, 0), (0, -piece.shape[1] % 256)))
    piece = jnp.sum(lax.all_to_all(piece[:, None], everyone, 0, 0, tiled=True)[:, 0], axis=0)
    return (
        layer_out[None],
        grad_input[None],
        sum_wqkv,
        piece[2 * part : 2 * part + bias_part],
        jnp.moveaxis(sum_wout, 0, 1).reshape(part, -1).T,
        piece[:part],
        piece[part : 2 * part],
        sum_wgate,
        sum_wup,
        sum_wdown,
    )


def solution(mesh):
    wide, narrow = mesh.shape["wide"], mesh.shape["narrow"]
    cores = 2 if narrow % 2 == 0 else 1
    along_x = narrow // cores
    along_y = along_x if wide % along_x == 0 else 1
    along_z = wide // along_y
    far = 2 if along_z % 2 == 0 else 1
    split = Mesh(
        mesh.devices.reshape(far, along_z // far, along_y, along_x, cores),
        ("zh", "zl", "y", "x", "c"),
    )
    w, n = ("zh", "zl", "y"), ("x", "c")
    placed = (
        P(w, n, None),
        P(w, None),
        P(w + n, None),
        P(w + n),
        P(None, w + n),
        P(w + n),
        P(w + n),
        P(w, n),
        P(w, n),
        P(n, w),
        P(w, n, None),
    )
    return jax.shard_map(
        shards,
        mesh=split,
        in_specs=placed,
        out_specs=(
            P(w, n, None),
            P(w, n, None),
            P(w + n, None),
            P(w + n),
            P(None, w + n),
            P(w + n),
            P(w + n),
            P(w, n),
            P(w, n),
            P(n, w),
        ),
        check_vma=False,
    )
```
